32 devices in a mesh: dp: 8 (over y, x, core), mp: 4 (over z).
Axes of the slice: x: 2, y: 2, z: 4, core: 2. Of those that a mesh axis runs over, the one named last changes fastest.
Arguments:
- tokens: bfloat16 [8192, 2048], P(('dp', 'mp')), may hold values from -6 to 6
- norm_gain: bfloat16 [2048], replicated, may hold values from 0.099609375 to 1.8984375
- layernorm_bias: bfloat16 [2048], replicated, may hold values from -4 to 4
- qkv_weight: bfloat16 [2048, 3, 2048], P(None, None, 'mp'), may hold values from -0.125 to 0.125
- qkv_bias: bfloat16 [3, 2048], P(None, 'mp'), may hold values from -6 to 6
- out_weight: bfloat16 [2048, 2048], P('mp'), may hold values from -0.5 to 0.5
- gate_up_weight: bfloat16 [2048, 2, 5632], P(None, None, 'mp'), may hold values from -0.125 to 0.125
- down_weight: bfloat16 [5632, 2048], P('mp'), may hold values from -0.15625 to 0.15625
- grad_out: bfloat16 [8192, 2048], P(('dp', 'mp')), may hold values from -6 to 6
Outputs:
- layer_out: bfloat16 [8192, 2048], P(('dp', 'mp'))
- grad_tokens: bfloat16 [8192, 2048], P(('dp', 'mp'))
- grad_norm_gain: float32 [2048], P('mp')
- grad_norm_bias: float32 [2048], P('mp')
- grad_qkv_weight: float32 [2048, 3, 2048], P(None, None, 'mp')
- grad_qkv_bias: float32 [3, 2048], P(None, 'mp')
- grad_out_weight: float32 [2048, 2048], P('mp')
- grad_gate_up_weight: float32 [2048, 2, 5632], P(None, None, 'mp')
- grad_down_weight: float32 [5632, 2048], P('mp')
The draws below stay inside these ranges and needn't reach their ends.
All inputs are finite; a program needn't handle non-finite values.
Results may differ from the reference program's by a relative error of at most 0.0097.
Values may be sent and summed in bfloat16 or wider, within the bound.
A program may use at most 320 MiB of HBM per device.

```python
import math
import jax
import jax.numpy as jnp
from jax import lax

D = 2048
HEADS = 32
HD = 64
FF = 5632
ROT = 16
SEQ = 1024
TOKENS = 8192
N_DP = 8


def block_levels(own_key, shape, shards, smallest, top_value):
    def one(axis_at, shards_of):
        draws = jax.random.uniform(jax.random.fold_in(jax.random.fold_in(own_key, 6), axis_at), (shards_of,), jnp.float32, smallest / len(shards), top_value / len(shards))
        return jnp.repeat(jnp.exp(draws), shape[axis_at] // shards_of).reshape((-1,) + (1,) * (len(shape) - axis_at - 1))

    factor_of = one(*shards[0])
    for cut in shards[1:]:
        factor_of = factor_of * one(*cut)
    return factor_of


def gaussian(own_key, shape, width, most, split=(), held_as=jnp.bfloat16):
    factor_of = block_levels(own_key, shape, split, -0.22, 0.18) if split else 1.0
    values = jax.random.normal(own_key, shape, jnp.float32) * width * factor_of
    return jnp.minimum(jnp.maximum(values, -most), most).astype(held_as)


def setup_inputs(seed: int = 0) -> dict:
    key_of = jax.random.split(jax.random.key(seed), 10)
    return {
        "tokens": gaussian(key_of[0], (TOKENS, D), 1.0, 6.0, ((0, 32),)),
        "norm_gain": jnp.clip(1.0 + 0.18 * jax.random.normal(key_of[1], (D,), jnp.float32), 0.099609375, 1.8984375).astype(jnp.bfloat16),
        "layernorm_bias": gaussian(key_of[2], (D,), 0.3, 4.0),
        "qkv_weight": gaussian(key_of[3], (D, 3, D), D ** -0.5, 0.125, ((2, 4),)),
        "qkv_bias": gaussian(key_of[4], (3, D), 0.5, 6.0, ((1, 4),)),
        "out_weight": gaussian(key_of[5], (D, D), (D // 16) ** -0.5, 0.5, ((0, 4),)),
        "gate_up_weight": gaussian(key_of[6], (D, 2, FF), D ** -0.5, 0.125, ((2, 4),)),
        "down_weight": gaussian(key_of[7], (FF, D), (FF // 4) ** -0.5, 0.15625, ((0, 4),)),
        "grad_out": gaussian(key_of[8], (TOKENS, D), 1.0, 6.0, ((0, 32),)),
    }


@jax.custom_vjp
def low(v):
    return lax.optimization_barrier(v.astype(jnp.bfloat16)).astype(jnp.float32)

@jax.custom_vjp
def low_back(v):
    return v

def low_keep(v):
    return (low(v), None)

def low_pass(kept, grad):
    return (grad,)

def back_keep(v):
    return (v, None)

def back_low(kept, grad):
    return (low(grad),)
low.defvjp(low_keep, low_pass)
low_back.defvjp(back_keep, back_low)
EPS = 1e-05

def matmul(left, right):
    return jnp.dot(left, right, precision=lax.Precision.HIGHEST)

def angles(seq_len):
    positions = jnp.arange(seq_len, dtype=jnp.float32)
    freqs = 1.0 / 10000.0 ** (jnp.arange(ROT // 2, dtype=jnp.float32) * 2.0 / ROT)
    phase = positions[:, None] * freqs[None, :]
    return (jnp.cos(phase), jnp.sin(phase))

def rotate(values, cosine, sine_part, direction):
    rot_half = cosine.shape[1]
    lead_part = values[..., :rot_half]
    pair_part = values[..., rot_half:2 * rot_half]
    cos_rows = cosine[:, None, :]
    sin_rows = direction * sine_part[:, None, :]
    return jnp.concatenate([lead_part * cos_rows - pair_part * sin_rows, pair_part * cos_rows + lead_part * sin_rows, values[..., 2 * rot_half:]], axis=-1)

def layer(tokens, norm_gain, layernorm_bias, qkv_weight, qkv_bias, out_weight, gate_up_weight, down_weight):
    row_mean = lax.optimization_barrier(jnp.mean(tokens, axis=1, keepdims=True))
    centered_rows = tokens - row_mean
    inverse_deviation = lax.rsqrt(lax.optimization_barrier(jnp.mean(centered_rows * centered_rows, axis=1, keepdims=True)) + EPS)
    normalized_rows = low(centered_rows * inverse_deviation * norm_gain + layernorm_bias)
    qkv = low_back(matmul(normalized_rows, qkv_weight.reshape(D, 3 * D)) + qkv_bias.reshape(3 * D))
    cosine, sine_part = angles(SEQ)
    queries = low(rotate(qkv[:, :D].reshape(SEQ, HEADS, HD), cosine, sine_part, 1.0))
    keys = low(rotate(qkv[:, D:2 * D].reshape(SEQ, HEADS, HD), cosine, sine_part, 1.0))
    values = low(qkv[:, 2 * D:].reshape(SEQ, HEADS, HD))
    block_rows = min(512, SEQ)
    num_blocks = SEQ // block_rows
    key_pos = jnp.arange(SEQ)
    score_scale = 1.0 / math.sqrt(HD)

    def attend(pair):
        q_block, first_row = pair
        scores = low_back(jnp.einsum('qhd,khd->hqk', q_block, keys, precision=lax.Precision.HIGHEST) * score_scale)
        allowed = (first_row + jnp.arange(block_rows))[:, None] >= key_pos[None, :]
        scores = jnp.where(allowed[None], scores, -1e+30)
        row_max = lax.optimization_barrier(jnp.max(scores, axis=-1, keepdims=True))
        exp_scores = jnp.exp(scores - row_max)
        attn_probs = low(exp_scores / lax.optimization_barrier(jnp.sum(exp_scores, axis=-1, keepdims=True)))
        return jnp.einsum('hqk,khd->qhd', attn_probs, values, precision=lax.Precision.HIGHEST)
    attended = lax.map(jax.checkpoint(attend), (queries.reshape(num_blocks, block_rows, HEADS, HD), jnp.arange(num_blocks) * block_rows))
    attended = low(low_back(attended.reshape(SEQ, D)))
    gate_up = low_back(matmul(normalized_rows, gate_up_weight.reshape(D, 2 * FF)))
    hidden = low(jax.nn.silu(gate_up[:, :FF]) * gate_up[:, FF:])
    return tokens + matmul(attended, out_weight) + matmul(hidden, down_weight)

def reference(tokens, norm_gain, layernorm_bias, qkv_weight, qkv_bias, out_weight, gate_up_weight, down_weight, grad_out):
    params = tuple((param.astype(jnp.float32) for param in (norm_gain, layernorm_bias, qkv_weight, qkv_bias, out_weight, gate_up_weight, down_weight)))
    seqs_in = tokens.astype(jnp.float32).reshape(N_DP, SEQ, D)
    seqs_grad = grad_out.astype(jnp.float32).reshape(N_DP, SEQ, D)

    def one_sequence(totals, pair):
        seq_in, seq_grad = pair
        result, pullback = jax.vjp(layer, seq_in, *params)
        grads = pullback(seq_grad)
        return (tuple((summed + extra for summed, extra in zip(totals, grads[1:]))), (result, grads[0]))
    totals, (outputs, grad_in) = lax.scan(one_sequence, tuple((jnp.zeros_like(param) for param in params)), (seqs_in, seqs_grad))
    return (outputs.reshape(TOKENS, D).astype(jnp.bfloat16), grad_in.reshape(TOKENS, D).astype(jnp.bfloat16), totals[0], totals[1], totals[2], totals[3], totals[4], totals[5], totals[6])
```

```python
import functools
import math

import jax
import jax.numpy as jnp
from jax import lax
from jax.experimental import pallas as pl
from jax.experimental.pallas import tpu as pltpu
from jax.sharding import PartitionSpec as P

HD = 64
ROT = 16
EPS = 1e-05
LANES = 128
QB = 256


F32 = jnp.float32
BF16 = jnp.bfloat16


def dot(a, b, ca, cb, out=F32):
    return lax.dot_general(
        a, b, (((ca,), (cb,)), ((), ())), preferred_element_type=F32
    ).astype(out)


def rotary_tables(seq_len):
    positions = jnp.arange(seq_len, dtype=F32)
    freqs = 1.0 / 10000.0 ** (jnp.arange(ROT // 2, dtype=F32) * 2.0 / ROT)
    phase = positions[:, None] * freqs[None, :]
    cosine, sine = jnp.cos(phase), jnp.sin(phase)
    half = ROT // 2
    rest = HD - ROT
    ones = jnp.ones((seq_len, rest), F32)
    zeros = jnp.zeros((seq_len, rest), F32)
    zhalf = jnp.zeros((seq_len, half), F32)
    c = jnp.concatenate([cosine, cosine, ones], axis=1)
    up = jnp.concatenate([-sine, zhalf, zeros], axis=1)
    down = jnp.concatenate([zhalf, sine, zeros], axis=1)
    two = LANES // HD
    return jnp.stack([jnp.tile(t, (1, two)) for t in (c, up, down)])


def turn(x, tables, sign):
    half = ROT // 2
    ahead = pltpu.roll(x, LANES - half, 1)
    behind = pltpu.roll(x, half, 1)
    return x * tables[0] + sign * (ahead * tables[1] + behind * tables[2])


def lane_mask(rows, j):
    lane = lax.broadcasted_iota(jnp.int32, (rows, LANES), 1)
    return (lane // HD) == j


def forward_kernel(
    q_in, k_in, v_in, bias_ref, tab_ref, q_out, k_out, v_out, o_ref, lse_ref
):
    seq_len = q_in.shape[0]
    j = pl.program_id(1)

    @pl.when(j == 0)
    def _():
        tables = (tab_ref[0], tab_ref[1], tab_ref[2])
        q_out[...] = turn(q_in[...] + bias_ref[0, 0:1], tables, 1.0).astype(BF16)
        k_out[...] = turn(k_in[...] + bias_ref[0, 1:2], tables, 1.0).astype(BF16)
        v_out[...] = (v_in[...] + bias_ref[0, 2:3]).astype(BF16)

    mask = lane_mask(QB, j)
    causal = lax.broadcasted_iota(jnp.int32, (QB, QB), 0) <= lax.broadcasted_iota(
        jnp.int32, (QB, QB), 1
    )
    for i in range(seq_len // QB):
        rows = pl.ds(i * QB, QB)
        span = (i + 1) * QB
        q = q_out[rows, :] * 0.125
        q = jnp.where(mask, q, jnp.zeros_like(q))
        parts = []
        if i:
            parts.append(dot(k_out[pl.ds(0, i * QB), :], q, 1, 1))
        diag = dot(k_out[rows, :], q, 1, 1)
        parts.append(jnp.where(causal, diag, -1e30))
        top = functools.reduce(
            jnp.maximum, [jnp.max(s, axis=0, keepdims=True) for s in parts]
        )
        exps = [jnp.exp(s - top) for s in parts]
        total = sum(jnp.sum(e, axis=0, keepdims=True) for e in exps)
        inv = 1.0 / total
        probs = jnp.concatenate([(e * inv).astype(BF16) for e in exps], axis=0)
        out = dot(probs, v_out[pl.ds(0, span), :], 0, 0).astype(BF16)
        before = o_ref[rows, :]
        o_ref[rows, :] = jnp.where(mask, out, before)
        lse_ref[0, 0, :, i * QB : (i + 1) * QB] = top + jnp.log(total)


def backward_kernel(
    q_ref, k_ref, v_ref, do_ref, lse_ref, tab_ref, dq_out, dk_out, dv_out, sums_out, dq, dk, dv
):
    seq_len = q_ref.shape[0]
    j = pl.program_id(1)
    mask = lane_mask(QB, j)
    causal = lax.broadcasted_iota(jnp.int32, (QB, QB), 0) <= lax.broadcasted_iota(
        jnp.int32, (QB, QB), 1
    )

    @pl.when(j == 0)
    def _():
        dk[...] = jnp.zeros_like(dk)
        dv[...] = jnp.zeros_like(dv)

    for i in range(seq_len // QB):
        rows = pl.ds(i * QB, QB)
        q = q_ref[rows, :] * 0.125
        q = jnp.where(mask, q, jnp.zeros_like(q))
        do = do_ref[rows, :]
        do = jnp.where(mask, do, jnp.zeros_like(do))
        lse = lse_ref[0, 0, :, i * QB : (i + 1) * QB]
        pieces = []
        if i:
            pieces.append((pl.ds(0, i * QB), False))
        pieces.append((rows, True))
        probs, grads = [], []
        inner = 0.0
        for where, diagonal in pieces:
            s = dot(k_ref[where, :], q, 1, 1)
            if diagonal:
                s = jnp.where(causal, s, -1e30)
            p = jnp.exp(s - lse)
            dp = dot(v_ref[where, :], do, 1, 1)
            inner = inner + jnp.sum(p * dp, axis=0, keepdims=True)
            probs.append(p)
            grads.append(dp)
        acc = 0.0
        for (where, diagonal), p, dp in zip(pieces, probs, grads):
            ds = (p * (dp - inner)).astype(BF16)
            dv[where, :] += dot(p.astype(BF16), do, 1, 0)
            dk[where, :] += dot(ds, q, 1, 0)
            acc = acc + dot(ds, k_ref[where, :], 0, 0)
        before = dq[rows, :]
        dq[rows, :] = jnp.where(mask, acc * 0.125, before)

    @pl.when(j == pl.num_programs(1) - 1)
    def _():
        tables = (tab_ref[0], tab_ref[1], tab_ref[2])
        gq = turn(dq[...], tables, -1.0).astype(BF16)
        gk = turn(dk[...], tables, -1.0).astype(BF16)
        gv = dv[...].astype(BF16)
        dq_out[...] = gq
        dk_out[...] = gk
        dv_out[...] = gv
        sums_out[0, 0:1] = jnp.sum(gq.astype(F32), axis=0, keepdims=True)
        sums_out[0, 1:2] = jnp.sum(gk.astype(F32), axis=0, keepdims=True)
        sums_out[0, 2:3] = jnp.sum(gv.astype(F32), axis=0, keepdims=True)


def attention_forward(qkv, bias, tables):
    seq_len, width = qkv.shape[0], qkv.shape[1] // 3
    pairs = width // LANES
    column = lambda part: pl.BlockSpec((seq_len, LANES), lambda p, j: (0, part * pairs + p))
    block = pl.BlockSpec((seq_len, LANES), lambda p, j: (0, p))
    bias_blocks = bias.reshape(3, pairs, LANES).swapaxes(0, 1)
    wide = jax.ShapeDtypeStruct((seq_len, width), BF16)
    elements = pairs * 2 * seq_len * seq_len // 2
    return pl.pallas_call(
        forward_kernel,
        grid=(pairs, LANES // HD),
        in_specs=[
            column(0),
            column(1),
            column(2),
            pl.BlockSpec((1, 3, LANES), lambda p, j: (p, 0, 0)),
            pl.BlockSpec((3, seq_len, LANES), lambda p, j: (0, 0, 0)),
        ],
        out_specs=[
            block,
            block,
            block,
            block,
            pl.BlockSpec((1, 1, 1, seq_len), lambda p, j: (p, j, 0, 0)),
        ],
        out_shape=[
            wide,
            wide,
            wide,
            wide,
            jax.ShapeDtypeStruct((pairs, LANES // HD, 1, seq_len), F32),
        ],
        cost_estimate=pl.CostEstimate(
            flops=elements * 4 * LANES,
            bytes_accessed=qkv.size * 4 + 4 * seq_len * width * 2,
            transcendentals=elements,
        ),
        name="attention_forward",
    )(qkv, qkv, qkv, bias_blocks, tables)


def attention_backward(q, k, v, grad, lse, tables):
    seq_len, width = q.shape
    pairs = width // LANES
    block = pl.BlockSpec((seq_len, LANES), lambda p, j: (0, p))
    wide = jax.ShapeDtypeStruct((seq_len, width), BF16)
    elements = pairs * 2 * seq_len * seq_len // 2
    return pl.pallas_call(
        backward_kernel,
        grid=(pairs, LANES // HD),
        in_specs=[
            block,
            block,
            block,
            block,
            pl.BlockSpec((1, 1, 1, seq_len), lambda p, j: (p, j, 0, 0)),
            pl.BlockSpec((3, seq_len, LANES), lambda p, j: (0, 0, 0)),
        ],
        out_specs=[block, block, block, pl.BlockSpec((1, 3, LANES), lambda p, j: (p, 0, 0))],
        out_shape=[wide, wide, wide, jax.ShapeDtypeStruct((pairs, 3, LANES), F32)],
        scratch_shapes=[pltpu.VMEM((seq_len, LANES), F32)] * 3,
        cost_estimate=pl.CostEstimate(
            flops=elements * 10 * LANES,
            bytes_accessed=7 * seq_len * width * 2,
            transcendentals=elements,
        ),
        name="attention_backward",
    )(q, k, v, grad, lse, tables)


def pick(x, index):
    return lax.dynamic_index_in_dim(x, index, 0, keepdims=False)


class Cube:
    def __init__(self, axis, size):
        self.axis, self.size = axis, size
        self.bits = [b for b in range(size.bit_length()) if 1 << b < size]
        me = lax.axis_index(axis)
        self.own = [lax.rem(lax.div(me, 1 << b), 2) for b in self.bits]

    def swap(self, x, b):
        return lax.ppermute(x, self.axis, [(i, i ^ (1 << b)) for i in range(self.size)])

    def sum_all(self, x):
        for b in self.bits:
            x = x + self.swap(x, b)
        return x

    def contract(self, left, right, finish):
        depth, rows = left.shape
        columns = right.shape[1]
        core, others = self.bits[0], self.bits[1:]
        half = rows // 2
        mine = self.own[0]
        first = lax.dynamic_slice_in_dim(left, (1 - mine) * half, half, 1)
        second = lax.dynamic_slice_in_dim(left, mine * half, half, 1)
        away = dot(first, right, 0, 0, BF16)
        came = self.swap(away, core)
        keep = dot(second, right, 0, 0, BF16)
        orders = [others, others[::-1]]
        quarter = half // 2
        done = []
        for n, order in enumerate(orders):
            small = quarter >> len(order)
            shape = (2,) * len(order) + (small, columns)
            cur = (
                keep[n * quarter : (n + 1) * quarter].astype(F32)
                + came[n * quarter : (n + 1) * quarter].astype(F32)
            ).reshape(shape)
            for b in order:
                own = self.own[b]
                send = pick(cur, 1 - own).astype(BF16)
                got = self.swap(send, b)
                cur = pick(cur, own) + got.astype(F32)
            buf = cur.astype(BF16)
            for b in order[::-1]:
                own = self.own[b]
                got = self.swap(buf, b)
                low = jnp.where(own == 0, buf, got)
                high = jnp.where(own == 0, got, buf)
                buf = jnp.stack([low, high])
            done.append(buf.reshape(quarter, columns))
        whole = jnp.concatenate(done, axis=0)
        other = self.swap(whole, core)
        low = jnp.where(mine == 0, whole, other)
        high = jnp.where(mine == 0, other, whole)
        return jnp.concatenate([low, high], axis=0).astype(F32)


def on_device(
    n_dp,
    n_mp,
    tokens,
    norm_gain,
    layernorm_bias,
    qkv_weight,
    qkv_bias,
    out_weight,
    gate_up_weight,
    down_weight,
    grad_out,
):
    cube = Cube("dp", n_dp)
    rows, model_width = tokens.shape
    local_width = qkv_weight.shape[2]
    seq_len = rows * n_mp
    gain = norm_gain.astype(F32)
    token_f32 = tokens.astype(F32)
    row_mean = jnp.mean(token_f32, axis=1, keepdims=True)
    centered = token_f32 - row_mean
    inv_std = lax.rsqrt(jnp.mean(centered * centered, axis=1, keepdims=True) + EPS)
    xhat = centered * inv_std
    normed_own = (xhat * gain + layernorm_bias.astype(F32)).astype(BF16)
    normed = lax.all_gather(normed_own, "mp", axis=0, tiled=True)
    dy = lax.all_gather(grad_out, "mp", axis=0, tiled=True)

    w_qkv = [qkv_weight[:, t, :] for t in range(3)]
    w_gate, w_up = gate_up_weight[:, 0, :], gate_up_weight[:, 1, :]
    tables = rotary_tables(seq_len)

    gate = dot(normed, w_gate, 1, 0)
    up = dot(normed, w_up, 1, 0)
    sig = jax.nn.sigmoid(gate)
    hidden = (gate * sig * up).astype(BF16)
    qkv = jnp.concatenate([dot(normed, w, 1, 0) for w in w_qkv], axis=1)
    q, k, v, attended, lse = attention_forward(qkv, qkv_bias.astype(F32), tables)
    branch = (dot(attended, out_weight, 1, 0) + dot(hidden, down_weight, 1, 0)).astype(BF16)
    share = lax.psum_scatter(branch, "mp", scatter_dimension=0, tiled=True)
    layer_out = (token_f32 + share.astype(F32)).astype(BF16)

    grad_down_w = cube.contract(hidden, dy, None)
    grad_out_w = cube.contract(attended, dy, None)
    d_hidden = dot(dy, down_weight, 1, 1)
    silu = gate * sig
    d_gate = (d_hidden * up * (sig + silu * (1.0 - sig))).astype(BF16)
    d_up = (d_hidden * silu).astype(BF16)
    grad_gate_w = cube.contract(normed, d_gate, None)
    grad_up_w = cube.contract(normed, d_up, None)

    d_attended = dot(dy, out_weight, 1, 1, BF16)
    dq, dk, dv, sums = attention_backward(q, k, v, d_attended, lse, tables)
    d_normed = (
        dot(d_gate, w_gate, 1, 1)
        + dot(d_up, w_up, 1, 1)
        + dot(dq, w_qkv[0], 1, 1)
        + dot(dk, w_qkv[1], 1, 1)
        + dot(dv, w_qkv[2], 1, 1)
    ).astype(BF16)
    d_own = lax.psum_scatter(d_normed, "mp", scatter_dimension=0, tiled=True).astype(F32)
    grad_qkv_w = cube.contract(normed, jnp.concatenate([dq, dk, dv], axis=1), None)

    scaled = d_own * gain
    grad_tokens = grad_out.astype(F32) + inv_std * (
        scaled
        - jnp.mean(scaled, axis=1, keepdims=True)
        - xhat * jnp.mean(scaled * xhat, axis=1, keepdims=True)
    )
    terms = jnp.stack([jnp.sum(d_own * xhat, axis=0), jnp.sum(d_own, axis=0)])
    bias_sum = cube.sum_all(sums)
    grad_bias = bias_sum.swapaxes(0, 1).reshape(3, local_width)
    terms = Cube("mp", n_mp).sum_all(cube.sum_all(terms))
    share_width = model_width // n_mp
    terms = lax.dynamic_slice_in_dim(
        terms, lax.axis_index("mp") * share_width, share_width, 1
    )
    return (
        layer_out,
        grad_tokens.astype(BF16),
        terms[0],
        terms[1],
        grad_qkv_w.reshape(model_width, 3, local_width),
        grad_bias,
        grad_out_w,
        jnp.stack([grad_gate_w, grad_up_w], axis=1),
        grad_down_w,
    )


def solution(mesh):
    return jax.shard_map(
        functools.partial(on_device, mesh.shape["dp"], mesh.shape["mp"]),
        mesh=mesh,
        in_specs=(
            P(("dp", "mp"), None),
            P(),
            P(),
            P(None, None, "mp"),
            P(None, "mp"),
            P("mp", None),
            P(None, None, "mp"),
            P("mp", None),
            P(("dp", "mp"), None),
        ),
        out_specs=(
            P(("dp", "mp"), None),
            P(("dp", "mp"), None),
            P("mp"),
            P("mp"),
            P(None, None, "mp"),
            P(None, "mp"),
            P("mp", None),
            P(None, None, "mp"),
            P("mp", None),
        ),
        check_vma=False,
    )
```

```python
import functools
import math

import jax
import jax.numpy as jnp
from jax import lax
from jax.experimental import pallas as pl
from jax.experimental.pallas import tpu as pltpu
from jax.sharding import PartitionSpec as P

HD = 64
ROT = 16
EPS = 1e-05
LANES = 128
QB = 256


F32 = jnp.float32
BF16 = jnp.bfloat16


def dot(a, b, ca, cb, out=F32):
    return lax.dot_general(
        a, b, (((ca,), (cb,)), ((), ())), preferred_element_type=F32
    ).astype(out)


def rotary_tables(seq_len):
    positions = jnp.arange(seq_len, dtype=F32)
    freqs = 1.0 / 10000.0 ** (jnp.arange(ROT // 2, dtype=F32) * 2.0 / ROT)
    phase = positions[:, None] * freqs[None, :]
    cosine, sine = jnp.cos(phase), jnp.sin(phase)
    half = ROT // 2
    rest = HD - ROT
    ones = jnp.ones((seq_len, rest), F32)
    zeros = jnp.zeros((seq_len, rest), F32)
    zhalf = jnp.zeros((seq_len, half), F32)
    c = jnp.concatenate([cosine, cosine, ones], axis=1)
    up = jnp.concatenate([-sine, zhalf, zeros], axis=1)
    down = jnp.concatenate([zhalf, sine, zeros], axis=1)
    two = LANES // HD
    return jnp.stack([jnp.tile(t, (1, two)) for t in (c, up, down)])


def turn(x, tables, sign):
    half = ROT // 2
    ahead = pltpu.roll(x, LANES - half, 1)
    behind = pltpu.roll(x, half, 1)
    return x * tables[0] + sign * (ahead * tables[1] + behind * tables[2])


def lane_mask(rows, j):
    lane = lax.broadcasted_iota(jnp.int32, (rows, LANES), 1)
    return (lane // HD) == j


def forward_kernel(
    q_in, k_in, v_in, bias_ref, tab_ref, q_out, k_out, v_out, o_ref, lse_ref
):
    seq_len = q_in.shape[0]
    j = pl.program_id(1)

    @pl.when(j == 0)
    def _():
        tables = (tab_ref[0], tab_ref[1], tab_ref[2])
        q_out[...] = turn(q_in[...] + bias_ref[0, 0:1], tables, 1.0).astype(BF16)
        k_out[...] = turn(k_in[...] + bias_ref[0, 1:2], tables, 1.0).astype(BF16)
        v_out[...] = (v_in[...] + bias_ref[0, 2:3]).astype(BF16)

    mask = lane_mask(QB, j)
    causal = lax.broadcasted_iota(jnp.int32, (QB, QB), 0) <= lax.broadcasted_iota(
        jnp.int32, (QB, QB), 1
    )
    for i in range(seq_len // QB):
        rows = pl.ds(i * QB, QB)
        span = (i + 1) * QB
        q = q_out[rows, :] * 0.125
        q = jnp.where(mask, q, jnp.zeros_like(q))
        parts = []
        if i:
            parts.append(dot(k_out[pl.ds(0, i * QB), :], q, 1, 1))
        diag = dot(k_out[rows, :], q, 1, 1)
        parts.append(jnp.where(causal, diag, -1e30))
        top = functools.reduce(
            jnp.maximum, [jnp.max(s, axis=0, keepdims=True) for s in parts]
        )
        exps = [jnp.exp(s - top) for s in parts]
        total = sum(jnp.sum(e, axis=0, keepdims=True) for e in exps)
        inv = 1.0 / total
        probs = jnp.concatenate([(e * inv).astype(BF16) for e in exps], axis=0)
        out = dot(probs, v_out[pl.ds(0, span), :], 0, 0).astype(BF16)
        before = o_ref[rows, :]
        o_ref[rows, :] = jnp.where(mask, out, before)
        lse_ref[0, 0, :, i * QB : (i + 1) * QB] = top + jnp.log(total)


def backward_kernel(
    q_ref, k_ref, v_ref, do_ref, lse_ref, tab_ref, dq_out, dk_out, dv_out, sums_out, dq, dk, dv
):
    seq_len = q_ref.shape[0]
    j = pl.program_id(1)
    mask = lane_mask(QB, j)
    causal = lax.broadcasted_iota(jnp.int32, (QB, QB), 0) <= lax.broadcasted_iota(
        jnp.int32, (QB, QB), 1
    )

    @pl.when(j == 0)
    def _():
        dk[...] = jnp.zeros_like(dk)
        dv[...] = jnp.zeros_like(dv)

    for i in range(seq_len // QB):
        rows = pl.ds(i * QB, QB)
        q = q_ref[rows, :] * 0.125
        q = jnp.where(mask, q, jnp.zeros_like(q))
        do = do_ref[rows, :]
        do = jnp.where(mask, do, jnp.zeros_like(do))
        lse = lse_ref[0, 0, :, i * QB : (i + 1) * QB]
        pieces = []
        if i:
            pieces.append((pl.ds(0, i * QB), False))
        pieces.append((rows, True))
        probs, grads = [], []
        inner = 0.0
        for where, diagonal in pieces:
            s = dot(k_ref[where, :], q, 1, 1)
            if diagonal:
                s = jnp.where(causal, s, -1e30)
            p = jnp.exp(s - lse)
            dp = dot(v_ref[where, :], do, 1, 1)
            inner = inner + jnp.sum(p * dp, axis=0, keepdims=True)
            probs.append(p)
            grads.append(dp)
        acc = 0.0
        for (where, diagonal), p, dp in zip(pieces, probs, grads):
            ds = (p * (dp - inner)).astype(BF16)
            dv[where, :] += dot(p.astype(BF16), do, 1, 0)
            dk[where, :] += dot(ds, q, 1, 0)
            acc = acc + dot(ds, k_ref[where, :], 0, 0)
        before = dq[rows, :]
        dq[rows, :] = jnp.where(mask, acc * 0.125, before)

    @pl.when(j == pl.num_programs(1) - 1)
    def _():
        tables = (tab_ref[0], tab_ref[1], tab_ref[2])
        gq = turn(dq[...], tables, -1.0).astype(BF16)
        gk = turn(dk[...], tables, -1.0).astype(BF16)
        gv = dv[...].astype(BF16)
        dq_out[...] = gq
        dk_out[...] = gk
        dv_out[...] = gv
        sums_out[0, 0:1] = jnp.sum(gq.astype(F32), axis=0, keepdims=True)
        sums_out[0, 1:2] = jnp.sum(gk.astype(F32), axis=0, keepdims=True)
        sums_out[0, 2:3] = jnp.sum(gv.astype(F32), axis=0, keepdims=True)


def attention_forward(qkv, bias, tables):
    seq_len, width = qkv.shape[0], qkv.shape[1] // 3
    pairs = width // LANES
    column = lambda part: pl.BlockSpec((seq_len, LANES), lambda p, j: (0, part * pairs + p))
    block = pl.BlockSpec((seq_len, LANES), lambda p, j: (0, p))
    bias_blocks = bias.reshape(3, pairs, LANES).swapaxes(0, 1)
    wide = jax.ShapeDtypeStruct((seq_len, width), BF16)
    elements = pairs * 2 * seq_len * seq_len // 2
    return pl.pallas_call(
        forward_kernel,
        grid=(pairs, LANES // HD),
        in_specs=[
            column(0),
            column(1),
            column(2),
            pl.BlockSpec((1, 3, LANES), lambda p, j: (p, 0, 0)),
            pl.BlockSpec((3, seq_len, LANES), lambda p, j: (0, 0, 0)),
        ],
        out_specs=[
            block,
            block,
            block,
            block,
            pl.BlockSpec((1, 1, 1, seq_len), lambda p, j: (p, j, 0, 0)),
        ],
        out_shape=[
            wide,
            wide,
            wide,
            wide,
            jax.ShapeDtypeStruct((pairs, LANES // HD, 1, seq_len), F32),
        ],
        cost_estimate=pl.CostEstimate(
            flops=elements * 4 * LANES,
            bytes_accessed=qkv.size * 4 + 4 * seq_len * width * 2,
            transcendentals=elements,
        ),
        name="attention_forward",
    )(qkv, qkv, qkv, bias_blocks, tables)


def attention_backward(q, k, v, grad, lse, tables):
    seq_len, width = q.shape
    pairs = width // LANES
    block = pl.BlockSpec((seq_len, LANES), lambda p, j: (0, p))
    wide = jax.ShapeDtypeStruct((seq_len, width), BF16)
    elements = pairs * 2 * seq_len * seq_len // 2
    return pl.pallas_call(
        backward_kernel,
        grid=(pairs, LANES // HD),
        in_specs=[
            block,
            block,
            block,
            block,
            pl.BlockSpec((1, 1, 1, seq_len), lambda p, j: (p, j, 0, 0)),
            pl.BlockSpec((3, seq_len, LANES), lambda p, j: (0, 0, 0)),
        ],
        out_specs=[block, block, block, pl.BlockSpec((1, 3, LANES), lambda p, j: (p, 0, 0))],
        out_shape=[wide, wide, wide, jax.ShapeDtypeStruct((pairs, 3, LANES), F32)],
        scratch_shapes=[pltpu.VMEM((seq_len, LANES), F32)] * 3,
        cost_estimate=pl.CostEstimate(
            flops=elements * 10 * LANES,
            bytes_accessed=7 * seq_len * width * 2,
            transcendentals=elements,
        ),
        name="attention_backward",
    )(q, k, v, grad, lse, tables)


def pick(x, index):
    return lax.dynamic_index_in_dim(x, index, 0, keepdims=False)


class Cube:
    def __init__(self, axis, size):
        self.axis, self.size = axis, size
        self.bits = [b for b in range(size.bit_length()) if 1 << b < size]
        me = lax.axis_index(axis)
        self.own = [lax.rem(lax.div(me, 1 << b), 2) for b in self.bits]

    def swap(self, x, b):
        return lax.ppermute(x, self.axis, [(i, i ^ (1 << b)) for i in range(self.size)])

    def sum_all(self, x):
        for b in self.bits:
            x = x + self.swap(x, b)
        return x

    def contract(self, left, right):
        depth, rows = left.shape
        columns = right.shape[1]
        core, others = self.bits[0], self.bits[1:]
        half = rows // 2
        mine = self.own[0]
        first = lax.dynamic_slice_in_dim(left, (1 - mine) * half, half, 1)
        second = lax.dynamic_slice_in_dim(left, mine * half, half, 1)
        away = dot(first, right, 0, 0, BF16)
        came = self.swap(away, core)
        keep = dot(second, right, 0, 0, BF16)
        orders = [others, others[::-1]]
        quarter = half // 2
        done = []
        for n, order in enumerate(orders):
            small = quarter >> len(order)
            shape = (2,) * len(order) + (small, columns)
            cur = (
                keep[n * quarter : (n + 1) * quarter].astype(F32)
                + came[n * quarter : (n + 1) * quarter].astype(F32)
            ).reshape(shape)
            for b in order:
                own = self.own[b]
                send = pick(cur, 1 - own).astype(BF16)
                got = self.swap(send, b)
                cur = pick(cur, own) + got.astype(F32)
            buf = cur.astype(BF16)
            for b in order[::-1]:
                own = self.own[b]
                got = self.swap(buf, b)
                low = jnp.where(own == 0, buf, got)
                high = jnp.where(own == 0, got, buf)
                buf = jnp.stack([low, high])
            done.append(buf.reshape(quarter, columns))
        whole = jnp.concatenate(done, axis=0)
        other = self.swap(whole, core)
        low = jnp.where(mine == 0, whole, other)
        high = jnp.where(mine == 0, other, whole)
        return jnp.concatenate([low, high], axis=0).astype(F32)


LAG = 2
BLOCK = 128
PIECES = 16
WIDE = 256
MESH = pl.DeviceIdType.MESH


class Places:
    def __init__(self):
        self.me = lax.axis_index("dp")
        self.z = lax.axis_index("mp")
        self.core = lax.rem(self.me, 2)
        self.x = lax.rem(lax.div(self.me, 2), 2)
        self.y = lax.div(self.me, 4)
        self.core_peer = (self.me + 1 - 2 * self.core, self.z)
        self.x_peer = (self.me + 2 - 4 * self.x, self.z)
        self.y_peer = (self.me + 4 - 8 * self.y, self.z)


def rdma(src, dst, sems, slot, peer):
    return pltpu.make_async_remote_copy(
        src_ref=src,
        dst_ref=dst,
        send_sem=sems.at[0, slot],
        recv_sem=sems.at[1, slot],
        device_id=peer,
        device_id_type=MESH,
    )


def grads_kernel(
    n_d, n_g, n_q, ha_ref, nt_ref, dy_ref, dgu_ref, dqkv_ref,
    down_out, out_out, gu_out, qkv_out,
    away, acc, rcv0, rcv1, rcv2, res, flat, pairs,
    s0, s1a, s1b, s2a, s2b, s3a, s3b, s4a, s4b, s5, s_flat, s_pair,
):
    at = Places()
    total = n_d + n_g + n_q
    n_down = down_out.shape[0]
    n_out = out_out.shape[0]
    qkv_items = n_q // 3

    def slot_of(buf, it):
        return lax.rem(it, buf.shape[0])

    def quarter(bit, half):
        return half * 4 + bit * 2

    def stage0(it):
        sa, s = slot_of(away, it), slot_of(rcv0, it)
        return [rdma(away.at[sa], rcv0.at[s], s0, s, at.core_peer)]

    def stage1(it):
        sa, s = slot_of(acc, it), slot_of(rcv1, it)
        return [
            rdma(acc.at[sa, pl.ds(quarter(1 - at.x, 0), 2)], rcv1.at[s, 0], s1a, s, at.x_peer),
            rdma(acc.at[sa, pl.ds(quarter(1 - at.y, 1), 2)], rcv1.at[s, 1], s1b, s, at.y_peer),
        ]

    def stage2(it):
        sa, s = slot_of(acc, it), slot_of(rcv2, it)
        return [
            rdma(acc.at[sa, quarter(at.x, 0) + 1 - at.y], rcv2.at[s, 0], s2a, s, at.y_peer),
            rdma(acc.at[sa, quarter(at.y, 1) + 1 - at.x], rcv2.at[s, 1], s2b, s, at.x_peer),
        ]

    def stage3(it):
        s = slot_of(res, it)
        a = at.core * 8 + quarter(at.x, 0) + at.y
        b = at.core * 8 + quarter(at.y, 1) + at.x
        return [
            rdma(res.at[s, a], res.at[s, a], s3a, s, at.y_peer),
            rdma(res.at[s, b], res.at[s, b], s3b, s, at.x_peer),
        ]

    def stage4(it):
        s = slot_of(res, it)
        a = pl.ds(at.core * 8 + quarter(at.x, 0), 2)
        b = pl.ds(at.core * 8 + quarter(at.y, 1), 2)
        return [
            rdma(res.at[s, a], res.at[s, a], s4a, s, at.x_peer),
            rdma(res.at[s, b], res.at[s, b], s4b, s, at.y_peer),
        ]

    def stage5(it):
        s = slot_of(res, it)
        part = pl.ds(at.core * 8, 8)
        return [rdma(res.at[s, part], res.at[s, part], s5, s, at.core_peer)]

    def start(copies):
        for copy in copies:
            copy.start()

    def wait(copies):
        for copy in copies:
            copy.wait()

    def product(it, left, right, offset):
        def half(which, dst):
            slot = slot_of(dst, it)

            @pl.loop(0, 4)
            def _(i):
                row = pl.multiple_of(which * (8 * BLOCK) + i * WIDE, WIDE)
                tile = dot(
                    left[pl.ds(row, WIDE), :],
                    right[:, pl.ds(pl.multiple_of(offset, WIDE), WIDE)],
                    1,
                    0,
                    BF16,
                )
                dst[slot, i * 2] = tile[:BLOCK]
                dst[slot, i * 2 + 1] = tile[BLOCK:]

        half(1 - at.core, away)
        start(stage0(it))
        half(at.core, acc)

    def flat_copies(it):
        slot = slot_of(flat, it)
        column = pl.ds(pl.multiple_of(it * WIDE, WIDE), WIDE)
        return [
            pltpu.make_async_copy(
                flat.at[slot, pl.ds(0, n_down)], down_out.at[:, column], s_flat.at[0, slot]
            ),
            pltpu.make_async_copy(
                flat.at[slot, pl.ds(n_down, n_out)], out_out.at[:, column], s_flat.at[1, slot]
            ),
        ]

    def pair_copies(it):
        slot = slot_of(pairs, it)
        column = pl.ds(pl.multiple_of((it - n_d) * BLOCK, BLOCK), BLOCK)
        return [pltpu.make_async_copy(pairs.at[slot], gu_out.at[:, :, column], s_pair.at[slot])]

    def qkv_copies(it):
        slot = slot_of(flat, it)
        n = it - n_d - n_g
        column = pl.ds(pl.multiple_of(lax.rem(n, qkv_items) * WIDE, WIDE), WIDE)
        return [
            pltpu.make_async_copy(
                flat.at[slot], qkv_out.at[lax.div(n, qkv_items), :, column], s_flat.at[0, slot]
            )
        ]

    def by_kind(it, valid, down, gate, attn):
        pl.when(jnp.logical_and(valid, it < n_d))(lambda: down(it))
        pl.when(jnp.logical_and(valid, jnp.logical_and(it >= n_d, it < n_d + n_g)))(
            lambda: gate(it)
        )
        pl.when(jnp.logical_and(valid, it >= n_d + n_g))(lambda: attn(it))

    def fill_flat(it):
        s, slot = slot_of(res, it), slot_of(flat, it)

        @pl.loop(0, PIECES)
        def _(p):
            flat[slot, pl.ds(pl.multiple_of(p * BLOCK, BLOCK), BLOCK), :] = res[s, p].astype(F32)

    def fill_pairs(it):
        s, slot = slot_of(res, it), slot_of(pairs, it)

        @pl.loop(0, PIECES)
        def _(p):
            rows = pl.ds(pl.multiple_of(p * BLOCK, BLOCK), BLOCK)
            pairs[slot, rows, 0, :] = res[s, p, :, :BLOCK].astype(F32)
            pairs[slot, rows, 1, :] = res[s, p, :, BLOCK:].astype(F32)

    def put_out(it):
        by_kind(
            it,
            it >= 0,
            lambda n: fill_flat(n) or start(flat_copies(n)),
            lambda n: fill_pairs(n) or start(pair_copies(n)),
            lambda n: fill_flat(n) or start(qkv_copies(n)),
        )

    def wait_out(it, valid):
        by_kind(
            it,
            valid,
            lambda n: wait(flat_copies(n)),
            lambda n: wait(pair_copies(n)),
            lambda n: wait(qkv_copies(n)),
        )

    barrier = pltpu.get_barrier_semaphore()
    for peer in (at.core_peer, at.x_peer, at.y_peer):
        pl.semaphore_signal(barrier, inc=1, device_id=peer, device_id_type=MESH)
    pl.semaphore_wait(barrier, 3)

    def live(it):
        return jnp.logical_and(it >= 0, it < total)

    @pl.loop(0, total + 6 * LAG + 2)
    def _(tick):
        one = tick - LAG

        @pl.when(live(one))
        def _():
            wait(stage0(one))
            sa, s = slot_of(acc, one), slot_of(rcv0, one)

            @pl.loop(0, 8)
            def _(p):
                acc[sa, p] = (acc[sa, p].astype(F32) + rcv0[s, p].astype(F32)).astype(BF16)

            start(stage1(one))

        two = tick - 2 * LAG

        @pl.when(live(two))
        def _():
            wait(stage1(two))
            sa, s = slot_of(acc, two), slot_of(rcv1, two)
            for n, bit in ((0, at.x), (1, at.y)):
                for k in range(2):
                    p = quarter(bit, n) + k
                    acc[sa, p] = (
                        acc[sa, p].astype(F32) + rcv1[s, n, k].astype(F32)
                    ).astype(BF16)
            start(stage2(two))

        three = tick - 3 * LAG

        @pl.when(live(three))
        def _():
            wait(stage2(three))
            sa, s, d = slot_of(acc, three), slot_of(rcv2, three), slot_of(res, three)
            for n, p in ((0, quarter(at.x, 0) + at.y), (1, quarter(at.y, 1) + at.x)):
                res[d, at.core * 8 + p] = (
                    acc[sa, p].astype(F32) + rcv2[s, n].astype(F32)
                ).astype(BF16)
            start(stage3(three))

        four = tick - 4 * LAG

        @pl.when(live(four))
        def _():
            wait(stage3(four))
            start(stage4(four))

        five = tick - 5 * LAG

        @pl.when(live(five))
        def _():
            wait(stage4(five))
            start(stage5(five))

        by_kind(
            tick,
            tick < total,
            lambda n: product(n, ha_ref, dy_ref, n * WIDE),
            lambda n: product(n, nt_ref, dgu_ref, (n - n_d) * WIDE),
            lambda n: product(n, nt_ref, dqkv_ref, (n - n_d - n_g) * WIDE),
        )

        six = tick - 6 * LAG
        wait_out(six - 2, live(six - 2))

        @pl.when(live(six))
        def _():
            wait(stage5(six))
            put_out(six)


def summed_grads(ha, nt, dy, dgu, dqkv, n_down, n_out):
    n_d = dy.shape[1] // WIDE
    n_g = dgu.shape[1] // WIDE
    n_q = dqkv.shape[1] // WIDE
    model = nt.shape[0]
    piece = lambda slots, *lead: pltpu.VMEM((slots, *lead, BLOCK, WIDE), BF16)
    sems = lambda slots: pltpu.SemaphoreType.DMA((2, slots))
    slots = 2 * LAG + 3
    final = 4 * LAG + 2
    return pl.pallas_call(
        functools.partial(grads_kernel, n_d, n_g, n_q),
        in_specs=[pl.BlockSpec(memory_space=pltpu.VMEM)] * 5,
        out_specs=[pl.BlockSpec(memory_space=pl.ANY)] * 4,
        out_shape=[
            jax.ShapeDtypeStruct((n_down, model), F32),
            jax.ShapeDtypeStruct((n_out, model), F32),
            jax.ShapeDtypeStruct((model, 2, dgu.shape[1] // 2), F32),
            jax.ShapeDtypeStruct((3, model, n_out), F32),
        ],
        scratch_shapes=[
            piece(LAG + 1, 8),
            piece(3 * LAG + 1, 8),
            piece(slots, 8),
            piece(slots, 2, 2),
            piece(slots, 2),
            piece(final, PIECES),
            pltpu.VMEM((2, model, WIDE), F32),
            pltpu.VMEM((2, model, 2, BLOCK), F32),
            sems(slots), sems(slots), sems(slots), sems(slots), sems(slots),
            sems(final), sems(final), sems(final), sems(final), sems(final),
            sems(2),
            pltpu.SemaphoreType.DMA((2,)),
        ],
        compiler_params=pltpu.CompilerParams(
            collective_id=0, has_side_effects=True, vmem_limit_bytes=63 << 20
        ),
        name="summed_grads",
    )(ha, nt, dy, dgu, dqkv)


def fast_path(n_dp, model_width, local_width, local_ff):
    return (
        n_dp == 8
        and model_width == PIECES * BLOCK
        and local_width % WIDE == 0
        and local_ff % BLOCK == 0
        and local_ff + local_width <= model_width
    )


def on_device(
    n_dp,
    n_mp,
    tokens,
    norm_gain,
    layernorm_bias,
    qkv_weight,
    qkv_bias,
    out_weight,
    gate_up_weight,
    down_weight,
    grad_out,
):
    cube = Cube("dp", n_dp)
    rows, model_width = tokens.shape
    local_width = qkv_weight.shape[2]
    seq_len = rows * n_mp
    fast = fast_path(n_dp, model_width, local_width, gate_up_weight.shape[2])
    gain = norm_gain.astype(F32)
    token_f32 = tokens.astype(F32)
    row_mean = jnp.mean(token_f32, axis=1, keepdims=True)
    centered = token_f32 - row_mean
    inv_std = lax.rsqrt(jnp.mean(centered * centered, axis=1, keepdims=True) + EPS)
    xhat = centered * inv_std
    normed_own = (xhat * gain + layernorm_bias.astype(F32)).astype(BF16)
    normed = lax.all_gather(normed_own, "mp", axis=0, tiled=True)
    dy = lax.all_gather(grad_out, "mp", axis=0, tiled=True)

    w_qkv = [qkv_weight[:, t, :] for t in range(3)]
    w_gate, w_up = gate_up_weight[:, 0, :], gate_up_weight[:, 1, :]
    tables = rotary_tables(seq_len)

    gate = dot(normed, w_gate, 1, 0)
    up = dot(normed, w_up, 1, 0)
    sig = jax.nn.sigmoid(gate)
    hidden = (gate * sig * up).astype(BF16)
    qkv = jnp.concatenate([dot(normed, w, 1, 0) for w in w_qkv], axis=1)
    q, k, v, attended, lse = attention_forward(qkv, qkv_bias.astype(F32), tables)
    branch = (dot(attended, out_weight, 1, 0) + dot(hidden, down_weight, 1, 0)).astype(BF16)
    share = lax.psum_scatter(branch, "mp", scatter_dimension=0, tiled=True)
    layer_out = (token_f32 + share.astype(F32)).astype(BF16)

    d_hidden = dot(dy, down_weight, 1, 1)
    silu = gate * sig
    d_gate = (d_hidden * up * (sig + silu * (1.0 - sig))).astype(BF16)
    d_up = (d_hidden * silu).astype(BF16)
    d_attended = dot(dy, out_weight, 1, 1, BF16)
    dq, dk, dv, sums = attention_backward(q, k, v, d_attended, lse, tables)
    d_normed = (
        dot(d_gate, w_gate, 1, 1)
        + dot(d_up, w_up, 1, 1)
        + dot(dq, w_qkv[0], 1, 1)
        + dot(dk, w_qkv[1], 1, 1)
        + dot(dv, w_qkv[2], 1, 1)
    ).astype(BF16)
    d_own = lax.psum_scatter(d_normed, "mp", scatter_dimension=0, tiled=True).astype(F32)
    d_qkv = jnp.concatenate([dq, dk, dv], axis=1)
    local_ff = hidden.shape[1]
    if fast:
        pad = model_width - local_ff - local_width
        ha = jnp.concatenate(
            [hidden, attended, jnp.zeros((seq_len, pad), BF16)], axis=1
        ).T
        d_gate_up = jnp.stack(
            [d.reshape(seq_len, local_ff // BLOCK, BLOCK) for d in (d_gate, d_up)], axis=2
        ).reshape(seq_len, 2 * local_ff)
        grad_down_w, grad_out_w, grad_gate_up_w, grad_qkv_w = summed_grads(
            ha, normed.T, dy, d_gate_up, d_qkv, local_ff, local_width
        )
        grad_qkv_w = grad_qkv_w.transpose(1, 0, 2)
    else:
        grad_down_w = cube.contract(hidden, dy)
        grad_out_w = cube.contract(attended, dy)
        grad_gate_up_w = jnp.stack(
            [cube.contract(normed, d_gate), cube.contract(normed, d_up)], axis=1
        )
        grad_qkv_w = cube.contract(normed, d_qkv).reshape(model_width, 3, local_width)

    scaled = d_own * gain
    grad_tokens = grad_out.astype(F32) + inv_std * (
        scaled
        - jnp.mean(scaled, axis=1, keepdims=True)
        - xhat * jnp.mean(scaled * xhat, axis=1, keepdims=True)
    )
    terms = jnp.stack([jnp.sum(d_own * xhat, axis=0), jnp.sum(d_own, axis=0)])
    bias_sum = cube.sum_all(sums)
    grad_bias = bias_sum.swapaxes(0, 1).reshape(3, local_width)
    terms = Cube("mp", n_mp).sum_all(cube.sum_all(terms))
    share_width = model_width // n_mp
    terms = lax.dynamic_slice_in_dim(
        terms, lax.axis_index("mp") * share_width, share_width, 1
    )
    return (
        layer_out,
        grad_tokens.astype(BF16),
        terms[0],
        terms[1],
        grad_qkv_w,
        grad_bias,
        grad_out_w,
        grad_gate_up_w,
        grad_down_w,
    )


def solution(mesh):
    return jax.shard_map(
        functools.partial(on_device, mesh.shape["dp"], mesh.shape["mp"]),
        mesh=mesh,
        in_specs=(
            P(("dp", "mp"), None),
            P(),
            P(),
            P(None, None, "mp"),
            P(None, "mp"),
            P("mp", None),
            P(None, None, "mp"),
            P("mp", None),
            P(("dp", "mp"), None),
        ),
        out_specs=(
            P(("dp", "mp"), None),
            P(("dp", "mp"), None),
            P("mp"),
            P("mp"),
            P(None, None, "mp"),
            P(None, "mp"),
            P("mp", None),
            P(None, None, "mp"),
            P("mp", None),
        ),
        check_vma=False,
    )
```

```python
import functools
import math

import jax
import jax.numpy as jnp
from jax import lax
from jax.experimental import pallas as pl
from jax.experimental.pallas import tpu as pltpu
from jax.sharding import PartitionSpec as P

HD = 64
ROT = 16
EPS = 1e-05
LANES = 128
QB = 256


F32 = jnp.float32
BF16 = jnp.bfloat16


def dot(a, b, ca, cb, out=F32):
    return lax.dot_general(
        a, b, (((ca,), (cb,)), ((), ())), preferred_element_type=F32
    ).astype(out)


def rotary_tables(seq_len):
    positions = jnp.arange(seq_len, dtype=F32)
    freqs = 1.0 / 10000.0 ** (jnp.arange(ROT // 2, dtype=F32) * 2.0 / ROT)
    phase = positions[:, None] * freqs[None, :]
    cosine, sine = jnp.cos(phase), jnp.sin(phase)
    half = ROT // 2
    rest = HD - ROT
    ones = jnp.ones((seq_len, rest), F32)
    zeros = jnp.zeros((seq_len, rest), F32)
    zhalf = jnp.zeros((seq_len, half), F32)
    c = jnp.concatenate([cosine, cosine, ones], axis=1)
    up = jnp.concatenate([-sine, zhalf, zeros], axis=1)
    down = jnp.concatenate([zhalf, sine, zeros], axis=1)
    two = LANES // HD
    return jnp.stack([jnp.tile(t, (1, two)) for t in (c, up, down)])


def turn(x, tables, sign):
    half = ROT // 2
    ahead = pltpu.roll(x, LANES - half, 1)
    behind = pltpu.roll(x, half, 1)
    return x * tables[0] + sign * (ahead * tables[1] + behind * tables[2])


def lane_mask(rows, j):
    lane = lax.broadcasted_iota(jnp.int32, (rows, LANES), 1)
    return (lane // HD) == j


def forward_kernel(
    q_in, k_in, v_in, bias_ref, tab_ref, q_out, k_out, v_out, o_ref, lse_ref
):
    seq_len = q_in.shape[0]
    j = pl.program_id(1)

    @pl.when(j == 0)
    def _():
        tables = (tab_ref[0], tab_ref[1], tab_ref[2])
        q_out[...] = turn(q_in[...] + bias_ref[0, 0:1], tables, 1.0).astype(BF16)
        k_out[...] = turn(k_in[...] + bias_ref[0, 1:2], tables, 1.0).astype(BF16)
        v_out[...] = (v_in[...] + bias_ref[0, 2:3]).astype(BF16)

    mask = lane_mask(QB, j)
    causal = lax.broadcasted_iota(jnp.int32, (QB, QB), 0) <= lax.broadcasted_iota(
        jnp.int32, (QB, QB), 1
    )
    for i in range(seq_len // QB):
        rows = pl.ds(i * QB, QB)
        span = (i + 1) * QB
        q = q_out[rows, :] * 0.125
        q = jnp.where(mask, q, jnp.zeros_like(q))
        parts = []
        if i:
            parts.append(dot(k_out[pl.ds(0, i * QB), :], q, 1, 1))
        diag = dot(k_out[rows, :], q, 1, 1)
        parts.append(jnp.where(causal, diag, -1e30))
        top = functools.reduce(
            jnp.maximum, [jnp.max(s, axis=0, keepdims=True) for s in parts]
        )
        exps = [jnp.exp(s - top) for s in parts]
        total = sum(jnp.sum(e, axis=0, keepdims=True) for e in exps)
        inv = 1.0 / total
        probs = jnp.concatenate([(e * inv).astype(BF16) for e in exps], axis=0)
        out = dot(probs, v_out[pl.ds(0, span), :], 0, 0).astype(BF16)
        before = o_ref[rows, :]
        o_ref[rows, :] = jnp.where(mask, out, before)
        lse_ref[0, 0, :, i * QB : (i + 1) * QB] = top + jnp.log(total)


def backward_kernel(
    q_ref, k_ref, v_ref, do_ref, lse_ref, tab_ref, dq_out, dk_out, dv_out, sums_out, dq, dk, dv
):
    seq_len = q_ref.shape[0]
    j = pl.program_id(1)
    mask = lane_mask(QB, j)
    causal = lax.broadcasted_iota(jnp.int32, (QB, QB), 0) <= lax.broadcasted_iota(
        jnp.int32, (QB, QB), 1
    )

    @pl.when(j == 0)
    def _():
        dk[...] = jnp.zeros_like(dk)
        dv[...] = jnp.zeros_like(dv)

    for i in range(seq_len // QB):
        rows = pl.ds(i * QB, QB)
        q = q_ref[rows, :] * 0.125
        q = jnp.where(mask, q, jnp.zeros_like(q))
        do = do_ref[rows, :]
        do = jnp.where(mask, do, jnp.zeros_like(do))
        lse = lse_ref[0, 0, :, i * QB : (i + 1) * QB]
        pieces = []
        if i:
            pieces.append((pl.ds(0, i * QB), False))
        pieces.append((rows, True))
        probs, grads = [], []
        inner = 0.0
        for where, diagonal in pieces:
            s = dot(k_ref[where, :], q, 1, 1)
            if diagonal:
                s = jnp.where(causal, s, -1e30)
            p = jnp.exp(s - lse)
            dp = dot(v_ref[where, :], do, 1, 1)
            inner = inner + jnp.sum(p * dp, axis=0, keepdims=True)
            probs.append(p)
            grads.append(dp)
        acc = 0.0
        for (where, diagonal), p, dp in zip(pieces, probs, grads):
            ds = (p * (dp - inner)).astype(BF16)
            dv[where, :] += dot(p.astype(BF16), do, 1, 0)
            dk[where, :] += dot(ds, q, 1, 0)
            acc = acc + dot(ds, k_ref[where, :], 0, 0)
        before = dq[rows, :]
        dq[rows, :] = jnp.where(mask, acc * 0.125, before)

    @pl.when(j == pl.num_programs(1) - 1)
    def _():
        tables = (tab_ref[0], tab_ref[1], tab_ref[2])
        gq = turn(dq[...], tables, -1.0).astype(BF16)
        gk = turn(dk[...], tables, -1.0).astype(BF16)
        gv = dv[...].astype(BF16)
        dq_out[...] = gq
        dk_out[...] = gk
        dv_out[...] = gv
        sums_out[0, 0:1] = jnp.sum(gq.astype(F32), axis=0, keepdims=True)
        sums_out[0, 1:2] = jnp.sum(gk.astype(F32), axis=0, keepdims=True)
        sums_out[0, 2:3] = jnp.sum(gv.astype(F32), axis=0, keepdims=True)


def attention_forward(qkv, bias, tables):
    seq_len, width = qkv.shape[0], qkv.shape[1] // 3
    pairs = width // LANES
    column = lambda part: pl.BlockSpec((seq_len, LANES), lambda p, j: (0, part * pairs + p))
    block = pl.BlockSpec((seq_len, LANES), lambda p, j: (0, p))
    bias_blocks = bias.reshape(3, pairs, LANES).swapaxes(0, 1)
    wide = jax.ShapeDtypeStruct((seq_len, width), BF16)
    elements = pairs * 2 * seq_len * seq_len // 2
    return pl.pallas_call(
        forward_kernel,
        grid=(pairs, LANES // HD),
        in_specs=[
            column(0),
            column(1),
            column(2),
            pl.BlockSpec((1, 3, LANES), lambda p, j: (p, 0, 0)),
            pl.BlockSpec((3, seq_len, LANES), lambda p, j: (0, 0, 0)),
        ],
        out_specs=[
            block,
            block,
            block,
            block,
            pl.BlockSpec((1, 1, 1, seq_len), lambda p, j: (p, j, 0, 0)),
        ],
        out_shape=[
            wide,
            wide,
            wide,
            wide,
            jax.ShapeDtypeStruct((pairs, LANES // HD, 1, seq_len), F32),
        ],
        cost_estimate=pl.CostEstimate(
            flops=elements * 4 * LANES,
            bytes_accessed=qkv.size * 4 + 4 * seq_len * width * 2,
            transcendentals=elements,
        ),
        name="attention_forward",
    )(qkv, qkv, qkv, bias_blocks, tables)


def attention_backward(q, k, v, grad, lse, tables):
    seq_len, width = q.shape
    pairs = width // LANES
    block = pl.BlockSpec((seq_len, LANES), lambda p, j: (0, p))
    wide = jax.ShapeDtypeStruct((seq_len, width), BF16)
    elements = pairs * 2 * seq_len * seq_len // 2
    return pl.pallas_call(
        backward_kernel,
        grid=(pairs, LANES // HD),
        in_specs=[
            block,
            block,
            block,
            block,
            pl.BlockSpec((1, 1, 1, seq_len), lambda p, j: (p, j, 0, 0)),
            pl.BlockSpec((3, seq_len, LANES), lambda p, j: (0, 0, 0)),
        ],
        out_specs=[block, block, block, pl.BlockSpec((1, 3, LANES), lambda p, j: (p, 0, 0))],
        out_shape=[wide, wide, wide, jax.ShapeDtypeStruct((pairs, 3, LANES), F32)],
        scratch_shapes=[pltpu.VMEM((seq_len, LANES), F32)] * 3,
        cost_estimate=pl.CostEstimate(
            flops=elements * 10 * LANES,
            bytes_accessed=7 * seq_len * width * 2,
            transcendentals=elements,
        ),
        name="attention_backward",
    )(q, k, v, grad, lse, tables)


def pick(x, index):
    return lax.dynamic_index_in_dim(x, index, 0, keepdims=False)


class Cube:
    def __init__(self, axis, size):
        self.axis, self.size = axis, size
        self.bits = [b for b in range(size.bit_length()) if 1 << b < size]
        me = lax.axis_index(axis)
        self.own = [lax.rem(lax.div(me, 1 << b), 2) for b in self.bits]

    def swap(self, x, b):
        return lax.ppermute(x, self.axis, [(i, i ^ (1 << b)) for i in range(self.size)])

    def sum_all(self, x):
        for b in self.bits:
            x = x + self.swap(x, b)
        return x

    def contract(self, left, right):
        depth, rows = left.shape
        columns = right.shape[1]
        core, others = self.bits[0], self.bits[1:]
        half = rows // 2
        mine = self.own[0]
        first = lax.dynamic_slice_in_dim(left, (1 - mine) * half, half, 1)
        second = lax.dynamic_slice_in_dim(left, mine * half, half, 1)
        away = dot(first, right, 0, 0, BF16)
        came = self.swap(away, core)
        keep = dot(second, right, 0, 0, BF16)
        orders = [others, others[::-1]]
        quarter = half // 2
        done = []
        for n, order in enumerate(orders):
            small = quarter >> len(order)
            shape = (2,) * len(order) + (small, columns)
            cur = (
                keep[n * quarter : (n + 1) * quarter].astype(F32)
                + came[n * quarter : (n + 1) * quarter].astype(F32)
            ).reshape(shape)
            for b in order:
                own = self.own[b]
                send = pick(cur, 1 - own).astype(BF16)
                got = self.swap(send, b)
                cur = pick(cur, own) + got.astype(F32)
            buf = cur.astype(BF16)
            for b in order[::-1]:
                own = self.own[b]
                got = self.swap(buf, b)
                low = jnp.where(own == 0, buf, got)
                high = jnp.where(own == 0, got, buf)
                buf = jnp.stack([low, high])
            done.append(buf.reshape(quarter, columns))
        whole = jnp.concatenate(done, axis=0)
        other = self.swap(whole, core)
        low = jnp.where(mine == 0, whole, other)
        high = jnp.where(mine == 0, other, whole)
        return jnp.concatenate([low, high], axis=0).astype(F32)


LAG = 2
BLOCK = 128
PIECES = 16
WIDE = 256
MESH = pl.DeviceIdType.MESH


class Places:
    def __init__(self, n_z):
        self.me = lax.axis_index("dp")
        self.z = lax.axis_index("mp")
        self.core = lax.rem(self.me, 2)
        self.x = lax.rem(lax.div(self.me, 2), 2)
        self.y = lax.div(self.me, 4)
        self.core_peer = (self.me + 1 - 2 * self.core, self.z)
        self.x_peer = (self.me + 2 - 4 * self.x, self.z)
        self.y_peer = (self.me + 4 - 8 * self.y, self.z)
        self.z_of = [lax.rem(self.z + d, n_z) for d in range(n_z)]
        self.z_peers = [(self.me, z) for z in self.z_of]


def rdma(src, dst, send_sem, recv_sem, peer):
    return pltpu.make_async_remote_copy(
        src_ref=src,
        dst_ref=dst,
        send_sem=send_sem,
        recv_sem=recv_sem,
        device_id=peer,
        device_id_type=MESH,
    )


def start(copies):
    for copy in copies:
        copy.start()


def wait(copies):
    for copy in copies:
        copy.wait()


def rows_at(i, size):
    return pl.ds(pl.multiple_of(i * size, size), size)


def attention_unit(u, q_v, k_v, v_v, do_v, lse_ref, tab_ref, dqkv_v, small, dq, dk, dv):
    seq_len, width = q_v.shape
    pair, j = lax.div(u, 2), lax.rem(u, 2)
    lanes = rows_at(pair, LANES)
    mask = lane_mask(QB, j)
    causal = lax.broadcasted_iota(jnp.int32, (QB, QB), 0) <= lax.broadcasted_iota(
        jnp.int32, (QB, QB), 1
    )

    @pl.when(j == 0)
    def _():
        dk[...] = jnp.zeros_like(dk)
        dv[...] = jnp.zeros_like(dv)
        dq[...] = jnp.zeros_like(dq)

    for i in range(seq_len // QB):
        rows = pl.ds(i * QB, QB)
        q = q_v[rows, lanes] * 0.125
        q = jnp.where(mask, q, jnp.zeros_like(q))
        do = do_v[rows, lanes]
        do = jnp.where(mask, do, jnp.zeros_like(do))
        lse = lse_ref[u, :, i * QB : (i + 1) * QB]
        pieces = []
        if i:
            pieces.append((pl.ds(0, i * QB), False))
        pieces.append((rows, True))
        probs, grads = [], []
        inner = 0.0
        for where, diagonal in pieces:
            s = dot(k_v[where, lanes], q, 1, 1)
            if diagonal:
                s = jnp.where(causal, s, -1e30)
            p = jnp.exp(s - lse)
            dp = dot(v_v[where, lanes], do, 1, 1)
            inner = inner + jnp.sum(p * dp, axis=0, keepdims=True)
            probs.append(p)
            grads.append(dp)
        acc = 0.0
        for (where, diagonal), p, dp in zip(pieces, probs, grads):
            ds = (p * (dp - inner)).astype(BF16)
            dv[where, :] += dot(p.astype(BF16), do, 1, 0)
            dk[where, :] += dot(ds, q, 1, 0)
            acc = acc + dot(ds, k_v[where, lanes], 0, 0)
        dq[rows, :] = jnp.where(mask, acc * 0.125, dq[rows, :])

    @pl.when(j == 1)
    def _():
        tables = (tab_ref[0], tab_ref[1], tab_ref[2])
        out = (
            turn(dq[...], tables, -1.0).astype(BF16),
            turn(dk[...], tables, -1.0).astype(BF16),
            dv[...].astype(BF16),
        )
        for t, g in enumerate(out):
            dqkv_v[:, pl.ds(pl.multiple_of(t * width + pair * LANES, LANES), LANES)] = g
            small[2 + t : 3 + t, lanes] = jnp.sum(g.astype(F32), axis=0, keepdims=True)


def backward_pass(
    n_d, n_g, n_q, n_z,
    hat, nt, dy, datt, a1, a2, q, k, v, lse_ref, tables, w_down, w_gate, w_up, w_qkv, tokens, gain_ref,
    sums_out, grad_tokens_out, small_out,
    hat_v, nt_v, dy_v, do_v, a1_v, a2_v, q_v, k_v, v_v, tab_v, tok_v,
    dqkv_v, dq, dk, dv, wd_v, wg_v, wu_v, wq_v, zsend, zin, dsum, small, small_in, share_in,
    away, acc, rcv0, rcv1, rcv2, fin,
    load, s_wd, s_wn, s_tok, z_sems, small_sems, share_sems,
    s0, s1, s2, s3, s4, s5, s_fin,
):
    at = Places(n_z)
    total = n_d + n_g + n_q
    own_rows = tok_v.shape[0]
    width = q_v.shape[1]
    chunks = dsum.shape[1] // WIDE

    def slot_of(buf, it):
        return lax.rem(it, buf.shape[0])

    loads = [
        pltpu.make_async_copy(src, dst, load.at[i])
        for i, (src, dst) in enumerate(
            [
                (hat, hat_v), (dy, dy_v), (a1, a1_v), (a2, a2_v), (datt, do_v),
                (q, q_v), (k, k_v), (v, v_v), (tables, tab_v), (nt, nt_v), (tokens, tok_v),
            ]
        )
    ]

    def load_wd(f):
        s = lax.rem(f, 2)
        return [pltpu.make_async_copy(w_down.at[rows_at(f, BLOCK)], wd_v.at[s], s_wd.at[s])]

    def load_wn(c):
        s = lax.rem(c, 2)
        rows = rows_at(c, WIDE)
        return [
            pltpu.make_async_copy(w_gate.at[rows], wg_v.at[s], s_wn.at[0, s]),
            pltpu.make_async_copy(w_up.at[rows], wu_v.at[s], s_wn.at[1, s]),
            pltpu.make_async_copy(w_qkv.at[:, rows], wq_v.at[s], s_wn.at[2, s]),
        ]

    def quarter(bit, half):
        return half * 4 + bit * 2

    def stage0(it):
        sa, s = slot_of(away, it), slot_of(rcv0, it)
        return [rdma(away.at[sa], rcv0.at[s], s0.at[0, s], s0.at[1, s], at.core_peer)]

    def stage1(it):
        sa, s = slot_of(acc, it), slot_of(rcv1, it)
        a, b = pl.ds(quarter(1 - at.x, 0), 2), pl.ds(quarter(1 - at.y, 1), 2)
        return [
            rdma(acc.at[sa, a], rcv1.at[s, 0], s1.at[0, s], s1.at[1, s], at.x_peer),
            rdma(acc.at[sa, b], rcv1.at[s, 1], s1.at[2, s], s1.at[3, s], at.y_peer),
        ]

    def stage2(it):
        sa, s = slot_of(acc, it), slot_of(rcv2, it)
        a, b = quarter(at.x, 0) + 1 - at.y, quarter(at.y, 1) + 1 - at.x
        return [
            rdma(acc.at[sa, a], rcv2.at[s, 0], s2.at[0, s], s2.at[1, s], at.y_peer),
            rdma(acc.at[sa, b], rcv2.at[s, 1], s2.at[2, s], s2.at[3, s], at.x_peer),
        ]

    def piece_a():
        return at.core * 8 + quarter(at.x, 0) + at.y

    def piece_b():
        return at.core * 8 + quarter(at.y, 1) + at.x

    def stage3(it):
        s, n = slot_of(fin, it), lax.rem(it, s3.shape[1])
        a, b = sums_out.at[it, piece_a()], sums_out.at[it, piece_b()]
        return [
            rdma(fin.at[s, 0], a, s3.at[0, n], s3.at[1, n], at.y_peer),
            rdma(fin.at[s, 1], b, s3.at[2, n], s3.at[3, n], at.x_peer),
        ]

    def keep3(it):
        s = slot_of(fin, it)
        return [
            pltpu.make_async_copy(fin.at[s, 0], sums_out.at[it, piece_a()], s_fin.at[0, s]),
            pltpu.make_async_copy(fin.at[s, 1], sums_out.at[it, piece_b()], s_fin.at[1, s]),
        ]

    def stage4(it):
        n = lax.rem(it, s4.shape[1])
        a = sums_out.at[it, pl.ds(at.core * 8 + quarter(at.x, 0), 2)]
        b = sums_out.at[it, pl.ds(at.core * 8 + quarter(at.y, 1), 2)]
        return [
            rdma(a, a, s4.at[0, n], s4.at[1, n], at.x_peer),
            rdma(b, b, s4.at[2, n], s4.at[3, n], at.y_peer),
        ]

    def stage5(it):
        n = lax.rem(it, s5.shape[1])
        part = sums_out.at[it, pl.ds(at.core * 8, 8)]
        return [rdma(part, part, s5.at[0, n], s5.at[1, n], at.core_peer)]

    def product(it, left, right):
        def half(which, dst):
            slot = slot_of(dst, it)

            @pl.loop(0, 4)
            def _(i):
                row = pl.multiple_of(which * (8 * BLOCK) + i * WIDE, WIDE)
                tile = dot(left[pl.ds(row, WIDE), :], right(), 1, 0, BF16)
                dst[slot, i * 2] = tile[:BLOCK]
                dst[slot, i * 2 + 1] = tile[BLOCK:]

        half(1 - at.core, away)
        start(stage0(it))
        half(at.core, acc)

    def gate_right(f):
        lanes = rows_at(f, BLOCK)
        return jnp.concatenate([a1_v[:, lanes], a2_v[:, lanes]], axis=1)

    def hidden_job(f):
        s = lax.rem(f, 2)
        wait(load_wd(f))

        @pl.when(f + 1 < n_g)
        def _():
            start(load_wd(f + 1))

        lanes = rows_at(f, BLOCK)

        @pl.loop(0, dy_v.shape[0] // WIDE)
        def _(r):
            rows = rows_at(r, WIDE)
            dh = dot(dy_v[rows, :], wd_v[s], 1, 1)
            a1_v[rows, lanes] = (dh * a1_v[rows, lanes].astype(F32)).astype(BF16)
            a2_v[rows, lanes] = (dh * a2_v[rows, lanes].astype(F32)).astype(BF16)

    def z_copies(c):
        s = slot_of(zsend, c)
        columns = rows_at(c, WIDE)
        return [
            rdma(
                zsend.at[s, rows_at(at.z_of[d], own_rows)],
                zin.at[d - 1, :, columns],
                z_sems.at[0, d - 1, c],
                z_sems.at[1, d - 1, c],
                at.z_peers[d],
            )
            for d in range(1, n_z)
        ]

    def normed_job(c):
        s, w = slot_of(zsend, c), lax.rem(c, 2)
        wait(load_wn(c))

        @pl.when(c + 1 < chunks)
        def _():
            start(load_wn(c + 1))

        @pl.when(c >= zsend.shape[0])
        def _():
            for copy in z_copies(c - zsend.shape[0]):
                copy.wait_send()

        @pl.loop(0, dy_v.shape[0] // WIDE)
        def _(r):
            rows = rows_at(r, WIDE)
            part = dot(a1_v[rows, :], wg_v[w], 1, 1) + dot(a2_v[rows, :], wu_v[w], 1, 1)
            for t in range(3):
                part = part + dot(
                    dqkv_v[rows, t * width : (t + 1) * width], wq_v[w, t], 1, 1
                )
            zsend[s, rows, :] = part.astype(BF16)

        start(z_copies(c))
        dsum[:, rows_at(c, WIDE)] = zsend[s, rows_at(at.z, own_rows), :].astype(F32)

    def norm_job():
        @pl.loop(0, chunks)
        def _(c):
            @pl.when(c >= chunks - zsend.shape[0])
            def _():
                for copy in z_copies(c):
                    copy.wait_send()

            for copy in z_copies(c):
                copy.wait_recv()

        gain = gain_ref[0:1, :]
        step = 32

        @pl.loop(0, own_rows // step)
        def _(r):
            rows = rows_at(r, step)
            d = dsum[rows, :]
            for n in range(n_z - 1):
                d = d + zin[n, rows, :].astype(F32)
            tok = tok_v[rows, :].astype(F32)
            centered = tok - jnp.mean(tok, axis=1, keepdims=True)
            inv_std = lax.rsqrt(jnp.mean(centered * centered, axis=1, keepdims=True) + EPS)
            xhat = centered * inv_std
            scaled = d * gain
            dy_own = dy_v[pl.ds(pl.multiple_of(at.z * own_rows + r * step, step), step), :]
            dsum[rows, :] = dy_own.astype(F32) + inv_std * (
                scaled
                - jnp.mean(scaled, axis=1, keepdims=True)
                - xhat * jnp.mean(scaled * xhat, axis=1, keepdims=True)
            )
            small[0:1, :] += jnp.sum(d * xhat, axis=0, keepdims=True)
            small[1:2, :] += jnp.sum(d, axis=0, keepdims=True)
            tok_v[rows, :] = dsum[rows, :].astype(BF16)

        start(tokens_out())

    def tokens_out():
        return [pltpu.make_async_copy(tok_v, grad_tokens_out, s_tok)]

    small_peers = (at.core_peer, at.x_peer, at.y_peer)

    def small_copy(n):
        return [
            rdma(small, small_in.at[n], small_sems.at[0, n], small_sems.at[1, n], small_peers[n])
        ]

    def share_copies():
        share = small.shape[1] // n_z
        return [
            rdma(
                small.at[:, rows_at(at.z_of[d], share)],
                share_in.at[d - 1],
                share_sems.at[0, d - 1],
                share_sems.at[1, d - 1],
                at.z_peers[d],
            )
            for d in range(1, n_z)
        ]

    def small_step(n):
        wait(small_copy(n))
        small[...] = small[...] + small_in[n]
        start(small_copy(n + 1) if n < 2 else share_copies())

    def small_end():
        wait(share_copies())
        share = small.shape[1] // n_z
        mine = small[0:2, rows_at(at.z, share)]
        for n in range(n_z - 1):
            mine = mine + share_in[n, 0:2, :]
        small_out[0:2, :] = mine
        small_out[2:5, :] = small[2:5, 0:share]

    barrier = pltpu.get_barrier_semaphore()
    peers = [at.core_peer, at.x_peer, at.y_peer] + at.z_peers[1:]
    for peer in peers:
        pl.semaphore_signal(barrier, inc=1, device_id=peer, device_id_type=MESH)
    start(loads)
    start(load_wd(0))
    small[...] = jnp.zeros_like(small)
    small_out[...] = jnp.zeros_like(small_out)
    pl.semaphore_wait(barrier, len(peers))
    wait(loads)

    def live(it):
        return jnp.logical_and(it >= 0, it < total)

    units = width // HD
    attention_at = 1
    normed_at = max(n_g, attention_at + units)
    norm_at = total + 1

    @pl.loop(0, total + 6 * LAG)
    def _(tick):
        one = tick - LAG

        @pl.when(live(one))
        def _():
            wait(stage0(one))
            sa, s = slot_of(acc, one), slot_of(rcv0, one)

            @pl.loop(0, 8)
            def _(p):
                acc[sa, p] = (acc[sa, p].astype(F32) + rcv0[s, p].astype(F32)).astype(BF16)

            start(stage1(one))

        two = tick - 2 * LAG

        @pl.when(live(two))
        def _():
            wait(stage1(two))
            sa, s = slot_of(acc, two), slot_of(rcv1, two)
            for n, bit in ((0, at.x), (1, at.y)):
                for m in range(2):
                    p = quarter(bit, n) + m
                    acc[sa, p] = (
                        acc[sa, p].astype(F32) + rcv1[s, n, m].astype(F32)
                    ).astype(BF16)
            start(stage2(two))

        three = tick - 3 * LAG

        @pl.when(live(three))
        def _():
            wait(stage2(three))
            sa, s, d = slot_of(acc, three), slot_of(rcv2, three), slot_of(fin, three)
            for n, p in ((0, quarter(at.x, 0) + at.y), (1, quarter(at.y, 1) + at.x)):
                fin[d, n] = (acc[sa, p].astype(F32) + rcv2[s, n].astype(F32)).astype(BF16)
            start(stage3(three))
            start(keep3(three))

        four = tick - 4 * LAG

        @pl.when(live(four))
        def _():
            wait(keep3(four))
            wait(stage3(four))
            start(stage4(four))

        five = tick - 5 * LAG

        @pl.when(live(five))
        def _():
            wait(stage4(five))
            start(stage5(five))

        six = tick - 6 * LAG

        @pl.when(live(six))
        def _():
            wait(stage5(six))

        @pl.when(tick < n_d)
        def _():
            product(tick, hat_v, lambda: dy_v[:, rows_at(tick, WIDE)])

        @pl.when(jnp.logical_and(tick >= n_d, tick < n_d + n_g))
        def _():
            product(tick, nt_v, lambda: gate_right(tick - n_d))

        @pl.when(jnp.logical_and(tick >= n_d + n_g, tick < total))
        def _():
            product(tick, nt_v, lambda: dqkv_v[:, rows_at(tick - n_d - n_g, WIDE)])

        @pl.when(tick < n_g)
        def _():
            hidden_job(tick)

        @pl.when(jnp.logical_and(tick >= attention_at, tick < attention_at + units))
        def _():
            attention_unit(
                tick - attention_at, q_v, k_v, v_v, do_v, lse_ref, tab_v, dqkv_v, small, dq, dk, dv
            )

        @pl.when(tick == normed_at - 1)
        def _():
            start(load_wn(0))

        @pl.when(jnp.logical_and(tick >= normed_at, tick < normed_at + chunks))
        def _():
            normed_job(tick - normed_at)

        @pl.when(tick == norm_at)
        def _():
            norm_job()
            start(small_copy(0))

        for n in range(3):

            @pl.when(tick == norm_at + 1 + n)
            def _(n=n):
                small_step(n)

        @pl.when(tick == norm_at + 4)
        def _():
            small_end()
            wait(tokens_out())


def run_backward(
    hat, nt, dy, datt, a1, a2, q, k, v, lse, tables, w_down, w_gate, w_up, w_qkv, tokens, gain, n_z
):
    seq_len, model = dy.shape
    local_ff, width = a1.shape[1], q.shape[1]
    own = tokens.shape[0]
    n_d, n_g, n_q = model // WIDE, local_ff // BLOCK, 3 * width // WIDE
    total = n_d + n_g + n_q
    bf = lambda *shape: pltpu.VMEM(shape, BF16)
    fl = lambda *shape: pltpu.VMEM(shape, F32)
    sems = lambda *shape: pltpu.SemaphoreType.DMA(shape)
    slots = 2 * LAG + 3
    hbm = pl.BlockSpec(memory_space=pl.ANY)
    vmem = pl.BlockSpec(memory_space=pltpu.VMEM)
    return pl.pallas_call(
        functools.partial(backward_pass, n_d, n_g, n_q, n_z),
        in_specs=[hbm] * 9 + [vmem] + [hbm] * 6 + [vmem],
        out_specs=[hbm, hbm, vmem],
        out_shape=[
            jax.ShapeDtypeStruct((total, PIECES, BLOCK, WIDE), BF16),
            jax.ShapeDtypeStruct((own, model), BF16),
            jax.ShapeDtypeStruct((8, model // n_z), F32),
        ],
        scratch_shapes=[
            bf(model, seq_len), bf(model, seq_len), bf(seq_len, model), bf(seq_len, width),
            bf(seq_len, local_ff), bf(seq_len, local_ff),
            bf(seq_len, width), bf(seq_len, width), bf(seq_len, width),
            fl(3, seq_len, LANES), bf(own, model),
            bf(seq_len, 3 * width), fl(seq_len, LANES), fl(seq_len, LANES), fl(seq_len, LANES),
            bf(2, BLOCK, model), bf(2, WIDE, local_ff), bf(2, WIDE, local_ff),
            bf(2, 3, WIDE, width),
            bf(3, seq_len, WIDE), bf(n_z - 1, own, model), fl(own, model),
            fl(8, model), fl(3, 8, model), fl(n_z - 1, 8, model // n_z),
            bf(LAG + 1, 8, BLOCK, WIDE), bf(3 * LAG + 1, 8, BLOCK, WIDE),
            bf(slots, 8, BLOCK, WIDE), bf(slots, 2, 2, BLOCK, WIDE), bf(slots, 2, BLOCK, WIDE),
            bf(LAG + 1, 2, BLOCK, WIDE),
            sems(11), sems(2), sems(3, 2), pltpu.SemaphoreType.DMA,
            sems(2, n_z - 1, model // WIDE), sems(2, 3), sems(2, n_z - 1),
            sems(2, slots), sems(4, slots), sems(4, slots),
            sems(4, slots), sems(4, slots), sems(2, slots), sems(2, LAG + 1),
        ],
        compiler_params=pltpu.CompilerParams(
            collective_id=0, has_side_effects=True, vmem_limit_bytes=67043328
        ),
        name="backward_pass",
    )(
        hat, nt, dy, datt, a1, a2, q, k, v, lse, tables, w_down, w_gate, w_up, w_qkv, tokens, gain
    )


def flat_kernel(item_ref, *outs):
    at = 0
    for out in outs:
        n = out.shape[-2] // BLOCK
        for p in range(n):
            value = item_ref[0, at + p].astype(F32)
            out[..., p * BLOCK : (p + 1) * BLOCK, :] = value.reshape(
                out.shape[:-2] + (BLOCK, WIDE)
            )
        at += n


def pair_kernel(item_ref, out):
    for p in range(PIECES):
        rows = pl.ds(p * BLOCK, BLOCK)
        out[rows, 0, :] = item_ref[0, p, :, :BLOCK].astype(F32)
        out[rows, 1, :] = item_ref[0, p, :, BLOCK:].astype(F32)


def unpack(items, local_ff, width, model):
    n_d, n_g, n_q = model // WIDE, local_ff // BLOCK, 3 * width // WIDE
    item = lambda base: pl.BlockSpec((1, PIECES, BLOCK, WIDE), lambda i: (base + i, 0, 0, 0))
    per = n_q // 3
    down, out = pl.pallas_call(
        flat_kernel,
        grid=(n_d,),
        in_specs=[item(0)],
        out_specs=[
            pl.BlockSpec((local_ff, WIDE), lambda i: (0, i)),
            pl.BlockSpec((width, WIDE), lambda i: (0, i)),
        ],
        out_shape=[
            jax.ShapeDtypeStruct((local_ff, model), F32),
            jax.ShapeDtypeStruct((width, model), F32),
        ],
        name="unpack_down",
    )(items)
    gate_up = pl.pallas_call(
        pair_kernel,
        grid=(n_g,),
        in_specs=[item(n_d)],
        out_specs=pl.BlockSpec((model, 2, BLOCK), lambda i: (0, 0, i)),
        out_shape=jax.ShapeDtypeStruct((model, 2, local_ff), F32),
        name="unpack_gate_up",
    )(items)
    qkv = pl.pallas_call(
        flat_kernel,
        grid=(n_q,),
        in_specs=[item(n_d + n_g)],
        out_specs=pl.BlockSpec((1, model, WIDE), lambda i: (i // per, 0, i % per)),
        out_shape=jax.ShapeDtypeStruct((3, model, width), F32),
        name="unpack_qkv",
    )(items)
    return down, out, gate_up, qkv.transpose(1, 0, 2)


def fast_path(n_dp, n_mp, model_width, local_width, local_ff):
    return (
        n_dp == 8
        and model_width == PIECES * BLOCK
        and local_width % WIDE == 0
        and model_width // n_mp == local_width
        and local_ff % BLOCK == 0
        and local_ff + local_width <= model_width
    )


def on_device(
    n_dp,
    n_mp,
    tokens,
    norm_gain,
    layernorm_bias,
    qkv_weight,
    qkv_bias,
    out_weight,
    gate_up_weight,
    down_weight,
    grad_out,
):
    cube = Cube("dp", n_dp)
    rows, model_width = tokens.shape
    local_width = qkv_weight.shape[2]
    seq_len = rows * n_mp
    fast = fast_path(n_dp, n_mp, model_width, local_width, gate_up_weight.shape[2])
    gain = norm_gain.astype(F32)
    token_f32 = tokens.astype(F32)
    row_mean = jnp.mean(token_f32, axis=1, keepdims=True)
    centered = token_f32 - row_mean
    inv_std = lax.rsqrt(jnp.mean(centered * centered, axis=1, keepdims=True) + EPS)
    xhat = centered * inv_std
    normed_own = (xhat * gain + layernorm_bias.astype(F32)).astype(BF16)
    normed = lax.all_gather(normed_own, "mp", axis=0, tiled=True)
    dy = lax.all_gather(grad_out, "mp", axis=0, tiled=True)

    w_qkv = [qkv_weight[:, t, :] for t in range(3)]
    w_gate, w_up = gate_up_weight[:, 0, :], gate_up_weight[:, 1, :]
    tables = rotary_tables(seq_len)

    gate = dot(normed, w_gate, 1, 0)
    up = dot(normed, w_up, 1, 0)
    sig = jax.nn.sigmoid(gate)
    hidden = (gate * sig * up).astype(BF16)
    qkv = jnp.concatenate([dot(normed, w, 1, 0) for w in w_qkv], axis=1)
    q, k, v, attended, lse = attention_forward(qkv, qkv_bias.astype(F32), tables)
    branch = (dot(attended, out_weight, 1, 0) + dot(hidden, down_weight, 1, 0)).astype(BF16)
    share = lax.psum_scatter(branch, "mp", scatter_dimension=0, tiled=True)
    layer_out = (token_f32 + share.astype(F32)).astype(BF16)

    share_width = model_width // n_mp
    if fast:
        silu = gate * sig
        by_gate = (up * (sig + silu * (1.0 - sig))).astype(BF16)
        by_up = silu.astype(BF16)
        local_ff = hidden.shape[1]
        pad = jnp.zeros((seq_len, model_width - local_ff - local_width), BF16)
        hat = jnp.concatenate([hidden, attended, pad], axis=1).T
        d_attended = dot(dy, out_weight, 1, 1, BF16)
        items, grad_tokens, small = run_backward(
            hat, normed.T, dy, d_attended, by_gate, by_up, q, k, v,
            lse.reshape(-1, 1, seq_len), tables, down_weight, w_gate, w_up,
            qkv_weight.transpose(1, 0, 2), tokens, gain[None], n_mp,
        )
        grad_down_w, grad_out_w, grad_gate_up_w, grad_qkv_w = unpack(
            items, local_ff, local_width, model_width
        )
        return (
            layer_out,
            grad_tokens,
            small[0],
            small[1],
            grad_qkv_w,
            small[2:5, :local_width],
            grad_out_w,
            grad_gate_up_w,
            grad_down_w,
        )

    d_hidden = dot(dy, down_weight, 1, 1)
    silu = gate * sig
    d_gate = (d_hidden * up * (sig + silu * (1.0 - sig))).astype(BF16)
    d_up = (d_hidden * silu).astype(BF16)
    d_attended = dot(dy, out_weight, 1, 1, BF16)
    dq, dk, dv, sums = attention_backward(q, k, v, d_attended, lse, tables)
    d_normed = (
        dot(d_gate, w_gate, 1, 1)
        + dot(d_up, w_up, 1, 1)
        + dot(dq, w_qkv[0], 1, 1)
        + dot(dk, w_qkv[1], 1, 1)
        + dot(dv, w_qkv[2], 1, 1)
    ).astype(BF16)
    d_own = lax.psum_scatter(d_normed, "mp", scatter_dimension=0, tiled=True).astype(F32)
    d_qkv = jnp.concatenate([dq, dk, dv], axis=1)
    grad_down_w = cube.contract(hidden, dy)
    grad_out_w = cube.contract(attended, dy)
    grad_gate_up_w = jnp.stack(
        [cube.contract(normed, d_gate), cube.contract(normed, d_up)], axis=1
    )
    grad_qkv_w = cube.contract(normed, d_qkv).reshape(model_width, 3, local_width)

    scaled = d_own * gain
    grad_tokens = grad_out.astype(F32) + inv_std * (
        scaled
        - jnp.mean(scaled, axis=1, keepdims=True)
        - xhat * jnp.mean(scaled * xhat, axis=1, keepdims=True)
    )
    terms = jnp.stack([jnp.sum(d_own * xhat, axis=0), jnp.sum(d_own, axis=0)])
    bias_sum = cube.sum_all(sums)
    grad_bias = bias_sum.swapaxes(0, 1).reshape(3, local_width)
    terms = Cube("mp", n_mp).sum_all(cube.sum_all(terms))
    terms = lax.dynamic_slice_in_dim(
        terms, lax.axis_index("mp") * share_width, share_width, 1
    )
    return (
        layer_out,
        grad_tokens.astype(BF16),
        terms[0],
        terms[1],
        grad_qkv_w,
        grad_bias,
        grad_out_w,
        grad_gate_up_w,
        grad_down_w,
    )


def solution(mesh):
    return jax.shard_map(
        functools.partial(on_device, mesh.shape["dp"], mesh.shape["mp"]),
        mesh=mesh,
        in_specs=(
            P(("dp", "mp"), None),
            P(),
            P(),
            P(None, None, "mp"),
            P(None, "mp"),
            P("mp", None),
            P(None, None, "mp"),
            P("mp", None),
            P(("dp", "mp"), None),
        ),
        out_specs=(
            P(("dp", "mp"), None),
            P(("dp", "mp"), None),
            P("mp"),
            P("mp"),
            P(None, None, "mp"),
            P(None, "mp"),
            P("mp", None),
            P(None, None, "mp"),
            P("mp", None),
        ),
        check_vma=False,
    )
```

```python
import functools
import math

import jax
import jax.numpy as jnp
from jax import lax
from jax.experimental import pallas as pl
from jax.experimental.pallas import tpu as pltpu
from jax.sharding import PartitionSpec as P

HD = 64
ROT = 16
EPS = 1e-05
LANES = 128
QB = 256


F32 = jnp.float32
BF16 = jnp.bfloat16


def dot(a, b, ca, cb, out=F32):
    return lax.dot_general(
        a, b, (((ca,), (cb,)), ((), ())), preferred_element_type=F32
    ).astype(out)


def rotary_tables(seq_len):
    positions = jnp.arange(seq_len, dtype=F32)
    freqs = 1.0 / 10000.0 ** (jnp.arange(ROT // 2, dtype=F32) * 2.0 / ROT)
    phase = positions[:, None] * freqs[None, :]
    cosine, sine = jnp.cos(phase), jnp.sin(phase)
    half = ROT // 2
    rest = HD - ROT
    ones = jnp.ones((seq_len, rest), F32)
    zeros = jnp.zeros((seq_len, rest), F32)
    zhalf = jnp.zeros((seq_len, half), F32)
    c = jnp.concatenate([cosine, cosine, ones], axis=1)
    up = jnp.concatenate([-sine, zhalf, zeros], axis=1)
    down = jnp.concatenate([zhalf, sine, zeros], axis=1)
    two = LANES // HD
    return jnp.stack([jnp.tile(t, (1, two)) for t in (c, up, down)])


def turn(x, tables, sign):
    half = ROT // 2
    ahead = pltpu.roll(x, LANES - half, 1)
    behind = pltpu.roll(x, half, 1)
    return x * tables[0] + sign * (ahead * tables[1] + behind * tables[2])


def lane_mask(rows, j):
    lane = lax.broadcasted_iota(jnp.int32, (rows, LANES), 1)
    return (lane // HD) == j


def forward_kernel(
    q_in, k_in, v_in, bias_ref, tab_ref, q_out, k_out, v_out, o_ref, lse_ref
):
    seq_len = q_in.shape[0]
    j = pl.program_id(1)

    @pl.when(j == 0)
    def _():
        tables = (tab_ref[0], tab_ref[1], tab_ref[2])
        q_out[...] = turn(q_in[...] + bias_ref[0, 0:1], tables, 1.0).astype(BF16)
        k_out[...] = turn(k_in[...] + bias_ref[0, 1:2], tables, 1.0).astype(BF16)
        v_out[...] = (v_in[...] + bias_ref[0, 2:3]).astype(BF16)

    mask = lane_mask(QB, j)
    causal = lax.broadcasted_iota(jnp.int32, (QB, QB), 0) <= lax.broadcasted_iota(
        jnp.int32, (QB, QB), 1
    )
    for i in range(seq_len // QB):
        rows = pl.ds(i * QB, QB)
        span = (i + 1) * QB
        q = q_out[rows, :] * 0.125
        q = jnp.where(mask, q, jnp.zeros_like(q))
        parts = []
        if i:
            parts.append(dot(k_out[pl.ds(0, i * QB), :], q, 1, 1))
        diag = dot(k_out[rows, :], q, 1, 1)
        parts.append(jnp.where(causal, diag, -1e30))
        top = functools.reduce(
            jnp.maximum, [jnp.max(s, axis=0, keepdims=True) for s in parts]
        )
        exps = [jnp.exp(s - top) for s in parts]
        total = sum(jnp.sum(e, axis=0, keepdims=True) for e in exps)
        inv = 1.0 / total
        probs = jnp.concatenate([(e * inv).astype(BF16) for e in exps], axis=0)
        out = dot(probs, v_out[pl.ds(0, span), :], 0, 0).astype(BF16)
        before = o_ref[rows, :]
        o_ref[rows, :] = jnp.where(mask, out, before)
        lse_ref[0, 0, :, i * QB : (i + 1) * QB] = top + jnp.log(total)


def backward_kernel(
    q_ref, k_ref, v_ref, do_ref, lse_ref, tab_ref, dq_out, dk_out, dv_out, sums_out, dq, dk, dv
):
    seq_len = q_ref.shape[0]
    j = pl.program_id(1)
    mask = lane_mask(QB, j)
    causal = lax.broadcasted_iota(jnp.int32, (QB, QB), 0) <= lax.broadcasted_iota(
        jnp.int32, (QB, QB), 1
    )

    @pl.when(j == 0)
    def _():
        dk[...] = jnp.zeros_like(dk)
        dv[...] = jnp.zeros_like(dv)

    for i in range(seq_len // QB):
        rows = pl.ds(i * QB, QB)
        q = q_ref[rows, :] * 0.125
        q = jnp.where(mask, q, jnp.zeros_like(q))
        do = do_ref[rows, :]
        do = jnp.where(mask, do, jnp.zeros_like(do))
        lse = lse_ref[0, 0, :, i * QB : (i + 1) * QB]
        pieces = []
        if i:
            pieces.append((pl.ds(0, i * QB), False))
        pieces.append((rows, True))
        probs, grads = [], []
        inner = 0.0
        for where, diagonal in pieces:
            s = dot(k_ref[where, :], q, 1, 1)
            if diagonal:
                s = jnp.where(causal, s, -1e30)
            p = jnp.exp(s - lse)
            dp = dot(v_ref[where, :], do, 1, 1)
            inner = inner + jnp.sum(p * dp, axis=0, keepdims=True)
            probs.append(p)
            grads.append(dp)
        acc = 0.0
        for (where, diagonal), p, dp in zip(pieces, probs, grads):
            ds = (p * (dp - inner)).astype(BF16)
            dv[where, :] += dot(p.astype(BF16), do, 1, 0)
            dk[where, :] += dot(ds, q, 1, 0)
            acc = acc + dot(ds, k_ref[where, :], 0, 0)
        before = dq[rows, :]
        dq[rows, :] = jnp.where(mask, acc * 0.125, before)

    @pl.when(j == pl.num_programs(1) - 1)
    def _():
        tables = (tab_ref[0], tab_ref[1], tab_ref[2])
        gq = turn(dq[...], tables, -1.0).astype(BF16)
        gk = turn(dk[...], tables, -1.0).astype(BF16)
        gv = dv[...].astype(BF16)
        dq_out[...] = gq
        dk_out[...] = gk
        dv_out[...] = gv
        sums_out[0, 0:1] = jnp.sum(gq.astype(F32), axis=0, keepdims=True)
        sums_out[0, 1:2] = jnp.sum(gk.astype(F32), axis=0, keepdims=True)
        sums_out[0, 2:3] = jnp.sum(gv.astype(F32), axis=0, keepdims=True)


def attention_forward(qkv, bias, tables):
    seq_len, width = qkv.shape[0], qkv.shape[1] // 3
    pairs = width // LANES
    column = lambda part: pl.BlockSpec((seq_len, LANES), lambda p, j: (0, part * pairs + p))
    block = pl.BlockSpec((seq_len, LANES), lambda p, j: (0, p))
    bias_blocks = bias.reshape(3, pairs, LANES).swapaxes(0, 1)
    wide = jax.ShapeDtypeStruct((seq_len, width), BF16)
    elements = pairs * 2 * seq_len * seq_len // 2
    return pl.pallas_call(
        forward_kernel,
        grid=(pairs, LANES // HD),
        in_specs=[
            column(0),
            column(1),
            column(2),
            pl.BlockSpec((1, 3, LANES), lambda p, j: (p, 0, 0)),
            pl.BlockSpec((3, seq_len, LANES), lambda p, j: (0, 0, 0)),
        ],
        out_specs=[
            block,
            block,
            block,
            block,
            pl.BlockSpec((1, 1, 1, seq_len), lambda p, j: (p, j, 0, 0)),
        ],
        out_shape=[
            wide,
            wide,
            wide,
            wide,
            jax.ShapeDtypeStruct((pairs, LANES // HD, 1, seq_len), F32),
        ],
        cost_estimate=pl.CostEstimate(
            flops=elements * 4 * LANES,
            bytes_accessed=qkv.size * 4 + 4 * seq_len * width * 2,
            transcendentals=elements,
        ),
        name="attention_forward",
    )(qkv, qkv, qkv, bias_blocks, tables)


def attention_backward(q, k, v, grad, lse, tables):
    seq_len, width = q.shape
    pairs = width // LANES
    block = pl.BlockSpec((seq_len, LANES), lambda p, j: (0, p))
    wide = jax.ShapeDtypeStruct((seq_len, width), BF16)
    elements = pairs * 2 * seq_len * seq_len // 2
    return pl.pallas_call(
        backward_kernel,
        grid=(pairs, LANES // HD),
        in_specs=[
            block,
            block,
            block,
            block,
            pl.BlockSpec((1, 1, 1, seq_len), lambda p, j: (p, j, 0, 0)),
            pl.BlockSpec((3, seq_len, LANES), lambda p, j: (0, 0, 0)),
        ],
        out_specs=[block, block, block, pl.BlockSpec((1, 3, LANES), lambda p, j: (p, 0, 0))],
        out_shape=[wide, wide, wide, jax.ShapeDtypeStruct((pairs, 3, LANES), F32)],
        scratch_shapes=[pltpu.VMEM((seq_len, LANES), F32)] * 3,
        cost_estimate=pl.CostEstimate(
            flops=elements * 10 * LANES,
            bytes_accessed=7 * seq_len * width * 2,
            transcendentals=elements,
        ),
        name="attention_backward",
    )(q, k, v, grad, lse, tables)


def pick(x, index):
    return lax.dynamic_index_in_dim(x, index, 0, keepdims=False)


class Cube:
    def __init__(self, axis, size):
        self.axis, self.size = axis, size
        self.bits = [b for b in range(size.bit_length()) if 1 << b < size]
        me = lax.axis_index(axis)
        self.own = [lax.rem(lax.div(me, 1 << b), 2) for b in self.bits]

    def swap(self, x, b):
        return lax.ppermute(x, self.axis, [(i, i ^ (1 << b)) for i in range(self.size)])

    def sum_all(self, x):
        for b in self.bits:
            x = x + self.swap(x, b)
        return x

    def contract(self, left, right):
        depth, rows = left.shape
        columns = right.shape[1]
        core, others = self.bits[0], self.bits[1:]
        half = rows // 2
        mine = self.own[0]
        first = lax.dynamic_slice_in_dim(left, (1 - mine) * half, half, 1)
        second = lax.dynamic_slice_in_dim(left, mine * half, half, 1)
        away = dot(first, right, 0, 0, BF16)
        came = self.swap(away, core)
        keep = dot(second, right, 0, 0, BF16)
        orders = [others, others[::-1]]
        quarter = half // 2
        done = []
        for n, order in enumerate(orders):
            small = quarter >> len(order)
            shape = (2,) * len(order) + (small, columns)
            cur = (
                keep[n * quarter : (n + 1) * quarter].astype(F32)
                + came[n * quarter : (n + 1) * quarter].astype(F32)
            ).reshape(shape)
            for b in order:
                own = self.own[b]
                send = pick(cur, 1 - own).astype(BF16)
                got = self.swap(send, b)
                cur = pick(cur, own) + got.astype(F32)
            buf = cur.astype(BF16)
            for b in order[::-1]:
                own = self.own[b]
                got = self.swap(buf, b)
                low = jnp.where(own == 0, buf, got)
                high = jnp.where(own == 0, got, buf)
                buf = jnp.stack([low, high])
            done.append(buf.reshape(quarter, columns))
        whole = jnp.concatenate(done, axis=0)
        other = self.swap(whole, core)
        low = jnp.where(mine == 0, whole, other)
        high = jnp.where(mine == 0, other, whole)
        return jnp.concatenate([low, high], axis=0).astype(F32)


LAG = 2
BLOCK = 128
PIECES = 16
WIDE = 256
STEP = 32
MESH = pl.DeviceIdType.MESH


class Places:
    def __init__(self, n_z):
        self.me = lax.axis_index("dp")
        self.z = z = lax.axis_index("mp")
        self.core = lax.rem(self.me, 2)
        self.x = lax.rem(lax.div(self.me, 2), 2)
        self.y = lax.div(self.me, 4)
        self.core_peer = (self.me + 1 - 2 * self.core, z)
        self.x_peer = (self.me + 2 - 4 * self.x, z)
        self.y_peer = (self.me + 4 - 8 * self.y, z)
        self.z_of = [lax.rem(z + d, n_z) for d in range(n_z)]
        self.z_peers = [(self.me, to) for to in self.z_of]
        self.above = jnp.minimum(z + 1, n_z - 1)
        self.below = jnp.maximum(z - 1, 0)
        self.far = n_z - 1 - z
        self.has_above, self.has_below = z < n_z - 1, z > 0
        self.end = jnp.logical_or(z == 0, z == n_z - 1)
        self.middle = jnp.logical_not(self.end)
        self.order = [
            z,
            jnp.where(z == 0, 1, z - 1),
            jnp.where(z == 0, 2, jnp.where(z == 1, 2, jnp.where(z == 2, 3, 1))),
            jnp.where(z <= 1, 3, 0),
        ]


def rdma(src, dst, send_sem, recv_sem, peer):
    return pltpu.make_async_remote_copy(
        src_ref=src,
        dst_ref=dst,
        send_sem=send_sem,
        recv_sem=recv_sem,
        device_id=peer,
        device_id_type=MESH,
    )


def start(copies):
    for copy in copies:
        copy.start()


def wait(copies):
    for copy in copies:
        copy.wait()


def at_block(i, size):
    return pl.ds(pl.multiple_of(i * size, size), size)


def both(a, b):
    return jnp.logical_and(a, b)


def causal_block():
    key = lax.broadcasted_iota(jnp.int32, (QB, QB), 0)
    query = lax.broadcasted_iota(jnp.int32, (QB, QB), 1)
    return key <= query


def head_part(x, mask):
    return jnp.where(mask, x, jnp.zeros_like(x))


def attend_unit(u, qkv_v, attn_v, hat_v, lse_v, first_row):
    seq_len = qkv_v.shape[1]
    pair, j = lax.div(u, 2), lax.rem(u, 2)
    lanes = at_block(pair, LANES)
    mask = lane_mask(QB, j)
    causal = causal_block()
    for i in range(seq_len // QB):
        rows = pl.ds(i * QB, QB)
        q = head_part(qkv_v[0, rows, lanes] * 0.125, mask)
        parts = []
        if i:
            parts.append(dot(qkv_v[1, pl.ds(0, i * QB), lanes], q, 1, 1))
        parts.append(jnp.where(causal, dot(qkv_v[1, rows, lanes], q, 1, 1), -1e30))
        top = functools.reduce(
            jnp.maximum, [jnp.max(s, axis=0, keepdims=True) for s in parts]
        )
        exps = [jnp.exp(s - top) for s in parts]
        total = sum(jnp.sum(e, axis=0, keepdims=True) for e in exps)
        inv = 1.0 / total
        probs = jnp.concatenate([(e * inv).astype(BF16) for e in exps], axis=0)
        out = dot(probs, qkv_v[2, pl.ds(0, (i + 1) * QB), lanes], 0, 0).astype(BF16)
        attn_v[rows, lanes] = jnp.where(mask, out, attn_v[rows, lanes])
        lse_v[u, :, i * QB : (i + 1) * QB] = top + jnp.log(total)

    @pl.when(j == 1)
    def _():
        for i in range(seq_len // QB):
            rows = pl.ds(i * QB, QB)
            to = pl.ds(pl.multiple_of(first_row + pair * LANES, LANES), LANES)
            hat_v[to, rows] = jnp.transpose(attn_v[rows, lanes])


def attend_back_unit(u, qkv_v, do_v, lse_v, tab_v, dqkv_v, small, dq, dk, dv):
    seq_len, width = qkv_v.shape[1:]
    pair, j = lax.div(u, 2), lax.rem(u, 2)
    lanes = at_block(pair, LANES)
    mask = lane_mask(QB, j)
    causal = causal_block()

    @pl.when(j == 0)
    def _():
        dk[...] = jnp.zeros_like(dk)
        dv[...] = jnp.zeros_like(dv)
        dq[...] = jnp.zeros_like(dq)

    for i in range(seq_len // QB):
        rows = pl.ds(i * QB, QB)
        q = head_part(qkv_v[0, rows, lanes] * 0.125, mask)
        do = head_part(do_v[rows, lanes], mask)
        lse = lse_v[u, :, i * QB : (i + 1) * QB]
        pieces = [(pl.ds(0, i * QB), False)] if i else []
        pieces.append((rows, True))
        probs, grads = [], []
        inner = 0.0
        for where, diagonal in pieces:
            s = dot(qkv_v[1, where, lanes], q, 1, 1)
            if diagonal:
                s = jnp.where(causal, s, -1e30)
            p = jnp.exp(s - lse)
            dp = dot(qkv_v[2, where, lanes], do, 1, 1)
            inner = inner + jnp.sum(p * dp, axis=0, keepdims=True)
            probs.append(p)
            grads.append(dp)
        acc = 0.0
        for (where, diagonal), p, dp in zip(pieces, probs, grads):
            ds = (p * (dp - inner)).astype(BF16)
            dv[where, :] += dot(p.astype(BF16), do, 1, 0)
            dk[where, :] += dot(ds, q, 1, 0)
            acc = acc + dot(ds, qkv_v[1, where, lanes], 0, 0)
        dq[rows, :] = jnp.where(mask, acc * 0.125, dq[rows, :])

    @pl.when(j == 1)
    def _():
        tables = (tab_v[0], tab_v[1], tab_v[2])
        out = (
            turn(dq[...], tables, -1.0).astype(BF16),
            turn(dk[...], tables, -1.0).astype(BF16),
            dv[...].astype(BF16),
        )
        for t, g in enumerate(out):
            dqkv_v[:, pl.ds(pl.multiple_of(t * width + pair * LANES, LANES), LANES)] = g
            small[2 + t : 3 + t, lanes] = jnp.sum(g.astype(F32), axis=0, keepdims=True)


def layer_kernel(
    n_z, tokens, grad_out, tables, w_gate_up, w_qkv, w_down, w_out, gain_ref, shift_ref, bias_ref,
    sums_out, layer_out, grad_tokens_out, small_out, w_gate, w_up,
    hat_v, nt_v, dy_v, nrm, a1_v, a2_v, qkv_v, attn_v, hq_v, do_v, lse_v, tab_v, tok_v,
    wf, zsend, zin, own, small, small_in, share_in,
    away, acc, rcv0, rcv1, rcv2, fin,
    load, s_raw, s_wf, s_back, s_wd, s_wn, s_tok, ready,
    n_send, n_recv, y_send, y_recv, z_sems, small_sems, share_sems,
    s0, s1, s2, s3, s4, s5, s_fin,
):
    at = Places(n_z)
    seq_len, model = dy_v.shape
    own_rows = tok_v.shape[0]
    width = qkv_v.shape[2]
    local_ff = a1_v.shape[1]
    blocks_h, blocks_o = local_ff // BLOCK, width // BLOCK
    columns = model // WIDE
    n_d = -(-(blocks_h + blocks_o) * columns // PIECES)
    n_g, n_q = blocks_h, 3 * width // WIDE
    total = n_d + n_g + n_q
    per = width // WIDE
    fill = n_g + n_q
    dy_chunks = y_recv.shape[1]
    dy_wide = model // dy_chunks
    units = width // HD

    def slot_of(buf, it):
        return lax.rem(it, buf.shape[0])

    def quarter(bit, half):
        return half * 4 + bit * 2

    def stage0(it):
        sa, s = slot_of(away, it), slot_of(rcv0, it)
        return [rdma(away.at[sa], rcv0.at[s], s0.at[0, s], s0.at[1, s], at.core_peer)]

    def stage1(it):
        sa, s = slot_of(acc, it), slot_of(rcv1, it)
        a, b = pl.ds(quarter(1 - at.x, 0), 2), pl.ds(quarter(1 - at.y, 1), 2)
        return [
            rdma(acc.at[sa, a], rcv1.at[s, 0], s1.at[0, s], s1.at[1, s], at.x_peer),
            rdma(acc.at[sa, b], rcv1.at[s, 1], s1.at[2, s], s1.at[3, s], at.y_peer),
        ]

    def stage2(it):
        sa, s = slot_of(acc, it), slot_of(rcv2, it)
        a, b = quarter(at.x, 0) + 1 - at.y, quarter(at.y, 1) + 1 - at.x
        return [
            rdma(acc.at[sa, a], rcv2.at[s, 0], s2.at[0, s], s2.at[1, s], at.y_peer),
            rdma(acc.at[sa, b], rcv2.at[s, 1], s2.at[2, s], s2.at[3, s], at.x_peer),
        ]

    def piece_a():
        return at.core * 8 + quarter(at.x, 0) + at.y

    def piece_b():
        return at.core * 8 + quarter(at.y, 1) + at.x

    def stage3(it):
        s, n = slot_of(fin, it), lax.rem(it, s3.shape[1])
        a, b = sums_out.at[it, piece_a()], sums_out.at[it, piece_b()]
        return [
            rdma(fin.at[s, 0], a, s3.at[0, n], s3.at[1, n], at.y_peer),
            rdma(fin.at[s, 1], b, s3.at[2, n], s3.at[3, n], at.x_peer),
        ]

    def keep3(it):
        s = slot_of(fin, it)
        return [
            pltpu.make_async_copy(fin.at[s, 0], sums_out.at[it, piece_a()], s_fin.at[0, s]),
            pltpu.make_async_copy(fin.at[s, 1], sums_out.at[it, piece_b()], s_fin.at[1, s]),
        ]

    def stage4(it):
        n = lax.rem(it, s4.shape[1])
        a = sums_out.at[it, pl.ds(at.core * 8 + quarter(at.x, 0), 2)]
        b = sums_out.at[it, pl.ds(at.core * 8 + quarter(at.y, 1), 2)]
        return [
            rdma(a, a, s4.at[0, n], s4.at[1, n], at.x_peer),
            rdma(b, b, s4.at[2, n], s4.at[3, n], at.y_peer),
        ]

    def stage5(it):
        n = lax.rem(it, s5.shape[1])
        part = sums_out.at[it, pl.ds(at.core * 8, 8)]
        return [rdma(part, part, s5.at[0, n], s5.at[1, n], at.core_peer)]

    def product(it, half):
        half(1 - at.core, away, slot_of(away, it))
        start(stage0(it))
        half(at.core, acc, slot_of(acc, it))

    def tall(right):
        def half(which, dst, slot):
            tile = dot(nt_v[at_block(which, 8 * BLOCK), :], right(), 1, 0, BF16)
            for p in range(8):
                dst[slot, p] = tile[p * BLOCK : (p + 1) * BLOCK]

        return half

    def by_block(it):
        def half(which, dst, slot):
            @pl.loop(0, 8)
            def _(p):
                b = it * PIECES + which * 8 + p
                c = jnp.maximum(b - blocks_h * columns, 0)
                first = b < blocks_h * columns
                row = jnp.where(first, lax.rem(b, blocks_h), blocks_h + lax.rem(c, blocks_o))
                col = jnp.where(first, lax.div(b, blocks_h), lax.div(c, blocks_o))
                col = jnp.minimum(col, columns - 1)
                dst[slot, p] = dot(
                    hat_v[at_block(row, BLOCK), :], dy_v[:, at_block(col, WIDE)], 1, 0, BF16
                )

        return half

    def gate_right(f):
        lanes = at_block(f, BLOCK)
        return jnp.concatenate([a1_v[:, lanes], a2_v[:, lanes]], axis=1)

    def shard(origin):
        return at_block(origin, own_rows)

    def n_copy(kind, origin, to):
        rows = nrm.at[shard(origin)]
        return rdma(rows, rows, n_send.at[kind], n_recv.at[origin], (at.me, to))

    def y_copy(kind, origin, to, c):
        part = dy_v.at[shard(origin), at_block(c, dy_wide)]
        return rdma(part, part, y_send.at[kind, c], y_recv.at[origin, c], (at.me, to))

    def route(make, what):
        def when(condition, copy):
            @pl.when(condition)
            def _():
                getattr(copy, what)()

        def first():
            when(at.has_above, make(0, at.z, at.above))
            when(at.has_below, make(1, at.z, at.below))
            when(at.end, make(2, at.z, at.far))

        def passed(up):
            if up:
                when(at.middle, make(3, at.below, at.above))
            else:
                when(at.middle, make(4, at.above, at.below))

        return first, passed

    def n_arrived(origin):
        n_copy(0, origin, at.z_of[1]).wait_recv()

    def y_arrived(origin, c):
        y_copy(0, origin, at.z_of[1], c).wait_recv()

    def norm_rows(rows):
        tok = tok_v[rows, :].astype(F32)
        centered = tok - jnp.mean(tok, axis=1, keepdims=True)
        inv_std = lax.rsqrt(jnp.mean(centered * centered, axis=1, keepdims=True) + EPS)
        return centered * inv_std, inv_std

    def normalize():
        @pl.loop(0, own_rows // STEP)
        def _(r):
            xhat, _ = norm_rows(at_block(r, STEP))
            to = pl.ds(pl.multiple_of(at.z * own_rows + r * STEP, STEP), STEP)
            nrm[to, :] = (xhat * gain_ref[0:1, :] + shift_ref[0:1, :]).astype(BF16)

    def raw_copy(wint, f):
        s = lax.rem(f, 2)
        return pltpu.make_async_copy(
            w_gate_up.at[:, :, at_block(f, BLOCK)], wint.at[s], s_raw.at[s]
        )

    def back_copies(f):
        s = lax.rem(f, 2)
        return [
            pltpu.make_async_copy(
                wf.at[s, :, pl.ds(n * BLOCK, BLOCK)], w.at[:, at_block(f, BLOCK)], s_back.at[n, s]
            )
            for n, w in enumerate((w_gate, w_up))
        ]

    def pair_copies(f, s):
        return [
            pltpu.make_async_copy(
                w.at[:, at_block(f, BLOCK)], wf.at[s, :, pl.ds(n * BLOCK, BLOCK)], s_wf.at[n, s]
            )
            for n, w in enumerate((w_gate, w_up))
        ]

    def qkv_copies(m, s):
        return [
            pltpu.make_async_copy(
                w_qkv.at[lax.div(m, per), :, at_block(lax.rem(m, per), WIDE)], wf.at[s], s_wf.at[0, s]
            )
        ]

    def hidden_tile(f, s, rows):
        both_parts = dot(nrm[rows, :], wf[s], 1, 0)
        g, u = both_parts[:, :BLOCK], both_parts[:, BLOCK:]
        sig = jax.nn.sigmoid(g)
        silu = g * sig
        lanes = at_block(f, BLOCK)
        h = (silu * u).astype(BF16)
        hq_v[rows, lanes] = h
        hat_v[lanes, rows] = jnp.transpose(h)
        a1_v[rows, lanes] = (u * (sig + silu * (1.0 - sig))).astype(BF16)
        a2_v[rows, lanes] = silu.astype(BF16)

    def qkv_tile(m, s, rows):
        t = lax.div(m, per)
        value = dot(nrm[rows, :], wf[s], 1, 0) + bias_ref[m]
        for n in range(WIDE // LANES):
            x = value[:, n * LANES : (n + 1) * LANES]
            turned = turn(x, (tab_v[0, rows, :], tab_v[1, rows, :], tab_v[2, rows, :]), 1.0)
            lanes = pl.ds(pl.multiple_of(lax.rem(m, per) * WIDE + n * LANES, LANES), LANES)
            qkv_v[t, rows, lanes] = jnp.where(t < 2, turned, x).astype(BF16)

    def turn_over(origin):
        rows = shard(origin)
        for n in range(columns):
            cols = pl.ds(n * WIDE, WIDE)
            nt_v[cols, rows] = jnp.transpose(nrm[rows, cols])

    def own_pass(wint):
        r = lax.broadcasted_iota(jnp.int32, (WIDE, WIDE), 0)
        c = lax.broadcasted_iota(jnp.int32, (WIDE, WIDE), 1)
        source = jnp.where(r < BLOCK, 2 * r, 2 * (r - BLOCK) + 1)
        parting = (source == c).astype(F32).astype(BF16)
        rows = shard(at.z)

        @pl.loop(0, n_g)
        def _(f):
            s = lax.rem(f, 2)

            @pl.when(f + 1 < n_g)
            def _():
                raw_copy(wint, f + 1).start()

            raw_copy(wint, f).wait()

            @pl.when(f >= 2)
            def _():
                wait(back_copies(f - 2))

            for n in range(model // BLOCK):
                part = pl.ds(n * BLOCK, BLOCK)
                raw = wint[s, part].reshape(WIDE, BLOCK)
                parted = dot(parting, raw, 1, 0, BF16)
                wf[s, part, :BLOCK] = parted[:BLOCK]
                wf[s, part, BLOCK:] = parted[BLOCK:]
            start(back_copies(f))
            hidden_tile(f, s, rows)

        for f in (n_g - 2, n_g - 1):
            wait(back_copies(f))
        start(qkv_copies(0, n_g % 2))

        @pl.loop(0, n_q)
        def _(m):
            n = n_g + m
            s = lax.rem(n, 2)

            @pl.when(m + 1 < n_q)
            def _():
                start(qkv_copies(m + 1, 1 - s))

            @pl.when(m + 1 == n_q)
            def _():
                start(pair_copies(0, 1 - s))

            wait(qkv_copies(m, s))
            qkv_tile(m, s, rows)

    def later_pass(k):
        rows = shard(at.order[k])
        base = k * fill

        @pl.loop(0, n_g)
        def _(f):
            s = lax.rem(base + f, 2)

            @pl.when(f + 1 < n_g)
            def _():
                start(pair_copies(f + 1, 1 - s))

            @pl.when(f + 1 == n_g)
            def _():
                start(qkv_copies(0, 1 - s))

            wait(pair_copies(f, s))
            hidden_tile(f, s, rows)

        @pl.loop(0, n_q)
        def _(m):
            s = lax.rem(base + n_g + m, 2)

            @pl.when(m + 1 < n_q)
            def _():
                start(qkv_copies(m + 1, 1 - s))

            if k + 1 < n_z:

                @pl.when(m + 1 == n_q)
                def _():
                    start(pair_copies(0, 1 - s))

            wait(qkv_copies(m, s))
            qkv_tile(m, s, rows)

        turn_over(at.order[k])

    def z_copies(n, which):
        s = slot_of(zsend, n)
        c = at_block(lax.rem(n, columns), WIDE)
        copies = []
        for d in range(1, n_z):
            if which == 0:
                dst = nrm.at[pl.ds((d - 1) * own_rows, own_rows), c]
            else:
                dst = zin.at[d - 1, :, c]
            src = zsend.at[s, shard(at.z_of[d])]
            sems = z_sems.at[0, d - 1, n], z_sems.at[1, d - 1, n]
            copies.append(rdma(src, dst, *sems, at.z_peers[d]))
        return copies

    def z_send(n, which, value):
        s = slot_of(zsend, n)

        @pl.when(n >= zsend.shape[0])
        def _():
            for copy in z_copies(n - zsend.shape[0], 1):
                copy.wait_send()

        zsend[s] = value.astype(BF16)
        start(z_copies(n, which))

    def branch_load(c):
        s = lax.rem(c, 2)
        cols = at_block(c, WIDE)
        return [
            pltpu.make_async_copy(
                w_down.at[:, cols], wf.at[s, pl.ds(0, local_ff)], s_wf.at[0, s]
            ),
            pltpu.make_async_copy(
                w_out.at[:, cols], wf.at[s, pl.ds(local_ff, width)], s_wf.at[1, s]
            ),
        ]

    def branch_job(c):
        s = lax.rem(c, 2)
        wait(branch_load(c))

        @pl.when(c + 1 < columns)
        def _():
            start(branch_load(c + 1))

        value = dot(hq_v[:, :local_ff], wf[s, :local_ff], 1, 0) + dot(
            attn_v[...], wf[s, local_ff : local_ff + width], 1, 0
        )
        z_send(c, 0, value)
        mine = zsend[slot_of(zsend, c), shard(at.z), :]
        nrm[pl.ds((n_z - 1) * own_rows, own_rows), at_block(c, WIDE)] = mine

    def layer_out_copy():
        rows = pl.ds((n_z - 1) * own_rows, own_rows)
        return pltpu.make_async_copy(nrm.at[rows], layer_out, s_tok.at[0])

    def layer_out_job():
        @pl.loop(0, columns)
        def _(c):
            for copy in z_copies(c, 0):
                copy.wait_recv()

        @pl.loop(0, own_rows // STEP)
        def _(r):
            value = tok_v[at_block(r, STEP), :].astype(F32)
            for n in range(n_z):
                rows = pl.ds(pl.multiple_of(n * own_rows + r * STEP, STEP), STEP)
                value = value + nrm[rows, :].astype(F32)
            nrm[rows, :] = value.astype(BF16)

        layer_out_copy().start()

    def hidden_load(g, wd):
        def one(n, what):
            b = 2 * g + n
            dst = wd.at[pl.ds(n * BLOCK, BLOCK)]

            @pl.when(b < blocks_h)
            def _():
                rows = at_block(jnp.minimum(b, blocks_h - 1), BLOCK)
                getattr(pltpu.make_async_copy(w_down.at[rows], dst, s_wd.at[n]), what)()

            @pl.when(both(b >= blocks_h, b < blocks_h + blocks_o))
            def _():
                rows = at_block(jnp.clip(b - blocks_h, 0, blocks_o - 1), BLOCK)
                getattr(pltpu.make_async_copy(w_out.at[rows], dst, s_wd.at[n]), what)()

        return one

    def hidden_job(g, wd):
        for n in range(2):
            hidden_load(g, wd)(n, "wait")
        dh = dot(dy_v[...], wd[...], 1, 1)
        for n in range(2):
            b = 2 * g + n
            part = dh[:, n * BLOCK : (n + 1) * BLOCK]

            @pl.when(b < blocks_h)
            def _(part=part, b=b):
                lanes = at_block(jnp.minimum(b, blocks_h - 1), BLOCK)
                a1_v[:, lanes] = (part * a1_v[:, lanes].astype(F32)).astype(BF16)
                a2_v[:, lanes] = (part * a2_v[:, lanes].astype(F32)).astype(BF16)

            @pl.when(both(b >= blocks_h, b < blocks_h + blocks_o))
            def _(part=part, b=b):
                do_v[:, at_block(jnp.clip(b - blocks_h, 0, blocks_o - 1), BLOCK)] = part.astype(BF16)

    def normed_load(c, wg, wu, wq):
        rows = at_block(c, WIDE)
        return [
            pltpu.make_async_copy(w_gate.at[rows], wg, s_wn.at[0]),
            pltpu.make_async_copy(w_up.at[rows], wu, s_wn.at[1]),
            pltpu.make_async_copy(w_qkv.at[:, rows], wq, s_wn.at[2]),
        ]

    def normed_job(c, wg, wu, wq):
        wait(normed_load(c, wg, wu, wq))
        part = dot(a1_v[...], wg[...], 1, 1) + dot(a2_v[...], wu[...], 1, 1)
        for t in range(3):
            part = part + dot(hq_v[:, t * width : (t + 1) * width], wq[t], 1, 1)
        z_send(columns + c, 1, part)

        @pl.when(c + 1 < columns)
        def _():
            start(normed_load(c + 1, wg, wu, wq))

        own[:, at_block(c, WIDE)] = zsend[slot_of(zsend, columns + c), shard(at.z), :]

    def tokens_copy():
        return pltpu.make_async_copy(tok_v, grad_tokens_out, s_tok.at[1])

    def norm_job():
        @pl.loop(columns, 2 * columns)
        def _(n):
            @pl.when(n >= 2 * columns - zsend.shape[0])
            def _():
                for copy in z_copies(n, 1):
                    copy.wait_send()

            for copy in z_copies(n, 1):
                copy.wait_recv()

        @pl.loop(0, own_rows // STEP)
        def _(r):
            rows = at_block(r, STEP)
            d = own[rows, :].astype(F32)
            for n in range(n_z - 1):
                d = d + zin[n, rows, :].astype(F32)
            xhat, inv_std = norm_rows(rows)
            scaled = d * gain_ref[0:1, :]
            here = pl.ds(pl.multiple_of(at.z * own_rows + r * STEP, STEP), STEP)
            out = dy_v[here, :].astype(F32) + inv_std * (
                scaled
                - jnp.mean(scaled, axis=1, keepdims=True)
                - xhat * jnp.mean(scaled * xhat, axis=1, keepdims=True)
            )
            small[0:1, :] += jnp.sum(d * xhat, axis=0, keepdims=True)
            small[1:2, :] += jnp.sum(d, axis=0, keepdims=True)
            tok_v[rows, :] = out.astype(BF16)

        tokens_copy().start()

    small_peers = (at.core_peer, at.x_peer, at.y_peer)

    def small_copy(n):
        return [
            rdma(small, small_in.at[n], small_sems.at[0, n], small_sems.at[1, n], small_peers[n])
        ]

    def share_copies():
        share = small.shape[1] // n_z
        return [
            rdma(
                small.at[:, at_block(at.z_of[d], share)],
                share_in.at[d - 1],
                share_sems.at[0, d - 1],
                share_sems.at[1, d - 1],
                at.z_peers[d],
            )
            for d in range(1, n_z)
        ]

    def small_step(n):
        wait(small_copy(n))
        small[...] = small[...] + small_in[n]
        start(small_copy(n + 1) if n < 2 else share_copies())

    def small_end():
        wait(share_copies())
        share = small.shape[1] // n_z
        mine = small[0:2, at_block(at.z, share)]
        for n in range(n_z - 1):
            mine = mine + share_in[n, 0:2, :]
        small_out[0:2, :] = mine
        small_out[2:5, :] = small[2:5, 0:share]

    loads = [
        pltpu.make_async_copy(tokens, tok_v, load.at[0]),
        pltpu.make_async_copy(grad_out, dy_v.at[shard(at.z)], load.at[1]),
        pltpu.make_async_copy(tables, tab_v, load.at[2]),
    ]
    barrier = pltpu.get_barrier_semaphore()
    peers = [at.core_peer, at.x_peer, at.y_peer] + at.z_peers[1:]
    for peer in peers:
        pl.semaphore_signal(barrier, inc=1, device_id=peer, device_id_type=MESH)
    start(loads)
    small[...] = jnp.zeros_like(small)
    small_out[...] = jnp.zeros_like(small_out)
    loads[0].wait()
    normalize()
    pl.semaphore_wait(barrier, len(peers))

    def forward(wint):
        raw_copy(wint, 0).start()
        route(n_copy, "start")[0]()
        loads[2].wait()
        own_pass(wint)
        turn_over(at.z)

    pl.run_scoped(forward, pltpu.VMEM((2, model, 2, BLOCK), BF16))
    n_arrived(at.order[1])
    route(n_copy, "start")[1](True)

    @pl.when(at.middle)
    def _():
        n_arrived(at.order[2])

    route(n_copy, "start")[1](False)
    loads[1].wait()
    for c in range(dy_chunks):
        route(lambda *a: y_copy(*a, c), "start")[0]()
    later_pass(1)

    @pl.when(at.end)
    def _():
        n_arrived(at.order[2])

    later_pass(2)
    n_arrived(at.order[3])
    later_pass(3)
    start(branch_load(0))

    first, passed = route(n_copy, "wait_send")
    first()
    passed(True)
    passed(False)
    for peer in at.z_peers[1:]:
        pl.semaphore_signal(ready, inc=1, device_id=peer, device_id_type=MESH)

    early = units - n_d // 2

    @pl.loop(0, dy_chunks)
    def _(c):
        @pl.when(at.middle)
        def _():
            y_arrived(at.order[1], c)
            y_arrived(at.order[2], c)

        _, onward = route(lambda *a: y_copy(*a, c), "start")
        onward(True)
        onward(False)
        attend_unit(c, qkv_v, attn_v, hat_v, lse_v, local_ff)

    def rest_of_dy(c):
        y_arrived(at.order[3], c)

        @pl.when(at.end)
        def _():
            y_arrived(at.order[1], c)
            y_arrived(at.order[2], c)

    def live(it):
        return both(it >= 0, it < total)

    attend_late = units - dy_chunks
    branch_at = attend_late
    hidden_jobs = -(-(blocks_h + blocks_o) // 2)
    back_first = hidden_jobs - blocks_h // 2
    hidden_at = branch_at
    back_at = hidden_at + back_first
    normed_at = max(back_at + units, hidden_at + hidden_jobs)
    out_at = 21
    norm_at = total + 2
    needs = {}
    for it in range(n_d):
        last = min(((it + 1) * PIECES - 1) // blocks_h, columns - 1)
        needs.setdefault(last * WIDE // dy_wide, it)

    def hidden_index(n):
        return jnp.where(n < back_first, n + blocks_h // 2, n - back_first)

    def ticks(wg, wu, wq, wd, dq, dk, dv):
        for n in range(2):
            hidden_load(hidden_index(0), wd)(n, "start")
        start(normed_load(0, wg, wu, wq))

        @pl.loop(0, total + 6 * LAG)
        def _(tick):
            one = tick - LAG

            @pl.when(live(one))
            def _():
                wait(stage0(one))
                sa, s = slot_of(acc, one), slot_of(rcv0, one)

                @pl.loop(0, 8)
                def _(p):
                    acc[sa, p] = (acc[sa, p].astype(F32) + rcv0[s, p].astype(F32)).astype(BF16)

                start(stage1(one))

            two = tick - 2 * LAG

            @pl.when(live(two))
            def _():
                wait(stage1(two))
                sa, s = slot_of(acc, two), slot_of(rcv1, two)
                for n, bit in ((0, at.x), (1, at.y)):
                    for m in range(2):
                        p = quarter(bit, n) + m
                        acc[sa, p] = (
                            acc[sa, p].astype(F32) + rcv1[s, n, m].astype(F32)
                        ).astype(BF16)
                start(stage2(two))

            three = tick - 3 * LAG

            @pl.when(live(three))
            def _():
                wait(stage2(three))
                sa, s, d = slot_of(acc, three), slot_of(rcv2, three), slot_of(fin, three)
                for n, p in ((0, quarter(at.x, 0) + at.y), (1, quarter(at.y, 1) + at.x)):
                    fin[d, n] = (acc[sa, p].astype(F32) + rcv2[s, n].astype(F32)).astype(BF16)
                start(stage3(three))
                start(keep3(three))

            four = tick - 4 * LAG

            @pl.when(live(four))
            def _():
                wait(keep3(four))
                wait(stage3(four))
                start(stage4(four))

            five = tick - 5 * LAG

            @pl.when(live(five))
            def _():
                wait(stage4(five))
                start(stage5(five))

            six = tick - 6 * LAG

            @pl.when(live(six))
            def _():
                wait(stage5(six))

            for c, it in needs.items():

                @pl.when(tick == it)
                def _(c=c):
                    rest_of_dy(c)

            @pl.when(tick < n_d)
            def _():
                product(tick, by_block(tick))

            @pl.when(both(tick >= n_d, tick < n_d + n_g))
            def _():
                product(tick, tall(lambda: gate_right(tick - n_d)))

            @pl.when(both(tick >= n_d + n_g, tick < total))
            def _():
                product(tick, tall(lambda: hq_v[:, at_block(tick - n_d - n_g, WIDE)]))

            @pl.when(tick < attend_late)
            def _():
                attend_unit(tick + dy_chunks, qkv_v, attn_v, hat_v, lse_v, local_ff)

            @pl.when(tick == branch_at)
            def _():
                pl.semaphore_wait(ready, n_z - 1)

            @pl.when(both(tick >= branch_at, tick < branch_at + columns // 2))
            def _():
                @pl.loop(0, 2)
                def _(n):
                    branch_job(2 * (tick - branch_at) + n)

            @pl.when(both(tick >= hidden_at, tick < hidden_at + hidden_jobs))
            def _():
                n = tick - hidden_at
                hidden_job(hidden_index(n), wd)

                @pl.when(n + 1 < hidden_jobs)
                def _():
                    for m in range(2):
                        hidden_load(hidden_index(n + 1), wd)(m, "start")

            @pl.when(both(tick >= back_at, tick < back_at + units))
            def _():
                attend_back_unit(
                    tick - back_at, qkv_v, do_v, lse_v, tab_v, hq_v, small, dq, dk, dv
                )

            @pl.when(both(tick >= normed_at, tick < normed_at + columns))
            def _():
                normed_job(tick - normed_at, wg, wu, wq)

            @pl.when(tick == out_at)
            def _():
                layer_out_job()
                for c in range(dy_chunks):
                    first, passed = route(lambda *a: y_copy(*a, c), "wait_send")
                    first()
                    passed(True)
                    passed(False)

            @pl.when(tick == norm_at)
            def _():
                norm_job()
                start(small_copy(0))

            for n in range(3):

                @pl.when(tick == norm_at + 1 + n)
                def _(n=n):
                    small_step(n)

            @pl.when(tick == norm_at + 4)
            def _():
                small_end()
                tokens_copy().wait()
                layer_out_copy().wait()

    pl.run_scoped(
        ticks,
        pltpu.VMEM((WIDE, local_ff), BF16),
        pltpu.VMEM((WIDE, local_ff), BF16),
        pltpu.VMEM((3, WIDE, width), BF16),
        pltpu.VMEM((2 * BLOCK, model), BF16),
        *[pltpu.VMEM((seq_len, LANES), F32)] * 3,
    )


def run_layer(
    tokens, grad_out, tables, w_gate_up, w_qkv, w_down, w_out, gain, shift, bias, n_z
):
    own, model = tokens.shape
    seq_len = own * n_z
    local_ff, width = w_down.shape[0], w_out.shape[0]
    blocks, columns = (local_ff + width) // BLOCK, model // WIDE
    n_d = -(-blocks * columns // PIECES)
    total = n_d + local_ff // BLOCK + 3 * width // WIDE
    bf = lambda *shape: pltpu.VMEM(shape, BF16)
    fl = lambda *shape: pltpu.VMEM(shape, F32)
    sems = lambda *shape: pltpu.SemaphoreType.DMA(shape)
    slots = 2 * LAG + 2
    dy_chunks = 4
    hbm = pl.BlockSpec(memory_space=pl.ANY)
    vmem = pl.BlockSpec(memory_space=pltpu.VMEM)
    return pl.pallas_call(
        functools.partial(layer_kernel, n_z),
        in_specs=[hbm] * 7 + [vmem] * 3,
        out_specs=[hbm, hbm, hbm, vmem, hbm, hbm],
        out_shape=[
            jax.ShapeDtypeStruct((total, PIECES, BLOCK, WIDE), BF16),
            jax.ShapeDtypeStruct((own, model), BF16),
            jax.ShapeDtypeStruct((own, model), BF16),
            jax.ShapeDtypeStruct((8, model // n_z), F32),
            jax.ShapeDtypeStruct((model, local_ff), BF16),
            jax.ShapeDtypeStruct((model, local_ff), BF16),
        ],
        scratch_shapes=[
            bf(local_ff + width, seq_len), bf(model, seq_len), bf(seq_len, model),
            bf(seq_len, model), bf(seq_len, local_ff), bf(seq_len, local_ff),
            bf(3, seq_len, width), bf(seq_len, width), bf(seq_len, max(local_ff, 3 * width)),
            bf(seq_len, width), fl(width // HD, 1, seq_len), fl(3, seq_len, LANES), bf(own, model),
            bf(2, model, WIDE), bf(3, seq_len, WIDE), bf(n_z - 1, own, model), bf(own, model),
            fl(8, model), fl(3, 8, model), fl(n_z - 1, 8, model // n_z),
            bf(LAG + 1, 8, BLOCK, WIDE), bf(3 * LAG + 1, 8, BLOCK, WIDE),
            bf(slots, 8, BLOCK, WIDE), bf(slots, 2, 2, BLOCK, WIDE), bf(slots, 2, BLOCK, WIDE),
            bf(LAG + 1, 2, BLOCK, WIDE),
            sems(3), sems(2), sems(2, 2), sems(2, 2), sems(2), sems(3), sems(2),
            pltpu.SemaphoreType.REGULAR,
            sems(5), sems(n_z), sems(5, dy_chunks), sems(n_z, dy_chunks),
            sems(2, n_z - 1, 2 * columns), sems(2, 3), sems(2, n_z - 1),
            sems(2, slots), sems(4, slots), sems(4, slots),
            sems(4, slots), sems(4, slots), sems(2, slots), sems(2, LAG + 1),
        ],
        compiler_params=pltpu.CompilerParams(
            collective_id=0, has_side_effects=True, vmem_limit_bytes=67043328
        ),
        name="layer",
    )(tokens, grad_out, tables, w_gate_up, w_qkv, w_down, w_out, gain, shift, bias)


def rows_kernel(block_ref, out):
    for p in range(block_ref.shape[0]):
        out[p * BLOCK : (p + 1) * BLOCK, :] = block_ref[p].astype(F32)


def lead_kernel(block_ref, out):
    for p in range(block_ref.shape[0]):
        out[0, p * BLOCK : (p + 1) * BLOCK, :] = block_ref[p].astype(F32)


def pair_kernel(block_ref, out):
    flat = out.reshape(2 * out.shape[0], BLOCK)
    for p in range(block_ref.shape[0]):
        value = block_ref[p].astype(F32)
        for n in range(2):
            rows = pl.ds(2 * p * BLOCK + n, BLOCK, stride=2)
            flat[rows, :] = value[:, n * BLOCK : (n + 1) * BLOCK]


def unpack(items, local_ff, width, model):
    columns, n_g, n_q = model // WIDE, local_ff // BLOCK, 3 * width // WIDE
    n_d = items.shape[0] - n_g - n_q
    blocks = items.reshape(-1, BLOCK, WIDE)
    h, o = local_ff // BLOCK, width // BLOCK
    per = n_q // 3

    def take(kernel, steps, n, base, out_block, out_index, out_shape, name):
        return pl.pallas_call(
            kernel,
            grid=(steps,),
            in_specs=[pl.BlockSpec((n, BLOCK, WIDE), lambda i: (base + i, 0, 0))],
            out_specs=pl.BlockSpec(out_block, out_index),
            out_shape=jax.ShapeDtypeStruct(out_shape, F32),
            name=name,
        )(blocks)

    down = take(
        rows_kernel, columns, h, 0, (local_ff, WIDE), lambda i: (0, i), (local_ff, model), "unpack_down"
    )
    out = take(
        rows_kernel, columns, o, columns * h // o, (width, WIDE), lambda i: (0, i), (width, model), "unpack_out"
    )
    gate_up = take(
        pair_kernel, n_g, PIECES, n_d, (model, 2, BLOCK), lambda i: (0, 0, i),
        (model, 2, local_ff), "unpack_gate_up",
    )
    qkv = take(
        lead_kernel, n_q, PIECES, n_d + n_g, (1, model, WIDE), lambda i: (i // per, 0, i % per),
        (3, model, width), "unpack_qkv",
    )
    return down, out, gate_up, qkv.transpose(1, 0, 2)


def fast_path(n_dp, n_mp, rows, model_width, local_width, local_ff):
    blocks_h, blocks_o = local_ff // BLOCK, local_width // BLOCK
    return (
        n_dp == 8
        and n_mp == 4
        and rows == QB
        and model_width == PIECES * BLOCK
        and local_width == model_width // n_mp
        and local_ff % BLOCK == 0
        and blocks_h % 2 == 1
        and blocks_h + blocks_o <= PIECES
        and blocks_h * (model_width // WIDE) % blocks_o == 0
    )


def fused_layer(
    n_mp,
    tables,
    tokens,
    norm_gain,
    layernorm_bias,
    qkv_weight,
    qkv_bias,
    out_weight,
    gate_up_weight,
    down_weight,
    grad_out,
):
    model_width = tokens.shape[1]
    local_width, local_ff = qkv_weight.shape[2], gate_up_weight.shape[2]
    items, layer_out, grad_tokens, small, _, _ = run_layer(
        tokens,
        grad_out,
        tables,
        gate_up_weight,
        qkv_weight.transpose(1, 0, 2),
        down_weight,
        out_weight,
        norm_gain.astype(F32)[None],
        layernorm_bias.astype(F32)[None],
        qkv_bias.astype(F32).reshape(-1, 1, WIDE),
        n_mp,
    )
    grad_down_w, grad_out_w, grad_gate_up_w, grad_qkv_w = unpack(
        items, local_ff, local_width, model_width
    )
    return (
        layer_out,
        grad_tokens,
        small[0],
        small[1],
        grad_qkv_w,
        small[2:5, :local_width],
        grad_out_w,
        grad_gate_up_w,
        grad_down_w,
    )


def on_device(
    n_dp,
    n_mp,
    tokens,
    norm_gain,
    layernorm_bias,
    qkv_weight,
    qkv_bias,
    out_weight,
    gate_up_weight,
    down_weight,
    grad_out,
):
    rows, model_width = tokens.shape
    local_width = qkv_weight.shape[2]
    seq_len = rows * n_mp
    tables = rotary_tables(seq_len)
    if fast_path(n_dp, n_mp, rows, model_width, local_width, gate_up_weight.shape[2]):
        return fused_layer(
            n_mp, tables, tokens, norm_gain, layernorm_bias, qkv_weight, qkv_bias, out_weight,
            gate_up_weight, down_weight, grad_out,
        )
    cube = Cube("dp", n_dp)
    gain = norm_gain.astype(F32)
    token_f32 = tokens.astype(F32)
    row_mean = jnp.mean(token_f32, axis=1, keepdims=True)
    centered = token_f32 - row_mean
    inv_std = lax.rsqrt(jnp.mean(centered * centered, axis=1, keepdims=True) + EPS)
    xhat = centered * inv_std
    normed_own = (xhat * gain + layernorm_bias.astype(F32)).astype(BF16)
    normed = lax.all_gather(normed_own, "mp", axis=0, tiled=True)
    dy = lax.all_gather(grad_out, "mp", axis=0, tiled=True)

    w_qkv = [qkv_weight[:, t, :] for t in range(3)]
    w_gate, w_up = gate_up_weight[:, 0, :], gate_up_weight[:, 1, :]

    gate = dot(normed, w_gate, 1, 0)
    up = dot(normed, w_up, 1, 0)
    sig = jax.nn.sigmoid(gate)
    hidden = (gate * sig * up).astype(BF16)
    qkv = jnp.concatenate([dot(normed, w, 1, 0) for w in w_qkv], axis=1)
    q, k, v, attended, lse = attention_forward(qkv, qkv_bias.astype(F32), tables)
    branch = (dot(attended, out_weight, 1, 0) + dot(hidden, down_weight, 1, 0)).astype(BF16)
    share = lax.psum_scatter(branch, "mp", scatter_dimension=0, tiled=True)
    layer_out = (token_f32 + share.astype(F32)).astype(BF16)

    share_width = model_width // n_mp
    d_hidden = dot(dy, down_weight, 1, 1)
    silu = gate * sig
    d_gate = (d_hidden * up * (sig + silu * (1.0 - sig))).astype(BF16)
    d_up = (d_hidden * silu).astype(BF16)
    d_attended = dot(dy, out_weight, 1, 1, BF16)
    dq, dk, dv, sums = attention_backward(q, k, v, d_attended, lse, tables)
    d_normed = (
        dot(d_gate, w_gate, 1, 1)
        + dot(d_up, w_up, 1, 1)
        + dot(dq, w_qkv[0], 1, 1)
        + dot(dk, w_qkv[1], 1, 1)
        + dot(dv, w_qkv[2], 1, 1)
    ).astype(BF16)
    d_own = lax.psum_scatter(d_normed, "mp", scatter_dimension=0, tiled=True).astype(F32)
    d_qkv = jnp.concatenate([dq, dk, dv], axis=1)
    grad_down_w = cube.contract(hidden, dy)
    grad_out_w = cube.contract(attended, dy)
    grad_gate_up_w = jnp.stack(
        [cube.contract(normed, d_gate), cube.contract(normed, d_up)], axis=1
    )
    grad_qkv_w = cube.contract(normed, d_qkv).reshape(model_width, 3, local_width)

    scaled = d_own * gain
    grad_tokens = grad_out.astype(F32) + inv_std * (
        scaled
        - jnp.mean(scaled, axis=1, keepdims=True)
        - xhat * jnp.mean(scaled * xhat, axis=1, keepdims=True)
    )
    terms = jnp.stack([jnp.sum(d_own * xhat, axis=0), jnp.sum(d_own, axis=0)])
    bias_sum = cube.sum_all(sums)
    grad_bias = bias_sum.swapaxes(0, 1).reshape(3, local_width)
    terms = Cube("mp", n_mp).sum_all(cube.sum_all(terms))
    terms = lax.dynamic_slice_in_dim(
        terms, lax.axis_index("mp") * share_width, share_width, 1
    )
    return (
        layer_out,
        grad_tokens.astype(BF16),
        terms[0],
        terms[1],
        grad_qkv_w,
        grad_bias,
        grad_out_w,
        grad_gate_up_w,
        grad_down_w,
    )


def solution(mesh):
    return jax.shard_map(
        functools.partial(on_device, mesh.shape["dp"], mesh.shape["mp"]),
        mesh=mesh,
        in_specs=(
            P(("dp", "mp"), None),
            P(),
            P(),
            P(None, None, "mp"),
            P(None, "mp"),
            P("mp", None),
            P(None, None, "mp"),
            P("mp", None),
            P(("dp", "mp"), None),
        ),
        out_specs=(
            P(("dp", "mp"), None),
            P(("dp", "mp"), None),
            P("mp"),
            P("mp"),
            P(None, None, "mp"),
            P(None, "mp"),
            P("mp", None),
            P(None, None, "mp"),
            P("mp", None),
        ),
        check_vma=False,
    )
```

```python
import functools
import math

import jax
import jax.numpy as jnp
from jax import lax
from jax.experimental import pallas as pl
from jax.experimental.pallas import tpu as pltpu
from jax.sharding import PartitionSpec as P

HD = 64
ROT = 16
EPS = 1e-05
LANES = 128
QB = 256


F32 = jnp.float32
BF16 = jnp.bfloat16


def dot(a, b, ca, cb, out=F32):
    return lax.dot_general(
        a, b, (((ca,), (cb,)), ((), ())), preferred_element_type=F32
    ).astype(out)


def rotary_tables(seq_len):
    positions = jnp.arange(seq_len, dtype=F32)
    freqs = 1.0 / 10000.0 ** (jnp.arange(ROT // 2, dtype=F32) * 2.0 / ROT)
    phase = positions[:, None] * freqs[None, :]
    cosine, sine = jnp.cos(phase), jnp.sin(phase)
    half = ROT // 2
    rest = HD - ROT
    ones = jnp.ones((seq_len, rest), F32)
    zeros = jnp.zeros((seq_len, rest), F32)
    zhalf = jnp.zeros((seq_len, half), F32)
    c = jnp.concatenate([cosine, cosine, ones], axis=1)
    up = jnp.concatenate([-sine, zhalf, zeros], axis=1)
    down = jnp.concatenate([zhalf, sine, zeros], axis=1)
    two = LANES // HD
    return jnp.stack([jnp.tile(t, (1, two)) for t in (c, up, down)])


def turn(x, tables, sign):
    half = ROT // 2
    ahead = pltpu.roll(x, LANES - half, 1)
    behind = pltpu.roll(x, half, 1)
    return x * tables[0] + sign * (ahead * tables[1] + behind * tables[2])


def lane_mask(rows, j):
    lane = lax.broadcasted_iota(jnp.int32, (rows, LANES), 1)
    return (lane // HD) == j


def forward_kernel(
    q_in, k_in, v_in, bias_ref, tab_ref, q_out, k_out, v_out, o_ref, lse_ref
):
    seq_len = q_in.shape[0]
    j = pl.program_id(1)

    @pl.when(j == 0)
    def _():
        tables = (tab_ref[0], tab_ref[1], tab_ref[2])
        q_out[...] = turn(q_in[...] + bias_ref[0, 0:1], tables, 1.0).astype(BF16)
        k_out[...] = turn(k_in[...] + bias_ref[0, 1:2], tables, 1.0).astype(BF16)
        v_out[...] = (v_in[...] + bias_ref[0, 2:3]).astype(BF16)

    mask = lane_mask(QB, j)
    causal = lax.broadcasted_iota(jnp.int32, (QB, QB), 0) <= lax.broadcasted_iota(
        jnp.int32, (QB, QB), 1
    )
    for i in range(seq_len // QB):
        rows = pl.ds(i * QB, QB)
        span = (i + 1) * QB
        q = q_out[rows, :] * 0.125
        q = jnp.where(mask, q, jnp.zeros_like(q))
        parts = []
        if i:
            parts.append(dot(k_out[pl.ds(0, i * QB), :], q, 1, 1))
        diag = dot(k_out[rows, :], q, 1, 1)
        parts.append(jnp.where(causal, diag, -1e30))
        top = functools.reduce(
            jnp.maximum, [jnp.max(s, axis=0, keepdims=True) for s in parts]
        )
        exps = [jnp.exp(s - top) for s in parts]
        total = sum(jnp.sum(e, axis=0, keepdims=True) for e in exps)
        inv = 1.0 / total
        probs = jnp.concatenate([(e * inv).astype(BF16) for e in exps], axis=0)
        out = dot(probs, v_out[pl.ds(0, span), :], 0, 0).astype(BF16)
        before = o_ref[rows, :]
        o_ref[rows, :] = jnp.where(mask, out, before)
        lse_ref[0, 0, :, i * QB : (i + 1) * QB] = top + jnp.log(total)


def backward_kernel(
    q_ref, k_ref, v_ref, do_ref, lse_ref, tab_ref, dq_out, dk_out, dv_out, sums_out, dq, dk, dv
):
    seq_len = q_ref.shape[0]
    j = pl.program_id(1)
    mask = lane_mask(QB, j)
    causal = lax.broadcasted_iota(jnp.int32, (QB, QB), 0) <= lax.broadcasted_iota(
        jnp.int32, (QB, QB), 1
    )

    @pl.when(j == 0)
    def _():
        dk[...] = jnp.zeros_like(dk)
        dv[...] = jnp.zeros_like(dv)

    for i in range(seq_len // QB):
        rows = pl.ds(i * QB, QB)
        q = q_ref[rows, :] * 0.125
        q = jnp.where(mask, q, jnp.zeros_like(q))
        do = do_ref[rows, :]
        do = jnp.where(mask, do, jnp.zeros_like(do))
        lse = lse_ref[0, 0, :, i * QB : (i + 1) * QB]
        pieces = []
        if i:
            pieces.append((pl.ds(0, i * QB), False))
        pieces.append((rows, True))
        probs, grads = [], []
        inner = 0.0
        for where, diagonal in pieces:
            s = dot(k_ref[where, :], q, 1, 1)
            if diagonal:
                s = jnp.where(causal, s, -1e30)
            p = jnp.exp(s - lse)
            dp = dot(v_ref[where, :], do, 1, 1)
            inner = inner + jnp.sum(p * dp, axis=0, keepdims=True)
            probs.append(p)
            grads.append(dp)
        acc = 0.0
        for (where, diagonal), p, dp in zip(pieces, probs, grads):
            ds = (p * (dp - inner)).astype(BF16)
            dv[where, :] += dot(p.astype(BF16), do, 1, 0)
            dk[where, :] += dot(ds, q, 1, 0)
            acc = acc + dot(ds, k_ref[where, :], 0, 0)
        before = dq[rows, :]
        dq[rows, :] = jnp.where(mask, acc * 0.125, before)

    @pl.when(j == pl.num_programs(1) - 1)
    def _():
        tables = (tab_ref[0], tab_ref[1], tab_ref[2])
        gq = turn(dq[...], tables, -1.0).astype(BF16)
        gk = turn(dk[...], tables, -1.0).astype(BF16)
        gv = dv[...].astype(BF16)
        dq_out[...] = gq
        dk_out[...] = gk
        dv_out[...] = gv
        sums_out[0, 0:1] = jnp.sum(gq.astype(F32), axis=0, keepdims=True)
        sums_out[0, 1:2] = jnp.sum(gk.astype(F32), axis=0, keepdims=True)
        sums_out[0, 2:3] = jnp.sum(gv.astype(F32), axis=0, keepdims=True)


def attention_forward(qkv, bias, tables):
    seq_len, width = qkv.shape[0], qkv.shape[1] // 3
    pairs = width // LANES
    column = lambda part: pl.BlockSpec((seq_len, LANES), lambda p, j: (0, part * pairs + p))
    block = pl.BlockSpec((seq_len, LANES), lambda p, j: (0, p))
    bias_blocks = bias.reshape(3, pairs, LANES).swapaxes(0, 1)
    wide = jax.ShapeDtypeStruct((seq_len, width), BF16)
    elements = pairs * 2 * seq_len * seq_len // 2
    return pl.pallas_call(
        forward_kernel,
        grid=(pairs, LANES // HD),
        in_specs=[
            column(0),
            column(1),
            column(2),
            pl.BlockSpec((1, 3, LANES), lambda p, j: (p, 0, 0)),
            pl.BlockSpec((3, seq_len, LANES), lambda p, j: (0, 0, 0)),
        ],
        out_specs=[
            block,
            block,
            block,
            block,
            pl.BlockSpec((1, 1, 1, seq_len), lambda p, j: (p, j, 0, 0)),
        ],
        out_shape=[
            wide,
            wide,
            wide,
            wide,
            jax.ShapeDtypeStruct((pairs, LANES // HD, 1, seq_len), F32),
        ],
        cost_estimate=pl.CostEstimate(
            flops=elements * 4 * LANES,
            bytes_accessed=qkv.size * 4 + 4 * seq_len * width * 2,
            transcendentals=elements,
        ),
        name="attention_forward",
    )(qkv, qkv, qkv, bias_blocks, tables)


def attention_backward(q, k, v, grad, lse, tables):
    seq_len, width = q.shape
    pairs = width // LANES
    block = pl.BlockSpec((seq_len, LANES), lambda p, j: (0, p))
    wide = jax.ShapeDtypeStruct((seq_len, width), BF16)
    elements = pairs * 2 * seq_len * seq_len // 2
    return pl.pallas_call(
        backward_kernel,
        grid=(pairs, LANES // HD),
        in_specs=[
            block,
            block,
            block,
            block,
            pl.BlockSpec((1, 1, 1, seq_len), lambda p, j: (p, j, 0, 0)),
            pl.BlockSpec((3, seq_len, LANES), lambda p, j: (0, 0, 0)),
        ],
        out_specs=[block, block, block, pl.BlockSpec((1, 3, LANES), lambda p, j: (p, 0, 0))],
        out_shape=[wide, wide, wide, jax.ShapeDtypeStruct((pairs, 3, LANES), F32)],
        scratch_shapes=[pltpu.VMEM((seq_len, LANES), F32)] * 3,
        cost_estimate=pl.CostEstimate(
            flops=elements * 10 * LANES,
            bytes_accessed=7 * seq_len * width * 2,
            transcendentals=elements,
        ),
        name="attention_backward",
    )(q, k, v, grad, lse, tables)


def pick(x, index):
    return lax.dynamic_index_in_dim(x, index, 0, keepdims=False)


class Cube:
    def __init__(self, axis, size):
        self.axis, self.size = axis, size
        self.bits = [b for b in range(size.bit_length()) if 1 << b < size]
        me = lax.axis_index(axis)
        self.own = [lax.rem(lax.div(me, 1 << b), 2) for b in self.bits]

    def swap(self, x, b):
        return lax.ppermute(x, self.axis, [(i, i ^ (1 << b)) for i in range(self.size)])

    def sum_all(self, x):
        for b in self.bits:
            x = x + self.swap(x, b)
        return x

    def contract(self, left, right):
        depth, rows = left.shape
        columns = right.shape[1]
        core, others = self.bits[0], self.bits[1:]
        half = rows // 2
        mine = self.own[0]
        first = lax.dynamic_slice_in_dim(left, (1 - mine) * half, half, 1)
        second = lax.dynamic_slice_in_dim(left, mine * half, half, 1)
        away = dot(first, right, 0, 0, BF16)
        came = self.swap(away, core)
        keep = dot(second, right, 0, 0, BF16)
        orders = [others, others[::-1]]
        quarter = half // 2
        done = []
        for n, order in enumerate(orders):
            small = quarter >> len(order)
            shape = (2,) * len(order) + (small, columns)
            cur = (
                keep[n * quarter : (n + 1) * quarter].astype(F32)
                + came[n * quarter : (n + 1) * quarter].astype(F32)
            ).reshape(shape)
            for b in order:
                own = self.own[b]
                send = pick(cur, 1 - own).astype(BF16)
                got = self.swap(send, b)
                cur = pick(cur, own) + got.astype(F32)
            buf = cur.astype(BF16)
            for b in order[::-1]:
                own = self.own[b]
                got = self.swap(buf, b)
                low = jnp.where(own == 0, buf, got)
                high = jnp.where(own == 0, got, buf)
                buf = jnp.stack([low, high])
            done.append(buf.reshape(quarter, columns))
        whole = jnp.concatenate(done, axis=0)
        other = self.swap(whole, core)
        low = jnp.where(mine == 0, whole, other)
        high = jnp.where(mine == 0, other, whole)
        return jnp.concatenate([low, high], axis=0).astype(F32)


LAG = 2
BLOCK = 128
PIECES = 16
WIDE = 256
STEP = 32
MESH = pl.DeviceIdType.MESH


class Places:
    def __init__(self, n_dp, n_z):
        self.me = lax.axis_index("dp")
        self.z = z = lax.axis_index("mp")
        self.core = lax.rem(self.me, 2)
        self.x = lax.rem(lax.div(self.me, 2), 2)
        self.y = lax.div(self.me, 4)
        self.core_peer = (self.me + 1 - 2 * self.core, z)
        self.x_peer = (self.me + 2 - 4 * self.x, z)
        self.y_peer = (self.me + 4 - 8 * self.y, z)
        self.dp_others = [lax.rem(self.me + n, n_dp) for n in range(1, n_dp)]
        self.dp_peers = [(other, z) for other in self.dp_others]
        self.z_of = [lax.rem(z + d, n_z) for d in range(n_z)]
        self.z_peers = [(self.me, to) for to in self.z_of]
        self.above = jnp.minimum(z + 1, n_z - 1)
        self.below = jnp.maximum(z - 1, 0)
        self.far = n_z - 1 - z
        self.has_above, self.has_below = z < n_z - 1, z > 0
        self.end = jnp.logical_or(z == 0, z == n_z - 1)
        self.middle = jnp.logical_not(self.end)
        self.order = [
            z,
            jnp.where(z == 0, 1, z - 1),
            jnp.where(z == 0, 2, jnp.where(z == 1, 2, jnp.where(z == 2, 3, 1))),
            jnp.where(z <= 1, 3, 0),
        ]


def rdma(src, dst, send_sem, recv_sem, peer):
    return pltpu.make_async_remote_copy(
        src_ref=src,
        dst_ref=dst,
        send_sem=send_sem,
        recv_sem=recv_sem,
        device_id=peer,
        device_id_type=MESH,
    )


def start(copies):
    for copy in copies:
        copy.start()


def wait(copies):
    for copy in copies:
        copy.wait()


def at_block(i, size):
    return pl.ds(pl.multiple_of(i * size, size), size)


def both(a, b):
    return jnp.logical_and(a, b)


def causal_block():
    key = lax.broadcasted_iota(jnp.int32, (QB, QB), 0)
    query = lax.broadcasted_iota(jnp.int32, (QB, QB), 1)
    return key <= query


def head_part(x, mask):
    return jnp.where(mask, x, jnp.zeros_like(x))


def attend_unit(u, qkv_v, attn_v, hat_v, lse_v, first_row):
    seq_len = qkv_v.shape[1]
    pair, j = lax.div(u, 2), lax.rem(u, 2)
    lanes = at_block(pair, LANES)
    mask = lane_mask(QB, j)
    causal = causal_block()
    for i in range(seq_len // QB):
        rows = pl.ds(i * QB, QB)
        q = head_part(qkv_v[0, rows, lanes] * 0.125, mask)
        parts = []
        if i:
            parts.append(dot(qkv_v[1, pl.ds(0, i * QB), lanes], q, 1, 1))
        parts.append(jnp.where(causal, dot(qkv_v[1, rows, lanes], q, 1, 1), -1e30))
        top = functools.reduce(
            jnp.maximum, [jnp.max(s, axis=0, keepdims=True) for s in parts]
        )
        exps = [jnp.exp(s - top) for s in parts]
        total = sum(jnp.sum(e, axis=0, keepdims=True) for e in exps)
        inv = 1.0 / total
        probs = jnp.concatenate([(e * inv).astype(BF16) for e in exps], axis=0)
        out = dot(probs, qkv_v[2, pl.ds(0, (i + 1) * QB), lanes], 0, 0).astype(BF16)
        attn_v[rows, lanes] = jnp.where(mask, out, attn_v[rows, lanes])
        lse_v[u, :, i * QB : (i + 1) * QB] = top + jnp.log(total)

    @pl.when(j == 1)
    def _():
        for i in range(seq_len // QB):
            rows = pl.ds(i * QB, QB)
            to = pl.ds(pl.multiple_of(first_row + pair * LANES, LANES), LANES)
            hat_v[to, rows] = jnp.transpose(attn_v[rows, lanes])


def attend_back_unit(u, qkv_v, do_v, lse_v, tab_v, dqkv_v, small, dq, dk, dv):
    seq_len, width = qkv_v.shape[1:]
    pair, j = lax.div(u, 2), lax.rem(u, 2)
    lanes = at_block(pair, LANES)
    mask = lane_mask(QB, j)
    causal = causal_block()

    @pl.when(j == 0)
    def _():
        dk[...] = jnp.zeros_like(dk)
        dv[...] = jnp.zeros_like(dv)
        dq[...] = jnp.zeros_like(dq)

    for i in range(seq_len // QB):
        rows = pl.ds(i * QB, QB)
        q = head_part(qkv_v[0, rows, lanes] * 0.125, mask)
        do = head_part(do_v[rows, lanes], mask)
        lse = lse_v[u, :, i * QB : (i + 1) * QB]
        pieces = [(pl.ds(0, i * QB), False)] if i else []
        pieces.append((rows, True))
        probs, grads = [], []
        inner = 0.0
        for where, diagonal in pieces:
            s = dot(qkv_v[1, where, lanes], q, 1, 1)
            if diagonal:
                s = jnp.where(causal, s, -1e30)
            p = jnp.exp(s - lse)
            dp = dot(qkv_v[2, where, lanes], do, 1, 1)
            inner = inner + jnp.sum(p * dp, axis=0, keepdims=True)
            probs.append(p)
            grads.append(dp)
        acc = 0.0
        for (where, diagonal), p, dp in zip(pieces, probs, grads):
            ds = (p * (dp - inner)).astype(BF16)
            dv[where, :] += dot(p.astype(BF16), do, 1, 0)
            dk[where, :] += dot(ds, q, 1, 0)
            acc = acc + dot(ds, qkv_v[1, where, lanes], 0, 0)
        dq[rows, :] = jnp.where(mask, acc * 0.125, dq[rows, :])

    @pl.when(j == 1)
    def _():
        tables = (tab_v[0], tab_v[1], tab_v[2])
        out = (
            turn(dq[...], tables, -1.0).astype(BF16),
            turn(dk[...], tables, -1.0).astype(BF16),
            dv[...].astype(BF16),
        )
        for t, g in enumerate(out):
            dqkv_v[:, pl.ds(pl.multiple_of(t * width + pair * LANES, LANES), LANES)] = g
            small[2 + t : 3 + t, lanes] = jnp.sum(g.astype(F32), axis=0, keepdims=True)


def layer_kernel(
    n_dp, n_z, tokens, grad_out, tables, w_gate_up, w_qkv, w_down, w_out, gain_ref, shift_ref, bias_ref,
    sums_out, layer_out, grad_tokens_out, small_out, w_gate, w_up,
    hat_v, nt_v, dy_v, nrm, a1_v, a2_v, qkv_v, attn_v, hq_v, dqkv_v, do_v, lse_v, tab_v, tok_v,
    wf, zsend, zin, own, small, small_in, share_in,
    away, acc, rcv0, rcv1, rcv2, fin,
    load, s_raw, s_wf, s_back, s_wd, s_wn, s_tok, ready,
    n_send, n_recv, y_send, y_recv, z_sems, small_sems, share_sems,
    s0, s1, s2, s3, s4, s5, s_fin,
):
    at = Places(n_dp, n_z)
    seq_len, model = dy_v.shape
    own_rows = tok_v.shape[0]
    width = qkv_v.shape[2]
    local_ff = a1_v.shape[1]
    blocks_h, blocks_o = local_ff // BLOCK, width // BLOCK
    columns = model // WIDE
    n_d = columns
    n_g, n_q = blocks_h, 3 * width // WIDE
    total = n_d + n_g + n_q
    per = width // WIDE
    fill = n_g + n_q
    dy_chunks = y_recv.shape[1]
    dy_wide = model // dy_chunks
    units = width // HD

    def slot_of(buf, it):
        return lax.rem(it, buf.shape[0])

    def quarter(bit, half):
        return half * 4 + bit * 2

    def stage0(it):
        sa, s = slot_of(away, it), slot_of(rcv0, it)
        return [rdma(away.at[sa], rcv0.at[s], s0.at[0, s], s0.at[1, s], at.core_peer)]

    def stage1(it):
        sa, s = slot_of(acc, it), slot_of(rcv1, it)
        a, b = pl.ds(quarter(1 - at.x, 0), 2), pl.ds(quarter(1 - at.y, 1), 2)
        return [
            rdma(acc.at[sa, a], rcv1.at[s, 0], s1.at[0, s], s1.at[1, s], at.x_peer),
            rdma(acc.at[sa, b], rcv1.at[s, 1], s1.at[2, s], s1.at[3, s], at.y_peer),
        ]

    def stage2(it):
        sa, s = slot_of(acc, it), slot_of(rcv2, it)
        a, b = quarter(at.x, 0) + 1 - at.y, quarter(at.y, 1) + 1 - at.x
        return [
            rdma(acc.at[sa, a], rcv2.at[s, 0], s2.at[0, s], s2.at[1, s], at.y_peer),
            rdma(acc.at[sa, b], rcv2.at[s, 1], s2.at[2, s], s2.at[3, s], at.x_peer),
        ]

    def piece_a():
        return at.core * 8 + quarter(at.x, 0) + at.y

    def piece_b():
        return at.core * 8 + quarter(at.y, 1) + at.x

    def stage3(it):
        s, n = slot_of(fin, it), lax.rem(it, s3.shape[1])
        a, b = sums_out.at[it, piece_a()], sums_out.at[it, piece_b()]
        return [
            rdma(fin.at[s, 0], a, s3.at[0, n], s3.at[1, n], at.y_peer),
            rdma(fin.at[s, 1], b, s3.at[2, n], s3.at[3, n], at.x_peer),
        ]

    def keep3(it):
        s = slot_of(fin, it)
        return [
            pltpu.make_async_copy(fin.at[s, 0], sums_out.at[it, piece_a()], s_fin.at[0, s]),
            pltpu.make_async_copy(fin.at[s, 1], sums_out.at[it, piece_b()], s_fin.at[1, s]),
        ]

    def stage4(it):
        n = lax.rem(it, s4.shape[1])
        a = sums_out.at[it, pl.ds(at.core * 8 + quarter(at.x, 0), 2)]
        b = sums_out.at[it, pl.ds(at.core * 8 + quarter(at.y, 1), 2)]
        return [
            rdma(a, a, s4.at[0, n], s4.at[1, n], at.x_peer),
            rdma(b, b, s4.at[2, n], s4.at[3, n], at.y_peer),
        ]

    def stage5(it):
        n = lax.rem(it, s5.shape[1])
        part = sums_out.at[it, pl.ds(at.core * 8, 8)]
        return [rdma(part, part, s5.at[0, n], s5.at[1, n], at.core_peer)]

    def product(it, half):
        half(1 - at.core, away, slot_of(away, it))
        start(stage0(it))
        half(at.core, acc, slot_of(acc, it))

    def tall(left, right):
        def half(which, dst, slot):
            tile = dot(left[at_block(which, 8 * BLOCK), :], right(), 1, 0, BF16)
            for p in range(8):
                dst[slot, p] = tile[p * BLOCK : (p + 1) * BLOCK]

        return half

    def gate_right(f):
        lanes = at_block(f, BLOCK)
        return jnp.concatenate([a1_v[:, lanes], a2_v[:, lanes]], axis=1)

    def shard(origin):
        return at_block(origin, own_rows)

    def n_copy(kind, origin, to):
        rows = nrm.at[shard(origin)]
        return rdma(rows, rows, n_send.at[kind], n_recv.at[origin], (at.me, to))

    def y_copy(kind, origin, to, c):
        part = dy_v.at[shard(origin), at_block(c, dy_wide)]
        return rdma(part, part, y_send.at[kind, c], y_recv.at[origin, c], (at.me, to))

    def route(make, what):
        def when(condition, copy):
            @pl.when(condition)
            def _():
                getattr(copy, what)()

        def first():
            when(at.has_above, make(0, at.z, at.above))
            when(at.has_below, make(1, at.z, at.below))
            when(at.end, make(2, at.z, at.far))

        def passed(up):
            if up:
                when(at.middle, make(3, at.below, at.above))
            else:
                when(at.middle, make(4, at.above, at.below))

        return first, passed

    def n_arrived(origin):
        n_copy(0, origin, at.z_of[1]).wait_recv()

    def y_arrived(origin, c):
        y_copy(0, origin, at.z_of[1], c).wait_recv()

    def norm_rows(rows):
        tok = tok_v[rows, :].astype(F32)
        centered = tok - jnp.mean(tok, axis=1, keepdims=True)
        inv_std = lax.rsqrt(jnp.mean(centered * centered, axis=1, keepdims=True) + EPS)
        return centered * inv_std, inv_std

    def normalize():
        @pl.loop(0, own_rows // STEP)
        def _(r):
            xhat, _ = norm_rows(at_block(r, STEP))
            to = pl.ds(pl.multiple_of(at.z * own_rows + r * STEP, STEP), STEP)
            nrm[to, :] = (xhat * gain_ref[0:1, :] + shift_ref[0:1, :]).astype(BF16)

    def raw_copy(wint, f):
        s = lax.rem(f, 2)
        return pltpu.make_async_copy(
            w_gate_up.at[:, :, at_block(f, BLOCK)], wint.at[s], s_raw.at[s]
        )

    def back_copies(f):
        s = lax.rem(f, 2)
        return [
            pltpu.make_async_copy(
                wf.at[s, :, pl.ds(n * BLOCK, BLOCK)], w.at[:, at_block(f, BLOCK)], s_back.at[n, s]
            )
            for n, w in enumerate((w_gate, w_up))
        ]

    def pair_copies(f, s):
        return [
            pltpu.make_async_copy(
                w.at[:, at_block(f, BLOCK)], wf.at[s, :, pl.ds(n * BLOCK, BLOCK)], s_wf.at[n, s]
            )
            for n, w in enumerate((w_gate, w_up))
        ]

    def qkv_copies(m, s):
        return [
            pltpu.make_async_copy(
                w_qkv.at[lax.div(m, per), :, at_block(lax.rem(m, per), WIDE)], wf.at[s], s_wf.at[0, s]
            )
        ]

    def rows_of(rows):
        parts = [nrm[r, :] for r in rows]
        return parts[0] if len(parts) == 1 else jnp.concatenate(parts, axis=0)

    def hidden_tile(f, s, rows):
        product_of = dot(rows_of(rows), wf[s], 1, 0)
        lanes = at_block(f, BLOCK)
        for n, r in enumerate(rows):
            part = product_of[n * own_rows : (n + 1) * own_rows]
            g, u = part[:, :BLOCK], part[:, BLOCK:]
            sig = jax.nn.sigmoid(g)
            silu = g * sig
            h = (silu * u).astype(BF16)
            hq_v[r, lanes] = h
            hat_v[lanes, r] = jnp.transpose(h)
            a1_v[r, lanes] = (u * (sig + silu * (1.0 - sig))).astype(BF16)
            a2_v[r, lanes] = silu.astype(BF16)

    def qkv_tile(m, s, rows):
        t = lax.div(m, per)
        product_of = dot(rows_of(rows), wf[s], 1, 0) + bias_ref[m]
        for k, r in enumerate(rows):
            for n in range(WIDE // LANES):
                x = product_of[k * own_rows : (k + 1) * own_rows, n * LANES : (n + 1) * LANES]
                turned = turn(x, (tab_v[0, r, :], tab_v[1, r, :], tab_v[2, r, :]), 1.0)
                lanes = pl.ds(pl.multiple_of(lax.rem(m, per) * WIDE + n * LANES, LANES), LANES)
                qkv_v[t, r, lanes] = jnp.where(t < 2, turned, x).astype(BF16)

    def turn_over(origin):
        rows = shard(origin)
        for n in range(columns):
            cols = pl.ds(n * WIDE, WIDE)
            nt_v[cols, rows] = jnp.transpose(nrm[rows, cols])

    def own_pass(wint):
        r = lax.broadcasted_iota(jnp.int32, (WIDE, WIDE), 0)
        c = lax.broadcasted_iota(jnp.int32, (WIDE, WIDE), 1)
        source = jnp.where(r < BLOCK, 2 * r, 2 * (r - BLOCK) + 1)
        parting = (source == c).astype(F32).astype(BF16)
        rows = shard(at.z)

        @pl.loop(0, n_g)
        def _(f):
            s = lax.rem(f, 2)

            @pl.when(f + 1 < n_g)
            def _():
                raw_copy(wint, f + 1).start()

            raw_copy(wint, f).wait()

            @pl.when(f >= 2)
            def _():
                wait(back_copies(f - 2))

            for n in range(model // BLOCK):
                part = pl.ds(n * BLOCK, BLOCK)
                raw = wint[s, part].reshape(WIDE, BLOCK)
                parted = dot(parting, raw, 1, 0, BF16)
                wf[s, part, :BLOCK] = parted[:BLOCK]
                wf[s, part, BLOCK:] = parted[BLOCK:]
            start(back_copies(f))
            hidden_tile(f, s, [rows])

        for f in (n_g - 2, n_g - 1):
            wait(back_copies(f))
        start(qkv_copies(0, n_g % 2))

        @pl.loop(0, n_q)
        def _(m):
            n = n_g + m
            s = lax.rem(n, 2)

            @pl.when(m + 1 < n_q)
            def _():
                start(qkv_copies(m + 1, 1 - s))

            @pl.when(m + 1 == n_q)
            def _():
                start(pair_copies(0, 1 - s))

            wait(qkv_copies(m, s))
            qkv_tile(m, s, [rows])

    def later_pass(k, origins):
        rows = [shard(origin) for origin in origins]
        base = k * fill

        @pl.loop(0, n_g)
        def _(f):
            s = lax.rem(base + f, 2)

            @pl.when(f + 1 < n_g)
            def _():
                start(pair_copies(f + 1, 1 - s))

            @pl.when(f + 1 == n_g)
            def _():
                start(qkv_copies(0, 1 - s))

            wait(pair_copies(f, s))
            hidden_tile(f, s, rows)

        @pl.loop(0, n_q)
        def _(m):
            s = lax.rem(base + n_g + m, 2)

            @pl.when(m + 1 < n_q)
            def _():
                start(qkv_copies(m + 1, 1 - s))

            if k < 2:

                @pl.when(m + 1 == n_q)
                def _():
                    start(pair_copies(0, 1 - s))

            wait(qkv_copies(m, s))
            qkv_tile(m, s, rows)

        for origin in origins:
            turn_over(origin)

    def z_copies(n, which):
        s = slot_of(zsend, n)
        c = at_block(lax.rem(n, columns), WIDE)
        copies = []
        for d in range(1, n_z):
            if which == 0:
                dst = nrm.at[pl.ds((d - 1) * own_rows, own_rows), c]
            else:
                dst = zin.at[d - 1, :, c]
            src = zsend.at[s, shard(at.z_of[d])]
            sems = z_sems.at[0, d - 1, n], z_sems.at[1, d - 1, n]
            copies.append(rdma(src, dst, *sems, at.z_peers[d]))
        return copies

    def z_send(n, which, value):
        s = slot_of(zsend, n)

        @pl.when(n >= zsend.shape[0])
        def _():
            for copy in z_copies(n - zsend.shape[0], 1):
                copy.wait_send()

        zsend[s] = value.astype(BF16)
        start(z_copies(n, which))

    def branch_load(c):
        s = lax.rem(c, 2)
        cols = at_block(c, WIDE)
        return [
            pltpu.make_async_copy(
                w_down.at[:, cols], wf.at[s, pl.ds(0, local_ff)], s_wf.at[0, s]
            ),
            pltpu.make_async_copy(
                w_out.at[:, cols], wf.at[s, pl.ds(local_ff, width)], s_wf.at[1, s]
            ),
        ]

    def branch_job(c):
        s = lax.rem(c, 2)
        wait(branch_load(c))

        @pl.when(c + 1 < columns)
        def _():
            start(branch_load(c + 1))

        value = dot(hq_v[...], wf[s, :local_ff], 1, 0) + dot(
            attn_v[...], wf[s, local_ff : local_ff + width], 1, 0
        )
        z_send(c, 0, value)
        mine = zsend[slot_of(zsend, c), shard(at.z), :]
        nrm[pl.ds((n_z - 1) * own_rows, own_rows), at_block(c, WIDE)] = mine

    def layer_out_copy():
        rows = pl.ds((n_z - 1) * own_rows, own_rows)
        return pltpu.make_async_copy(nrm.at[rows], layer_out, s_tok.at[0])

    def layer_out_job():
        @pl.loop(0, columns)
        def _(c):
            for copy in z_copies(c, 0):
                copy.wait_recv()

        @pl.loop(0, own_rows // STEP)
        def _(r):
            value = tok_v[at_block(r, STEP), :].astype(F32)
            for n in range(n_z):
                rows = pl.ds(pl.multiple_of(n * own_rows + r * STEP, STEP), STEP)
                value = value + nrm[rows, :].astype(F32)
            nrm[rows, :] = value.astype(BF16)

        layer_out_copy().start()

    def hidden_load(g, wd):
        def one(n, what):
            b = 2 * g + n
            if b < blocks_h + blocks_o:
                w, row = (w_down, b) if b < blocks_h else (w_out, b - blocks_h)
                src = w.at[pl.ds(row * BLOCK, BLOCK)]
                dst = wd.at[pl.ds(n * BLOCK, BLOCK)]
                getattr(pltpu.make_async_copy(src, dst, s_wd.at[n]), what)()

        return one

    def hidden_job(g, wd):
        for n in range(2):
            hidden_load(g, wd)(n, "wait")
        blocks = min(2, blocks_h + blocks_o - 2 * g)
        dh = dot(dy_v[...], wd[: blocks * BLOCK], 1, 1)
        for n in range(blocks):
            b = 2 * g + n
            part = dh[:, n * BLOCK : (n + 1) * BLOCK]
            if b < blocks_h:
                lanes = pl.ds(b * BLOCK, BLOCK)
                a1_v[:, lanes] = (part * a1_v[:, lanes].astype(F32)).astype(BF16)
                a2_v[:, lanes] = (part * a2_v[:, lanes].astype(F32)).astype(BF16)
            else:
                do_v[:, pl.ds((b - blocks_h) * BLOCK, BLOCK)] = part.astype(BF16)

    def normed_load(c, wg, wu, wq):
        rows = at_block(c, WIDE)
        return [
            pltpu.make_async_copy(w_gate.at[rows], wg, s_wn.at[0]),
            pltpu.make_async_copy(w_up.at[rows], wu, s_wn.at[1]),
            pltpu.make_async_copy(w_qkv.at[:, rows], wq, s_wn.at[2]),
        ]

    def normed_job(c, wg, wu, wq):
        wait(normed_load(c, wg, wu, wq))
        part = dot(a1_v[...], wg[...], 1, 1) + dot(a2_v[...], wu[...], 1, 1)
        for t in range(3):
            part = part + dot(dqkv_v[:, t * width : (t + 1) * width], wq[t], 1, 1)
        z_send(columns + c, 1, part)

        @pl.when(c + 1 < columns)
        def _():
            start(normed_load(c + 1, wg, wu, wq))

        own[:, at_block(c, WIDE)] = zsend[slot_of(zsend, columns + c), shard(at.z), :]

    def tokens_copy():
        return pltpu.make_async_copy(tok_v, grad_tokens_out, s_tok.at[1])

    def norm_job():
        @pl.loop(columns, 2 * columns)
        def _(n):
            @pl.when(n >= 2 * columns - zsend.shape[0])
            def _():
                for copy in z_copies(n, 1):
                    copy.wait_send()

            for copy in z_copies(n, 1):
                copy.wait_recv()

        @pl.loop(0, own_rows // STEP)
        def _(r):
            rows = at_block(r, STEP)
            d = own[rows, :].astype(F32)
            for n in range(n_z - 1):
                d = d + zin[n, rows, :].astype(F32)
            xhat, inv_std = norm_rows(rows)
            scaled = d * gain_ref[0:1, :]
            here = pl.ds(pl.multiple_of(at.z * own_rows + r * STEP, STEP), STEP)
            out = dy_v[here, :].astype(F32) + inv_std * (
                scaled
                - jnp.mean(scaled, axis=1, keepdims=True)
                - xhat * jnp.mean(scaled * xhat, axis=1, keepdims=True)
            )
            small[0:1, :] += jnp.sum(d * xhat, axis=0, keepdims=True)
            small[1:2, :] += jnp.sum(d, axis=0, keepdims=True)
            tok_v[rows, :] = out.astype(BF16)

        tokens_copy().start()

    share = model // n_z

    def share_copies():
        return [
            rdma(
                small.at[:, at_block(at.z_of[d], share)],
                share_in.at[d - 1],
                share_sems.at[0, d - 1],
                share_sems.at[1, d - 1],
                at.z_peers[d],
            )
            for d in range(1, n_z)
        ]

    def spread_copies():
        return [
            rdma(
                small_in.at[at.me],
                small_in.at[at.me],
                small_sems.at[0, n],
                small_sems.at[1, at.me],
                peer,
            )
            for n, peer in enumerate(at.dp_peers)
        ]

    def small_spread():
        wait(share_copies())
        mine = small[0:2, at_block(at.z, share)]
        for n in range(n_z - 1):
            mine = mine + share_in[n, 0:2, :]
        small_in[at.me] = small[:, 0:share]
        small_in[at.me, 0:2, :] = mine
        start(spread_copies())

    def small_end():
        for copy in spread_copies():
            copy.wait_send()
        for n, source in enumerate(at.dp_others):
            rdma(
                small_in.at[source], small_in.at[source], small_sems.at[0, n],
                small_sems.at[1, source], at.dp_peers[n],
            ).wait_recv()
        value = small_in[0]
        for n in range(1, small_in.shape[0]):
            value = value + small_in[n]
        small_out[...] = value

    loads = [
        pltpu.make_async_copy(tokens, tok_v, load.at[0]),
        pltpu.make_async_copy(grad_out, dy_v.at[shard(at.z)], load.at[1]),
        pltpu.make_async_copy(tables, tab_v, load.at[2]),
    ]
    barrier = pltpu.get_barrier_semaphore()
    peers = at.dp_peers + at.z_peers[1:]
    for peer in peers:
        pl.semaphore_signal(barrier, inc=1, device_id=peer, device_id_type=MESH)
    start(loads)
    small[...] = jnp.zeros_like(small)
    hat_v[pl.ds(local_ff + width, model - local_ff - width), :] = jnp.zeros(
        (model - local_ff - width, seq_len), BF16
    )
    loads[0].wait()
    normalize()
    pl.semaphore_wait(barrier, len(peers))

    def forward(wint):
        raw_copy(wint, 0).start()
        route(n_copy, "start")[0]()
        loads[2].wait()
        own_pass(wint)
        turn_over(at.z)

    pl.run_scoped(forward, pltpu.VMEM((2, model, 2, BLOCK), BF16))
    o1, o2, o3 = at.order[1:]
    n_arrived(o1)
    onward = route(n_copy, "start")[1]

    @pl.when(at.middle)
    def _():
        n_arrived(o2)
        onward(True)
        onward(False)
        later_pass(1, [o1, o2])
        n_arrived(o3)

    @pl.when(at.end)
    def _():
        later_pass(1, [o1])
        n_arrived(o2)
        n_arrived(o3)

    def dy_route(c, what):
        return route(lambda *a: y_copy(*a, c), what)

    def send_dy(c):
        dy_route(c, "start")[0]()

    def pass_dy_on(c):
        @pl.when(at.middle)
        def _():
            y_arrived(o1, c)
            y_arrived(o2, c)

        onward = dy_route(c, "start")[1]
        onward(True)
        onward(False)

    def rest_of_dy(c):
        y_arrived(o3, c)

        @pl.when(at.end)
        def _():
            y_arrived(o1, c)
            y_arrived(o2, c)

    loads[1].wait()
    send_dy(0)

    @pl.when(at.middle)
    def _():
        later_pass(2, [o3])

    @pl.when(at.end)
    def _():
        later_pass(2, [o2, o3])

    start(branch_load(0))
    pass_dy_on(0)
    send_dy(1)

    first, passed = route(n_copy, "wait_send")
    first()
    passed(True)
    passed(False)
    for peer in at.z_peers[1:]:
        pl.semaphore_signal(ready, inc=1, device_id=peer, device_id_type=MESH)

    @pl.loop(0, units)
    def _(u):
        attend_unit(u, qkv_v, attn_v, hat_v, lse_v, local_ff)

    pass_dy_on(1)
    send_dy(2)

    def live(it):
        return both(it >= 0, it < total)

    branch_at = 5
    hidden_jobs = -(-(blocks_h + blocks_o) // 2)
    split = blocks_h // 2
    hidden_plan = [0, *range(split, hidden_jobs), *range(1, split)]
    hidden_at = n_d - 2
    hidden_tick = [hidden_at, hidden_at, hidden_at + 1, hidden_at + 1]
    hidden_tick += [hidden_at + 2 + n for n in range(hidden_jobs - 4)]
    back_at = hidden_at + 2
    normed_at = max(back_at + units, hidden_at + 2 + hidden_jobs - 4)
    out_at = total - 1
    norm_at = total + 3

    def ticks(wg, wu, wq, wd, dq, dk, dv):
        for n in range(2):
            hidden_load(hidden_plan[0], wd)(n, "start")
        start(normed_load(0, wg, wu, wq))

        @pl.loop(0, total + 6 * LAG)
        def _(tick):
            one = tick - LAG

            @pl.when(live(one))
            def _():
                wait(stage0(one))
                sa, s = slot_of(acc, one), slot_of(rcv0, one)

                @pl.loop(0, 8)
                def _(p):
                    acc[sa, p] = (acc[sa, p].astype(F32) + rcv0[s, p].astype(F32)).astype(BF16)

                start(stage1(one))

            two = tick - 2 * LAG

            @pl.when(live(two))
            def _():
                wait(stage1(two))
                sa, s = slot_of(acc, two), slot_of(rcv1, two)
                for n, bit in ((0, at.x), (1, at.y)):
                    for m in range(2):
                        p = quarter(bit, n) + m
                        acc[sa, p] = (
                            acc[sa, p].astype(F32) + rcv1[s, n, m].astype(F32)
                        ).astype(BF16)
                start(stage2(two))

            three = tick - 3 * LAG

            @pl.when(live(three))
            def _():
                wait(stage2(three))
                sa, s, d = slot_of(acc, three), slot_of(rcv2, three), slot_of(fin, three)
                for n, p in ((0, quarter(at.x, 0) + at.y), (1, quarter(at.y, 1) + at.x)):
                    fin[d, n] = (acc[sa, p].astype(F32) + rcv2[s, n].astype(F32)).astype(BF16)
                start(stage3(three))
                start(keep3(three))

            four = tick - 4 * LAG

            @pl.when(live(four))
            def _():
                wait(keep3(four))
                wait(stage3(four))
                start(stage4(four))

            five = tick - 5 * LAG

            @pl.when(live(five))
            def _():
                wait(stage4(five))
                start(stage5(five))

            six = tick - 6 * LAG

            @pl.when(live(six))
            def _():
                wait(stage5(six))

            for c in range(dy_chunks):

                @pl.when(tick == 2 * c)
                def _(c=c):
                    if c >= 1 and c + 1 < dy_chunks:
                        pass_dy_on(c + 1)
                        if c + 2 < dy_chunks:
                            send_dy(c + 2)
                    rest_of_dy(c)

            @pl.when(tick < n_d)
            def _():
                product(tick, tall(hat_v, lambda: dy_v[:, at_block(tick, WIDE)]))

            @pl.when(both(tick >= n_d, tick < n_d + n_g))
            def _():
                product(tick, tall(nt_v, lambda: gate_right(tick - n_d)))

            @pl.when(both(tick >= n_d + n_g, tick < total))
            def _():
                product(
                    tick, tall(nt_v, lambda: dqkv_v[:, at_block(tick - n_d - n_g, WIDE)])
                )

            @pl.when(tick == branch_at)
            def _():
                pl.semaphore_wait(ready, n_z - 1)

            @pl.when(both(tick >= branch_at, tick < branch_at + columns))
            def _():
                branch_job(tick - branch_at)

            for n in range(hidden_jobs):

                @pl.when(tick == hidden_tick[n])
                def _(n=n):
                    hidden_job(hidden_plan[n], wd)
                    if n + 1 < hidden_jobs:
                        for m in range(2):
                            hidden_load(hidden_plan[n + 1], wd)(m, "start")

            @pl.when(both(tick >= back_at, tick < back_at + units))
            def _():
                attend_back_unit(
                    tick - back_at, qkv_v, do_v, lse_v, tab_v, dqkv_v, small, dq, dk, dv
                )

            @pl.when(both(tick >= normed_at, tick < normed_at + columns))
            def _():
                normed_job(tick - normed_at, wg, wu, wq)

            @pl.when(tick == out_at)
            def _():
                layer_out_job()
                for c in range(dy_chunks):
                    first, passed = dy_route(c, "wait_send")
                    first()
                    passed(True)
                    passed(False)

            @pl.when(tick == norm_at)
            def _():
                norm_job()
                start(share_copies())

            @pl.when(tick == norm_at + 2)
            def _():
                small_spread()

            @pl.when(tick == norm_at + 5)
            def _():
                small_end()
                tokens_copy().wait()
                layer_out_copy().wait()

    pl.run_scoped(
        ticks,
        pltpu.VMEM((WIDE, local_ff), BF16),
        pltpu.VMEM((WIDE, local_ff), BF16),
        pltpu.VMEM((3, WIDE, width), BF16),
        pltpu.VMEM((2 * BLOCK, model), BF16),
        *[pltpu.VMEM((seq_len, LANES), F32)] * 3,
    )


def run_layer(
    tokens, grad_out, tables, w_gate_up, w_qkv, w_down, w_out, gain, shift, bias, n_dp, n_z
):
    own, model = tokens.shape
    seq_len = own * n_z
    local_ff, width = w_down.shape[0], w_out.shape[0]
    columns = model // WIDE
    total = columns + local_ff // BLOCK + 3 * width // WIDE
    bf = lambda *shape: pltpu.VMEM(shape, BF16)
    fl = lambda *shape: pltpu.VMEM(shape, F32)
    sems = lambda *shape: pltpu.SemaphoreType.DMA(shape)
    slots = 2 * LAG + 2
    dy_chunks = 4
    hbm = pl.BlockSpec(memory_space=pl.ANY)
    vmem = pl.BlockSpec(memory_space=pltpu.VMEM)
    return pl.pallas_call(
        functools.partial(layer_kernel, n_dp, n_z),
        in_specs=[hbm] * 7 + [vmem] * 3,
        out_specs=[hbm, hbm, hbm, vmem, hbm, hbm],
        out_shape=[
            jax.ShapeDtypeStruct((total, PIECES, BLOCK, WIDE), BF16),
            jax.ShapeDtypeStruct((own, model), BF16),
            jax.ShapeDtypeStruct((own, model), BF16),
            jax.ShapeDtypeStruct((8, model // n_z), F32),
            jax.ShapeDtypeStruct((model, local_ff), BF16),
            jax.ShapeDtypeStruct((model, local_ff), BF16),
        ],
        scratch_shapes=[
            bf(model, seq_len), bf(model, seq_len), bf(seq_len, model),
            bf(seq_len, model), bf(seq_len, local_ff), bf(seq_len, local_ff),
            bf(3, seq_len, width), bf(seq_len, width), bf(seq_len, local_ff), bf(seq_len, 3 * width),
            bf(seq_len, width), fl(width // HD, 1, seq_len), fl(3, seq_len, LANES), bf(own, model),
            bf(2, model, WIDE), bf(3, seq_len, WIDE), bf(n_z - 1, own, model), bf(own, model),
            fl(8, model), fl(n_dp, 8, model // n_z), fl(n_z - 1, 8, model // n_z),
            bf(LAG + 1, 8, BLOCK, WIDE), bf(3 * LAG + 1, 8, BLOCK, WIDE),
            bf(slots, 8, BLOCK, WIDE), bf(slots, 2, 2, BLOCK, WIDE), bf(slots, 2, BLOCK, WIDE),
            bf(LAG + 1, 2, BLOCK, WIDE),
            sems(3), sems(2), sems(2, 2), sems(2, 2), sems(2), sems(3), sems(2),
            pltpu.SemaphoreType.REGULAR,
            sems(5), sems(n_z), sems(5, dy_chunks), sems(n_z, dy_chunks),
            sems(2, n_z - 1, 2 * columns), sems(2, n_dp), sems(2, n_z - 1),
            sems(2, slots), sems(4, slots), sems(4, slots),
            sems(4, slots), sems(4, slots), sems(2, slots), sems(2, LAG + 1),
        ],
        compiler_params=pltpu.CompilerParams(
            collective_id=0, has_side_effects=True, vmem_limit_bytes=67043328
        ),
        name="layer",
    )(tokens, grad_out, tables, w_gate_up, w_qkv, w_down, w_out, gain, shift, bias)


def unpack_kernel(n_d, n_g, item_ref, down, out, gate_up, qkv):
    i = pl.program_id(0)
    n_down = down.shape[0] // BLOCK

    def rows(p):
        return pl.ds(p * BLOCK, BLOCK)

    @pl.when(i < n_d)
    def _():
        for p in range(n_down):
            down[rows(p), :] = item_ref[0, p].astype(F32)
        for p in range(out.shape[0] // BLOCK):
            out[rows(p), :] = item_ref[0, n_down + p].astype(F32)

    @pl.when(both(i >= n_d, i < n_d + n_g))
    def _():
        flat = gate_up.reshape(2 * gate_up.shape[0], BLOCK)
        for p in range(PIECES):
            value = item_ref[0, p].astype(F32)
            for n in range(2):
                flat[pl.ds(2 * p * BLOCK + n, BLOCK, stride=2), :] = value[
                    :, n * BLOCK : (n + 1) * BLOCK
                ]

    @pl.when(i >= n_d + n_g)
    def _():
        for p in range(PIECES):
            qkv[0, rows(p), :] = item_ref[0, p].astype(F32)


def unpack(items, local_ff, width, model):
    n_d, n_g, n_q = model // WIDE, local_ff // BLOCK, 3 * width // WIDE
    per = n_q // 3

    def of_d(i):
        return (0, jnp.minimum(i, n_d - 1))

    def of_q(i):
        q = jnp.maximum(i - n_d - n_g, 0)
        return (lax.div(q, per), 0, lax.rem(q, per))

    down, out, gate_up, qkv = pl.pallas_call(
        functools.partial(unpack_kernel, n_d, n_g),
        grid=(n_d + n_g + n_q,),
        in_specs=[pl.BlockSpec((1, PIECES, BLOCK, WIDE), lambda i: (i, 0, 0, 0))],
        out_specs=[
            pl.BlockSpec((local_ff, WIDE), of_d),
            pl.BlockSpec((width, WIDE), of_d),
            pl.BlockSpec((model, 2, BLOCK), lambda i: (0, 0, jnp.clip(i - n_d, 0, n_g - 1))),
            pl.BlockSpec((1, model, WIDE), of_q),
        ],
        out_shape=[
            jax.ShapeDtypeStruct((local_ff, model), F32),
            jax.ShapeDtypeStruct((width, model), F32),
            jax.ShapeDtypeStruct((model, 2, local_ff), F32),
            jax.ShapeDtypeStruct((3, model, width), F32),
        ],
        name="unpack",
    )(items)
    return down, out, gate_up, qkv.transpose(1, 0, 2)


def fast_path(n_dp, n_mp, rows, model_width, local_width, local_ff):
    blocks_h, blocks_o = local_ff // BLOCK, local_width // BLOCK
    return (
        n_dp == 8
        and n_mp == 4
        and rows == QB
        and model_width == PIECES * BLOCK
        and local_width == model_width // n_mp
        and local_ff % BLOCK == 0
        and blocks_h % 2 == 1
        and blocks_h + blocks_o <= PIECES
        and blocks_h * (model_width // WIDE) % blocks_o == 0
    )


def fused_layer(
    n_dp,
    n_mp,
    tables,
    tokens,
    norm_gain,
    layernorm_bias,
    qkv_weight,
    qkv_bias,
    out_weight,
    gate_up_weight,
    down_weight,
    grad_out,
):
    model_width = tokens.shape[1]
    local_width, local_ff = qkv_weight.shape[2], gate_up_weight.shape[2]
    items, layer_out, grad_tokens, small, _, _ = run_layer(
        tokens,
        grad_out,
        tables,
        gate_up_weight,
        qkv_weight.transpose(1, 0, 2),
        down_weight,
        out_weight,
        norm_gain.astype(F32)[None],
        layernorm_bias.astype(F32)[None],
        qkv_bias.astype(F32).reshape(-1, 1, WIDE),
        n_dp,
        n_mp,
    )
    grad_down_w, grad_out_w, grad_gate_up_w, grad_qkv_w = unpack(
        items, local_ff, local_width, model_width
    )
    return (
        layer_out,
        grad_tokens,
        small[0],
        small[1],
        grad_qkv_w,
        small[2:5, :local_width],
        grad_out_w,
        grad_gate_up_w,
        grad_down_w,
    )


def on_device(
    n_dp,
    n_mp,
    tokens,
    norm_gain,
    layernorm_bias,
    qkv_weight,
    qkv_bias,
    out_weight,
    gate_up_weight,
    down_weight,
    grad_out,
):
    rows, model_width = tokens.shape
    local_width = qkv_weight.shape[2]
    seq_len = rows * n_mp
    tables = rotary_tables(seq_len)
    if fast_path(n_dp, n_mp, rows, model_width, local_width, gate_up_weight.shape[2]):
        return fused_layer(
            n_dp, n_mp, tables, tokens, norm_gain, layernorm_bias, qkv_weight, qkv_bias, out_weight,
            gate_up_weight, down_weight, grad_out,
        )
    cube = Cube("dp", n_dp)
    gain = norm_gain.astype(F32)
    token_f32 = tokens.astype(F32)
    row_mean = jnp.mean(token_f32, axis=1, keepdims=True)
    centered = token_f32 - row_mean
    inv_std = lax.rsqrt(jnp.mean(centered * centered, axis=1, keepdims=True) + EPS)
    xhat = centered * inv_std
    normed_own = (xhat * gain + layernorm_bias.astype(F32)).astype(BF16)
    normed = lax.all_gather(normed_own, "mp", axis=0, tiled=True)
    dy = lax.all_gather(grad_out, "mp", axis=0, tiled=True)

    w_qkv = [qkv_weight[:, t, :] for t in range(3)]
    w_gate, w_up = gate_up_weight[:, 0, :], gate_up_weight[:, 1, :]

    gate = dot(normed, w_gate, 1, 0)
    up = dot(normed, w_up, 1, 0)
    sig = jax.nn.sigmoid(gate)
    hidden = (gate * sig * up).astype(BF16)
    qkv = jnp.concatenate([dot(normed, w, 1, 0) for w in w_qkv], axis=1)
    q, k, v, attended, lse = attention_forward(qkv, qkv_bias.astype(F32), tables)
    branch = (dot(attended, out_weight, 1, 0) + dot(hidden, down_weight, 1, 0)).astype(BF16)
    share = lax.psum_scatter(branch, "mp", scatter_dimension=0, tiled=True)
    layer_out = (token_f32 + share.astype(F32)).astype(BF16)

    share_width = model_width // n_mp
    d_hidden = dot(dy, down_weight, 1, 1)
    silu = gate * sig
    d_gate = (d_hidden * up * (sig + silu * (1.0 - sig))).astype(BF16)
    d_up = (d_hidden * silu).astype(BF16)
    d_attended = dot(dy, out_weight, 1, 1, BF16)
    dq, dk, dv, sums = attention_backward(q, k, v, d_attended, lse, tables)
    d_normed = (
        dot(d_gate, w_gate, 1, 1)
        + dot(d_up, w_up, 1, 1)
        + dot(dq, w_qkv[0], 1, 1)
        + dot(dk, w_qkv[1], 1, 1)
        + dot(dv, w_qkv[2], 1, 1)
    ).astype(BF16)
    d_own = lax.psum_scatter(d_normed, "mp", scatter_dimension=0, tiled=True).astype(F32)
    d_qkv = jnp.concatenate([dq, dk, dv], axis=1)
    grad_down_w = cube.contract(hidden, dy)
    grad_out_w = cube.contract(attended, dy)
    grad_gate_up_w = jnp.stack(
        [cube.contract(normed, d_gate), cube.contract(normed, d_up)], axis=1
    )
    grad_qkv_w = cube.contract(normed, d_qkv).reshape(model_width, 3, local_width)

    scaled = d_own * gain
    grad_tokens = grad_out.astype(F32) + inv_std * (
        scaled
        - jnp.mean(scaled, axis=1, keepdims=True)
        - xhat * jnp.mean(scaled * xhat, axis=1, keepdims=True)
    )
    terms = jnp.stack([jnp.sum(d_own * xhat, axis=0), jnp.sum(d_own, axis=0)])
    bias_sum = cube.sum_all(sums)
    grad_bias = bias_sum.swapaxes(0, 1).reshape(3, local_width)
    terms = Cube("mp", n_mp).sum_all(cube.sum_all(terms))
    terms = lax.dynamic_slice_in_dim(
        terms, lax.axis_index("mp") * share_width, share_width, 1
    )
    return (
        layer_out,
        grad_tokens.astype(BF16),
        terms[0],
        terms[1],
        grad_qkv_w,
        grad_bias,
        grad_out_w,
        grad_gate_up_w,
        grad_down_w,
    )


def solution(mesh):
    return jax.shard_map(
        functools.partial(on_device, mesh.shape["dp"], mesh.shape["mp"]),
        mesh=mesh,
        in_specs=(
            P(("dp", "mp"), None),
            P(),
            P(),
            P(None, None, "mp"),
            P(None, "mp"),
            P("mp", None),
            P(None, None, "mp"),
            P("mp", None),
            P(("dp", "mp"), None),
        ),
        out_specs=(
            P(("dp", "mp"), None),
            P(("dp", "mp"), None),
            P("mp"),
            P("mp"),
            P(None, None, "mp"),
            P(None, "mp"),
            P("mp", None),
            P(None, None, "mp"),
            P("mp", None),
        ),
        check_vma=False,
    )
```

```python
import functools
import math

import jax
import jax.numpy as jnp
from jax import lax
from jax.experimental import pallas as pl
from jax.experimental.pallas import tpu as pltpu
from jax.sharding import PartitionSpec as P

HD = 64
ROT = 16
EPS = 1e-05
LANES = 128
QB = 256


F32 = jnp.float32
BF16 = jnp.bfloat16


def dot(a, b, ca, cb, out=F32):
    return lax.dot_general(
        a, b, (((ca,), (cb,)), ((), ())), preferred_element_type=F32
    ).astype(out)


def rotary_tables(seq_len):
    half = ROT // 2
    shape = (seq_len, LANES)
    dim = lax.rem(lax.broadcasted_iota(jnp.int32, shape, 1), HD)
    positions = lax.broadcasted_iota(jnp.int32, shape, 0).astype(F32)
    freqs = 1.0 / 10000.0 ** (lax.rem(dim, half).astype(F32) * 2.0 / ROT)
    phase = positions * freqs
    cosine, sine = jnp.cos(phase), jnp.sin(phase)
    return jnp.stack(
        [
            jnp.where(dim < ROT, cosine, 1.0),
            jnp.where(dim < half, -sine, jnp.where(dim < ROT, sine, 0.0)),
        ]
    )


def turn(x, tables, sign):
    half = ROT // 2
    dim = lax.rem(lax.broadcasted_iota(jnp.int32, x.shape, 1), HD)
    partner = jnp.where(dim < half, pltpu.roll(x, LANES - half, 1), pltpu.roll(x, half, 1))
    return x * tables[0] + sign * (partner * tables[1])


def lane_mask(rows, j):
    lane = lax.broadcasted_iota(jnp.int32, (rows, LANES), 1)
    return (lane // HD) == j


def forward_kernel(
    q_in, k_in, v_in, bias_ref, tab_ref, q_out, k_out, v_out, o_ref, lse_ref
):
    seq_len = q_in.shape[0]
    j = pl.program_id(1)

    @pl.when(j == 0)
    def _():
        tables = (tab_ref[0], tab_ref[1])
        q_out[...] = turn(q_in[...] + bias_ref[0, 0:1], tables, 1.0).astype(BF16)
        k_out[...] = turn(k_in[...] + bias_ref[0, 1:2], tables, 1.0).astype(BF16)
        v_out[...] = (v_in[...] + bias_ref[0, 2:3]).astype(BF16)

    mask = lane_mask(QB, j)
    causal = lax.broadcasted_iota(jnp.int32, (QB, QB), 0) <= lax.broadcasted_iota(
        jnp.int32, (QB, QB), 1
    )
    for i in range(seq_len // QB):
        rows = pl.ds(i * QB, QB)
        span = (i + 1) * QB
        q = q_out[rows, :] * 0.125
        q = jnp.where(mask, q, jnp.zeros_like(q))
        parts = []
        if i:
            parts.append(dot(k_out[pl.ds(0, i * QB), :], q, 1, 1))
        diag = dot(k_out[rows, :], q, 1, 1)
        parts.append(jnp.where(causal, diag, -1e30))
        top = functools.reduce(
            jnp.maximum, [jnp.max(s, axis=0, keepdims=True) for s in parts]
        )
        exps = [jnp.exp(s - top) for s in parts]
        total = sum(jnp.sum(e, axis=0, keepdims=True) for e in exps)
        inv = 1.0 / total
        probs = jnp.concatenate([(e * inv).astype(BF16) for e in exps], axis=0)
        out = dot(probs, v_out[pl.ds(0, span), :], 0, 0).astype(BF16)
        before = o_ref[rows, :]
        o_ref[rows, :] = jnp.where(mask, out, before)
        lse_ref[0, 0, :, i * QB : (i + 1) * QB] = top + jnp.log(total)


def backward_kernel(
    q_ref, k_ref, v_ref, do_ref, lse_ref, tab_ref, dq_out, dk_out, dv_out, sums_out, dq, dk, dv
):
    seq_len = q_ref.shape[0]
    j = pl.program_id(1)
    mask = lane_mask(QB, j)
    causal = lax.broadcasted_iota(jnp.int32, (QB, QB), 0) <= lax.broadcasted_iota(
        jnp.int32, (QB, QB), 1
    )

    @pl.when(j == 0)
    def _():
        dk[...] = jnp.zeros_like(dk)
        dv[...] = jnp.zeros_like(dv)

    for i in range(seq_len // QB):
        rows = pl.ds(i * QB, QB)
        q = q_ref[rows, :] * 0.125
        q = jnp.where(mask, q, jnp.zeros_like(q))
        do = do_ref[rows, :]
        do = jnp.where(mask, do, jnp.zeros_like(do))
        lse = lse_ref[0, 0, :, i * QB : (i + 1) * QB]
        pieces = []
        if i:
            pieces.append((pl.ds(0, i * QB), False))
        pieces.append((rows, True))
        probs, grads = [], []
        inner = 0.0
        for where, diagonal in pieces:
            s = dot(k_ref[where, :], q, 1, 1)
            if diagonal:
                s = jnp.where(causal, s, -1e30)
            p = jnp.exp(s - lse)
            dp = dot(v_ref[where, :], do, 1, 1)
            inner = inner + jnp.sum(p * dp, axis=0, keepdims=True)
            probs.append(p)
            grads.append(dp)
        acc = 0.0
        for (where, diagonal), p, dp in zip(pieces, probs, grads):
            ds = (p * (dp - inner)).astype(BF16)
            dv[where, :] += dot(p.astype(BF16), do, 1, 0)
            dk[where, :] += dot(ds, q, 1, 0)
            acc = acc + dot(ds, k_ref[where, :], 0, 0)
        before = dq[rows, :]
        dq[rows, :] = jnp.where(mask, acc * 0.125, before)

    @pl.when(j == pl.num_programs(1) - 1)
    def _():
        tables = (tab_ref[0], tab_ref[1])
        gq = turn(dq[...], tables, -1.0).astype(BF16)
        gk = turn(dk[...], tables, -1.0).astype(BF16)
        gv = dv[...].astype(BF16)
        dq_out[...] = gq
        dk_out[...] = gk
        dv_out[...] = gv
        sums_out[0, 0:1] = jnp.sum(gq.astype(F32), axis=0, keepdims=True)
        sums_out[0, 1:2] = jnp.sum(gk.astype(F32), axis=0, keepdims=True)
        sums_out[0, 2:3] = jnp.sum(gv.astype(F32), axis=0, keepdims=True)


def attention_forward(qkv, bias, tables):
    seq_len, width = qkv.shape[0], qkv.shape[1] // 3
    pairs = width // LANES
    column = lambda part: pl.BlockSpec((seq_len, LANES), lambda p, j: (0, part * pairs + p))
    block = pl.BlockSpec((seq_len, LANES), lambda p, j: (0, p))
    bias_blocks = bias.reshape(3, pairs, LANES).swapaxes(0, 1)
    wide = jax.ShapeDtypeStruct((seq_len, width), BF16)
    elements = pairs * 2 * seq_len * seq_len // 2
    return pl.pallas_call(
        forward_kernel,
        grid=(pairs, LANES // HD),
        in_specs=[
            column(0),
            column(1),
            column(2),
            pl.BlockSpec((1, 3, LANES), lambda p, j: (p, 0, 0)),
            pl.BlockSpec((2, seq_len, LANES), lambda p, j: (0, 0, 0)),
        ],
        out_specs=[
            block,
            block,
            block,
            block,
            pl.BlockSpec((1, 1, 1, seq_len), lambda p, j: (p, j, 0, 0)),
        ],
        out_shape=[
            wide,
            wide,
            wide,
            wide,
            jax.ShapeDtypeStruct((pairs, LANES // HD, 1, seq_len), F32),
        ],
        cost_estimate=pl.CostEstimate(
            flops=elements * 4 * LANES,
            bytes_accessed=qkv.size * 4 + 4 * seq_len * width * 2,
            transcendentals=elements,
        ),
        name="attention_forward",
    )(qkv, qkv, qkv, bias_blocks, tables)


def attention_backward(q, k, v, grad, lse, tables):
    seq_len, width = q.shape
    pairs = width // LANES
    block = pl.BlockSpec((seq_len, LANES), lambda p, j: (0, p))
    wide = jax.ShapeDtypeStruct((seq_len, width), BF16)
    elements = pairs * 2 * seq_len * seq_len // 2
    return pl.pallas_call(
        backward_kernel,
        grid=(pairs, LANES // HD),
        in_specs=[
            block,
            block,
            block,
            block,
            pl.BlockSpec((1, 1, 1, seq_len), lambda p, j: (p, j, 0, 0)),
            pl.BlockSpec((2, seq_len, LANES), lambda p, j: (0, 0, 0)),
        ],
        out_specs=[block, block, block, pl.BlockSpec((1, 3, LANES), lambda p, j: (p, 0, 0))],
        out_shape=[wide, wide, wide, jax.ShapeDtypeStruct((pairs, 3, LANES), F32)],
        scratch_shapes=[pltpu.VMEM((seq_len, LANES), F32)] * 3,
        cost_estimate=pl.CostEstimate(
            flops=elements * 10 * LANES,
            bytes_accessed=7 * seq_len * width * 2,
            transcendentals=elements,
        ),
        name="attention_backward",
    )(q, k, v, grad, lse, tables)


def pick(x, index):
    return lax.dynamic_index_in_dim(x, index, 0, keepdims=False)


class Cube:
    def __init__(self, axis, size):
        self.axis, self.size = axis, size
        self.bits = [b for b in range(size.bit_length()) if 1 << b < size]
        me = lax.axis_index(axis)
        self.own = [lax.rem(lax.div(me, 1 << b), 2) for b in self.bits]

    def swap(self, x, b):
        return lax.ppermute(x, self.axis, [(i, i ^ (1 << b)) for i in range(self.size)])

    def sum_all(self, x):
        for b in self.bits:
            x = x + self.swap(x, b)
        return x

    def contract(self, left, right):
        depth, rows = left.shape
        columns = right.shape[1]
        core, others = self.bits[0], self.bits[1:]
        half = rows // 2
        mine = self.own[0]
        first = lax.dynamic_slice_in_dim(left, (1 - mine) * half, half, 1)
        second = lax.dynamic_slice_in_dim(left, mine * half, half, 1)
        away = dot(first, right, 0, 0, BF16)
        came = self.swap(away, core)
        keep = dot(second, right, 0, 0, BF16)
        orders = [others, others[::-1]]
        quarter = half // 2
        done = []
        for n, order in enumerate(orders):
            small = quarter >> len(order)
            shape = (2,) * len(order) + (small, columns)
            cur = (
                keep[n * quarter : (n + 1) * quarter].astype(F32)
                + came[n * quarter : (n + 1) * quarter].astype(F32)
            ).reshape(shape)
            for b in order:
                own = self.own[b]
                send = pick(cur, 1 - own).astype(BF16)
                got = self.swap(send, b)
                cur = pick(cur, own) + got.astype(F32)
            buf = cur.astype(BF16)
            for b in order[::-1]:
                own = self.own[b]
                got = self.swap(buf, b)
                low = jnp.where(own == 0, buf, got)
                high = jnp.where(own == 0, got, buf)
                buf = jnp.stack([low, high])
            done.append(buf.reshape(quarter, columns))
        whole = jnp.concatenate(done, axis=0)
        other = self.swap(whole, core)
        low = jnp.where(mine == 0, whole, other)
        high = jnp.where(mine == 0, other, whole)
        return jnp.concatenate([low, high], axis=0).astype(F32)


LAG = 2
BLOCK = 128
PIECES = 16
WIDE = 256
STEP = 32
MESH = pl.DeviceIdType.MESH


class Places:
    def __init__(self, n_dp, n_z):
        self.me = lax.axis_index("dp")
        self.z = z = lax.axis_index("mp")
        self.core = lax.rem(self.me, 2)
        self.x = lax.rem(lax.div(self.me, 2), 2)
        self.y = lax.div(self.me, 4)
        self.core_peer = (self.me + 1 - 2 * self.core, z)
        self.x_peer = (self.me + 2 - 4 * self.x, z)
        self.y_peer = (self.me + 4 - 8 * self.y, z)
        self.dp_others = [lax.rem(self.me + n, n_dp) for n in range(1, n_dp)]
        self.dp_peers = [(other, z) for other in self.dp_others]
        self.z_of = [lax.rem(z + d, n_z) for d in range(n_z)]
        self.z_peers = [(self.me, to) for to in self.z_of]
        self.above = jnp.minimum(z + 1, n_z - 1)
        self.below = jnp.maximum(z - 1, 0)
        self.far = n_z - 1 - z
        self.has_above, self.has_below = z < n_z - 1, z > 0
        self.end = jnp.logical_or(z == 0, z == n_z - 1)
        self.inner = jnp.where(z == 0, 1, n_z - 2)
        self.middle = jnp.logical_not(self.end)
        self.order = [
            z,
            jnp.where(z == 0, 1, z - 1),
            jnp.where(z == 0, 2, jnp.where(z == 1, 2, jnp.where(z == 2, 3, 1))),
            jnp.where(z <= 1, 3, 0),
        ]


def rdma(src, dst, send_sem, recv_sem, peer):
    return pltpu.make_async_remote_copy(
        src_ref=src,
        dst_ref=dst,
        send_sem=send_sem,
        recv_sem=recv_sem,
        device_id=peer,
        device_id_type=MESH,
    )


def start(copies):
    for copy in copies:
        copy.start()


def wait(copies):
    for copy in copies:
        copy.wait()


def at_block(i, size):
    return pl.ds(pl.multiple_of(i * size, size), size)


def both(a, b):
    return jnp.logical_and(a, b)


def causal_block():
    key = lax.broadcasted_iota(jnp.int32, (QB, QB), 0)
    query = lax.broadcasted_iota(jnp.int32, (QB, QB), 1)
    return key <= query


def head_part(x, mask):
    return jnp.where(mask, x, jnp.zeros_like(x))


def attend_unit(u, qkv_v, attn_v, hat_v, lse_v, first_row):
    seq_len = qkv_v.shape[1]
    pair, j = lax.div(u, 2), lax.rem(u, 2)
    lanes = at_block(pair, LANES)
    mask = lane_mask(QB, j)
    causal = causal_block()
    for i in range(seq_len // QB):
        rows = pl.ds(i * QB, QB)
        q = head_part(qkv_v[0, rows, lanes] * 0.125, mask)
        parts = []
        if i:
            parts.append(dot(qkv_v[1, pl.ds(0, i * QB), lanes], q, 1, 1))
        parts.append(jnp.where(causal, dot(qkv_v[1, rows, lanes], q, 1, 1), -1e30))
        top = functools.reduce(
            jnp.maximum, [jnp.max(s, axis=0, keepdims=True) for s in parts]
        )
        exps = [jnp.exp(s - top) for s in parts]
        total = sum(jnp.sum(e, axis=0, keepdims=True) for e in exps)
        inv = 1.0 / total
        probs = jnp.concatenate([(e * inv).astype(BF16) for e in exps], axis=0)
        out = dot(probs, qkv_v[2, pl.ds(0, (i + 1) * QB), lanes], 0, 0).astype(BF16)
        attn_v[rows, lanes] = jnp.where(mask, out, attn_v[rows, lanes])
        lse_v[u, :, i * QB : (i + 1) * QB] = top + jnp.log(total)

    @pl.when(j == 1)
    def _():
        for i in range(seq_len // QB):
            rows = pl.ds(i * QB, QB)
            to = pl.ds(pl.multiple_of(first_row + pair * LANES, LANES), LANES)
            hat_v[to, rows] = jnp.transpose(attn_v[rows, lanes])


def attend_back_unit(u, qkv_v, do_v, lse_v, tab_v, dqkv_v, small, dq, dk, dv):
    seq_len, width = qkv_v.shape[1:]
    pair, j = lax.div(u, 2), lax.rem(u, 2)
    lanes = at_block(pair, LANES)
    mask = lane_mask(QB, j)
    causal = causal_block()

    @pl.when(j == 0)
    def _():
        dk[...] = jnp.zeros_like(dk)
        dv[...] = jnp.zeros_like(dv)
        dq[...] = jnp.zeros_like(dq)

    for i in range(seq_len // QB):
        rows = pl.ds(i * QB, QB)
        q = head_part(qkv_v[0, rows, lanes] * 0.125, mask)
        do = head_part(do_v[rows, lanes], mask)
        lse = lse_v[u, :, i * QB : (i + 1) * QB]
        pieces = [(pl.ds(0, i * QB), False)] if i else []
        pieces.append((rows, True))
        probs, grads = [], []
        inner = 0.0
        for where, diagonal in pieces:
            s = dot(qkv_v[1, where, lanes], q, 1, 1)
            if diagonal:
                s = jnp.where(causal, s, -1e30)
            p = jnp.exp(s - lse)
            dp = dot(qkv_v[2, where, lanes], do, 1, 1)
            inner = inner + jnp.sum(p * dp, axis=0, keepdims=True)
            probs.append(p)
            grads.append(dp)
        acc = 0.0
        for (where, diagonal), p, dp in zip(pieces, probs, grads):
            ds = (p * (dp - inner)).astype(BF16)
            dv[where, :] += dot(p.astype(BF16), do, 1, 0)
            dk[where, :] += dot(ds, q, 1, 0)
            acc = acc + dot(ds, qkv_v[1, where, lanes], 0, 0)
        dq[rows, :] = jnp.where(mask, acc * 0.125, dq[rows, :])

    @pl.when(j == 1)
    def _():
        tables = (tab_v[0], tab_v[1])
        out = (
            turn(dq[...], tables, -1.0).astype(BF16),
            turn(dk[...], tables, -1.0).astype(BF16),
            dv[...].astype(BF16),
        )
        for t, g in enumerate(out):
            dqkv_v[:, pl.ds(pl.multiple_of(t * width + pair * LANES, LANES), LANES)] = g
            small[2 + t : 3 + t, lanes] = jnp.sum(g.astype(F32), axis=0, keepdims=True)


def layer_kernel(
    n_dp, n_z, tokens, grad_out, tables, w_gate_up, w_qkv, w_down, w_out, norm_ref, bias_ref,
    sums_out, layer_out, grad_tokens_out, gain_out, shift_out, bias_out, w_gate, w_up,
    lhs_v, dy_v, nrm, rhs, a1_v, a2_v, qkv_v, attn_v, hq_v, do_v, lse_v, tab_v, tok_v,
    wf, zsend, zin, zout, far_v, mid, own, small, small_in, share_in,
    acc, rcv0, rcv1, rcv2, fin,
    load, s_raw, s_wf, s_back, s_wd, s_wn, s_tok, b_sems, m_sems,
    n_send, n_recv, y_send, y_recv, z_sems, small_sems, share_sems,
    s0, s1, s2, s3, s4, s5, s_fin,
):
    at = Places(n_dp, n_z)
    seq_len, model = dy_v.shape
    own_rows = tok_v.shape[0]
    width = qkv_v.shape[2]
    local_ff = a1_v.shape[1]
    blocks_h, blocks_o = local_ff // BLOCK, width // BLOCK
    columns = model // WIDE
    n_d = columns
    n_g, n_q = blocks_h, 3 * width // WIDE
    total = n_d + n_g + n_q
    per = width // WIDE
    fill = n_g + n_q
    dy_chunks = y_recv.shape[1]
    dy_wide = model // dy_chunks
    units = width // HD

    dqkv_v = hq_v
    away_slots = LAG + 1
    own_slots = acc.shape[0] - away_slots
    hat_v, nt_v = lhs_v.at[0], lhs_v.at[1]

    def slot_of(buf, it):
        return lax.rem(it, own_slots if buf is acc else buf.shape[0])

    def quarter(bit, half):
        return half * 4 + bit * 2

    def stage0(it):
        sa, s = own_slots + lax.rem(it, away_slots), slot_of(rcv0, it)
        return [rdma(acc.at[sa], rcv0.at[s], s0.at[0, s], s0.at[1, s], at.core_peer)]

    def stage1(it):
        sa, s = slot_of(acc, it), slot_of(rcv1, it)
        a, b = pl.ds(quarter(1 - at.x, 0), 2), pl.ds(quarter(1 - at.y, 1), 2)
        return [
            rdma(acc.at[sa, a], rcv1.at[s, 0], s1.at[0, s], s1.at[1, s], at.x_peer),
            rdma(acc.at[sa, b], rcv1.at[s, 1], s1.at[2, s], s1.at[3, s], at.y_peer),
        ]

    def stage2(it):
        sa, s = slot_of(acc, it), slot_of(rcv2, it)
        a, b = quarter(at.x, 0) + 1 - at.y, quarter(at.y, 1) + 1 - at.x
        return [
            rdma(acc.at[sa, a], rcv2.at[s, 0], s2.at[0, s], s2.at[1, s], at.y_peer),
            rdma(acc.at[sa, b], rcv2.at[s, 1], s2.at[2, s], s2.at[3, s], at.x_peer),
        ]

    def piece_a():
        return at.core * 8 + quarter(at.x, 0) + at.y

    def piece_b():
        return at.core * 8 + quarter(at.y, 1) + at.x

    def stage3(it):
        s, n = slot_of(fin, it), lax.rem(it, s3.shape[1])
        a, b = sums_out.at[it, piece_a()], sums_out.at[it, piece_b()]
        return [
            rdma(fin.at[s, 0], a, s3.at[0, n], s3.at[1, n], at.y_peer),
            rdma(fin.at[s, 1], b, s3.at[2, n], s3.at[3, n], at.x_peer),
        ]

    def keep3(it):
        s = slot_of(fin, it)
        return [
            pltpu.make_async_copy(fin.at[s, 0], sums_out.at[it, piece_a()], s_fin.at[0, s]),
            pltpu.make_async_copy(fin.at[s, 1], sums_out.at[it, piece_b()], s_fin.at[1, s]),
        ]

    def stage4(it):
        n = lax.rem(it, s4.shape[1])
        a = sums_out.at[it, pl.ds(at.core * 8 + quarter(at.x, 0), 2)]
        b = sums_out.at[it, pl.ds(at.core * 8 + quarter(at.y, 1), 2)]
        return [
            rdma(a, a, s4.at[0, n], s4.at[1, n], at.x_peer),
            rdma(b, b, s4.at[2, n], s4.at[3, n], at.y_peer),
        ]

    def stage5(it):
        n = lax.rem(it, s5.shape[1])
        part = sums_out.at[it, pl.ds(at.core * 8, 8)]
        return [rdma(part, part, s5.at[0, n], s5.at[1, n], at.core_peer)]

    def product(it):
        left = jnp.where(it < n_d, 0, 1)

        @pl.when(it < n_d)
        def _():
            rhs[...] = dy_v[:, at_block(it, WIDE)]

        @pl.when(both(it >= n_d, it < n_d + n_g))
        def _():
            lanes = at_block(it - n_d, BLOCK)
            rhs[:, :BLOCK] = a1_v[:, lanes]
            rhs[:, BLOCK:] = a2_v[:, lanes]

        @pl.when(it >= n_d + n_g)
        def _():
            rhs[...] = dqkv_v[:, at_block(it - n_d - n_g, WIDE)]

        @pl.loop(0, 2)
        def _(h):
            which = jnp.where(h == 0, 1 - at.core, at.core)
            slot = jnp.where(h == 0, own_slots + lax.rem(it, away_slots), lax.rem(it, own_slots))
            tile = dot(lhs_v[left, at_block(which, 8 * BLOCK), :], rhs[...], 1, 0, BF16)
            for p in range(8):
                acc[slot, p] = tile[p * BLOCK : (p + 1) * BLOCK]

            @pl.when(h == 0)
            def _():
                start(stage0(it))

    def shard(origin):
        return at_block(origin, own_rows)

    def n_copy(kind, origin, to):
        rows = nrm.at[shard(origin)]
        return rdma(rows, rows, n_send.at[kind], n_recv.at[origin], (at.me, to))

    def y_copy(kind, origin, to, c):
        part = dy_v.at[shard(origin), at_block(c, dy_wide)]
        return rdma(part, part, y_send.at[kind, c], y_recv.at[origin, c], (at.me, to))

    def route(make, what):
        def when(condition, copy):
            @pl.when(condition)
            def _():
                getattr(copy, what)()

        def first():
            when(at.has_above, make(0, at.z, at.above))
            when(at.has_below, make(1, at.z, at.below))
            when(at.end, make(2, at.z, at.far))

        def passed(up):
            if up:
                when(at.middle, make(3, at.below, at.above))
            else:
                when(at.middle, make(4, at.above, at.below))

        return first, passed

    def n_arrived(origin):
        n_copy(0, origin, at.z_of[1]).wait_recv()

    def y_arrived(origin, c):
        y_copy(0, origin, at.z_of[1], c).wait_recv()

    def norm_rows(rows):
        tok = tok_v[rows, :].astype(F32)
        centered = tok - jnp.mean(tok, axis=1, keepdims=True)
        inv_std = lax.rsqrt(jnp.mean(centered * centered, axis=1, keepdims=True) + EPS)
        return centered * inv_std, inv_std

    def normalize():
        @pl.loop(0, own_rows // STEP)
        def _(r):
            xhat, _ = norm_rows(at_block(r, STEP))
            to = pl.ds(pl.multiple_of(at.z * own_rows + r * STEP, STEP), STEP)
            nrm[to, :] = (xhat * norm_ref[0:1, :] + norm_ref[1:2, :]).astype(BF16)

    def raw_copy(wint, f):
        s = lax.rem(f, 2)
        return pltpu.make_async_copy(
            w_gate_up.at[:, :, at_block(f, BLOCK)], wint.at[s], s_raw.at[s]
        )

    def back_copies(f):
        s = lax.rem(f, 2)
        return [
            pltpu.make_async_copy(
                wf.at[s, :, pl.ds(n * BLOCK, BLOCK)], w.at[:, at_block(f, BLOCK)], s_back.at[n, s]
            )
            for n, w in enumerate((w_gate, w_up))
        ]

    def pair_copies(f, s):
        return [
            pltpu.make_async_copy(
                w.at[:, at_block(f, BLOCK)], wf.at[s, :, pl.ds(n * BLOCK, BLOCK)], s_wf.at[n, s]
            )
            for n, w in enumerate((w_gate, w_up))
        ]

    def qkv_copies(m, s):
        return [
            pltpu.make_async_copy(
                w_qkv.at[lax.div(m, per), :, at_block(lax.rem(m, per), WIDE)], wf.at[s], s_wf.at[0, s]
            )
        ]

    def rows_of(rows):
        parts = [nrm[r, :] for r in rows]
        return parts[0] if len(parts) == 1 else jnp.concatenate(parts, axis=0)

    def hidden_tile(f, s, rows):
        product_of = dot(rows_of(rows), wf[s], 1, 0)
        lanes = at_block(f, BLOCK)
        for n, r in enumerate(rows):
            part = product_of[n * own_rows : (n + 1) * own_rows]
            g, u = part[:, :BLOCK], part[:, BLOCK:]
            sig = jax.nn.sigmoid(g)
            silu = g * sig
            h = (silu * u).astype(BF16)
            hq_v[r, lanes] = h
            hat_v[lanes, r] = jnp.transpose(h)
            a1_v[r, lanes] = (u * (sig + silu * (1.0 - sig))).astype(BF16)
            a2_v[r, lanes] = silu.astype(BF16)

    def qkv_tile(m, s, rows):
        t = lax.div(m, per)
        biases = bias_ref[...].astype(F32)
        bias = jnp.where(t == 0, biases[0:1], jnp.where(t == 1, biases[1:2], biases[2:3]))
        part = bias[:, :WIDE]
        for n in range(1, per):
            part = jnp.where(lax.rem(m, per) == n, bias[:, n * WIDE : (n + 1) * WIDE], part)
        product_of = dot(rows_of(rows), wf[s], 1, 0) + part
        for k, r in enumerate(rows):
            for n in range(WIDE // LANES):
                x = product_of[k * own_rows : (k + 1) * own_rows, n * LANES : (n + 1) * LANES]
                turned = turn(x, (tab_v[0, r, :], tab_v[1, r, :]), 1.0)
                lanes = pl.ds(pl.multiple_of(lax.rem(m, per) * WIDE + n * LANES, LANES), LANES)
                qkv_v[t, r, lanes] = jnp.where(t < 2, turned, x).astype(BF16)

    def turn_over(origin):
        rows = shard(origin)
        for n in range(columns):
            cols = pl.ds(n * WIDE, WIDE)
            nt_v[cols, rows] = jnp.transpose(nrm[rows, cols])

    def own_pass(wint):
        r = lax.broadcasted_iota(jnp.int32, (WIDE, WIDE), 0)
        c = lax.broadcasted_iota(jnp.int32, (WIDE, WIDE), 1)
        source = jnp.where(r < BLOCK, 2 * r, 2 * (r - BLOCK) + 1)
        parting = (source == c).astype(F32).astype(BF16)
        rows = shard(at.z)

        @pl.loop(0, n_g)
        def _(f):
            s = lax.rem(f, 2)

            @pl.when(f + 1 < n_g)
            def _():
                raw_copy(wint, f + 1).start()

            raw_copy(wint, f).wait()

            @pl.when(f >= 2)
            def _():
                wait(back_copies(f - 2))

            for n in range(model // BLOCK):
                part = pl.ds(n * BLOCK, BLOCK)
                raw = wint[s, part].reshape(WIDE, BLOCK)
                parted = dot(parting, raw, 1, 0, BF16)
                wf[s, part, :BLOCK] = parted[:BLOCK]
                wf[s, part, BLOCK:] = parted[BLOCK:]
            start(back_copies(f))
            hidden_tile(f, s, [rows])

        for f in (n_g - 2, n_g - 1):
            wait(back_copies(f))
        start(qkv_copies(0, n_g % 2))

        @pl.loop(0, n_q)
        def _(m):
            n = n_g + m
            s = lax.rem(n, 2)

            @pl.when(m + 1 < n_q)
            def _():
                start(qkv_copies(m + 1, 1 - s))

            @pl.when(m + 1 == n_q)
            def _():
                start(pair_copies(0, 1 - s))

            wait(qkv_copies(m, s))
            qkv_tile(m, s, [rows])

    def later_pass(k, origins, aside=None):
        rows = [shard(origin) for origin in origins]
        base = k * fill

        @pl.loop(0, n_g)
        def _(f):
            s = lax.rem(base + f, 2)

            @pl.when(f + 1 < n_g)
            def _():
                start(pair_copies(f + 1, 1 - s))

            @pl.when(f + 1 == n_g)
            def _():
                start(qkv_copies(0, 1 - s))

            if aside is not None:

                @pl.when(f == n_g - 1)
                def _():
                    aside()

            wait(pair_copies(f, s))
            hidden_tile(f, s, rows)

        @pl.loop(0, n_q)
        def _(m):
            s = lax.rem(base + n_g + m, 2)

            @pl.when(m + 1 < n_q)
            def _():
                start(qkv_copies(m + 1, 1 - s))

            if k < 2:

                @pl.when(m + 1 == n_q)
                def _():
                    start(pair_copies(0, 1 - s))

            wait(qkv_copies(m, s))
            qkv_tile(m, s, rows)

        for origin in origins:
            turn_over(origin)

    def straight(d):
        return {1: at.z != n_z - 1, 2: at.end, n_z - 1: at.z != 0}[d]

    def comes(d):
        return {1: at.z != 0, 2: at.z >= 0, n_z - 1: at.z != n_z - 1}[d]

    def under(condition, act):
        @pl.when(condition)
        def _():
            act()

    def z_copy(c, d, onward=False):
        columns_c = at_block(c, WIDE)
        src = far_v.at[:, columns_c] if onward else zsend.at[slot_of(zsend, c), shard(at.z_of[d])]
        dst = zin.at[d - 1, :, columns_c]
        return rdma(src, dst, z_sems.at[0, d - 1, c], z_sems.at[1, d - 1, c], at.z_peers[d])

    def mid_copy(c):
        src = zsend.at[slot_of(zsend, c), shard(at.far)]
        dst = mid.at[:, at_block(c, WIDE)]
        return rdma(src, dst, m_sems.at[0, c], m_sems.at[1, c], (at.me, at.inner))

    def z_out(c, what):
        for d in range(1, n_z):
            under(straight(d), getattr(z_copy(c, d), what))
        under(at.end, getattr(mid_copy(c), what))

    def far_job(c):
        @pl.when(at.middle)
        def _():
            mid_copy(c).wait_recv()
            cols = at_block(c, WIDE)
            far_v[:, cols] = (far_v[:, cols].astype(F32) + mid[:, cols].astype(F32)).astype(BF16)
            z_copy(c, 2, True).start()

    def branch_load(c):
        s = lax.rem(c, 2)
        cols = at_block(c, WIDE)
        return [
            pltpu.make_async_copy(
                w_down.at[:, cols], wf.at[s, pl.ds(0, local_ff)], s_wf.at[0, s]
            ),
            pltpu.make_async_copy(
                w_out.at[:, cols], wf.at[s, pl.ds(local_ff, width)], s_wf.at[1, s]
            ),
        ]

    def branch_job(c):
        s = lax.rem(c, 2)
        wait(branch_load(c))

        @pl.when(c + 1 < columns)
        def _():
            start(branch_load(c + 1))

        value = dot(hq_v[:, :local_ff], wf[s, :local_ff], 1, 0) + dot(
            attn_v[...], wf[s, local_ff : local_ff + width], 1, 0
        )
        nrm[:, at_block(c, WIDE)] = value.astype(BF16)

    def branch_copy(d):
        src, dst = nrm.at[shard(at.z_of[d])], zout.at[d - 1]
        return rdma(src, dst, b_sems.at[0, d - 1], b_sems.at[1, d - 1], at.z_peers[d])

    def branch_mid():
        return rdma(
            nrm.at[shard(at.far)], far_v, b_sems.at[0, n_z - 1], b_sems.at[1, n_z - 1],
            (at.me, at.inner),
        )

    def branch_first():
        under(at.end, lambda: branch_mid().start())

        @pl.when(at.middle)
        def _():
            for d in (1, n_z - 1):
                branch_copy(d).start()

    def branch_second():
        @pl.when(at.end)
        def _():
            for d in range(1, n_z):
                under(straight(d), branch_copy(d).start)

        @pl.when(at.middle)
        def _():
            branch_mid().wait_recv()

            @pl.loop(0, own_rows // STEP)
            def _(r):
                rows = at_block(r, STEP)
                to = pl.ds(pl.multiple_of(at.z_of[2] * own_rows + r * STEP, STEP), STEP)
                nrm[to, :] = (nrm[to, :].astype(F32) + far_v[rows, :].astype(F32)).astype(BF16)

            branch_copy(2).start()

    def layer_out_copy():
        return pltpu.make_async_copy(nrm.at[shard(at.z)], layer_out, s_tok.at[0])

    def layer_out_job():
        under(at.end, branch_mid().wait_send)
        under(at.middle, branch_copy(2).wait_send)
        for d in range(1, n_z):
            under(straight(d), branch_copy(d).wait_send)
            under(comes(d), branch_copy(d).wait_recv)

        @pl.loop(0, own_rows // STEP)
        def _(r):
            rows = at_block(r, STEP)
            here = pl.ds(pl.multiple_of(at.z * own_rows + r * STEP, STEP), STEP)
            value = tok_v[rows, :].astype(F32) + nrm[here, :].astype(F32)
            for n in range(n_z - 1):
                value = value + jnp.where(comes(n + 1), zout[n, rows, :].astype(F32), 0.0)
            nrm[here, :] = value.astype(BF16)

        layer_out_copy().start()

    def hidden_load(g, wd):
        def one(n, what):
            b = 2 * g + n
            dst = wd.at[pl.ds(n * BLOCK, BLOCK)]

            @pl.when(b < blocks_h)
            def _():
                rows = at_block(jnp.minimum(b, blocks_h - 1), BLOCK)
                getattr(pltpu.make_async_copy(w_down.at[rows], dst, s_wd.at[n]), what)()

            @pl.when(both(b >= blocks_h, b < blocks_h + blocks_o))
            def _():
                rows = at_block(jnp.clip(b - blocks_h, 0, blocks_o - 1), BLOCK)
                getattr(pltpu.make_async_copy(w_out.at[rows], dst, s_wd.at[n]), what)()

        return one

    def hidden_job(g, wd):
        for n in range(2):
            hidden_load(g, wd)(n, "wait")
        dh = dot(dy_v[...], wd[...], 1, 1)
        for n in range(2):
            b = 2 * g + n
            part = dh[:, n * BLOCK : (n + 1) * BLOCK]

            @pl.when(b < blocks_h)
            def _(part=part, b=b):
                lanes = at_block(jnp.minimum(b, blocks_h - 1), BLOCK)
                a1_v[:, lanes] = (part * a1_v[:, lanes].astype(F32)).astype(BF16)
                a2_v[:, lanes] = (part * a2_v[:, lanes].astype(F32)).astype(BF16)

            @pl.when(both(b >= blocks_h, b < blocks_h + blocks_o))
            def _(part=part, b=b):
                do_v[:, at_block(jnp.clip(b - blocks_h, 0, blocks_o - 1), BLOCK)] = part.astype(BF16)

    def normed_load(c, wg, wu, wq):
        rows = at_block(c, WIDE)
        return [
            pltpu.make_async_copy(w_gate.at[rows], wg, s_wn.at[0]),
            pltpu.make_async_copy(w_up.at[rows], wu, s_wn.at[1]),
            pltpu.make_async_copy(w_qkv.at[:, rows], wq, s_wn.at[2]),
        ]

    def normed_job(c, wg, wu, wq):
        wait(normed_load(c, wg, wu, wq))
        part = dot(a1_v[...], wg[...], 1, 1) + dot(a2_v[...], wu[...], 1, 1)
        for t in range(3):
            part = part + dot(dqkv_v[:, t * width : (t + 1) * width], wq[t], 1, 1)
        s = slot_of(zsend, c)

        @pl.when(c >= zsend.shape[0])
        def _():
            z_out(c - zsend.shape[0], "wait_send")

        zsend[s] = part.astype(BF16)
        z_out(c, "start")

        @pl.when(at.middle)
        def _():
            far_v[:, at_block(c, WIDE)] = zsend[s, shard(at.z_of[2]), :]

        @pl.when(c + 1 < columns)
        def _():
            start(normed_load(c + 1, wg, wu, wq))

        own[:, at_block(c, WIDE)] = zsend[s, shard(at.z), :]

    def tokens_copy():
        return pltpu.make_async_copy(tok_v, grad_tokens_out, s_tok.at[1])

    def norm_job():
        @pl.loop(0, columns)
        def _(c):
            @pl.when(c >= columns - zsend.shape[0])
            def _():
                z_out(c, "wait_send")

            under(at.middle, z_copy(c, 2, True).wait_send)
            for d in range(1, n_z):
                under(comes(d), z_copy(c, d).wait_recv)

        @pl.loop(0, own_rows // STEP)
        def _(r):
            rows = at_block(r, STEP)
            d = own[rows, :].astype(F32)
            for n in range(n_z - 1):
                d = d + jnp.where(comes(n + 1), zin[n, rows, :].astype(F32), 0.0)
            xhat, inv_std = norm_rows(rows)
            scaled = d * norm_ref[0:1, :]
            here = pl.ds(pl.multiple_of(at.z * own_rows + r * STEP, STEP), STEP)
            out = dy_v[here, :].astype(F32) + inv_std * (
                scaled
                - jnp.mean(scaled, axis=1, keepdims=True)
                - xhat * jnp.mean(scaled * xhat, axis=1, keepdims=True)
            )
            small[0:1, :] += jnp.sum(d * xhat, axis=0, keepdims=True)
            small[1:2, :] += jnp.sum(d, axis=0, keepdims=True)
            tok_v[rows, :] = out.astype(BF16)

        tokens_copy().start()

    share = model // n_z

    def share_copies():
        return [
            rdma(
                small.at[:, at_block(at.z_of[d], share)],
                share_in.at[d - 1],
                share_sems.at[0, d - 1],
                share_sems.at[1, d - 1],
                at.z_peers[d],
            )
            for d in range(1, n_z)
        ]

    def spread_copies():
        return [
            rdma(
                small_in.at[at.me],
                small_in.at[at.me],
                small_sems.at[0, n],
                small_sems.at[1, at.me],
                peer,
            )
            for n, peer in enumerate(at.dp_peers)
        ]

    def small_spread():
        wait(share_copies())
        mine = small[0:2, at_block(at.z, share)]
        for n in range(n_z - 1):
            mine = mine + share_in[n, 0:2, :]
        small_in[at.me] = small[:, 0:share]
        small_in[at.me, 0:2, :] = mine
        start(spread_copies())

    def small_end():
        for copy in spread_copies():
            copy.wait_send()
        for n, source in enumerate(at.dp_others):
            rdma(
                small_in.at[source], small_in.at[source], small_sems.at[0, n],
                small_sems.at[1, source], at.dp_peers[n],
            ).wait_recv()
        value = small_in[0]
        for n in range(1, small_in.shape[0]):
            value = value + small_in[n]
        gain_out[...] = value[0]
        shift_out[...] = value[1]
        bias_out[...] = value[2:5]

    loads = [
        pltpu.make_async_copy(tokens, tok_v, load.at[0]),
        pltpu.make_async_copy(grad_out, dy_v.at[shard(at.z)], load.at[1]),
        pltpu.make_async_copy(tables, tab_v, load.at[2]),
    ]
    start(loads)
    barrier = pltpu.get_barrier_semaphore()
    peers = at.dp_peers + at.z_peers[1:]
    for peer in peers:
        pl.semaphore_signal(barrier, inc=1, device_id=peer, device_id_type=MESH)
    loads[0].wait()
    normalize()
    pl.semaphore_wait(barrier, len(peers))

    def forward(wint):
        raw_copy(wint, 0).start()
        route(n_copy, "start")[0]()
        small[...] = jnp.zeros_like(small)
        rest = model - local_ff - width
        hat_v[pl.ds(local_ff + width, rest), :] = jnp.zeros((rest, seq_len), BF16)
        loads[2].wait()
        own_pass(wint)
        turn_over(at.z)

    pl.run_scoped(forward, pltpu.VMEM((2, model, 2, BLOCK), BF16))
    o1, o2, o3 = at.order[1:]
    n_arrived(o1)
    onward = route(n_copy, "start")[1]

    @pl.when(at.middle)
    def _():
        n_arrived(o2)
        onward(True)
        onward(False)
        later_pass(1, [o1, o2])
        n_arrived(o3)

    @pl.when(at.end)
    def _():
        later_pass(1, [o1])
        n_arrived(o2)
        n_arrived(o3)

    def dy_route(c, what):
        return route(lambda *a: y_copy(*a, c), what)

    def send_dy(c):
        dy_route(c, "start")[0]()

    def pass_dy_on(c):
        @pl.when(at.middle)
        def _():
            y_arrived(o1, c)
            y_arrived(o2, c)

        onward = dy_route(c, "start")[1]
        onward(True)
        onward(False)

    def rest_of_dy(c):
        y_arrived(o3, c)

        @pl.when(at.end)
        def _():
            y_arrived(o1, c)
            y_arrived(o2, c)

    loads[1].wait()
    send_dy(0)

    @pl.when(at.middle)
    def _():
        later_pass(2, [o3], lambda: send_dy(1))

    @pl.when(at.end)
    def _():
        later_pass(2, [o2, o3], lambda: send_dy(1))

    start(branch_load(0))
    pass_dy_on(0)

    first, passed = route(n_copy, "wait_send")
    first()
    passed(True)
    passed(False)

    def attend(first, count):
        @pl.loop(first, first + count)
        def _(u):
            attend_unit(u, qkv_v, attn_v, hat_v, lse_v, local_ff)

    attend(0, units // 2)
    pass_dy_on(1)
    send_dy(2)
    attend(units // 2, units - units // 2)

    early = [0, 1, 2, 3, 6, 7]
    behind = 4
    branches = {4: 0, 5: 2, 8: 4, 9: 6}

    def meanwhile(tick):
        for t, c in ((2, 2), (5, 3)):

            @pl.when(tick == t)
            def _(c=c):
                pass_dy_on(c)
                if c + 1 < dy_chunks:
                    send_dy(c + 1)

        from_, to = 0, 0
        for t, c in branches.items():
            from_ = jnp.where(tick == t, c, from_)
            to = jnp.where(tick == t, c + 2, to)

        @pl.loop(from_, to)
        def _(c):
            branch_job(c)

        for t, c in ((0, 0), (2, 1), (6, 2), (10, 3)):

            @pl.when(tick == t)
            def _(c=c):
                rest_of_dy(c)

    def item_at(tick):
        it = tick - behind
        for n, t in enumerate(early):
            it = jnp.where(tick == t, n, it)
        return it

    def live(tick):
        ready_tick = both(tick >= len(early) + behind, tick < total + behind)
        for t in early:
            ready_tick = jnp.logical_or(ready_tick, tick == t)
        return ready_tick

    hidden_jobs = -(-(blocks_h + blocks_o) // 2)
    split = blocks_h // 2
    hidden_at = len(early) + behind
    back_at = hidden_at + 2 + hidden_jobs - split
    normed_at = max(back_at + units, hidden_at + hidden_jobs)
    out_at = total + behind - 1
    norm_at = total + behind + 4

    def hidden_index(n):
        late = hidden_jobs - split
        return jnp.where(n < 2, n, jnp.where(n < late + 2, n + split - 2, n - late))

    def ticks(wide, wq, dq, dk, dv):
        wd = wide.at[0]
        wg, wu = wide.at[0, :, pl.ds(0, local_ff)], wide.at[1, :, pl.ds(0, local_ff)]

        for n in range(2):
            hidden_load(hidden_index(0), wd)(n, "start")

        @pl.loop(0, total + behind + 6 * LAG)
        def _(tick):
            one = item_at(tick - LAG)

            @pl.when(live(tick - LAG))
            def _():
                wait(stage0(one))
                sa, s = slot_of(acc, one), slot_of(rcv0, one)

                @pl.loop(0, 8)
                def _(p):
                    acc[sa, p] = (acc[sa, p].astype(F32) + rcv0[s, p].astype(F32)).astype(BF16)

                start(stage1(one))

            two = item_at(tick - 2 * LAG)

            @pl.when(live(tick - 2 * LAG))
            def _():
                wait(stage1(two))
                sa, s = slot_of(acc, two), slot_of(rcv1, two)
                for n, bit in ((0, at.x), (1, at.y)):
                    for m in range(2):
                        p = quarter(bit, n) + m
                        acc[sa, p] = (
                            acc[sa, p].astype(F32) + rcv1[s, n, m].astype(F32)
                        ).astype(BF16)
                start(stage2(two))

            three = item_at(tick - 3 * LAG)

            @pl.when(live(tick - 3 * LAG))
            def _():
                wait(stage2(three))
                sa, s, d = slot_of(acc, three), slot_of(rcv2, three), slot_of(fin, three)
                for n, p in ((0, quarter(at.x, 0) + at.y), (1, quarter(at.y, 1) + at.x)):
                    fin[d, n] = (acc[sa, p].astype(F32) + rcv2[s, n].astype(F32)).astype(BF16)
                start(stage3(three))
                start(keep3(three))

            four = item_at(tick - 4 * LAG)

            @pl.when(live(tick - 4 * LAG))
            def _():
                wait(keep3(four))
                wait(stage3(four))
                start(stage4(four))

            five = item_at(tick - 5 * LAG)

            @pl.when(live(tick - 5 * LAG))
            def _():
                wait(stage4(five))
                start(stage5(five))

            six = item_at(tick - 6 * LAG)

            @pl.when(live(tick - 6 * LAG))
            def _():
                wait(stage5(six))

            meanwhile(tick)
            item = item_at(tick)

            @pl.when(live(tick))
            def _():
                product(item)

            @pl.when(tick == hidden_at)
            def _():
                branch_first()

            @pl.when(tick == hidden_at + 4)
            def _():
                branch_second()

            @pl.when(both(tick >= hidden_at, tick < hidden_at + hidden_jobs))
            def _():
                n = tick - hidden_at
                hidden_job(hidden_index(n), wd)

                @pl.when(n + 1 < hidden_jobs)
                def _():
                    for m in range(2):
                        hidden_load(hidden_index(n + 1), wd)(m, "start")

            @pl.when(both(tick >= back_at, tick < back_at + units))
            def _():
                attend_back_unit(
                    tick - back_at, qkv_v, do_v, lse_v, tab_v, dqkv_v, small, dq, dk, dv
                )

            @pl.when(tick == normed_at - 1)
            def _():
                start(normed_load(0, wg, wu, wq))

            @pl.when(both(tick >= normed_at, tick < normed_at + columns))
            def _():
                normed_job(tick - normed_at, wg, wu, wq)

            @pl.when(both(tick >= normed_at + 2, tick < normed_at + 2 + columns))
            def _():
                far_job(tick - normed_at - 2)

            @pl.when(tick == out_at)
            def _():
                layer_out_job()
                for c in range(dy_chunks):
                    first, passed = dy_route(c, "wait_send")
                    first()
                    passed(True)
                    passed(False)

            @pl.when(tick == norm_at)
            def _():
                norm_job()
                start(share_copies())

            @pl.when(tick == norm_at + 2)
            def _():
                small_spread()

            @pl.when(tick == norm_at + 5)
            def _():
                small_end()
                tokens_copy().wait()
                layer_out_copy().wait()

    pl.run_scoped(
        ticks,
        pltpu.VMEM((2, WIDE, model), BF16),
        pltpu.VMEM((3, WIDE, width), BF16),
        *[pltpu.VMEM((seq_len, LANES), F32)] * 3,
    )


def run_layer(
    tokens, grad_out, tables, w_gate_up, w_qkv, w_down, w_out, norm, bias, n_dp, n_z
):
    own, model = tokens.shape
    seq_len = own * n_z
    local_ff, width = w_down.shape[0], w_out.shape[0]
    columns = model // WIDE
    total = columns + local_ff // BLOCK + 3 * width // WIDE
    bf = lambda *shape: pltpu.VMEM(shape, BF16)
    fl = lambda *shape: pltpu.VMEM(shape, F32)
    sems = lambda *shape: pltpu.SemaphoreType.DMA(shape)
    slots = 2 * LAG + 2
    dy_chunks = 4
    hbm = pl.BlockSpec(memory_space=pl.ANY)
    vmem = pl.BlockSpec(memory_space=pltpu.VMEM)
    return pl.pallas_call(
        functools.partial(layer_kernel, n_dp, n_z),
        in_specs=[hbm] * 7 + [vmem] * 2,
        out_specs=[hbm, hbm, hbm, vmem, vmem, vmem, hbm, hbm],
        out_shape=[
            jax.ShapeDtypeStruct((total, PIECES, BLOCK, WIDE), BF16),
            jax.ShapeDtypeStruct((own, model), BF16),
            jax.ShapeDtypeStruct((own, model), BF16),
            jax.ShapeDtypeStruct((model // n_z,), F32),
            jax.ShapeDtypeStruct((model // n_z,), F32),
            jax.ShapeDtypeStruct((3, width), F32),
            jax.ShapeDtypeStruct((model, local_ff), BF16),
            jax.ShapeDtypeStruct((model, local_ff), BF16),
        ],
        scratch_shapes=[
            bf(2, model, seq_len), bf(seq_len, model), bf(seq_len, model), bf(seq_len, WIDE),
            bf(seq_len, local_ff), bf(seq_len, local_ff),
            bf(3, seq_len, width), bf(seq_len, width), bf(seq_len, max(local_ff, 3 * width)),
            bf(seq_len, width), fl(width // HD, 1, seq_len), fl(2, seq_len, LANES), bf(own, model),
            bf(2, model, WIDE), bf(3, seq_len, WIDE), bf(n_z - 1, own, model), bf(n_z - 1, own, model), bf(own, model), bf(own, model), bf(own, model),
            fl(8, model), fl(n_dp, 8, model // n_z), fl(n_z - 1, 8, model // n_z),
            bf(4 * LAG + 2, 8, BLOCK, WIDE),
            bf(slots - 1, 8, BLOCK, WIDE), bf(slots, 2, 2, BLOCK, WIDE), bf(slots, 2, BLOCK, WIDE),
            bf(LAG + 1, 2, BLOCK, WIDE),
            sems(3), sems(2), sems(2, 2), sems(2, 2), sems(2), sems(3), sems(2),
            sems(2, n_z), sems(2, columns),
            sems(5), sems(n_z), sems(5, dy_chunks), sems(n_z, dy_chunks),
            sems(2, n_z - 1, columns), sems(2, n_dp), sems(2, n_z - 1),
            sems(2, slots), sems(4, slots), sems(4, slots),
            sems(4, slots), sems(4, slots), sems(2, slots), sems(2, LAG + 1),
        ],
        compiler_params=pltpu.CompilerParams(
            collective_id=0, has_side_effects=True, vmem_limit_bytes=67043328
        ),
        name="layer",
    )(tokens, grad_out, tables, w_gate_up, w_qkv, w_down, w_out, norm, bias)


def unpack_kernel(n_d, n_g, item_ref, down, out, gate_up, qkv):
    i = pl.program_id(0)
    n_down = down.shape[0] // BLOCK

    def rows(p):
        return pl.ds(p * BLOCK, BLOCK)

    @pl.when(i < n_d)
    def _():
        for p in range(n_down):
            down[rows(p), :] = item_ref[0, p].astype(F32)
        for p in range(out.shape[0] // BLOCK):
            out[rows(p), :] = item_ref[0, n_down + p].astype(F32)

    @pl.when(both(i >= n_d, i < n_d + n_g))
    def _():
        flat = gate_up.reshape(2 * gate_up.shape[0], BLOCK)
        for p in range(PIECES):
            value = item_ref[0, p].astype(F32)
            for n in range(2):
                flat[pl.ds(2 * p * BLOCK + n, BLOCK, stride=2), :] = value[
                    :, n * BLOCK : (n + 1) * BLOCK
                ]

    @pl.when(i >= n_d + n_g)
    def _():
        for p in range(PIECES):
            qkv[0, rows(p), :] = item_ref[0, p].astype(F32)


def unpack(items, local_ff, width, model):
    n_d, n_g, n_q = model // WIDE, local_ff // BLOCK, 3 * width // WIDE
    per = n_q // 3

    def of_d(i):
        return (0, jnp.minimum(i, n_d - 1))

    def of_q(i):
        q = jnp.maximum(i - n_d - n_g, 0)
        return (lax.div(q, per), 0, lax.rem(q, per))

    down, out, gate_up, qkv = pl.pallas_call(
        functools.partial(unpack_kernel, n_d, n_g),
        grid=(n_d + n_g + n_q,),
        in_specs=[pl.BlockSpec((1, PIECES, BLOCK, WIDE), lambda i: (i, 0, 0, 0))],
        out_specs=[
            pl.BlockSpec((local_ff, WIDE), of_d),
            pl.BlockSpec((width, WIDE), of_d),
            pl.BlockSpec((model, 2, BLOCK), lambda i: (0, 0, jnp.clip(i - n_d, 0, n_g - 1))),
            pl.BlockSpec((1, model, WIDE), of_q),
        ],
        out_shape=[
            jax.ShapeDtypeStruct((local_ff, model), F32),
            jax.ShapeDtypeStruct((width, model), F32),
            jax.ShapeDtypeStruct((model, 2, local_ff), F32),
            jax.ShapeDtypeStruct((3, model, width), F32),
        ],
        name="unpack",
    )(items)
    return down, out, gate_up, qkv.transpose(1, 0, 2)


def fast_path(n_dp, n_mp, rows, model_width, local_width, local_ff):
    blocks_h, blocks_o = local_ff // BLOCK, local_width // BLOCK
    return (
        n_dp == 8
        and n_mp == 4
        and rows == QB
        and model_width == PIECES * BLOCK
        and local_width == model_width // n_mp
        and local_ff % BLOCK == 0
        and blocks_h % 2 == 1
        and blocks_h + blocks_o <= PIECES
        and blocks_h * (model_width // WIDE) % blocks_o == 0
    )


def fused_layer(
    n_dp,
    n_mp,
    tables,
    tokens,
    norm_gain,
    layernorm_bias,
    qkv_weight,
    qkv_bias,
    out_weight,
    gate_up_weight,
    down_weight,
    grad_out,
):
    model_width = tokens.shape[1]
    local_width, local_ff = qkv_weight.shape[2], gate_up_weight.shape[2]
    items, layer_out, grad_tokens, grad_gain, grad_shift, grad_bias, _, _ = run_layer(
        tokens,
        grad_out,
        tables,
        gate_up_weight,
        qkv_weight.transpose(1, 0, 2),
        down_weight,
        out_weight,
        jnp.stack([norm_gain, layernorm_bias]).astype(F32),
        qkv_bias,
        n_dp,
        n_mp,
    )
    grad_down_w, grad_out_w, grad_gate_up_w, grad_qkv_w = unpack(
        items, local_ff, local_width, model_width
    )
    return (
        layer_out,
        grad_tokens,
        grad_gain,
        grad_shift,
        grad_qkv_w,
        grad_bias,
        grad_out_w,
        grad_gate_up_w,
        grad_down_w,
    )


def on_device(
    n_dp,
    n_mp,
    tokens,
    norm_gain,
    layernorm_bias,
    qkv_weight,
    qkv_bias,
    out_weight,
    gate_up_weight,
    down_weight,
    grad_out,
):
    rows, model_width = tokens.shape
    local_width = qkv_weight.shape[2]
    seq_len = rows * n_mp
    tables = rotary_tables(seq_len)
    if fast_path(n_dp, n_mp, rows, model_width, local_width, gate_up_weight.shape[2]):
        return fused_layer(
            n_dp, n_mp, tables, tokens, norm_gain, layernorm_bias, qkv_weight, qkv_bias, out_weight,
            gate_up_weight, down_weight, grad_out,
        )
    cube = Cube("dp", n_dp)
    gain = norm_gain.astype(F32)
    token_f32 = tokens.astype(F32)
    row_mean = jnp.mean(token_f32, axis=1, keepdims=True)
    centered = token_f32 - row_mean
    inv_std = lax.rsqrt(jnp.mean(centered * centered, axis=1, keepdims=True) + EPS)
    xhat = centered * inv_std
    normed_own = (xhat * gain + layernorm_bias.astype(F32)).astype(BF16)
    normed = lax.all_gather(normed_own, "mp", axis=0, tiled=True)
    dy = lax.all_gather(grad_out, "mp", axis=0, tiled=True)

    w_qkv = [qkv_weight[:, t, :] for t in range(3)]
    w_gate, w_up = gate_up_weight[:, 0, :], gate_up_weight[:, 1, :]

    gate = dot(normed, w_gate, 1, 0)
    up = dot(normed, w_up, 1, 0)
    sig = jax.nn.sigmoid(gate)
    hidden = (gate * sig * up).astype(BF16)
    qkv = jnp.concatenate([dot(normed, w, 1, 0) for w in w_qkv], axis=1)
    q, k, v, attended, lse = attention_forward(qkv, qkv_bias.astype(F32), tables)
    branch = (dot(attended, out_weight, 1, 0) + dot(hidden, down_weight, 1, 0)).astype(BF16)
    share = lax.psum_scatter(branch, "mp", scatter_dimension=0, tiled=True)
    layer_out = (token_f32 + share.astype(F32)).astype(BF16)

    share_width = model_width // n_mp
    d_hidden = dot(dy, down_weight, 1, 1)
    silu = gate * sig
    d_gate = (d_hidden * up * (sig + silu * (1.0 - sig))).astype(BF16)
    d_up = (d_hidden * silu).astype(BF16)
    d_attended = dot(dy, out_weight, 1, 1, BF16)
    dq, dk, dv, sums = attention_backward(q, k, v, d_attended, lse, tables)
    d_normed = (
        dot(d_gate, w_gate, 1, 1)
        + dot(d_up, w_up, 1, 1)
        + dot(dq, w_qkv[0], 1, 1)
        + dot(dk, w_qkv[1], 1, 1)
        + dot(dv, w_qkv[2], 1, 1)
    ).astype(BF16)
    d_own = lax.psum_scatter(d_normed, "mp", scatter_dimension=0, tiled=True).astype(F32)
    d_qkv = jnp.concatenate([dq, dk, dv], axis=1)
    grad_down_w = cube.contract(hidden, dy)
    grad_out_w = cube.contract(attended, dy)
    grad_gate_up_w = jnp.stack(
        [cube.contract(normed, d_gate), cube.contract(normed, d_up)], axis=1
    )
    grad_qkv_w = cube.contract(normed, d_qkv).reshape(model_width, 3, local_width)

    scaled = d_own * gain
    grad_tokens = grad_out.astype(F32) + inv_std * (
        scaled
        - jnp.mean(scaled, axis=1, keepdims=True)
        - xhat * jnp.mean(scaled * xhat, axis=1, keepdims=True)
    )
    terms = jnp.stack([jnp.sum(d_own * xhat, axis=0), jnp.sum(d_own, axis=0)])
    bias_sum = cube.sum_all(sums)
    grad_bias = bias_sum.swapaxes(0, 1).reshape(3, local_width)
    terms = Cube("mp", n_mp).sum_all(cube.sum_all(terms))
    terms = lax.dynamic_slice_in_dim(
        terms, lax.axis_index("mp") * share_width, share_width, 1
    )
    return (
        layer_out,
        grad_tokens.astype(BF16),
        terms[0],
        terms[1],
        grad_qkv_w,
        grad_bias,
        grad_out_w,
        grad_gate_up_w,
        grad_down_w,
    )


def solution(mesh):
    return jax.shard_map(
        functools.partial(on_device, mesh.shape["dp"], mesh.shape["mp"]),
        mesh=mesh,
        in_specs=(
            P(("dp", "mp"), None),
            P(),
            P(),
            P(None, None, "mp"),
            P(None, "mp"),
            P("mp", None),
            P(None, None, "mp"),
            P("mp", None),
            P(("dp", "mp"), None),
        ),
        out_specs=(
            P(("dp", "mp"), None),
            P(("dp", "mp"), None),
            P("mp"),
            P("mp"),
            P(None, None, "mp"),
            P(None, "mp"),
            P("mp", None),
            P(None, None, "mp"),
            P("mp", None),
        ),
        check_vma=False,
    )
```

```python
import functools
import math

import jax
import jax.numpy as jnp
from jax import lax
from jax.experimental import pallas as pl
from jax.experimental.pallas import tpu as pltpu
from jax.sharding import PartitionSpec as P

HD = 64
ROT = 16
EPS = 1e-05
LANES = 128
QB = 256


F32 = jnp.float32
BF16 = jnp.bfloat16


def dot(a, b, ca, cb, out=F32):
    return lax.dot_general(
        a, b, (((ca,), (cb,)), ((), ())), preferred_element_type=F32
    ).astype(out)


def rotary_tables(seq_len):
    half = ROT // 2
    shape = (seq_len, LANES)
    dim = lax.rem(lax.broadcasted_iota(jnp.int32, shape, 1), HD)
    positions = lax.broadcasted_iota(jnp.int32, shape, 0).astype(F32)
    freqs = 1.0 / 10000.0 ** (lax.rem(dim, half).astype(F32) * 2.0 / ROT)
    phase = positions * freqs
    cosine, sine = jnp.cos(phase), jnp.sin(phase)
    return (
        jnp.where(dim < ROT, cosine, 1.0),
        jnp.where(dim < half, -sine, jnp.where(dim < ROT, sine, 0.0)),
    )


def turn(x, tables, sign):
    half = ROT // 2
    dim = lax.rem(lax.broadcasted_iota(jnp.int32, x.shape, 1), HD)
    partner = jnp.where(dim < half, pltpu.roll(x, LANES - half, 1), pltpu.roll(x, half, 1))
    return x * tables[0] + sign * (partner * tables[1])


def lane_mask(rows, j):
    lane = lax.broadcasted_iota(jnp.int32, (rows, LANES), 1)
    return (lane // HD) == j


def forward_kernel(
    q_in, k_in, v_in, bias_ref, tab_ref, q_out, k_out, v_out, o_ref, lse_ref
):
    seq_len = q_in.shape[0]
    j = pl.program_id(1)

    @pl.when(j == 0)
    def _():
        tables = (tab_ref[0], tab_ref[1])
        q_out[...] = turn(q_in[...] + bias_ref[0, 0:1], tables, 1.0).astype(BF16)
        k_out[...] = turn(k_in[...] + bias_ref[0, 1:2], tables, 1.0).astype(BF16)
        v_out[...] = (v_in[...] + bias_ref[0, 2:3]).astype(BF16)

    mask = lane_mask(QB, j)
    causal = lax.broadcasted_iota(jnp.int32, (QB, QB), 0) <= lax.broadcasted_iota(
        jnp.int32, (QB, QB), 1
    )
    for i in range(seq_len // QB):
        rows = pl.ds(i * QB, QB)
        span = (i + 1) * QB
        q = q_out[rows, :] * 0.125
        q = jnp.where(mask, q, jnp.zeros_like(q))
        parts = []
        if i:
            parts.append(dot(k_out[pl.ds(0, i * QB), :], q, 1, 1))
        diag = dot(k_out[rows, :], q, 1, 1)
        parts.append(jnp.where(causal, diag, -1e30))
        top = functools.reduce(
            jnp.maximum, [jnp.max(s, axis=0, keepdims=True) for s in parts]
        )
        exps = [jnp.exp(s - top) for s in parts]
        total = sum(jnp.sum(e, axis=0, keepdims=True) for e in exps)
        inv = 1.0 / total
        probs = jnp.concatenate([(e * inv).astype(BF16) for e in exps], axis=0)
        out = dot(probs, v_out[pl.ds(0, span), :], 0, 0).astype(BF16)
        before = o_ref[rows, :]
        o_ref[rows, :] = jnp.where(mask, out, before)
        lse_ref[0, 0, :, i * QB : (i + 1) * QB] = top + jnp.log(total)


def backward_kernel(
    q_ref, k_ref, v_ref, do_ref, lse_ref, tab_ref, dq_out, dk_out, dv_out, sums_out, dq, dk, dv
):
    seq_len = q_ref.shape[0]
    j = pl.program_id(1)
    mask = lane_mask(QB, j)
    causal = lax.broadcasted_iota(jnp.int32, (QB, QB), 0) <= lax.broadcasted_iota(
        jnp.int32, (QB, QB), 1
    )

    @pl.when(j == 0)
    def _():
        dk[...] = jnp.zeros_like(dk)
        dv[...] = jnp.zeros_like(dv)

    for i in range(seq_len // QB):
        rows = pl.ds(i * QB, QB)
        q = q_ref[rows, :] * 0.125
        q = jnp.where(mask, q, jnp.zeros_like(q))
        do = do_ref[rows, :]
        do = jnp.where(mask, do, jnp.zeros_like(do))
        lse = lse_ref[0, 0, :, i * QB : (i + 1) * QB]
        pieces = []
        if i:
            pieces.append((pl.ds(0, i * QB), False))
        pieces.append((rows, True))
        probs, grads = [], []
        inner = 0.0
        for where, diagonal in pieces:
            s = dot(k_ref[where, :], q, 1, 1)
            if diagonal:
                s = jnp.where(causal, s, -1e30)
            p = jnp.exp(s - lse)
            dp = dot(v_ref[where, :], do, 1, 1)
            inner = inner + jnp.sum(p * dp, axis=0, keepdims=True)
            probs.append(p)
            grads.append(dp)
        acc = 0.0
        for (where, diagonal), p, dp in zip(pieces, probs, grads):
            ds = (p * (dp - inner)).astype(BF16)
            dv[where, :] += dot(p.astype(BF16), do, 1, 0)
            dk[where, :] += dot(ds, q, 1, 0)
            acc = acc + dot(ds, k_ref[where, :], 0, 0)
        before = dq[rows, :]
        dq[rows, :] = jnp.where(mask, acc * 0.125, before)

    @pl.when(j == pl.num_programs(1) - 1)
    def _():
        tables = (tab_ref[0], tab_ref[1])
        gq = turn(dq[...], tables, -1.0).astype(BF16)
        gk = turn(dk[...], tables, -1.0).astype(BF16)
        gv = dv[...].astype(BF16)
        dq_out[...] = gq
        dk_out[...] = gk
        dv_out[...] = gv
        sums_out[0, 0:1] = jnp.sum(gq.astype(F32), axis=0, keepdims=True)
        sums_out[0, 1:2] = jnp.sum(gk.astype(F32), axis=0, keepdims=True)
        sums_out[0, 2:3] = jnp.sum(gv.astype(F32), axis=0, keepdims=True)


def attention_forward(qkv, bias, tables):
    seq_len, width = qkv.shape[0], qkv.shape[1] // 3
    pairs = width // LANES
    column = lambda part: pl.BlockSpec((seq_len, LANES), lambda p, j: (0, part * pairs + p))
    block = pl.BlockSpec((seq_len, LANES), lambda p, j: (0, p))
    bias_blocks = bias.reshape(3, pairs, LANES).swapaxes(0, 1)
    wide = jax.ShapeDtypeStruct((seq_len, width), BF16)
    elements = pairs * 2 * seq_len * seq_len // 2
    return pl.pallas_call(
        forward_kernel,
        grid=(pairs, LANES // HD),
        in_specs=[
            column(0),
            column(1),
            column(2),
            pl.BlockSpec((1, 3, LANES), lambda p, j: (p, 0, 0)),
            pl.BlockSpec((2, seq_len, LANES), lambda p, j: (0, 0, 0)),
        ],
        out_specs=[
            block,
            block,
            block,
            block,
            pl.BlockSpec((1, 1, 1, seq_len), lambda p, j: (p, j, 0, 0)),
        ],
        out_shape=[
            wide,
            wide,
            wide,
            wide,
            jax.ShapeDtypeStruct((pairs, LANES // HD, 1, seq_len), F32),
        ],
        cost_estimate=pl.CostEstimate(
            flops=elements * 4 * LANES,
            bytes_accessed=qkv.size * 4 + 4 * seq_len * width * 2,
            transcendentals=elements,
        ),
        name="attention_forward",
    )(qkv, qkv, qkv, bias_blocks, tables)


def attention_backward(q, k, v, grad, lse, tables):
    seq_len, width = q.shape
    pairs = width // LANES
    block = pl.BlockSpec((seq_len, LANES), lambda p, j: (0, p))
    wide = jax.ShapeDtypeStruct((seq_len, width), BF16)
    elements = pairs * 2 * seq_len * seq_len // 2
    return pl.pallas_call(
        backward_kernel,
        grid=(pairs, LANES // HD),
        in_specs=[
            block,
            block,
            block,
            block,
            pl.BlockSpec((1, 1, 1, seq_len), lambda p, j: (p, j, 0, 0)),
            pl.BlockSpec((2, seq_len, LANES), lambda p, j: (0, 0, 0)),
        ],
        out_specs=[block, block, block, pl.BlockSpec((1, 3, LANES), lambda p, j: (p, 0, 0))],
        out_shape=[wide, wide, wide, jax.ShapeDtypeStruct((pairs, 3, LANES), F32)],
        scratch_shapes=[pltpu.VMEM((seq_len, LANES), F32)] * 3,
        cost_estimate=pl.CostEstimate(
            flops=elements * 10 * LANES,
            bytes_accessed=7 * seq_len * width * 2,
            transcendentals=elements,
        ),
        name="attention_backward",
    )(q, k, v, grad, lse, tables)


def pick(x, index):
    return lax.dynamic_index_in_dim(x, index, 0, keepdims=False)


class Cube:
    def __init__(self, axis, size):
        self.axis, self.size = axis, size
        self.bits = [b for b in range(size.bit_length()) if 1 << b < size]
        me = lax.axis_index(axis)
        self.own = [lax.rem(lax.div(me, 1 << b), 2) for b in self.bits]

    def swap(self, x, b):
        return lax.ppermute(x, self.axis, [(i, i ^ (1 << b)) for i in range(self.size)])

    def sum_all(self, x):
        for b in self.bits:
            x = x + self.swap(x, b)
        return x

    def contract(self, left, right):
        depth, rows = left.shape
        columns = right.shape[1]
        core, others = self.bits[0], self.bits[1:]
        half = rows // 2
        mine = self.own[0]
        first = lax.dynamic_slice_in_dim(left, (1 - mine) * half, half, 1)
        second = lax.dynamic_slice_in_dim(left, mine * half, half, 1)
        away = dot(first, right, 0, 0, BF16)
        came = self.swap(away, core)
        keep = dot(second, right, 0, 0, BF16)
        orders = [others, others[::-1]]
        quarter = half // 2
        done = []
        for n, order in enumerate(orders):
            small = quarter >> len(order)
            shape = (2,) * len(order) + (small, columns)
            cur = (
                keep[n * quarter : (n + 1) * quarter].astype(F32)
                + came[n * quarter : (n + 1) * quarter].astype(F32)
            ).reshape(shape)
            for b in order:
                own = self.own[b]
                send = pick(cur, 1 - own).astype(BF16)
                got = self.swap(send, b)
                cur = pick(cur, own) + got.astype(F32)
            buf = cur.astype(BF16)
            for b in order[::-1]:
                own = self.own[b]
                got = self.swap(buf, b)
                low = jnp.where(own == 0, buf, got)
                high = jnp.where(own == 0, got, buf)
                buf = jnp.stack([low, high])
            done.append(buf.reshape(quarter, columns))
        whole = jnp.concatenate(done, axis=0)
        other = self.swap(whole, core)
        low = jnp.where(mine == 0, whole, other)
        high = jnp.where(mine == 0, other, whole)
        return jnp.concatenate([low, high], axis=0).astype(F32)


LAG = 2
BLOCK = 128
PIECES = 16
WIDE = 256
STEP = 32
MESH = pl.DeviceIdType.MESH


class Places:
    def __init__(self, n_dp, n_z):
        self.me = lax.axis_index("dp")
        self.z = z = lax.axis_index("mp")
        self.core = lax.rem(self.me, 2)
        self.x = lax.rem(lax.div(self.me, 2), 2)
        self.y = lax.div(self.me, 4)
        self.core_peer = (self.me + 1 - 2 * self.core, z)
        self.x_peer = (self.me + 2 - 4 * self.x, z)
        self.y_peer = (self.me + 4 - 8 * self.y, z)
        self.dp_others = [lax.rem(self.me + n, n_dp) for n in range(1, n_dp)]
        self.dp_peers = [(other, z) for other in self.dp_others]
        self.z_of = [lax.rem(z + d, n_z) for d in range(n_z)]
        self.z_peers = [(self.me, to) for to in self.z_of]
        self.above = jnp.minimum(z + 1, n_z - 1)
        self.below = jnp.maximum(z - 1, 0)
        self.far = n_z - 1 - z
        self.has_above, self.has_below = z < n_z - 1, z > 0
        self.end = jnp.logical_or(z == 0, z == n_z - 1)
        self.inner = jnp.where(z == 0, 1, n_z - 2)
        self.middle = jnp.logical_not(self.end)
        self.order = [
            z,
            jnp.where(z == 0, 1, z - 1),
            jnp.where(z == 0, 2, jnp.where(z == 1, 2, jnp.where(z == 2, 3, 1))),
            jnp.where(z <= 1, 3, 0),
        ]


def rdma(src, dst, send_sem, recv_sem, peer):
    return pltpu.make_async_remote_copy(
        src_ref=src,
        dst_ref=dst,
        send_sem=send_sem,
        recv_sem=recv_sem,
        device_id=peer,
        device_id_type=MESH,
    )


def start(copies):
    for copy in copies:
        copy.start()


def wait(copies):
    for copy in copies:
        copy.wait()


def at_block(i, size):
    return pl.ds(pl.multiple_of(i * size, size), size)


def both(a, b):
    return jnp.logical_and(a, b)


def causal_block():
    key = lax.broadcasted_iota(jnp.int32, (QB, QB), 0)
    query = lax.broadcasted_iota(jnp.int32, (QB, QB), 1)
    return key <= query


def head_part(x, mask):
    return jnp.where(mask, x, jnp.zeros_like(x))


def attend_unit(u, qkv_v, attn_v, hat_v, lse_v, first_row):
    seq_len = qkv_v.shape[1]
    pair, j = lax.div(u, 2), lax.rem(u, 2)
    lanes = at_block(pair, LANES)
    mask = lane_mask(QB, j)
    causal = causal_block()
    for i in range(seq_len // QB):
        rows = pl.ds(i * QB, QB)
        q = head_part(qkv_v[0, rows, lanes] * 0.125, mask)
        parts = []
        if i:
            parts.append(dot(qkv_v[1, pl.ds(0, i * QB), lanes], q, 1, 1))
        parts.append(jnp.where(causal, dot(qkv_v[1, rows, lanes], q, 1, 1), -1e30))
        top = functools.reduce(
            jnp.maximum, [jnp.max(s, axis=0, keepdims=True) for s in parts]
        )
        exps = [jnp.exp(s - top) for s in parts]
        total = sum(jnp.sum(e, axis=0, keepdims=True) for e in exps)
        inv = 1.0 / total
        probs = jnp.concatenate([(e * inv).astype(BF16) for e in exps], axis=0)
        out = dot(probs, qkv_v[2, pl.ds(0, (i + 1) * QB), lanes], 0, 0).astype(BF16)
        attn_v[rows, lanes] = jnp.where(mask, out, attn_v[rows, lanes])
        lse_v[u, :, i * QB : (i + 1) * QB] = top + jnp.log(total)

    @pl.when(j == 1)
    def _():
        for i in range(seq_len // QB):
            rows = pl.ds(i * QB, QB)
            to = pl.ds(pl.multiple_of(first_row + pair * LANES, LANES), LANES)
            hat_v[to, rows] = jnp.transpose(attn_v[rows, lanes])


def attend_back_unit(u, qkv_v, do_v, lse_v, tab_v, dqkv_v, small, dq, dk, dv):
    seq_len, width = qkv_v.shape[1:]
    pair, j = lax.div(u, 2), lax.rem(u, 2)
    lanes = at_block(pair, LANES)
    mask = lane_mask(QB, j)
    causal = causal_block()

    @pl.when(j == 0)
    def _():
        dk[...] = jnp.zeros_like(dk)
        dv[...] = jnp.zeros_like(dv)
        dq[...] = jnp.zeros_like(dq)

    for i in range(seq_len // QB):
        rows = pl.ds(i * QB, QB)
        q = head_part(qkv_v[0, rows, lanes] * 0.125, mask)
        do = head_part(do_v[rows, lanes], mask)
        lse = lse_v[u, :, i * QB : (i + 1) * QB]
        pieces = [(pl.ds(0, i * QB), False)] if i else []
        pieces.append((rows, True))
        probs, grads = [], []
        inner = 0.0
        for where, diagonal in pieces:
            s = dot(qkv_v[1, where, lanes], q, 1, 1)
            if diagonal:
                s = jnp.where(causal, s, -1e30)
            p = jnp.exp(s - lse)
            dp = dot(qkv_v[2, where, lanes], do, 1, 1)
            inner = inner + jnp.sum(p * dp, axis=0, keepdims=True)
            probs.append(p)
            grads.append(dp)
        acc = 0.0
        for (where, diagonal), p, dp in zip(pieces, probs, grads):
            ds = (p * (dp - inner)).astype(BF16)
            dv[where, :] += dot(p.astype(BF16), do, 1, 0)
            dk[where, :] += dot(ds, q, 1, 0)
            acc = acc + dot(ds, qkv_v[1, where, lanes], 0, 0)
        dq[rows, :] = jnp.where(mask, acc * 0.125, dq[rows, :])

    @pl.when(j == 1)
    def _():
        tables = (tab_v[0], tab_v[1])
        out = (
            turn(dq[...], tables, -1.0).astype(BF16),
            turn(dk[...], tables, -1.0).astype(BF16),
            dv[...].astype(BF16),
        )
        for t, g in enumerate(out):
            dqkv_v[:, pl.ds(pl.multiple_of(t * width + pair * LANES, LANES), LANES)] = g
            small[2 + t : 3 + t, lanes] = jnp.sum(g.astype(F32), axis=0, keepdims=True)


def layer_kernel(
    n_dp, n_z, tokens, grad_out, table_c, table_s, w_gate_up, w_qkv, w_down, w_out, gain_ref, shift_ref, bias_ref,
    sums_out, layer_out, grad_tokens_out, gain_out, shift_out, bias_out, w_gate, w_up,
    lhs_v, dy_v, nrm, rhs, a1_v, a2_v, qkv_v, attn_v, hq_v, do_v, lse_v, tab_v, tok_v,
    wf, zsend, zin, zout, far_v, mid, own, small, small_in, share_in,
    acc, rcv0, rcv1, rcv2, fin,
    load, s_raw, s_wf, s_back, s_wd, s_wn, s_tok, b_sems, m_sems,
    n_send, n_recv, y_send, y_recv, z_sems, small_sems, share_sems,
    s0, s1, s2, s3, s4, s5, s_fin,
):
    at = Places(n_dp, n_z)
    seq_len, model = dy_v.shape
    own_rows = tok_v.shape[0]
    width = qkv_v.shape[2]
    local_ff = a1_v.shape[1]
    blocks_h, blocks_o = local_ff // BLOCK, width // BLOCK
    columns = model // WIDE
    n_d = columns
    n_g, n_q = blocks_h, 3 * width // WIDE
    total = n_d + n_g + n_q
    per = width // WIDE
    fill = n_g + n_q
    dy_chunks = y_recv.shape[1]
    dy_wide = model // dy_chunks
    units = width // HD

    dqkv_v = hq_v
    away_slots = LAG + 1
    own_slots = acc.shape[0] - away_slots
    hat_v, nt_v = lhs_v.at[0], lhs_v.at[1]

    def slot_of(buf, it):
        return lax.rem(it, own_slots if buf is acc else buf.shape[0])

    def quarter(bit, half):
        return half * 4 + bit * 2

    def stage0(it):
        sa, s = own_slots + lax.rem(it, away_slots), slot_of(rcv0, it)
        return [rdma(acc.at[sa], rcv0.at[s], s0.at[0, s], s0.at[1, s], at.core_peer)]

    def stage1(it):
        sa, s = slot_of(acc, it), slot_of(rcv1, it)
        a, b = pl.ds(quarter(1 - at.x, 0), 2), pl.ds(quarter(1 - at.y, 1), 2)
        return [
            rdma(acc.at[sa, a], rcv1.at[s, 0], s1.at[0, s], s1.at[1, s], at.x_peer),
            rdma(acc.at[sa, b], rcv1.at[s, 1], s1.at[2, s], s1.at[3, s], at.y_peer),
        ]

    def stage2(it):
        sa, s = slot_of(acc, it), slot_of(rcv2, it)
        a, b = quarter(at.x, 0) + 1 - at.y, quarter(at.y, 1) + 1 - at.x
        return [
            rdma(acc.at[sa, a], rcv2.at[s, 0], s2.at[0, s], s2.at[1, s], at.y_peer),
            rdma(acc.at[sa, b], rcv2.at[s, 1], s2.at[2, s], s2.at[3, s], at.x_peer),
        ]

    def piece_a():
        return at.core * 8 + quarter(at.x, 0) + at.y

    def piece_b():
        return at.core * 8 + quarter(at.y, 1) + at.x

    def stage3(it):
        s, n = slot_of(fin, it), lax.rem(it, s3.shape[1])
        a, b = sums_out.at[it, piece_a()], sums_out.at[it, piece_b()]
        return [
            rdma(fin.at[s, 0], a, s3.at[0, n], s3.at[1, n], at.y_peer),
            rdma(fin.at[s, 1], b, s3.at[2, n], s3.at[3, n], at.x_peer),
        ]

    def keep3(it):
        s = slot_of(fin, it)
        return [
            pltpu.make_async_copy(fin.at[s, 0], sums_out.at[it, piece_a()], s_fin.at[0, s]),
            pltpu.make_async_copy(fin.at[s, 1], sums_out.at[it, piece_b()], s_fin.at[1, s]),
        ]

    def stage4(it):
        n = lax.rem(it, s4.shape[1])
        a = sums_out.at[it, pl.ds(at.core * 8 + quarter(at.x, 0), 2)]
        b = sums_out.at[it, pl.ds(at.core * 8 + quarter(at.y, 1), 2)]
        return [
            rdma(a, a, s4.at[0, n], s4.at[1, n], at.x_peer),
            rdma(b, b, s4.at[2, n], s4.at[3, n], at.y_peer),
        ]

    def stage5(it):
        n = lax.rem(it, s5.shape[1])
        part = sums_out.at[it, pl.ds(at.core * 8, 8)]
        return [rdma(part, part, s5.at[0, n], s5.at[1, n], at.core_peer)]

    def product(it):
        left = jnp.where(it < n_d, 0, 1)

        @pl.when(it < n_d)
        def _():
            rhs[...] = dy_v[:, at_block(it, WIDE)]

        @pl.when(both(it >= n_d, it < n_d + n_g))
        def _():
            lanes = at_block(it - n_d, BLOCK)
            rhs[:, :BLOCK] = a1_v[:, lanes]
            rhs[:, BLOCK:] = a2_v[:, lanes]

        @pl.when(it >= n_d + n_g)
        def _():
            rhs[...] = dqkv_v[:, at_block(it - n_d - n_g, WIDE)]

        @pl.loop(0, 2)
        def _(h):
            which = jnp.where(h == 0, 1 - at.core, at.core)
            slot = jnp.where(h == 0, own_slots + lax.rem(it, away_slots), lax.rem(it, own_slots))
            tile = dot(lhs_v[left, at_block(which, 8 * BLOCK), :], rhs[...], 1, 0, BF16)
            for p in range(8):
                acc[slot, p] = tile[p * BLOCK : (p + 1) * BLOCK]

            @pl.when(h == 0)
            def _():
                start(stage0(it))

    def shard(origin):
        return at_block(origin, own_rows)

    def n_copy(kind, origin, to):
        rows = nrm.at[shard(origin)]
        return rdma(rows, rows, n_send.at[kind], n_recv.at[origin], (at.me, to))

    def y_copy(kind, origin, to, c):
        part = dy_v.at[shard(origin), at_block(c, dy_wide)]
        return rdma(part, part, y_send.at[kind, c], y_recv.at[origin, c], (at.me, to))

    def route(make, what):
        def when(condition, copy):
            @pl.when(condition)
            def _():
                getattr(copy, what)()

        def first():
            when(at.has_above, make(0, at.z, at.above))
            when(at.has_below, make(1, at.z, at.below))
            when(at.end, make(2, at.z, at.far))

        def passed(up):
            if up:
                when(at.middle, make(3, at.below, at.above))
            else:
                when(at.middle, make(4, at.above, at.below))

        return first, passed

    def n_arrived(origin):
        n_copy(0, origin, at.z_of[1]).wait_recv()

    def y_arrived(origin, c):
        y_copy(0, origin, at.z_of[1], c).wait_recv()

    def norm_rows(rows):
        tok = tok_v[rows, :].astype(F32)
        centered = tok - jnp.mean(tok, axis=1, keepdims=True)
        inv_std = lax.rsqrt(jnp.mean(centered * centered, axis=1, keepdims=True) + EPS)
        return centered * inv_std, inv_std

    gain = gain_ref[...].astype(F32).reshape(1, model)
    shift = shift_ref[...].astype(F32).reshape(1, model)

    def normalize():
        @pl.loop(0, own_rows // STEP)
        def _(r):
            xhat, _ = norm_rows(at_block(r, STEP))
            to = pl.ds(pl.multiple_of(at.z * own_rows + r * STEP, STEP), STEP)
            nrm[to, :] = (xhat * gain + shift).astype(BF16)

    def raw_copy(wint, f):
        s = lax.rem(f, 2)
        return pltpu.make_async_copy(
            w_gate_up.at[:, :, at_block(f, BLOCK)], wint.at[s], s_raw.at[s]
        )

    def back_copies(f):
        s = lax.rem(f, 2)
        return [
            pltpu.make_async_copy(
                wf.at[s, :, pl.ds(n * BLOCK, BLOCK)], w.at[:, at_block(f, BLOCK)], s_back.at[n, s]
            )
            for n, w in enumerate((w_gate, w_up))
        ]

    def pair_copies(f, s):
        return [
            pltpu.make_async_copy(
                w.at[:, at_block(f, BLOCK)], wf.at[s, :, pl.ds(n * BLOCK, BLOCK)], s_wf.at[n, s]
            )
            for n, w in enumerate((w_gate, w_up))
        ]

    def qkv_copies(m, s):
        return [
            pltpu.make_async_copy(
                w_qkv.at[lax.div(m, per), :, at_block(lax.rem(m, per), WIDE)], wf.at[s], s_wf.at[0, s]
            )
        ]

    def rows_of(rows):
        parts = [nrm[r, :] for r in rows]
        return parts[0] if len(parts) == 1 else jnp.concatenate(parts, axis=0)

    def hidden_tile(f, s, rows):
        product_of = dot(rows_of(rows), wf[s], 1, 0)
        lanes = at_block(f, BLOCK)
        for n, r in enumerate(rows):
            part = product_of[n * own_rows : (n + 1) * own_rows]
            g, u = part[:, :BLOCK], part[:, BLOCK:]
            sig = jax.nn.sigmoid(g)
            silu = g * sig
            h = (silu * u).astype(BF16)
            hq_v[r, lanes] = h
            hat_v[lanes, r] = jnp.transpose(h)
            a1_v[r, lanes] = (u * (sig + silu * (1.0 - sig))).astype(BF16)
            a2_v[r, lanes] = silu.astype(BF16)

    def qkv_tile(m, s, rows):
        t = lax.div(m, per)
        biases = bias_ref[...].astype(F32)
        bias = jnp.where(t == 0, biases[0:1], jnp.where(t == 1, biases[1:2], biases[2:3]))
        part = bias[:, :WIDE]
        for n in range(1, per):
            part = jnp.where(lax.rem(m, per) == n, bias[:, n * WIDE : (n + 1) * WIDE], part)
        product_of = dot(rows_of(rows), wf[s], 1, 0) + part
        for k, r in enumerate(rows):
            for n in range(WIDE // LANES):
                x = product_of[k * own_rows : (k + 1) * own_rows, n * LANES : (n + 1) * LANES]
                turned = turn(x, (tab_v[0, r, :], tab_v[1, r, :]), 1.0)
                lanes = pl.ds(pl.multiple_of(lax.rem(m, per) * WIDE + n * LANES, LANES), LANES)
                qkv_v[t, r, lanes] = jnp.where(t < 2, turned, x).astype(BF16)

    def turn_over(origin):
        rows = shard(origin)
        for n in range(columns):
            cols = pl.ds(n * WIDE, WIDE)
            nt_v[cols, rows] = jnp.transpose(nrm[rows, cols])

    def own_pass(wint):
        r = lax.broadcasted_iota(jnp.int32, (WIDE, WIDE), 0)
        c = lax.broadcasted_iota(jnp.int32, (WIDE, WIDE), 1)
        source = jnp.where(r < BLOCK, 2 * r, 2 * (r - BLOCK) + 1)
        parting = (source == c).astype(F32).astype(BF16)
        rows = shard(at.z)

        @pl.loop(0, n_g)
        def _(f):
            s = lax.rem(f, 2)

            @pl.when(f + 1 < n_g)
            def _():
                raw_copy(wint, f + 1).start()

            raw_copy(wint, f).wait()

            @pl.when(f >= 2)
            def _():
                wait(back_copies(f - 2))

            for n in range(model // BLOCK):
                part = pl.ds(n * BLOCK, BLOCK)
                raw = wint[s, part].reshape(WIDE, BLOCK)
                parted = dot(parting, raw, 1, 0, BF16)
                wf[s, part, :BLOCK] = parted[:BLOCK]
                wf[s, part, BLOCK:] = parted[BLOCK:]
            start(back_copies(f))
            hidden_tile(f, s, [rows])

        for f in (n_g - 2, n_g - 1):
            wait(back_copies(f))
        start(qkv_copies(0, n_g % 2))

        @pl.loop(0, n_q)
        def _(m):
            n = n_g + m
            s = lax.rem(n, 2)

            @pl.when(m + 1 < n_q)
            def _():
                start(qkv_copies(m + 1, 1 - s))

            @pl.when(m + 1 == n_q)
            def _():
                start(pair_copies(0, 1 - s))

            wait(qkv_copies(m, s))
            qkv_tile(m, s, [rows])

    def later_pass(k, origins, aside=None):
        rows = [shard(origin) for origin in origins]
        base = k * fill

        @pl.loop(0, n_g)
        def _(f):
            s = lax.rem(base + f, 2)

            @pl.when(f + 1 < n_g)
            def _():
                start(pair_copies(f + 1, 1 - s))

            @pl.when(f + 1 == n_g)
            def _():
                start(qkv_copies(0, 1 - s))

            if aside is not None:

                @pl.when(f == n_g - 1)
                def _():
                    aside()

            wait(pair_copies(f, s))
            hidden_tile(f, s, rows)

        @pl.loop(0, n_q)
        def _(m):
            s = lax.rem(base + n_g + m, 2)

            @pl.when(m + 1 < n_q)
            def _():
                start(qkv_copies(m + 1, 1 - s))

            if k < 2:

                @pl.when(m + 1 == n_q)
                def _():
                    start(pair_copies(0, 1 - s))

            wait(qkv_copies(m, s))
            qkv_tile(m, s, rows)

        for origin in origins:
            turn_over(origin)

    def straight(d):
        return {1: at.z != n_z - 1, 2: at.end, n_z - 1: at.z != 0}[d]

    def comes(d):
        return {1: at.z != 0, 2: at.z >= 0, n_z - 1: at.z != n_z - 1}[d]

    def under(condition, act):
        @pl.when(condition)
        def _():
            act()

    def z_copy(c, d, onward=False):
        columns_c = at_block(c, WIDE)
        src = far_v.at[:, columns_c] if onward else zsend.at[slot_of(zsend, c), shard(at.z_of[d])]
        dst = zin.at[d - 1, :, columns_c]
        return rdma(src, dst, z_sems.at[0, d - 1, c], z_sems.at[1, d - 1, c], at.z_peers[d])

    def mid_copy(c):
        src = zsend.at[slot_of(zsend, c), shard(at.far)]
        dst = mid.at[:, at_block(c, WIDE)]
        return rdma(src, dst, m_sems.at[0, c], m_sems.at[1, c], (at.me, at.inner))

    def z_out(c, what):
        for d in range(1, n_z):
            under(straight(d), getattr(z_copy(c, d), what))
        under(at.end, getattr(mid_copy(c), what))

    def far_job(c):
        @pl.when(at.middle)
        def _():
            mid_copy(c).wait_recv()
            cols = at_block(c, WIDE)
            far_v[:, cols] = (far_v[:, cols].astype(F32) + mid[:, cols].astype(F32)).astype(BF16)
            z_copy(c, 2, True).start()

    def branch_load(c):
        s = lax.rem(c, 2)
        cols = at_block(c, WIDE)
        return [
            pltpu.make_async_copy(
                w_down.at[:, cols], wf.at[s, pl.ds(0, local_ff)], s_wf.at[0, s]
            ),
            pltpu.make_async_copy(
                w_out.at[:, cols], wf.at[s, pl.ds(local_ff, width)], s_wf.at[1, s]
            ),
        ]

    def branch_job(c):
        s = lax.rem(c, 2)
        wait(branch_load(c))

        @pl.when(c + 1 < columns)
        def _():
            start(branch_load(c + 1))

        value = dot(hq_v[:, :local_ff], wf[s, :local_ff], 1, 0) + dot(
            attn_v[...], wf[s, local_ff : local_ff + width], 1, 0
        )
        nrm[:, at_block(c, WIDE)] = value.astype(BF16)

    def branch_copy(d):
        src, dst = nrm.at[shard(at.z_of[d])], zout.at[d - 1]
        return rdma(src, dst, b_sems.at[0, d - 1], b_sems.at[1, d - 1], at.z_peers[d])

    def branch_mid():
        return rdma(
            nrm.at[shard(at.far)], far_v, b_sems.at[0, n_z - 1], b_sems.at[1, n_z - 1],
            (at.me, at.inner),
        )

    def branch_first():
        under(at.end, lambda: branch_mid().start())

        @pl.when(at.middle)
        def _():
            for d in (1, n_z - 1):
                branch_copy(d).start()

    def branch_second():
        @pl.when(at.end)
        def _():
            for d in range(1, n_z):
                under(straight(d), branch_copy(d).start)

        @pl.when(at.middle)
        def _():
            branch_mid().wait_recv()

            @pl.loop(0, own_rows // STEP)
            def _(r):
                rows = at_block(r, STEP)
                to = pl.ds(pl.multiple_of(at.z_of[2] * own_rows + r * STEP, STEP), STEP)
                nrm[to, :] = (nrm[to, :].astype(F32) + far_v[rows, :].astype(F32)).astype(BF16)

            branch_copy(2).start()

    def layer_out_copy():
        return pltpu.make_async_copy(nrm.at[shard(at.z)], layer_out, s_tok.at[0])

    def layer_out_job():
        under(at.end, branch_mid().wait_send)
        under(at.middle, branch_copy(2).wait_send)
        for d in range(1, n_z):
            under(straight(d), branch_copy(d).wait_send)
            under(comes(d), branch_copy(d).wait_recv)

        @pl.loop(0, own_rows // STEP)
        def _(r):
            rows = at_block(r, STEP)
            here = pl.ds(pl.multiple_of(at.z * own_rows + r * STEP, STEP), STEP)
            value = tok_v[rows, :].astype(F32) + nrm[here, :].astype(F32)
            for n in range(n_z - 1):
                value = value + jnp.where(comes(n + 1), zout[n, rows, :].astype(F32), 0.0)
            nrm[here, :] = value.astype(BF16)

        layer_out_copy().start()

    def hidden_load(g, wd):
        def one(n, what):
            b = 2 * g + n
            dst = wd.at[pl.ds(n * BLOCK, BLOCK)]

            @pl.when(b < blocks_h)
            def _():
                rows = at_block(jnp.minimum(b, blocks_h - 1), BLOCK)
                getattr(pltpu.make_async_copy(w_down.at[rows], dst, s_wd.at[n]), what)()

            @pl.when(both(b >= blocks_h, b < blocks_h + blocks_o))
            def _():
                rows = at_block(jnp.clip(b - blocks_h, 0, blocks_o - 1), BLOCK)
                getattr(pltpu.make_async_copy(w_out.at[rows], dst, s_wd.at[n]), what)()

        return one

    def hidden_job(g, wd):
        for n in range(2):
            hidden_load(g, wd)(n, "wait")
        dh = dot(dy_v[...], wd[...], 1, 1)
        for n in range(2):
            b = 2 * g + n
            part = dh[:, n * BLOCK : (n + 1) * BLOCK]

            @pl.when(b < blocks_h)
            def _(part=part, b=b):
                lanes = at_block(jnp.minimum(b, blocks_h - 1), BLOCK)
                a1_v[:, lanes] = (part * a1_v[:, lanes].astype(F32)).astype(BF16)
                a2_v[:, lanes] = (part * a2_v[:, lanes].astype(F32)).astype(BF16)

            @pl.when(both(b >= blocks_h, b < blocks_h + blocks_o))
            def _(part=part, b=b):
                do_v[:, at_block(jnp.clip(b - blocks_h, 0, blocks_o - 1), BLOCK)] = part.astype(BF16)

    def normed_load(c, wg, wu, wq):
        rows = at_block(c, WIDE)
        return [
            pltpu.make_async_copy(w_gate.at[rows], wg, s_wn.at[0]),
            pltpu.make_async_copy(w_up.at[rows], wu, s_wn.at[1]),
            pltpu.make_async_copy(w_qkv.at[:, rows], wq, s_wn.at[2]),
        ]

    def normed_job(c, wg, wu, wq):
        wait(normed_load(c, wg, wu, wq))
        part = dot(a1_v[...], wg[...], 1, 1) + dot(a2_v[...], wu[...], 1, 1)
        for t in range(3):
            part = part + dot(dqkv_v[:, t * width : (t + 1) * width], wq[t], 1, 1)
        s = slot_of(zsend, c)

        @pl.when(c >= zsend.shape[0])
        def _():
            z_out(c - zsend.shape[0], "wait_send")

        zsend[s] = part.astype(BF16)
        z_out(c, "start")

        @pl.when(at.middle)
        def _():
            far_v[:, at_block(c, WIDE)] = zsend[s, shard(at.z_of[2]), :]

        @pl.when(c + 1 < columns)
        def _():
            start(normed_load(c + 1, wg, wu, wq))

        own[:, at_block(c, WIDE)] = zsend[s, shard(at.z), :]

    def tokens_copy():
        return pltpu.make_async_copy(tok_v, grad_tokens_out, s_tok.at[1])

    def norm_job():
        @pl.loop(0, columns)
        def _(c):
            @pl.when(c >= columns - zsend.shape[0])
            def _():
                z_out(c, "wait_send")

            under(at.middle, z_copy(c, 2, True).wait_send)
            for d in range(1, n_z):
                under(comes(d), z_copy(c, d).wait_recv)

        @pl.loop(0, own_rows // STEP)
        def _(r):
            rows = at_block(r, STEP)
            d = own[rows, :].astype(F32)
            for n in range(n_z - 1):
                d = d + jnp.where(comes(n + 1), zin[n, rows, :].astype(F32), 0.0)
            xhat, inv_std = norm_rows(rows)
            scaled = d * gain
            here = pl.ds(pl.multiple_of(at.z * own_rows + r * STEP, STEP), STEP)
            out = dy_v[here, :].astype(F32) + inv_std * (
                scaled
                - jnp.mean(scaled, axis=1, keepdims=True)
                - xhat * jnp.mean(scaled * xhat, axis=1, keepdims=True)
            )
            small[0:1, :] += jnp.sum(d * xhat, axis=0, keepdims=True)
            small[1:2, :] += jnp.sum(d, axis=0, keepdims=True)
            tok_v[rows, :] = out.astype(BF16)

        tokens_copy().start()

    share = model // n_z

    def share_copies():
        return [
            rdma(
                small.at[:, at_block(at.z_of[d], share)],
                share_in.at[d - 1],
                share_sems.at[0, d - 1],
                share_sems.at[1, d - 1],
                at.z_peers[d],
            )
            for d in range(1, n_z)
        ]

    def spread_copies():
        return [
            rdma(
                small_in.at[at.me],
                small_in.at[at.me],
                small_sems.at[0, n],
                small_sems.at[1, at.me],
                peer,
            )
            for n, peer in enumerate(at.dp_peers)
        ]

    def small_spread():
        wait(share_copies())
        mine = small[0:2, at_block(at.z, share)]
        for n in range(n_z - 1):
            mine = mine + share_in[n, 0:2, :]
        small_in[at.me] = small[:, 0:share]
        small_in[at.me, 0:2, :] = mine
        start(spread_copies())

    def small_end():
        for copy in spread_copies():
            copy.wait_send()
        for n, source in enumerate(at.dp_others):
            rdma(
                small_in.at[source], small_in.at[source], small_sems.at[0, n],
                small_sems.at[1, source], at.dp_peers[n],
            ).wait_recv()
        value = small_in[0]
        for n in range(1, small_in.shape[0]):
            value = value + small_in[n]
        gain_out[...] = value[0]
        shift_out[...] = value[1]
        bias_out[...] = value[2:5]

    loads = [
        pltpu.make_async_copy(tokens, tok_v, load.at[0]),
        pltpu.make_async_copy(grad_out, dy_v.at[shard(at.z)], load.at[1]),
        pltpu.make_async_copy(table_c, tab_v.at[0], load.at[2]),
        pltpu.make_async_copy(table_s, tab_v.at[1], load.at[3]),
    ]
    start(loads)
    barrier = pltpu.get_barrier_semaphore()
    peers = at.dp_peers + at.z_peers[1:]
    for peer in peers:
        pl.semaphore_signal(barrier, inc=1, device_id=peer, device_id_type=MESH)
    loads[0].wait()
    normalize()
    pl.semaphore_wait(barrier, len(peers))

    def forward(wint):
        raw_copy(wint, 0).start()
        route(n_copy, "start")[0]()
        small[...] = jnp.zeros_like(small)
        rest = model - local_ff
        hat_v[pl.ds(local_ff, rest), :] = jnp.zeros((rest, seq_len), BF16)
        loads[2].wait()
        loads[3].wait()
        own_pass(wint)
        turn_over(at.z)

    pl.run_scoped(forward, pltpu.VMEM((2, model, 2, BLOCK), BF16))
    o1, o2, o3 = at.order[1:]
    n_arrived(o1)
    onward = route(n_copy, "start")[1]

    @pl.when(at.middle)
    def _():
        n_arrived(o2)
        onward(True)
        onward(False)
        later_pass(1, [o1, o2])
        n_arrived(o3)

    @pl.when(at.end)
    def _():
        later_pass(1, [o1])
        n_arrived(o2)
        n_arrived(o3)

    def dy_route(c, what):
        return route(lambda *a: y_copy(*a, c), what)

    def send_dy(c):
        dy_route(c, "start")[0]()

    def pass_dy_on(c):
        @pl.when(at.middle)
        def _():
            y_arrived(o1, c)
            y_arrived(o2, c)

        onward = dy_route(c, "start")[1]
        onward(True)
        onward(False)

    def rest_of_dy(c):
        y_arrived(o3, c)

        @pl.when(at.end)
        def _():
            y_arrived(o1, c)
            y_arrived(o2, c)

    loads[1].wait()
    send_dy(0)

    @pl.when(at.middle)
    def _():
        later_pass(2, [o3], lambda: send_dy(1))

    @pl.when(at.end)
    def _():
        later_pass(2, [o2, o3], lambda: send_dy(1))

    start(branch_load(0))
    pass_dy_on(0)

    first, passed = route(n_copy, "wait_send")
    first()
    passed(True)
    passed(False)

    def attend(first, count):
        @pl.loop(first, first + count)
        def _(u):
            attend_unit(u, qkv_v, attn_v, hat_v, lse_v, local_ff)

    attend(0, units // 2)
    pass_dy_on(1)
    send_dy(2)
    attend(units // 2, units - units // 2)

    early = [0, 1, 2, 3, 6, 7]
    behind = 4
    branches = {4: 0, 5: 2, 8: 4, 9: 6}

    def meanwhile(tick):
        for t, c in ((2, 2), (5, 3)):

            @pl.when(tick == t)
            def _(c=c):
                pass_dy_on(c)
                if c + 1 < dy_chunks:
                    send_dy(c + 1)

        from_, to = 0, 0
        for t, c in branches.items():
            from_ = jnp.where(tick == t, c, from_)
            to = jnp.where(tick == t, c + 2, to)

        @pl.loop(from_, to)
        def _(c):
            branch_job(c)

        for t, c in ((0, 0), (2, 1), (6, 2), (10, 3)):

            @pl.when(tick == t)
            def _(c=c):
                rest_of_dy(c)

    def item_at(tick):
        it = tick - behind
        for n, t in enumerate(early):
            it = jnp.where(tick == t, n, it)
        return it

    def live(tick):
        ready_tick = both(tick >= len(early) + behind, tick < total + behind)
        for t in early:
            ready_tick = jnp.logical_or(ready_tick, tick == t)
        return ready_tick

    hidden_jobs = -(-(blocks_h + blocks_o) // 2)
    split = blocks_h // 2
    hidden_at = len(early) + behind
    back_at = hidden_at + 2 + hidden_jobs - split
    normed_at = max(back_at + units // 2 + units // 4, hidden_at + hidden_jobs)
    out_at = normed_at + 4
    norm_at = normed_at + columns + 3

    def hidden_index(n):
        late = hidden_jobs - split
        return jnp.where(n < 2, n, jnp.where(n < late + 2, n + split - 2, n - late))

    def ticks(wide, wq, dq, dk, dv):
        wd = wide.at[0]
        wg, wu = wide.at[0, :, pl.ds(0, local_ff)], wide.at[1, :, pl.ds(0, local_ff)]

        for n in range(2):
            hidden_load(hidden_index(0), wd)(n, "start")

        @pl.loop(0, total + behind + 6 * LAG)
        def _(tick):
            one = item_at(tick - LAG)

            @pl.when(live(tick - LAG))
            def _():
                wait(stage0(one))
                sa, s = slot_of(acc, one), slot_of(rcv0, one)

                @pl.loop(0, 8)
                def _(p):
                    acc[sa, p] = (acc[sa, p].astype(F32) + rcv0[s, p].astype(F32)).astype(BF16)

                start(stage1(one))

            two = item_at(tick - 2 * LAG)

            @pl.when(live(tick - 2 * LAG))
            def _():
                wait(stage1(two))
                sa, s = slot_of(acc, two), slot_of(rcv1, two)
                for n, bit in ((0, at.x), (1, at.y)):
                    for m in range(2):
                        p = quarter(bit, n) + m
                        acc[sa, p] = (
                            acc[sa, p].astype(F32) + rcv1[s, n, m].astype(F32)
                        ).astype(BF16)
                start(stage2(two))

            three = item_at(tick - 3 * LAG)

            @pl.when(live(tick - 3 * LAG))
            def _():
                wait(stage2(three))
                sa, s, d = slot_of(acc, three), slot_of(rcv2, three), slot_of(fin, three)
                for n, p in ((0, quarter(at.x, 0) + at.y), (1, quarter(at.y, 1) + at.x)):
                    fin[d, n] = (acc[sa, p].astype(F32) + rcv2[s, n].astype(F32)).astype(BF16)
                start(stage3(three))
                start(keep3(three))

            four = item_at(tick - 4 * LAG)

            @pl.when(live(tick - 4 * LAG))
            def _():
                wait(keep3(four))
                wait(stage3(four))
                start(stage4(four))

            five = item_at(tick - 5 * LAG)

            @pl.when(live(tick - 5 * LAG))
            def _():
                wait(stage4(five))
                start(stage5(five))

            six = item_at(tick - 6 * LAG)

            @pl.when(live(tick - 6 * LAG))
            def _():
                wait(stage5(six))

            meanwhile(tick)
            item = item_at(tick)

            @pl.when(live(tick))
            def _():
                product(item)

            @pl.when(tick == hidden_at)
            def _():
                branch_first()

            @pl.when(tick == hidden_at + 4)
            def _():
                branch_second()

            @pl.when(both(tick >= hidden_at, tick < hidden_at + hidden_jobs))
            def _():
                n = tick - hidden_at
                hidden_job(hidden_index(n), wd)

                @pl.when(n + 1 < hidden_jobs)
                def _():
                    for m in range(2):
                        hidden_load(hidden_index(n + 1), wd)(m, "start")

            half = units // 2
            first = tick - back_at + jnp.clip(tick - back_at - half, 0, half)
            count = jnp.where(tick - back_at < half, 1, 2)

            @pl.loop(first, jnp.where(both(first >= 0, first < units), first + count, first))
            def _(u):
                attend_back_unit(
                    u, qkv_v, do_v, lse_v, tab_v, dqkv_v, small, dq, dk, dv
                )

            @pl.when(tick == normed_at - 1)
            def _():
                start(normed_load(0, wg, wu, wq))

            @pl.when(both(tick >= normed_at, tick < normed_at + columns))
            def _():
                normed_job(tick - normed_at, wg, wu, wq)

            @pl.when(both(tick >= normed_at + 1, tick < normed_at + 1 + columns))
            def _():
                far_job(tick - normed_at - 1)

            @pl.when(tick == out_at)
            def _():
                layer_out_job()
                for c in range(dy_chunks):
                    first, passed = dy_route(c, "wait_send")
                    first()
                    passed(True)
                    passed(False)

            @pl.when(tick == norm_at)
            def _():
                norm_job()
                start(share_copies())

            @pl.when(tick == norm_at + 2)
            def _():
                small_spread()

            @pl.when(tick == norm_at + 5)
            def _():
                small_end()
                tokens_copy().wait()
                layer_out_copy().wait()

    pl.run_scoped(
        ticks,
        pltpu.VMEM((2, WIDE, model), BF16),
        pltpu.VMEM((3, WIDE, width), BF16),
        *[pltpu.VMEM((seq_len, LANES), F32)] * 3,
    )


def run_layer(
    tokens, grad_out, tables, w_gate_up, w_qkv, w_down, w_out, gain, shift, bias, n_dp, n_z
):
    own, model = tokens.shape
    seq_len = own * n_z
    local_ff, width = w_down.shape[0], w_out.shape[0]
    columns = model // WIDE
    total = columns + local_ff // BLOCK + 3 * width // WIDE
    bf = lambda *shape: pltpu.VMEM(shape, BF16)
    fl = lambda *shape: pltpu.VMEM(shape, F32)
    sems = lambda *shape: pltpu.SemaphoreType.DMA(shape)
    slots = 2 * LAG + 2
    dy_chunks = 4
    hbm = pl.BlockSpec(memory_space=pl.ANY)
    vmem = pl.BlockSpec(memory_space=pltpu.VMEM)
    return pl.pallas_call(
        functools.partial(layer_kernel, n_dp, n_z),
        in_specs=[hbm] * 8 + [vmem] * 3,
        out_specs=[hbm, hbm, hbm, vmem, vmem, vmem, hbm, hbm],
        out_shape=[
            jax.ShapeDtypeStruct((total, PIECES, BLOCK, WIDE), BF16),
            jax.ShapeDtypeStruct((own, model), BF16),
            jax.ShapeDtypeStruct((own, model), BF16),
            jax.ShapeDtypeStruct((model // n_z,), F32),
            jax.ShapeDtypeStruct((model // n_z,), F32),
            jax.ShapeDtypeStruct((3, width), F32),
            jax.ShapeDtypeStruct((model, local_ff), BF16),
            jax.ShapeDtypeStruct((model, local_ff), BF16),
        ],
        scratch_shapes=[
            bf(2, model, seq_len), bf(seq_len, model), bf(seq_len, model), bf(seq_len, WIDE),
            bf(seq_len, local_ff), bf(seq_len, local_ff),
            bf(3, seq_len, width), bf(seq_len, width), bf(seq_len, max(local_ff, 3 * width)),
            bf(seq_len, width), fl(width // HD, 1, seq_len), fl(2, seq_len, LANES), bf(own, model),
            bf(2, model, WIDE), bf(3, seq_len, WIDE), bf(n_z - 1, own, model), bf(n_z - 1, own, model), bf(own, model), bf(own, model), bf(own, model),
            fl(8, model), fl(n_dp, 8, model // n_z), fl(n_z - 1, 8, model // n_z),
            bf(4 * LAG + 2, 8, BLOCK, WIDE),
            bf(slots - 1, 8, BLOCK, WIDE), bf(slots, 2, 2, BLOCK, WIDE), bf(slots, 2, BLOCK, WIDE),
            bf(LAG + 1, 2, BLOCK, WIDE),
            sems(4), sems(2), sems(2, 2), sems(2, 2), sems(2), sems(3), sems(2),
            sems(2, n_z), sems(2, columns),
            sems(5), sems(n_z), sems(5, dy_chunks), sems(n_z, dy_chunks),
            sems(2, n_z - 1, columns), sems(2, n_dp), sems(2, n_z - 1),
            sems(2, slots), sems(4, slots), sems(4, slots),
            sems(4, slots), sems(4, slots), sems(2, slots), sems(2, LAG + 1),
        ],
        compiler_params=pltpu.CompilerParams(
            collective_id=0, has_side_effects=True, vmem_limit_bytes=67043328
        ),
        name="layer",
    )(tokens, grad_out, *tables, w_gate_up, w_qkv, w_down, w_out, gain, shift, bias)


def unpack_kernel(n_d, n_g, item_ref, *refs):
    passed = len(refs) // 2 - 2
    kept, (down, out, gate_up, qkv), outs = refs[:passed], refs[passed : passed + 4], refs[passed + 4 :]
    i = pl.program_id(0)
    n_down = down.shape[0] // BLOCK
    for src, dst in zip(kept, outs):
        dst[...] = src[...]

    def rows(p):
        return pl.ds(p * BLOCK, BLOCK)

    @pl.when(i < n_d)
    def _():
        for p in range(n_down):
            down[rows(p), :] = item_ref[0, p].astype(F32)
        for p in range(out.shape[0] // BLOCK):
            out[rows(p), :] = item_ref[0, n_down + p].astype(F32)

    @pl.when(both(i >= n_d, i < n_d + n_g))
    def _():
        flat = gate_up.reshape(2 * gate_up.shape[0], BLOCK)
        for p in range(PIECES):
            value = item_ref[0, p].astype(F32)
            for n in range(2):
                flat[pl.ds(2 * p * BLOCK + n, BLOCK, stride=2), :] = value[
                    :, n * BLOCK : (n + 1) * BLOCK
                ]

    @pl.when(i >= n_d + n_g)
    def _():
        for p in range(PIECES):
            qkv[0, rows(p), :] = item_ref[0, p].astype(F32)


def unpack(items, kept, local_ff, width, model):
    n_d, n_g, n_q = model // WIDE, local_ff // BLOCK, 3 * width // WIDE
    per = n_q // 3

    def of_d(i):
        return (0, jnp.minimum(i, n_d - 1))

    def of_q(i):
        q = jnp.maximum(i - n_d - n_g, 0)
        return (lax.div(q, per), 0, lax.rem(q, per))

    def whole(x):
        if x.ndim == 2 and x.shape[0] % 256 == 0:
            return pl.BlockSpec((x.shape[0] // 16, x.shape[1]), lambda i: (jnp.minimum(i, 15), 0))
        return pl.BlockSpec(x.shape, lambda i: (0,) * x.ndim)

    down, out, gate_up, qkv, *kept = pl.pallas_call(
        functools.partial(unpack_kernel, n_d, n_g),
        grid=(n_d + n_g + n_q,),
        in_specs=[
            pl.BlockSpec((1, PIECES, BLOCK, WIDE), lambda i: (i, 0, 0, 0)),
            *[whole(x) for x in kept],
        ],
        out_specs=[
            pl.BlockSpec((local_ff, WIDE), of_d),
            pl.BlockSpec((width, WIDE), of_d),
            pl.BlockSpec((model, 2, BLOCK), lambda i: (0, 0, jnp.clip(i - n_d, 0, n_g - 1))),
            pl.BlockSpec((1, model, WIDE), of_q),
            *[whole(x) for x in kept],
        ],
        out_shape=[
            jax.ShapeDtypeStruct((local_ff, model), F32),
            jax.ShapeDtypeStruct((width, model), F32),
            jax.ShapeDtypeStruct((model, 2, local_ff), F32),
            jax.ShapeDtypeStruct((3, model, width), F32),
            *[jax.ShapeDtypeStruct(x.shape, x.dtype) for x in kept],
        ],
        name="unpack",
    )(items, *kept)
    return (down, out, gate_up, qkv.transpose(1, 0, 2), *kept)


def fast_path(n_dp, n_mp, rows, model_width, local_width, local_ff):
    blocks_h, blocks_o = local_ff // BLOCK, local_width // BLOCK
    return (
        n_dp == 8
        and n_mp == 4
        and rows == QB
        and model_width == PIECES * BLOCK
        and local_width == model_width // n_mp
        and local_ff % BLOCK == 0
        and blocks_h % 2 == 1
        and blocks_h + blocks_o < PIECES
    )


def fused_layer(
    n_dp,
    n_mp,
    tables,
    tokens,
    norm_gain,
    layernorm_bias,
    qkv_weight,
    qkv_bias,
    out_weight,
    gate_up_weight,
    down_weight,
    grad_out,
):
    model_width = tokens.shape[1]
    local_width, local_ff = qkv_weight.shape[2], gate_up_weight.shape[2]
    items, *kept = run_layer(
        tokens,
        grad_out,
        tables,
        gate_up_weight,
        qkv_weight.transpose(1, 0, 2),
        down_weight,
        out_weight,
        norm_gain,
        layernorm_bias,
        qkv_bias,
        n_dp,
        n_mp,
    )
    grad_down_w, grad_out_w, grad_gate_up_w, grad_qkv_w, *kept = unpack(
        items, kept[:5], local_ff, local_width, model_width
    )
    layer_out, grad_tokens, grad_gain, grad_shift, grad_bias = kept
    return (
        layer_out,
        grad_tokens,
        grad_gain,
        grad_shift,
        grad_qkv_w,
        grad_bias,
        grad_out_w,
        grad_gate_up_w,
        grad_down_w,
    )


def on_device(
    n_dp,
    n_mp,
    tokens,
    norm_gain,
    layernorm_bias,
    qkv_weight,
    qkv_bias,
    out_weight,
    gate_up_weight,
    down_weight,
    grad_out,
):
    rows, model_width = tokens.shape
    local_width = qkv_weight.shape[2]
    seq_len = rows * n_mp
    tables = rotary_tables(seq_len)
    if fast_path(n_dp, n_mp, rows, model_width, local_width, gate_up_weight.shape[2]):
        return fused_layer(
            n_dp, n_mp, tables, tokens, norm_gain, layernorm_bias, qkv_weight, qkv_bias, out_weight,
            gate_up_weight, down_weight, grad_out,
        )
    cube = Cube("dp", n_dp)
    tables = jnp.stack(tables)
    gain = norm_gain.astype(F32)
    token_f32 = tokens.astype(F32)
    row_mean = jnp.mean(token_f32, axis=1, keepdims=True)
    centered = token_f32 - row_mean
    inv_std = lax.rsqrt(jnp.mean(centered * centered, axis=1, keepdims=True) + EPS)
    xhat = centered * inv_std
    normed_own = (xhat * gain + layernorm_bias.astype(F32)).astype(BF16)
    normed = lax.all_gather(normed_own, "mp", axis=0, tiled=True)
    dy = lax.all_gather(grad_out, "mp", axis=0, tiled=True)

    w_qkv = [qkv_weight[:, t, :] for t in range(3)]
    w_gate, w_up = gate_up_weight[:, 0, :], gate_up_weight[:, 1, :]

    gate = dot(normed, w_gate, 1, 0)
    up = dot(normed, w_up, 1, 0)
    sig = jax.nn.sigmoid(gate)
    hidden = (gate * sig * up).astype(BF16)
    qkv = jnp.concatenate([dot(normed, w, 1, 0) for w in w_qkv], axis=1)
    q, k, v, attended, lse = attention_forward(qkv, qkv_bias.astype(F32), tables)
    branch = (dot(attended, out_weight, 1, 0) + dot(hidden, down_weight, 1, 0)).astype(BF16)
    share = lax.psum_scatter(branch, "mp", scatter_dimension=0, tiled=True)
    layer_out = (token_f32 + share.astype(F32)).astype(BF16)

    share_width = model_width // n_mp
    d_hidden = dot(dy, down_weight, 1, 1)
    silu = gate * sig
    d_gate = (d_hidden * up * (sig + silu * (1.0 - sig))).astype(BF16)
    d_up = (d_hidden * silu).astype(BF16)
    d_attended = dot(dy, out_weight, 1, 1, BF16)
    dq, dk, dv, sums = attention_backward(q, k, v, d_attended, lse, tables)
    d_normed = (
        dot(d_gate, w_gate, 1, 1)
        + dot(d_up, w_up, 1, 1)
        + dot(dq, w_qkv[0], 1, 1)
        + dot(dk, w_qkv[1], 1, 1)
        + dot(dv, w_qkv[2], 1, 1)
    ).astype(BF16)
    d_own = lax.psum_scatter(d_normed, "mp", scatter_dimension=0, tiled=True).astype(F32)
    d_qkv = jnp.concatenate([dq, dk, dv], axis=1)
    grad_down_w = cube.contract(hidden, dy)
    grad_out_w = cube.contract(attended, dy)
    grad_gate_up_w = jnp.stack(
        [cube.contract(normed, d_gate), cube.contract(normed, d_up)], axis=1
    )
    grad_qkv_w = cube.contract(normed, d_qkv).reshape(model_width, 3, local_width)

    scaled = d_own * gain
    grad_tokens = grad_out.astype(F32) + inv_std * (
        scaled
        - jnp.mean(scaled, axis=1, keepdims=True)
        - xhat * jnp.mean(scaled * xhat, axis=1, keepdims=True)
    )
    terms = jnp.stack([jnp.sum(d_own * xhat, axis=0), jnp.sum(d_own, axis=0)])
    bias_sum = cube.sum_all(sums)
    grad_bias = bias_sum.swapaxes(0, 1).reshape(3, local_width)
    terms = Cube("mp", n_mp).sum_all(cube.sum_all(terms))
    terms = lax.dynamic_slice_in_dim(
        terms, lax.axis_index("mp") * share_width, share_width, 1
    )
    return (
        layer_out,
        grad_tokens.astype(BF16),
        terms[0],
        terms[1],
        grad_qkv_w,
        grad_bias,
        grad_out_w,
        grad_gate_up_w,
        grad_down_w,
    )


def solution(mesh):
    return jax.shard_map(
        functools.partial(on_device, mesh.shape["dp"], mesh.shape["mp"]),
        mesh=mesh,
        in_specs=(
            P(("dp", "mp"), None),
            P(),
            P(),
            P(None, None, "mp"),
            P(None, "mp"),
            P("mp", None),
            P(None, None, "mp"),
            P("mp", None),
            P(("dp", "mp"), None),
        ),
        out_specs=(
            P(("dp", "mp"), None),
            P(("dp", "mp"), None),
            P("mp"),
            P("mp"),
            P(None, None, "mp"),
            P(None, "mp"),
            P("mp", None),
            P(None, None, "mp"),
            P("mp", None),
        ),
        check_vma=False,
    )
```

```python
import functools
import math

import jax
import jax.numpy as jnp
from jax import lax
from jax.experimental import pallas as pl
from jax.experimental.pallas import tpu as pltpu
from jax.sharding import PartitionSpec as P

HD = 64
ROT = 16
EPS = 1e-05
LANES = 128
QB = 256


F32 = jnp.float32
BF16 = jnp.bfloat16


def dot(a, b, ca, cb, out=F32):
    return lax.dot_general(
        a, b, (((ca,), (cb,)), ((), ())), preferred_element_type=F32
    ).astype(out)


def rotary_tables(seq_len):
    half = ROT // 2
    shape = (seq_len, LANES)
    dim = lax.rem(lax.broadcasted_iota(jnp.int32, shape, 1), HD)
    positions = lax.broadcasted_iota(jnp.int32, shape, 0).astype(F32)
    freqs = 1.0 / 10000.0 ** (lax.rem(dim, half).astype(F32) * 2.0 / ROT)
    phase = positions * freqs
    cosine, sine = jnp.cos(phase), jnp.sin(phase)
    return (
        jnp.where(dim < ROT, cosine, 1.0),
        jnp.where(dim < half, -sine, jnp.where(dim < ROT, sine, 0.0)),
    )


def turn(x, tables, sign):
    half = ROT // 2
    dim = lax.rem(lax.broadcasted_iota(jnp.int32, x.shape, 1), HD)
    partner = jnp.where(dim < half, pltpu.roll(x, LANES - half, 1), pltpu.roll(x, half, 1))
    return x * tables[0] + sign * (partner * tables[1])


def lane_mask(rows, j):
    lane = lax.broadcasted_iota(jnp.int32, (rows, LANES), 1)
    return (lane // HD) == j


def forward_kernel(
    q_in, k_in, v_in, bias_ref, tab_ref, q_out, k_out, v_out, o_ref, lse_ref
):
    seq_len = q_in.shape[0]
    j = pl.program_id(1)

    @pl.when(j == 0)
    def _():
        tables = (tab_ref[0], tab_ref[1])
        q_out[...] = turn(q_in[...] + bias_ref[0, 0:1], tables, 1.0).astype(BF16)
        k_out[...] = turn(k_in[...] + bias_ref[0, 1:2], tables, 1.0).astype(BF16)
        v_out[...] = (v_in[...] + bias_ref[0, 2:3]).astype(BF16)

    mask = lane_mask(QB, j)
    causal = lax.broadcasted_iota(jnp.int32, (QB, QB), 0) <= lax.broadcasted_iota(
        jnp.int32, (QB, QB), 1
    )
    for i in range(seq_len // QB):
        rows = pl.ds(i * QB, QB)
        span = (i + 1) * QB
        q = q_out[rows, :] * 0.125
        q = jnp.where(mask, q, jnp.zeros_like(q))
        parts = []
        if i:
            parts.append(dot(k_out[pl.ds(0, i * QB), :], q, 1, 1))
        diag = dot(k_out[rows, :], q, 1, 1)
        parts.append(jnp.where(causal, diag, -1e30))
        top = functools.reduce(
            jnp.maximum, [jnp.max(s, axis=0, keepdims=True) for s in parts]
        )
        exps = [jnp.exp(s - top) for s in parts]
        total = sum(jnp.sum(e, axis=0, keepdims=True) for e in exps)
        inv = 1.0 / total
        probs = jnp.concatenate([(e * inv).astype(BF16) for e in exps], axis=0)
        out = dot(probs, v_out[pl.ds(0, span), :], 0, 0).astype(BF16)
        before = o_ref[rows, :]
        o_ref[rows, :] = jnp.where(mask, out, before)
        lse_ref[0, 0, :, i * QB : (i + 1) * QB] = top + jnp.log(total)


def backward_kernel(
    q_ref, k_ref, v_ref, do_ref, lse_ref, tab_ref, dq_out, dk_out, dv_out, sums_out, dq, dk, dv
):
    seq_len = q_ref.shape[0]
    j = pl.program_id(1)
    mask = lane_mask(QB, j)
    causal = lax.broadcasted_iota(jnp.int32, (QB, QB), 0) <= lax.broadcasted_iota(
        jnp.int32, (QB, QB), 1
    )

    @pl.when(j == 0)
    def _():
        dk[...] = jnp.zeros_like(dk)
        dv[...] = jnp.zeros_like(dv)

    for i in range(seq_len // QB):
        rows = pl.ds(i * QB, QB)
        q = q_ref[rows, :] * 0.125
        q = jnp.where(mask, q, jnp.zeros_like(q))
        do = do_ref[rows, :]
        do = jnp.where(mask, do, jnp.zeros_like(do))
        lse = lse_ref[0, 0, :, i * QB : (i + 1) * QB]
        pieces = []
        if i:
            pieces.append((pl.ds(0, i * QB), False))
        pieces.append((rows, True))
        probs, grads = [], []
        inner = 0.0
        for where, diagonal in pieces:
            s = dot(k_ref[where, :], q, 1, 1)
            if diagonal:
                s = jnp.where(causal, s, -1e30)
            p = jnp.exp(s - lse)
            dp = dot(v_ref[where, :], do, 1, 1)
            inner = inner + jnp.sum(p * dp, axis=0, keepdims=True)
            probs.append(p)
            grads.append(dp)
        acc = 0.0
        for (where, diagonal), p, dp in zip(pieces, probs, grads):
            ds = (p * (dp - inner)).astype(BF16)
            dv[where, :] += dot(p.astype(BF16), do, 1, 0)
            dk[where, :] += dot(ds, q, 1, 0)
            acc = acc + dot(ds, k_ref[where, :], 0, 0)
        before = dq[rows, :]
        dq[rows, :] = jnp.where(mask, acc * 0.125, before)

    @pl.when(j == pl.num_programs(1) - 1)
    def _():
        tables = (tab_ref[0], tab_ref[1])
        gq = turn(dq[...], tables, -1.0).astype(BF16)
        gk = turn(dk[...], tables, -1.0).astype(BF16)
        gv = dv[...].astype(BF16)
        dq_out[...] = gq
        dk_out[...] = gk
        dv_out[...] = gv
        sums_out[0, 0:1] = jnp.sum(gq.astype(F32), axis=0, keepdims=True)
        sums_out[0, 1:2] = jnp.sum(gk.astype(F32), axis=0, keepdims=True)
        sums_out[0, 2:3] = jnp.sum(gv.astype(F32), axis=0, keepdims=True)


def attention_forward(qkv, bias, tables):
    seq_len, width = qkv.shape[0], qkv.shape[1] // 3
    pairs = width // LANES
    column = lambda part: pl.BlockSpec((seq_len, LANES), lambda p, j: (0, part * pairs + p))
    block = pl.BlockSpec((seq_len, LANES), lambda p, j: (0, p))
    bias_blocks = bias.reshape(3, pairs, LANES).swapaxes(0, 1)
    wide = jax.ShapeDtypeStruct((seq_len, width), BF16)
    elements = pairs * 2 * seq_len * seq_len // 2
    return pl.pallas_call(
        forward_kernel,
        grid=(pairs, LANES // HD),
        in_specs=[
            column(0),
            column(1),
            column(2),
            pl.BlockSpec((1, 3, LANES), lambda p, j: (p, 0, 0)),
            pl.BlockSpec((2, seq_len, LANES), lambda p, j: (0, 0, 0)),
        ],
        out_specs=[
            block,
            block,
            block,
            block,
            pl.BlockSpec((1, 1, 1, seq_len), lambda p, j: (p, j, 0, 0)),
        ],
        out_shape=[
            wide,
            wide,
            wide,
            wide,
            jax.ShapeDtypeStruct((pairs, LANES // HD, 1, seq_len), F32),
        ],
        cost_estimate=pl.CostEstimate(
            flops=elements * 4 * LANES,
            bytes_accessed=qkv.size * 4 + 4 * seq_len * width * 2,
            transcendentals=elements,
        ),
        name="attention_forward",
    )(qkv, qkv, qkv, bias_blocks, tables)


def attention_backward(q, k, v, grad, lse, tables):
    seq_len, width = q.shape
    pairs = width // LANES
    block = pl.BlockSpec((seq_len, LANES), lambda p, j: (0, p))
    wide = jax.ShapeDtypeStruct((seq_len, width), BF16)
    elements = pairs * 2 * seq_len * seq_len // 2
    return pl.pallas_call(
        backward_kernel,
        grid=(pairs, LANES // HD),
        in_specs=[
            block,
            block,
            block,
            block,
            pl.BlockSpec((1, 1, 1, seq_len), lambda p, j: (p, j, 0, 0)),
            pl.BlockSpec((2, seq_len, LANES), lambda p, j: (0, 0, 0)),
        ],
        out_specs=[block, block, block, pl.BlockSpec((1, 3, LANES), lambda p, j: (p, 0, 0))],
        out_shape=[wide, wide, wide, jax.ShapeDtypeStruct((pairs, 3, LANES), F32)],
        scratch_shapes=[pltpu.VMEM((seq_len, LANES), F32)] * 3,
        cost_estimate=pl.CostEstimate(
            flops=elements * 10 * LANES,
            bytes_accessed=7 * seq_len * width * 2,
            transcendentals=elements,
        ),
        name="attention_backward",
    )(q, k, v, grad, lse, tables)


def pick(x, index):
    return lax.dynamic_index_in_dim(x, index, 0, keepdims=False)


class Cube:
    def __init__(self, axis, size):
        self.axis, self.size = axis, size
        self.bits = [b for b in range(size.bit_length()) if 1 << b < size]
        me = lax.axis_index(axis)
        self.own = [lax.rem(lax.div(me, 1 << b), 2) for b in self.bits]

    def swap(self, x, b):
        return lax.ppermute(x, self.axis, [(i, i ^ (1 << b)) for i in range(self.size)])

    def sum_all(self, x):
        for b in self.bits:
            x = x + self.swap(x, b)
        return x

    def contract(self, left, right):
        depth, rows = left.shape
        columns = right.shape[1]
        core, others = self.bits[0], self.bits[1:]
        half = rows // 2
        mine = self.own[0]
        first = lax.dynamic_slice_in_dim(left, (1 - mine) * half, half, 1)
        second = lax.dynamic_slice_in_dim(left, mine * half, half, 1)
        away = dot(first, right, 0, 0, BF16)
        came = self.swap(away, core)
        keep = dot(second, right, 0, 0, BF16)
        orders = [others, others[::-1]]
        quarter = half // 2
        done = []
        for n, order in enumerate(orders):
            small = quarter >> len(order)
            shape = (2,) * len(order) + (small, columns)
            cur = (
                keep[n * quarter : (n + 1) * quarter].astype(F32)
                + came[n * quarter : (n + 1) * quarter].astype(F32)
            ).reshape(shape)
            for b in order:
                own = self.own[b]
                send = pick(cur, 1 - own).astype(BF16)
                got = self.swap(send, b)
                cur = pick(cur, own) + got.astype(F32)
            buf = cur.astype(BF16)
            for b in order[::-1]:
                own = self.own[b]
                got = self.swap(buf, b)
                low = jnp.where(own == 0, buf, got)
                high = jnp.where(own == 0, got, buf)
                buf = jnp.stack([low, high])
            done.append(buf.reshape(quarter, columns))
        whole = jnp.concatenate(done, axis=0)
        other = self.swap(whole, core)
        low = jnp.where(mine == 0, whole, other)
        high = jnp.where(mine == 0, other, whole)
        return jnp.concatenate([low, high], axis=0).astype(F32)


LAG = 2
BLOCK = 128
PIECES = 16
WIDE = 256
STEP = 32
MESH = pl.DeviceIdType.MESH


def item_places(n_d, n_g, n_q):
    d_at = -(-n_g // n_d) * n_d
    q_at = -(-(d_at + n_d) // n_q) * n_q
    return d_at, 0, q_at, q_at + n_q


class Places:
    def __init__(self, n_dp, n_z):
        self.me = lax.axis_index("dp")
        self.z = z = lax.axis_index("mp")
        self.core = lax.rem(self.me, 2)
        self.x = lax.rem(lax.div(self.me, 2), 2)
        self.y = lax.div(self.me, 4)
        self.core_peer = (self.me + 1 - 2 * self.core, z)
        self.x_peer = (self.me + 2 - 4 * self.x, z)
        self.y_peer = (self.me + 4 - 8 * self.y, z)
        self.dp_others = [lax.rem(self.me + n, n_dp) for n in range(1, n_dp)]
        self.dp_peers = [(other, z) for other in self.dp_others]
        self.z_of = [lax.rem(z + d, n_z) for d in range(n_z)]
        self.z_peers = [(self.me, to) for to in self.z_of]
        self.above = jnp.minimum(z + 1, n_z - 1)
        self.below = jnp.maximum(z - 1, 0)
        self.far = n_z - 1 - z
        self.has_above, self.has_below = z < n_z - 1, z > 0
        self.end = jnp.logical_or(z == 0, z == n_z - 1)
        self.inner = jnp.where(z == 0, 1, n_z - 2)
        self.middle = jnp.logical_not(self.end)
        self.order = [
            z,
            jnp.where(z == 0, 1, z - 1),
            jnp.where(z == 0, 2, jnp.where(z == 1, 2, jnp.where(z == 2, 3, 1))),
            jnp.where(z <= 1, 3, 0),
        ]


def rdma(src, dst, send_sem, recv_sem, peer):
    return pltpu.make_async_remote_copy(
        src_ref=src,
        dst_ref=dst,
        send_sem=send_sem,
        recv_sem=recv_sem,
        device_id=peer,
        device_id_type=MESH,
    )


def start(copies):
    for copy in copies:
        copy.start()


def wait(copies):
    for copy in copies:
        copy.wait()


def at_block(i, size):
    return pl.ds(pl.multiple_of(i * size, size), size)


def both(a, b):
    return jnp.logical_and(a, b)


def causal_block():
    key = lax.broadcasted_iota(jnp.int32, (QB, QB), 0)
    query = lax.broadcasted_iota(jnp.int32, (QB, QB), 1)
    return key <= query


def head_part(x, mask):
    return jnp.where(mask, x, jnp.zeros_like(x))


def attend_unit(u, qkv_v, attn_v, hat_v, lse_v, first_row):
    seq_len = qkv_v.shape[1]
    pair, j = lax.div(u, 2), lax.rem(u, 2)
    lanes = at_block(pair, LANES)
    mask = lane_mask(QB, j)
    causal = causal_block()
    for i in range(seq_len // QB):
        rows = pl.ds(i * QB, QB)
        q = head_part(qkv_v[0, rows, lanes] * 0.125, mask)
        parts = []
        if i:
            parts.append(dot(qkv_v[1, pl.ds(0, i * QB), lanes], q, 1, 1))
        parts.append(jnp.where(causal, dot(qkv_v[1, rows, lanes], q, 1, 1), -1e30))
        top = functools.reduce(
            jnp.maximum, [jnp.max(s, axis=0, keepdims=True) for s in parts]
        )
        exps = [jnp.exp(s - top) for s in parts]
        total = sum(jnp.sum(e, axis=0, keepdims=True) for e in exps)
        inv = 1.0 / total
        probs = jnp.concatenate([(e * inv).astype(BF16) for e in exps], axis=0)
        out = dot(probs, qkv_v[2, pl.ds(0, (i + 1) * QB), lanes], 0, 0).astype(BF16)
        attn_v[rows, lanes] = jnp.where(mask, out, attn_v[rows, lanes])
        lse_v[u, :, i * QB : (i + 1) * QB] = top + jnp.log(total)

    @pl.when(j == 1)
    def _():
        for i in range(seq_len // QB):
            rows = pl.ds(i * QB, QB)
            to = pl.ds(pl.multiple_of(first_row + pair * LANES, LANES), LANES)
            hat_v[to, rows] = jnp.transpose(attn_v[rows, lanes])


def attend_back_unit(u, qkv_v, do_v, lse_v, tab_v, dqkv_v, small, dq, dk, dv):
    seq_len, width = qkv_v.shape[1:]
    pair, j = lax.div(u, 2), lax.rem(u, 2)
    lanes = at_block(pair, LANES)
    mask = lane_mask(QB, j)
    causal = causal_block()

    @pl.when(j == 0)
    def _():
        dk[...] = jnp.zeros_like(dk)
        dv[...] = jnp.zeros_like(dv)
        dq[...] = jnp.zeros_like(dq)

    for i in range(seq_len // QB):
        rows = pl.ds(i * QB, QB)
        q = head_part(qkv_v[0, rows, lanes] * 0.125, mask)
        do = head_part(do_v[rows, lanes], mask)
        lse = lse_v[u, :, i * QB : (i + 1) * QB]
        pieces = [(pl.ds(0, i * QB), False)] if i else []
        pieces.append((rows, True))
        probs, grads = [], []
        inner = 0.0
        for where, diagonal in pieces:
            s = dot(qkv_v[1, where, lanes], q, 1, 1)
            if diagonal:
                s = jnp.where(causal, s, -1e30)
            p = jnp.exp(s - lse)
            dp = dot(qkv_v[2, where, lanes], do, 1, 1)
            inner = inner + jnp.sum(p * dp, axis=0, keepdims=True)
            probs.append(p)
            grads.append(dp)
        acc = 0.0
        for (where, diagonal), p, dp in zip(pieces, probs, grads):
            ds = (p * (dp - inner)).astype(BF16)
            dv[where, :] += dot(p.astype(BF16), do, 1, 0)
            dk[where, :] += dot(ds, q, 1, 0)
            acc = acc + dot(ds, qkv_v[1, where, lanes], 0, 0)
        dq[rows, :] = jnp.where(mask, acc * 0.125, dq[rows, :])

    @pl.when(j == 1)
    def _():
        tables = (tab_v[0], tab_v[1])
        out = (
            turn(dq[...], tables, -1.0).astype(BF16),
            turn(dk[...], tables, -1.0).astype(BF16),
            dv[...].astype(BF16),
        )
        for t, g in enumerate(out):
            dqkv_v[:, pl.ds(pl.multiple_of(t * width + pair * LANES, LANES), LANES)] = g
            small[2 + t : 3 + t, lanes] = jnp.sum(g.astype(F32), axis=0, keepdims=True)


def layer_kernel(
    n_dp, n_z, tokens, grad_out, table_c, table_s, w_gate_up, w_qkv, w_down, w_out, gain_ref, shift_ref, bias_ref,
    sums_out, layer_out, grad_tokens_out, gain_out, shift_out, bias_out, w_gate, w_up,
    lhs_v, dy_v, nrm, rhs, a1_v, a2_v, qkv_v, attn_v, hq_v, do_v, lse_v, tab_v, tok_v,
    wf, zsend, zin, zout, far_v, mid, own, small, small_in, share_in,
    acc, rcv0, rcv1, rcv2, fin,
    load, s_raw, s_wf, s_back, s_wd, s_wn, s_tok, b_sems, m_sems,
    n_send, n_recv, y_send, y_recv, z_sems, small_sems, share_sems,
    s0, s1, s2, s3, s4, s5, s_fin,
):
    at = Places(n_dp, n_z)
    seq_len, model = dy_v.shape
    own_rows = tok_v.shape[0]
    width = qkv_v.shape[2]
    local_ff = a1_v.shape[1]
    blocks_h, blocks_o = local_ff // BLOCK, width // BLOCK
    columns = model // WIDE
    n_d = columns
    n_g, n_q = blocks_h, 3 * width // WIDE
    total = n_d + n_g + n_q
    d_place, g_place, q_place, _ = item_places(n_d, n_g, n_q)
    per = width // WIDE
    fill = n_g + n_q
    dy_chunks = y_recv.shape[1]
    dy_wide = model // dy_chunks
    units = width // HD

    dqkv_v = hq_v
    away_slots = LAG + 1
    own_slots = acc.shape[0] - away_slots
    hat_v, nt_v = lhs_v.at[0], lhs_v.at[1]

    def slot_of(buf, it):
        return lax.rem(it, own_slots if buf is acc else buf.shape[0])

    def quarter(bit, half):
        return half * 4 + bit * 2

    def stage0(it):
        sa, s = own_slots + lax.rem(it, away_slots), slot_of(rcv0, it)
        return [rdma(acc.at[sa], rcv0.at[s], s0.at[0, s], s0.at[1, s], at.core_peer)]

    def stage1(it):
        sa, s = slot_of(acc, it), slot_of(rcv1, it)
        a, b = pl.ds(quarter(1 - at.x, 0), 2), pl.ds(quarter(1 - at.y, 1), 2)
        return [
            rdma(acc.at[sa, a], rcv1.at[s, 0], s1.at[0, s], s1.at[1, s], at.x_peer),
            rdma(acc.at[sa, b], rcv1.at[s, 1], s1.at[2, s], s1.at[3, s], at.y_peer),
        ]

    def stage2(it):
        sa, s = slot_of(acc, it), slot_of(rcv2, it)
        a, b = quarter(at.x, 0) + 1 - at.y, quarter(at.y, 1) + 1 - at.x
        return [
            rdma(acc.at[sa, a], rcv2.at[s, 0], s2.at[0, s], s2.at[1, s], at.y_peer),
            rdma(acc.at[sa, b], rcv2.at[s, 1], s2.at[2, s], s2.at[3, s], at.x_peer),
        ]

    def piece_a():
        return at.core * 8 + quarter(at.x, 0) + at.y

    def piece_b():
        return at.core * 8 + quarter(at.y, 1) + at.x

    def place(it):
        late = jnp.where(it < n_d + n_g, g_place - n_d, q_place - n_d - n_g)
        return it + jnp.where(it < n_d, d_place, late)

    def stage3(it):
        s, n = slot_of(fin, it), lax.rem(it, s3.shape[1])
        a, b = sums_out.at[place(it), piece_a()], sums_out.at[place(it), piece_b()]
        return [
            rdma(fin.at[s, 0], a, s3.at[0, n], s3.at[1, n], at.y_peer),
            rdma(fin.at[s, 1], b, s3.at[2, n], s3.at[3, n], at.x_peer),
        ]

    def keep3(it):
        s = slot_of(fin, it)
        return [
            pltpu.make_async_copy(fin.at[s, 0], sums_out.at[place(it), piece_a()], s_fin.at[0, s]),
            pltpu.make_async_copy(fin.at[s, 1], sums_out.at[place(it), piece_b()], s_fin.at[1, s]),
        ]

    def stage4(it):
        n = lax.rem(it, s4.shape[1])
        a = sums_out.at[place(it), pl.ds(at.core * 8 + quarter(at.x, 0), 2)]
        b = sums_out.at[place(it), pl.ds(at.core * 8 + quarter(at.y, 1), 2)]
        return [
            rdma(a, a, s4.at[0, n], s4.at[1, n], at.x_peer),
            rdma(b, b, s4.at[2, n], s4.at[3, n], at.y_peer),
        ]

    def stage5(it):
        n = lax.rem(it, s5.shape[1])
        part = sums_out.at[place(it), pl.ds(at.core * 8, 8)]
        return [rdma(part, part, s5.at[0, n], s5.at[1, n], at.core_peer)]

    def product(it):
        left = jnp.where(it < n_d, 0, 1)

        @pl.when(it < n_d)
        def _():
            rhs[...] = dy_v[:, at_block(it, WIDE)]

        @pl.when(both(it >= n_d, it < n_d + n_g))
        def _():
            lanes = at_block(it - n_d, BLOCK)
            rhs[:, :BLOCK] = a1_v[:, lanes]
            rhs[:, BLOCK:] = a2_v[:, lanes]

        @pl.when(it >= n_d + n_g)
        def _():
            rhs[...] = dqkv_v[:, at_block(it - n_d - n_g, WIDE)]

        @pl.loop(0, 2)
        def _(h):
            which = jnp.where(h == 0, 1 - at.core, at.core)
            slot = jnp.where(h == 0, own_slots + lax.rem(it, away_slots), lax.rem(it, own_slots))
            tile = dot(lhs_v[left, at_block(which, 8 * BLOCK), :], rhs[...], 1, 0, BF16)
            for p in range(8):
                acc[slot, p] = tile[p * BLOCK : (p + 1) * BLOCK]

            @pl.when(h == 0)
            def _():
                start(stage0(it))

    def shard(origin):
        return at_block(origin, own_rows)

    def n_copy(kind, origin, to):
        rows = nrm.at[shard(origin)]
        return rdma(rows, rows, n_send.at[kind], n_recv.at[origin], (at.me, to))

    def y_copy(kind, origin, to, c):
        part = dy_v.at[shard(origin), at_block(c, dy_wide)]
        return rdma(part, part, y_send.at[kind, c], y_recv.at[origin, c], (at.me, to))

    def route(make, what):
        def when(condition, copy):
            @pl.when(condition)
            def _():
                getattr(copy, what)()

        def first():
            when(at.has_above, make(0, at.z, at.above))
            when(at.has_below, make(1, at.z, at.below))
            when(at.end, make(2, at.z, at.far))

        def passed(up):
            if up:
                when(at.middle, make(3, at.below, at.above))
            else:
                when(at.middle, make(4, at.above, at.below))

        return first, passed

    def n_arrived(origin):
        n_copy(0, origin, at.z_of[1]).wait_recv()

    def y_arrived(origin, c):
        y_copy(0, origin, at.z_of[1], c).wait_recv()

    def norm_rows(rows):
        tok = tok_v[rows, :].astype(F32)
        centered = tok - jnp.mean(tok, axis=1, keepdims=True)
        inv_std = lax.rsqrt(jnp.mean(centered * centered, axis=1, keepdims=True) + EPS)
        return centered * inv_std, inv_std

    gain = gain_ref[...].astype(F32).reshape(1, model)
    shift = shift_ref[...].astype(F32).reshape(1, model)

    def normalize():
        @pl.loop(0, own_rows // STEP)
        def _(r):
            xhat, _ = norm_rows(at_block(r, STEP))
            to = pl.ds(pl.multiple_of(at.z * own_rows + r * STEP, STEP), STEP)
            nrm[to, :] = (xhat * gain + shift).astype(BF16)

    def raw_copy(wint, f):
        s = lax.rem(f, 2)
        return pltpu.make_async_copy(
            w_gate_up.at[:, :, at_block(f, BLOCK)], wint.at[s], s_raw.at[s]
        )

    def back_copies(f):
        s = lax.rem(f, 2)
        return [
            pltpu.make_async_copy(
                wf.at[s, :, pl.ds(n * BLOCK, BLOCK)], w.at[:, at_block(f, BLOCK)], s_back.at[n, s]
            )
            for n, w in enumerate((w_gate, w_up))
        ]

    def pair_copies(f, s):
        return [
            pltpu.make_async_copy(
                w.at[:, at_block(f, BLOCK)], wf.at[s, :, pl.ds(n * BLOCK, BLOCK)], s_wf.at[n, s]
            )
            for n, w in enumerate((w_gate, w_up))
        ]

    def qkv_copies(m, s):
        return [
            pltpu.make_async_copy(
                w_qkv.at[lax.div(m, per), :, at_block(lax.rem(m, per), WIDE)], wf.at[s], s_wf.at[0, s]
            )
        ]

    def rows_of(rows):
        parts = [nrm[r, :] for r in rows]
        return parts[0] if len(parts) == 1 else jnp.concatenate(parts, axis=0)

    def hidden_tile(f, s, rows):
        product_of = dot(rows_of(rows), wf[s], 1, 0)
        lanes = at_block(f, BLOCK)
        for n, r in enumerate(rows):
            part = product_of[n * own_rows : (n + 1) * own_rows]
            g, u = part[:, :BLOCK], part[:, BLOCK:]
            sig = jax.nn.sigmoid(g)
            silu = g * sig
            h = (silu * u).astype(BF16)
            hq_v[r, lanes] = h
            hat_v[lanes, r] = jnp.transpose(h)
            a1_v[r, lanes] = (u * (sig + silu * (1.0 - sig))).astype(BF16)
            a2_v[r, lanes] = silu.astype(BF16)

    def qkv_tile(m, s, rows):
        t = lax.div(m, per)
        biases = bias_ref[...].astype(F32)
        bias = jnp.where(t == 0, biases[0:1], jnp.where(t == 1, biases[1:2], biases[2:3]))
        part = bias[:, :WIDE]
        for n in range(1, per):
            part = jnp.where(lax.rem(m, per) == n, bias[:, n * WIDE : (n + 1) * WIDE], part)
        product_of = dot(rows_of(rows), wf[s], 1, 0) + part
        for k, r in enumerate(rows):
            for n in range(WIDE // LANES):
                x = product_of[k * own_rows : (k + 1) * own_rows, n * LANES : (n + 1) * LANES]
                turned = turn(x, (tab_v[0, r, :], tab_v[1, r, :]), 1.0)
                lanes = pl.ds(pl.multiple_of(lax.rem(m, per) * WIDE + n * LANES, LANES), LANES)
                qkv_v[t, r, lanes] = jnp.where(t < 2, turned, x).astype(BF16)

    def turn_over(origin):
        rows = shard(origin)
        for n in range(columns):
            cols = pl.ds(n * WIDE, WIDE)
            nt_v[cols, rows] = jnp.transpose(nrm[rows, cols])

    def own_pass(wint):
        r = lax.broadcasted_iota(jnp.int32, (WIDE, WIDE), 0)
        c = lax.broadcasted_iota(jnp.int32, (WIDE, WIDE), 1)
        source = jnp.where(r < BLOCK, 2 * r, 2 * (r - BLOCK) + 1)
        parting = (source == c).astype(F32).astype(BF16)
        rows = shard(at.z)

        @pl.loop(0, n_g)
        def _(f):
            s = lax.rem(f, 2)

            @pl.when(f + 1 < n_g)
            def _():
                raw_copy(wint, f + 1).start()

            raw_copy(wint, f).wait()

            @pl.when(f >= 2)
            def _():
                wait(back_copies(f - 2))

            for n in range(model // BLOCK):
                part = pl.ds(n * BLOCK, BLOCK)
                raw = wint[s, part].reshape(WIDE, BLOCK)
                parted = dot(parting, raw, 1, 0, BF16)
                wf[s, part, :BLOCK] = parted[:BLOCK]
                wf[s, part, BLOCK:] = parted[BLOCK:]
            start(back_copies(f))
            hidden_tile(f, s, [rows])

        for f in (n_g - 2, n_g - 1):
            wait(back_copies(f))
        start(qkv_copies(0, n_g % 2))

        @pl.loop(0, n_q)
        def _(m):
            n = n_g + m
            s = lax.rem(n, 2)

            @pl.when(m + 1 < n_q)
            def _():
                start(qkv_copies(m + 1, 1 - s))

            @pl.when(m + 1 == n_q)
            def _():
                start(pair_copies(0, 1 - s))

            wait(qkv_copies(m, s))
            qkv_tile(m, s, [rows])

    def later_pass(k, origins, aside=None):
        rows = [shard(origin) for origin in origins]
        base = k * fill

        @pl.loop(0, n_g)
        def _(f):
            s = lax.rem(base + f, 2)

            @pl.when(f + 1 < n_g)
            def _():
                start(pair_copies(f + 1, 1 - s))

            @pl.when(f + 1 == n_g)
            def _():
                start(qkv_copies(0, 1 - s))

            if aside is not None:

                @pl.when(f == n_g - 1)
                def _():
                    aside()

            wait(pair_copies(f, s))
            hidden_tile(f, s, rows)

        @pl.loop(0, n_q)
        def _(m):
            s = lax.rem(base + n_g + m, 2)

            @pl.when(m + 1 < n_q)
            def _():
                start(qkv_copies(m + 1, 1 - s))

            if k < 2:

                @pl.when(m + 1 == n_q)
                def _():
                    start(pair_copies(0, 1 - s))

            wait(qkv_copies(m, s))
            qkv_tile(m, s, rows)

        for origin in origins:
            turn_over(origin)

    def straight(d):
        return {1: at.z != n_z - 1, 2: at.end, n_z - 1: at.z != 0}[d]

    def comes(d):
        return {1: at.z != 0, 2: at.z >= 0, n_z - 1: at.z != n_z - 1}[d]

    def under(condition, act):
        @pl.when(condition)
        def _():
            act()

    def z_copy(c, d, onward=False):
        columns_c = at_block(c, WIDE)
        src = far_v.at[:, columns_c] if onward else zsend.at[slot_of(zsend, c), shard(at.z_of[d])]
        dst = zin.at[d - 1, :, columns_c]
        return rdma(src, dst, z_sems.at[0, d - 1, c], z_sems.at[1, d - 1, c], at.z_peers[d])

    def mid_copy(c):
        src = zsend.at[slot_of(zsend, c), shard(at.far)]
        dst = mid.at[:, at_block(c, WIDE)]
        return rdma(src, dst, m_sems.at[0, c], m_sems.at[1, c], (at.me, at.inner))

    def z_out(c, what):
        for d in range(1, n_z):
            under(straight(d), getattr(z_copy(c, d), what))
        under(at.end, getattr(mid_copy(c), what))

    def far_job(c):
        @pl.when(at.middle)
        def _():
            mid_copy(c).wait_recv()
            cols = at_block(c, WIDE)
            far_v[:, cols] = (far_v[:, cols].astype(F32) + mid[:, cols].astype(F32)).astype(BF16)
            z_copy(c, 2, True).start()

    def branch_load(c):
        s = lax.rem(c, 2)
        cols = at_block(c, WIDE)
        return [
            pltpu.make_async_copy(
                w_down.at[:, cols], wf.at[s, pl.ds(0, local_ff)], s_wf.at[0, s]
            ),
            pltpu.make_async_copy(
                w_out.at[:, cols], wf.at[s, pl.ds(local_ff, width)], s_wf.at[1, s]
            ),
        ]

    def branch_job(c):
        s = lax.rem(c, 2)
        wait(branch_load(c))

        @pl.when(c + 1 < columns)
        def _():
            start(branch_load(c + 1))

        value = dot(hq_v[:, :local_ff], wf[s, :local_ff], 1, 0) + dot(
            attn_v[...], wf[s, local_ff : local_ff + width], 1, 0
        )
        nrm[:, at_block(c, WIDE)] = value.astype(BF16)

    def branch_copy(d):
        src, dst = nrm.at[shard(at.z_of[d])], zout.at[d - 1]
        return rdma(src, dst, b_sems.at[0, d - 1], b_sems.at[1, d - 1], at.z_peers[d])

    def branch_mid():
        return rdma(
            nrm.at[shard(at.far)], far_v, b_sems.at[0, n_z - 1], b_sems.at[1, n_z - 1],
            (at.me, at.inner),
        )

    def branch_first():
        under(at.end, lambda: branch_mid().start())

        @pl.when(at.middle)
        def _():
            for d in (1, n_z - 1):
                branch_copy(d).start()

    def branch_second():
        @pl.when(at.end)
        def _():
            for d in range(1, n_z):
                under(straight(d), branch_copy(d).start)

        @pl.when(at.middle)
        def _():
            branch_mid().wait_recv()

            @pl.loop(0, own_rows // STEP)
            def _(r):
                rows = at_block(r, STEP)
                to = pl.ds(pl.multiple_of(at.z_of[2] * own_rows + r * STEP, STEP), STEP)
                nrm[to, :] = (nrm[to, :].astype(F32) + far_v[rows, :].astype(F32)).astype(BF16)

            branch_copy(2).start()

    def layer_out_copy():
        return pltpu.make_async_copy(nrm.at[shard(at.z)], layer_out, s_tok.at[0])

    def layer_out_job():
        under(at.end, branch_mid().wait_send)
        under(at.middle, branch_copy(2).wait_send)
        for d in range(1, n_z):
            under(straight(d), branch_copy(d).wait_send)
            under(comes(d), branch_copy(d).wait_recv)

        @pl.loop(0, own_rows // STEP)
        def _(r):
            rows = at_block(r, STEP)
            here = pl.ds(pl.multiple_of(at.z * own_rows + r * STEP, STEP), STEP)
            value = tok_v[rows, :].astype(F32) + nrm[here, :].astype(F32)
            for n in range(n_z - 1):
                value = value + jnp.where(comes(n + 1), zout[n, rows, :].astype(F32), 0.0)
            nrm[here, :] = value.astype(BF16)

        layer_out_copy().start()

    def hidden_load(g, wd):
        def one(n, what):
            b = 2 * g + n
            dst = wd.at[pl.ds(n * BLOCK, BLOCK)]

            @pl.when(b < blocks_h)
            def _():
                rows = at_block(jnp.minimum(b, blocks_h - 1), BLOCK)
                getattr(pltpu.make_async_copy(w_down.at[rows], dst, s_wd.at[n]), what)()

            @pl.when(both(b >= blocks_h, b < blocks_h + blocks_o))
            def _():
                rows = at_block(jnp.clip(b - blocks_h, 0, blocks_o - 1), BLOCK)
                getattr(pltpu.make_async_copy(w_out.at[rows], dst, s_wd.at[n]), what)()

        return one

    def hidden_job(g, wd):
        for n in range(2):
            hidden_load(g, wd)(n, "wait")
        dh = dot(dy_v[...], wd[...], 1, 1)
        for n in range(2):
            b = 2 * g + n
            part = dh[:, n * BLOCK : (n + 1) * BLOCK]

            @pl.when(b < blocks_h)
            def _(part=part, b=b):
                lanes = at_block(jnp.minimum(b, blocks_h - 1), BLOCK)
                a1_v[:, lanes] = (part * a1_v[:, lanes].astype(F32)).astype(BF16)
                a2_v[:, lanes] = (part * a2_v[:, lanes].astype(F32)).astype(BF16)

            @pl.when(both(b >= blocks_h, b < blocks_h + blocks_o))
            def _(part=part, b=b):
                do_v[:, at_block(jnp.clip(b - blocks_h, 0, blocks_o - 1), BLOCK)] = part.astype(BF16)

    def normed_load(c, wg, wu, wq):
        rows = at_block(c, WIDE)
        return [
            pltpu.make_async_copy(w_gate.at[rows], wg, s_wn.at[0]),
            pltpu.make_async_copy(w_up.at[rows], wu, s_wn.at[1]),
            pltpu.make_async_copy(w_qkv.at[:, rows], wq, s_wn.at[2]),
        ]

    def normed_job(c, wg, wu, wq):
        wait(normed_load(c, wg, wu, wq))
        part = dot(a1_v[...], wg[...], 1, 1) + dot(a2_v[...], wu[...], 1, 1)
        for t in range(3):
            part = part + dot(dqkv_v[:, t * width : (t + 1) * width], wq[t], 1, 1)
        s = slot_of(zsend, c)

        @pl.when(c >= zsend.shape[0])
        def _():
            z_out(c - zsend.shape[0], "wait_send")

        zsend[s] = part.astype(BF16)
        z_out(c, "start")

        @pl.when(at.middle)
        def _():
            far_v[:, at_block(c, WIDE)] = zsend[s, shard(at.z_of[2]), :]

        @pl.when(c + 1 < columns)
        def _():
            start(normed_load(c + 1, wg, wu, wq))

        own[:, at_block(c, WIDE)] = zsend[s, shard(at.z), :]

    def tokens_copy():
        return pltpu.make_async_copy(tok_v, grad_tokens_out, s_tok.at[1])

    def norm_job():
        @pl.loop(0, columns)
        def _(c):
            @pl.when(c >= columns - zsend.shape[0])
            def _():
                z_out(c, "wait_send")

            under(at.middle, z_copy(c, 2, True).wait_send)
            for d in range(1, n_z):
                under(comes(d), z_copy(c, d).wait_recv)

        @pl.loop(0, own_rows // STEP)
        def _(r):
            rows = at_block(r, STEP)
            d = own[rows, :].astype(F32)
            for n in range(n_z - 1):
                d = d + jnp.where(comes(n + 1), zin[n, rows, :].astype(F32), 0.0)
            xhat, inv_std = norm_rows(rows)
            scaled = d * gain
            here = pl.ds(pl.multiple_of(at.z * own_rows + r * STEP, STEP), STEP)
            out = dy_v[here, :].astype(F32) + inv_std * (
                scaled
                - jnp.mean(scaled, axis=1, keepdims=True)
                - xhat * jnp.mean(scaled * xhat, axis=1, keepdims=True)
            )
            small[0:1, :] += jnp.sum(d * xhat, axis=0, keepdims=True)
            small[1:2, :] += jnp.sum(d, axis=0, keepdims=True)
            tok_v[rows, :] = out.astype(BF16)

        tokens_copy().start()

    share = model // n_z

    def share_copies():
        return [
            rdma(
                small.at[:, at_block(at.z_of[d], share)],
                share_in.at[d - 1],
                share_sems.at[0, d - 1],
                share_sems.at[1, d - 1],
                at.z_peers[d],
            )
            for d in range(1, n_z)
        ]

    def spread_copies():
        return [
            rdma(
                small_in.at[at.me],
                small_in.at[at.me],
                small_sems.at[0, n],
                small_sems.at[1, at.me],
                peer,
            )
            for n, peer in enumerate(at.dp_peers)
        ]

    def small_spread():
        wait(share_copies())
        mine = small[0:2, at_block(at.z, share)]
        for n in range(n_z - 1):
            mine = mine + share_in[n, 0:2, :]
        small_in[at.me] = small[:, 0:share]
        small_in[at.me, 0:2, :] = mine
        start(spread_copies())

    def small_end():
        for copy in spread_copies():
            copy.wait_send()
        for n, source in enumerate(at.dp_others):
            rdma(
                small_in.at[source], small_in.at[source], small_sems.at[0, n],
                small_sems.at[1, source], at.dp_peers[n],
            ).wait_recv()
        value = small_in[0]
        for n in range(1, small_in.shape[0]):
            value = value + small_in[n]
        gain_out[...] = value[0]
        shift_out[...] = value[1]
        bias_out[...] = value[2:5]

    loads = [
        pltpu.make_async_copy(tokens, tok_v, load.at[0]),
        pltpu.make_async_copy(grad_out, dy_v.at[shard(at.z)], load.at[1]),
        pltpu.make_async_copy(table_c, tab_v.at[0], load.at[2]),
        pltpu.make_async_copy(table_s, tab_v.at[1], load.at[3]),
    ]
    start(loads)
    barrier = pltpu.get_barrier_semaphore()
    peers = at.dp_peers + at.z_peers[1:]
    for peer in peers:
        pl.semaphore_signal(barrier, inc=1, device_id=peer, device_id_type=MESH)
    loads[0].wait()
    normalize()
    pl.semaphore_wait(barrier, len(peers))

    def forward(wint):
        raw_copy(wint, 0).start()
        route(n_copy, "start")[0]()
        small[...] = jnp.zeros_like(small)
        rest = model - local_ff
        hat_v[pl.ds(local_ff, rest), :] = jnp.zeros((rest, seq_len), BF16)
        loads[2].wait()
        loads[3].wait()
        own_pass(wint)
        turn_over(at.z)

    pl.run_scoped(forward, pltpu.VMEM((2, model, 2, BLOCK), BF16))
    o1, o2, o3 = at.order[1:]
    n_arrived(o1)
    onward = route(n_copy, "start")[1]

    @pl.when(at.middle)
    def _():
        n_arrived(o2)
        onward(True)
        onward(False)
        later_pass(1, [o1, o2])
        n_arrived(o3)

    @pl.when(at.end)
    def _():
        later_pass(1, [o1])
        n_arrived(o2)
        n_arrived(o3)

    def dy_route(c, what):
        return route(lambda *a: y_copy(*a, c), what)

    def send_dy(c):
        dy_route(c, "start")[0]()

    def pass_dy_on(c):
        @pl.when(at.middle)
        def _():
            y_arrived(o1, c)
            y_arrived(o2, c)

        onward = dy_route(c, "start")[1]
        onward(True)
        onward(False)

    def rest_of_dy(c):
        y_arrived(o3, c)

        @pl.when(at.end)
        def _():
            y_arrived(o1, c)
            y_arrived(o2, c)

    loads[1].wait()
    send_dy(0)

    @pl.when(at.middle)
    def _():
        later_pass(2, [o3], lambda: send_dy(1))

    @pl.when(at.end)
    def _():
        later_pass(2, [o2, o3], lambda: send_dy(1))

    start(branch_load(0))
    pass_dy_on(0)

    first, passed = route(n_copy, "wait_send")
    first()
    passed(True)
    passed(False)

    def attend(first, count):
        @pl.loop(first, first + count)
        def _(u):
            attend_unit(u, qkv_v, attn_v, hat_v, lse_v, local_ff)

    attend(0, units // 2)
    pass_dy_on(1)
    send_dy(2)
    attend(units // 2, units - units // 2)

    early = [0, 1, 2, 3, 6, 7]
    behind = 4
    branches = {4: 0, 5: 2, 8: 4, 9: 6}

    def meanwhile(tick):
        for t, c in ((2, 2), (5, 3)):

            @pl.when(tick == t)
            def _(c=c):
                pass_dy_on(c)
                if c + 1 < dy_chunks:
                    send_dy(c + 1)

        from_, to = 0, 0
        for t, c in branches.items():
            from_ = jnp.where(tick == t, c, from_)
            to = jnp.where(tick == t, c + 2, to)

        @pl.loop(from_, to)
        def _(c):
            branch_job(c)

        for t, c in ((0, 0), (2, 1), (6, 2), (10, 3)):

            @pl.when(tick == t)
            def _(c=c):
                rest_of_dy(c)

    def item_at(tick):
        it = tick - behind
        for n, t in enumerate(early):
            it = jnp.where(tick == t, n, it)
        return it

    def live(tick):
        ready_tick = both(tick >= len(early) + behind, tick < total + behind)
        for t in early:
            ready_tick = jnp.logical_or(ready_tick, tick == t)
        return ready_tick

    hidden_jobs = -(-(blocks_h + blocks_o) // 2)
    split = blocks_h // 2
    hidden_at = len(early) + behind
    back_at = hidden_at + 2 + hidden_jobs - split
    normed_at = max(back_at + units // 2 + units // 4, hidden_at + hidden_jobs)
    out_at = normed_at + 4
    norm_at = normed_at + columns + 3

    def hidden_index(n):
        late = hidden_jobs - split
        return jnp.where(n < 2, n, jnp.where(n < late + 2, n + split - 2, n - late))

    def ticks(wide, wq, dq, dk, dv):
        wd = wide.at[0]
        wg, wu = wide.at[0, :, pl.ds(0, local_ff)], wide.at[1, :, pl.ds(0, local_ff)]

        for n in range(2):
            hidden_load(hidden_index(0), wd)(n, "start")

        @pl.loop(0, total + behind + 6 * LAG)
        def _(tick):
            one = item_at(tick - LAG)

            @pl.when(live(tick - LAG))
            def _():
                wait(stage0(one))
                sa, s = slot_of(acc, one), slot_of(rcv0, one)

                @pl.loop(0, 8)
                def _(p):
                    acc[sa, p] = (acc[sa, p].astype(F32) + rcv0[s, p].astype(F32)).astype(BF16)

                start(stage1(one))

            two = item_at(tick - 2 * LAG)

            @pl.when(live(tick - 2 * LAG))
            def _():
                wait(stage1(two))
                sa, s = slot_of(acc, two), slot_of(rcv1, two)
                for n, bit in ((0, at.x), (1, at.y)):
                    for m in range(2):
                        p = quarter(bit, n) + m
                        acc[sa, p] = (
                            acc[sa, p].astype(F32) + rcv1[s, n, m].astype(F32)
                        ).astype(BF16)
                start(stage2(two))

            three = item_at(tick - 3 * LAG)

            @pl.when(live(tick - 3 * LAG))
            def _():
                wait(stage2(three))
                sa, s, d = slot_of(acc, three), slot_of(rcv2, three), slot_of(fin, three)
                for n, p in ((0, quarter(at.x, 0) + at.y), (1, quarter(at.y, 1) + at.x)):
                    fin[d, n] = (acc[sa, p].astype(F32) + rcv2[s, n].astype(F32)).astype(BF16)
                start(stage3(three))
                start(keep3(three))

            four = item_at(tick - 4 * LAG)

            @pl.when(live(tick - 4 * LAG))
            def _():
                wait(keep3(four))
                wait(stage3(four))
                start(stage4(four))

            five = item_at(tick - 5 * LAG)

            @pl.when(live(tick - 5 * LAG))
            def _():
                wait(stage4(five))
                start(stage5(five))

            six = item_at(tick - 6 * LAG)

            @pl.when(live(tick - 6 * LAG))
            def _():
                wait(stage5(six))

            meanwhile(tick)
            item = item_at(tick)

            @pl.when(live(tick))
            def _():
                product(item)

            @pl.when(tick == hidden_at)
            def _():
                branch_first()

            @pl.when(tick == hidden_at + 4)
            def _():
                branch_second()

            @pl.when(both(tick >= hidden_at, tick < hidden_at + hidden_jobs))
            def _():
                n = tick - hidden_at
                hidden_job(hidden_index(n), wd)

                @pl.when(n + 1 < hidden_jobs)
                def _():
                    for m in range(2):
                        hidden_load(hidden_index(n + 1), wd)(m, "start")

            half = units // 2
            first = tick - back_at + jnp.clip(tick - back_at - half, 0, half)
            count = jnp.where(tick - back_at < half, 1, 2)

            @pl.loop(first, jnp.where(both(first >= 0, first < units), first + count, first))
            def _(u):
                attend_back_unit(
                    u, qkv_v, do_v, lse_v, tab_v, dqkv_v, small, dq, dk, dv
                )

            @pl.when(tick == normed_at - 1)
            def _():
                start(normed_load(0, wg, wu, wq))

            @pl.when(both(tick >= normed_at, tick < normed_at + columns))
            def _():
                normed_job(tick - normed_at, wg, wu, wq)

            @pl.when(both(tick >= normed_at + 1, tick < normed_at + 1 + columns))
            def _():
                far_job(tick - normed_at - 1)

            @pl.when(tick == out_at)
            def _():
                layer_out_job()
                for c in range(dy_chunks):
                    first, passed = dy_route(c, "wait_send")
                    first()
                    passed(True)
                    passed(False)

            @pl.when(tick == norm_at)
            def _():
                norm_job()
                start(share_copies())

            @pl.when(tick == norm_at + 2)
            def _():
                small_spread()

            @pl.when(tick == norm_at + 5)
            def _():
                small_end()
                tokens_copy().wait()
                layer_out_copy().wait()

    pl.run_scoped(
        ticks,
        pltpu.VMEM((2, WIDE, model), BF16),
        pltpu.VMEM((3, WIDE, width), BF16),
        *[pltpu.VMEM((seq_len, LANES), F32)] * 3,
    )


def run_layer(
    tokens, grad_out, tables, w_gate_up, w_qkv, w_down, w_out, gain, shift, bias, n_dp, n_z
):
    own, model = tokens.shape
    seq_len = own * n_z
    local_ff, width = w_down.shape[0], w_out.shape[0]
    columns = model // WIDE
    places = item_places(columns, local_ff // BLOCK, 3 * width // WIDE)[3]
    bf = lambda *shape: pltpu.VMEM(shape, BF16)
    fl = lambda *shape: pltpu.VMEM(shape, F32)
    sems = lambda *shape: pltpu.SemaphoreType.DMA(shape)
    slots = 2 * LAG + 2
    dy_chunks = 4
    hbm = pl.BlockSpec(memory_space=pl.ANY)
    vmem = pl.BlockSpec(memory_space=pltpu.VMEM)
    return pl.pallas_call(
        functools.partial(layer_kernel, n_dp, n_z),
        in_specs=[hbm] * 8 + [vmem] * 3,
        out_specs=[hbm, hbm, hbm, vmem, vmem, vmem, hbm, hbm],
        out_shape=[
            jax.ShapeDtypeStruct((places, PIECES, BLOCK, WIDE), BF16),
            jax.ShapeDtypeStruct((own, model), BF16),
            jax.ShapeDtypeStruct((own, model), BF16),
            jax.ShapeDtypeStruct((model // n_z,), F32),
            jax.ShapeDtypeStruct((model // n_z,), F32),
            jax.ShapeDtypeStruct((3, width), F32),
            jax.ShapeDtypeStruct((model, local_ff), BF16),
            jax.ShapeDtypeStruct((model, local_ff), BF16),
        ],
        scratch_shapes=[
            bf(2, model, seq_len), bf(seq_len, model), bf(seq_len, model), bf(seq_len, WIDE),
            bf(seq_len, local_ff), bf(seq_len, local_ff),
            bf(3, seq_len, width), bf(seq_len, width), bf(seq_len, max(local_ff, 3 * width)),
            bf(seq_len, width), fl(width // HD, 1, seq_len), fl(2, seq_len, LANES), bf(own, model),
            bf(2, model, WIDE), bf(3, seq_len, WIDE), bf(n_z - 1, own, model), bf(n_z - 1, own, model), bf(own, model), bf(own, model), bf(own, model),
            fl(8, model), fl(n_dp, 8, model // n_z), fl(n_z - 1, 8, model // n_z),
            bf(4 * LAG + 2, 8, BLOCK, WIDE),
            bf(slots - 1, 8, BLOCK, WIDE), bf(slots, 2, 2, BLOCK, WIDE), bf(slots, 2, BLOCK, WIDE),
            bf(LAG + 1, 2, BLOCK, WIDE),
            sems(4), sems(2), sems(2, 2), sems(2, 2), sems(2), sems(3), sems(2),
            sems(2, n_z), sems(2, columns),
            sems(5), sems(n_z), sems(5, dy_chunks), sems(n_z, dy_chunks),
            sems(2, n_z - 1, columns), sems(2, n_dp), sems(2, n_z - 1),
            sems(2, slots), sems(4, slots), sems(4, slots),
            sems(4, slots), sems(4, slots), sems(2, slots), sems(2, LAG + 1),
        ],
        compiler_params=pltpu.CompilerParams(
            collective_id=0, has_side_effects=True, vmem_limit_bytes=67043328
        ),
        name="layer",
    )(tokens, grad_out, *tables, w_gate_up, w_qkv, w_down, w_out, gain, shift, bias)


def unpack_kernel(n_down, n_out, n_g, d_ref, g_ref, q_ref, *refs):
    passed = len(refs) // 2 - 2
    kept, (down, out, gate_up, qkv), outs = refs[:passed], refs[passed : passed + 4], refs[passed + 4 :]
    i = pl.program_id(0)
    for src, dst in zip(kept, outs):
        dst[...] = src[...]

    def columns(n):
        return pl.ds(n * WIDE, WIDE)

    @pl.when(i < n_down)
    def _():
        for n in range(d_ref.shape[0]):
            down[:, columns(n)] = d_ref[n, 0].astype(F32)

    @pl.when(both(i >= n_down, i < n_down + n_out))
    def _():
        for n in range(d_ref.shape[0]):
            out[:, columns(n)] = d_ref[n, 0].astype(F32)

    @pl.when(i < n_g)
    def _():
        flat = gate_up.reshape(2 * gate_up.shape[0], BLOCK)
        for p in range(PIECES):
            value = g_ref[0, p].astype(F32)
            for n in range(2):
                flat[pl.ds(2 * p * BLOCK + n, BLOCK, stride=2), :] = value[
                    :, n * BLOCK : (n + 1) * BLOCK
                ]

    per = q_ref.shape[0] // 3
    for n in range(q_ref.shape[0]):
        qkv[n // per, :, columns(n % per)] = q_ref[n, 0].astype(F32)


def unpack(items, kept, local_ff, width, model):
    n_d, n_g, n_q = model // WIDE, local_ff // BLOCK, 3 * width // WIDE
    d_at, g_at, q_at, _ = item_places(n_d, n_g, n_q)
    n_down, n_out = local_ff // BLOCK, width // BLOCK

    def piece(n, at):
        return pl.BlockSpec((n, 1, BLOCK, WIDE), lambda i: (at // n, i, 0, 0))

    def whole(x):
        if x.ndim == 2 and x.shape[0] % 256 == 0:
            return pl.BlockSpec((x.shape[0] // PIECES, x.shape[1]), lambda i: (i, 0))
        return pl.BlockSpec(x.shape, lambda i: (0,) * x.ndim)

    down, out, gate_up, qkv, *kept = pl.pallas_call(
        functools.partial(unpack_kernel, n_down, n_out, n_g),
        grid=(PIECES,),
        in_specs=[
            piece(n_d, d_at),
            pl.BlockSpec(
                (1, PIECES, BLOCK, WIDE), lambda i: (g_at + jnp.minimum(i, n_g - 1), 0, 0, 0)
            ),
            piece(n_q, q_at),
            *[whole(x) for x in kept],
        ],
        out_specs=[
            pl.BlockSpec((BLOCK, model), lambda i: (jnp.minimum(i, n_down - 1), 0)),
            pl.BlockSpec((BLOCK, model), lambda i: (jnp.clip(i - n_down, 0, n_out - 1), 0)),
            pl.BlockSpec((model, 2, BLOCK), lambda i: (0, 0, jnp.minimum(i, n_g - 1))),
            pl.BlockSpec((3, BLOCK, width), lambda i: (0, i, 0)),
            *[whole(x) for x in kept],
        ],
        out_shape=[
            jax.ShapeDtypeStruct((local_ff, model), F32),
            jax.ShapeDtypeStruct((width, model), F32),
            jax.ShapeDtypeStruct((model, 2, local_ff), F32),
            jax.ShapeDtypeStruct((3, model, width), F32),
            *[jax.ShapeDtypeStruct(x.shape, x.dtype) for x in kept],
        ],
        name="unpack",
    )(items, items, items, *kept)
    return (down, out, gate_up, qkv.transpose(1, 0, 2), *kept)


def fast_path(n_dp, n_mp, rows, model_width, local_width, local_ff):
    blocks_h, blocks_o = local_ff // BLOCK, local_width // BLOCK
    return (
        n_dp == 8
        and n_mp == 4
        and rows == QB
        and model_width == PIECES * BLOCK
        and local_width == model_width // n_mp
        and local_ff % BLOCK == 0
        and blocks_h % 2 == 1
        and blocks_h + blocks_o < PIECES
    )


def fused_layer(
    n_dp,
    n_mp,
    tables,
    tokens,
    norm_gain,
    layernorm_bias,
    qkv_weight,
    qkv_bias,
    out_weight,
    gate_up_weight,
    down_weight,
    grad_out,
):
    model_width = tokens.shape[1]
    local_width, local_ff = qkv_weight.shape[2], gate_up_weight.shape[2]
    items, *kept = run_layer(
        tokens,
        grad_out,
        tables,
        gate_up_weight,
        qkv_weight.transpose(1, 0, 2),
        down_weight,
        out_weight,
        norm_gain,
        layernorm_bias,
        qkv_bias,
        n_dp,
        n_mp,
    )
    grad_down_w, grad_out_w, grad_gate_up_w, grad_qkv_w, *kept = unpack(
        items, kept[:5], local_ff, local_width, model_width
    )
    layer_out, grad_tokens, grad_gain, grad_shift, grad_bias = kept
    return (
        layer_out,
        grad_tokens,
        grad_gain,
        grad_shift,
        grad_qkv_w,
        grad_bias,
        grad_out_w,
        grad_gate_up_w,
        grad_down_w,
    )


def on_device(
    n_dp,
    n_mp,
    tokens,
    norm_gain,
    layernorm_bias,
    qkv_weight,
    qkv_bias,
    out_weight,
    gate_up_weight,
    down_weight,
    grad_out,
):
    rows, model_width = tokens.shape
    local_width = qkv_weight.shape[2]
    seq_len = rows * n_mp
    tables = rotary_tables(seq_len)
    if fast_path(n_dp, n_mp, rows, model_width, local_width, gate_up_weight.shape[2]):
        return fused_layer(
            n_dp, n_mp, tables, tokens, norm_gain, layernorm_bias, qkv_weight, qkv_bias, out_weight,
            gate_up_weight, down_weight, grad_out,
        )
    cube = Cube("dp", n_dp)
    tables = jnp.stack(tables)
    gain = norm_gain.astype(F32)
    token_f32 = tokens.astype(F32)
    row_mean = jnp.mean(token_f32, axis=1, keepdims=True)
    centered = token_f32 - row_mean
    inv_std = lax.rsqrt(jnp.mean(centered * centered, axis=1, keepdims=True) + EPS)
    xhat = centered * inv_std
    normed_own = (xhat * gain + layernorm_bias.astype(F32)).astype(BF16)
    normed = lax.all_gather(normed_own, "mp", axis=0, tiled=True)
    dy = lax.all_gather(grad_out, "mp", axis=0, tiled=True)

    w_qkv = [qkv_weight[:, t, :] for t in range(3)]
    w_gate, w_up = gate_up_weight[:, 0, :], gate_up_weight[:, 1, :]

    gate = dot(normed, w_gate, 1, 0)
    up = dot(normed, w_up, 1, 0)
    sig = jax.nn.sigmoid(gate)
    hidden = (gate * sig * up).astype(BF16)
    qkv = jnp.concatenate([dot(normed, w, 1, 0) for w in w_qkv], axis=1)
    q, k, v, attended, lse = attention_forward(qkv, qkv_bias.astype(F32), tables)
    branch = (dot(attended, out_weight, 1, 0) + dot(hidden, down_weight, 1, 0)).astype(BF16)
    share = lax.psum_scatter(branch, "mp", scatter_dimension=0, tiled=True)
    layer_out = (token_f32 + share.astype(F32)).astype(BF16)

    share_width = model_width // n_mp
    d_hidden = dot(dy, down_weight, 1, 1)
    silu = gate * sig
    d_gate = (d_hidden * up * (sig + silu * (1.0 - sig))).astype(BF16)
    d_up = (d_hidden * silu).astype(BF16)
    d_attended = dot(dy, out_weight, 1, 1, BF16)
    dq, dk, dv, sums = attention_backward(q, k, v, d_attended, lse, tables)
    d_normed = (
        dot(d_gate, w_gate, 1, 1)
        + dot(d_up, w_up, 1, 1)
        + dot(dq, w_qkv[0], 1, 1)
        + dot(dk, w_qkv[1], 1, 1)
        + dot(dv, w_qkv[2], 1, 1)
    ).astype(BF16)
    d_own = lax.psum_scatter(d_normed, "mp", scatter_dimension=0, tiled=True).astype(F32)
    d_qkv = jnp.concatenate([dq, dk, dv], axis=1)
    grad_down_w = cube.contract(hidden, dy)
    grad_out_w = cube.contract(attended, dy)
    grad_gate_up_w = jnp.stack(
        [cube.contract(normed, d_gate), cube.contract(normed, d_up)], axis=1
    )
    grad_qkv_w = cube.contract(normed, d_qkv).reshape(model_width, 3, local_width)

    scaled = d_own * gain
    grad_tokens = grad_out.astype(F32) + inv_std * (
        scaled
        - jnp.mean(scaled, axis=1, keepdims=True)
        - xhat * jnp.mean(scaled * xhat, axis=1, keepdims=True)
    )
    terms = jnp.stack([jnp.sum(d_own * xhat, axis=0), jnp.sum(d_own, axis=0)])
    bias_sum = cube.sum_all(sums)
    grad_bias = bias_sum.swapaxes(0, 1).reshape(3, local_width)
    terms = Cube("mp", n_mp).sum_all(cube.sum_all(terms))
    terms = lax.dynamic_slice_in_dim(
        terms, lax.axis_index("mp") * share_width, share_width, 1
    )
    return (
        layer_out,
        grad_tokens.astype(BF16),
        terms[0],
        terms[1],
        grad_qkv_w,
        grad_bias,
        grad_out_w,
        grad_gate_up_w,
        grad_down_w,
    )


def solution(mesh):
    return jax.shard_map(
        functools.partial(on_device, mesh.shape["dp"], mesh.shape["mp"]),
        mesh=mesh,
        in_specs=(
            P(("dp", "mp"), None),
            P(),
            P(),
            P(None, None, "mp"),
            P(None, "mp"),
            P("mp", None),
            P(None, None, "mp"),
            P("mp", None),
            P(("dp", "mp"), None),
        ),
        out_specs=(
            P(("dp", "mp"), None),
            P(("dp", "mp"), None),
            P("mp"),
            P("mp"),
            P(None, None, "mp"),
            P(None, "mp"),
            P("mp", None),
            P(None, None, "mp"),
            P("mp", None),
        ),
        check_vma=False,
    )
```

```python
import functools
import math

import jax
import jax.numpy as jnp
from jax import lax
from jax.experimental import pallas as pl
from jax.experimental.pallas import tpu as pltpu
from jax.sharding import PartitionSpec as P

HD = 64
ROT = 16
EPS = 1e-05
LANES = 128
QB = 256


F32 = jnp.float32
BF16 = jnp.bfloat16


def dot(a, b, ca, cb, out=F32):
    return lax.dot_general(
        a, b, (((ca,), (cb,)), ((), ())), preferred_element_type=F32
    ).astype(out)


def rotary_tables(seq_len):
    half = ROT // 2
    shape = (seq_len, LANES)
    dim = lax.rem(lax.broadcasted_iota(jnp.int32, shape, 1), HD)
    positions = lax.broadcasted_iota(jnp.int32, shape, 0).astype(F32)
    freqs = 1.0 / 10000.0 ** (lax.rem(dim, half).astype(F32) * 2.0 / ROT)
    phase = positions * freqs
    cosine, sine = jnp.cos(phase), jnp.sin(phase)
    return (
        jnp.where(dim < ROT, cosine, 1.0),
        jnp.where(dim < half, -sine, jnp.where(dim < ROT, sine, 0.0)),
    )


def turn(x, tables, sign):
    half = ROT // 2
    dim = lax.rem(lax.broadcasted_iota(jnp.int32, x.shape, 1), HD)
    partner = jnp.where(dim < half, pltpu.roll(x, LANES - half, 1), pltpu.roll(x, half, 1))
    return x * tables[0] + sign * (partner * tables[1])


def lane_mask(rows, j):
    lane = lax.broadcasted_iota(jnp.int32, (rows, LANES), 1)
    return (lane // HD) == j


def forward_kernel(
    q_in, k_in, v_in, bias_ref, tab_ref, q_out, k_out, v_out, o_ref, lse_ref
):
    seq_len = q_in.shape[0]
    j = pl.program_id(1)

    @pl.when(j == 0)
    def _():
        tables = (tab_ref[0], tab_ref[1])
        q_out[...] = turn(q_in[...] + bias_ref[0, 0:1], tables, 1.0).astype(BF16)
        k_out[...] = turn(k_in[...] + bias_ref[0, 1:2], tables, 1.0).astype(BF16)
        v_out[...] = (v_in[...] + bias_ref[0, 2:3]).astype(BF16)

    mask = lane_mask(QB, j)
    causal = lax.broadcasted_iota(jnp.int32, (QB, QB), 0) <= lax.broadcasted_iota(
        jnp.int32, (QB, QB), 1
    )
    for i in range(seq_len // QB):
        rows = pl.ds(i * QB, QB)
        span = (i + 1) * QB
        q = q_out[rows, :] * 0.125
        q = jnp.where(mask, q, jnp.zeros_like(q))
        parts = []
        if i:
            parts.append(dot(k_out[pl.ds(0, i * QB), :], q, 1, 1))
        diag = dot(k_out[rows, :], q, 1, 1)
        parts.append(jnp.where(causal, diag, -1e30))
        top = functools.reduce(
            jnp.maximum, [jnp.max(s, axis=0, keepdims=True) for s in parts]
        )
        exps = [jnp.exp(s - top) for s in parts]
        total = sum(jnp.sum(e, axis=0, keepdims=True) for e in exps)
        inv = 1.0 / total
        probs = jnp.concatenate([(e * inv).astype(BF16) for e in exps], axis=0)
        out = dot(probs, v_out[pl.ds(0, span), :], 0, 0).astype(BF16)
        before = o_ref[rows, :]
        o_ref[rows, :] = jnp.where(mask, out, before)
        lse_ref[0, 0, :, i * QB : (i + 1) * QB] = top + jnp.log(total)


def backward_kernel(
    q_ref, k_ref, v_ref, do_ref, lse_ref, tab_ref, dq_out, dk_out, dv_out, sums_out, dq, dk, dv
):
    seq_len = q_ref.shape[0]
    j = pl.program_id(1)
    mask = lane_mask(QB, j)
    causal = lax.broadcasted_iota(jnp.int32, (QB, QB), 0) <= lax.broadcasted_iota(
        jnp.int32, (QB, QB), 1
    )

    @pl.when(j == 0)
    def _():
        dk[...] = jnp.zeros_like(dk)
        dv[...] = jnp.zeros_like(dv)

    for i in range(seq_len // QB):
        rows = pl.ds(i * QB, QB)
        q = q_ref[rows, :] * 0.125
        q = jnp.where(mask, q, jnp.zeros_like(q))
        do = do_ref[rows, :]
        do = jnp.where(mask, do, jnp.zeros_like(do))
        lse = lse_ref[0, 0, :, i * QB : (i + 1) * QB]
        pieces = []
        if i:
            pieces.append((pl.ds(0, i * QB), False))
        pieces.append((rows, True))
        probs, grads = [], []
        inner = 0.0
        for where, diagonal in pieces:
            s = dot(k_ref[where, :], q, 1, 1)
            if diagonal:
                s = jnp.where(causal, s, -1e30)
            p = jnp.exp(s - lse)
            dp = dot(v_ref[where, :], do, 1, 1)
            inner = inner + jnp.sum(p * dp, axis=0, keepdims=True)
            probs.append(p)
            grads.append(dp)
        acc = 0.0
        for (where, diagonal), p, dp in zip(pieces, probs, grads):
            ds = (p * (dp - inner)).astype(BF16)
            dv[where, :] += dot(p.astype(BF16), do, 1, 0)
            dk[where, :] += dot(ds, q, 1, 0)
            acc = acc + dot(ds, k_ref[where, :], 0, 0)
        before = dq[rows, :]
        dq[rows, :] = jnp.where(mask, acc * 0.125, before)

    @pl.when(j == pl.num_programs(1) - 1)
    def _():
        tables = (tab_ref[0], tab_ref[1])
        gq = turn(dq[...], tables, -1.0).astype(BF16)
        gk = turn(dk[...], tables, -1.0).astype(BF16)
        gv = dv[...].astype(BF16)
        dq_out[...] = gq
        dk_out[...] = gk
        dv_out[...] = gv
        sums_out[0, 0:1] = jnp.sum(gq.astype(F32), axis=0, keepdims=True)
        sums_out[0, 1:2] = jnp.sum(gk.astype(F32), axis=0, keepdims=True)
        sums_out[0, 2:3] = jnp.sum(gv.astype(F32), axis=0, keepdims=True)


def attention_forward(qkv, bias, tables):
    seq_len, width = qkv.shape[0], qkv.shape[1] // 3
    pairs = width // LANES
    column = lambda part: pl.BlockSpec((seq_len, LANES), lambda p, j: (0, part * pairs + p))
    block = pl.BlockSpec((seq_len, LANES), lambda p, j: (0, p))
    bias_blocks = bias.reshape(3, pairs, LANES).swapaxes(0, 1)
    wide = jax.ShapeDtypeStruct((seq_len, width), BF16)
    elements = pairs * 2 * seq_len * seq_len // 2
    return pl.pallas_call(
        forward_kernel,
        grid=(pairs, LANES // HD),
        in_specs=[
            column(0),
            column(1),
            column(2),
            pl.BlockSpec((1, 3, LANES), lambda p, j: (p, 0, 0)),
            pl.BlockSpec((2, seq_len, LANES), lambda p, j: (0, 0, 0)),
        ],
        out_specs=[
            block,
            block,
            block,
            block,
            pl.BlockSpec((1, 1, 1, seq_len), lambda p, j: (p, j, 0, 0)),
        ],
        out_shape=[
            wide,
            wide,
            wide,
            wide,
            jax.ShapeDtypeStruct((pairs, LANES // HD, 1, seq_len), F32),
        ],
        cost_estimate=pl.CostEstimate(
            flops=elements * 4 * LANES,
            bytes_accessed=qkv.size * 4 + 4 * seq_len * width * 2,
            transcendentals=elements,
        ),
        name="attention_forward",
    )(qkv, qkv, qkv, bias_blocks, tables)


def attention_backward(q, k, v, grad, lse, tables):
    seq_len, width = q.shape
    pairs = width // LANES
    block = pl.BlockSpec((seq_len, LANES), lambda p, j: (0, p))
    wide = jax.ShapeDtypeStruct((seq_len, width), BF16)
    elements = pairs * 2 * seq_len * seq_len // 2
    return pl.pallas_call(
        backward_kernel,
        grid=(pairs, LANES // HD),
        in_specs=[
            block,
            block,
            block,
            block,
            pl.BlockSpec((1, 1, 1, seq_len), lambda p, j: (p, j, 0, 0)),
            pl.BlockSpec((2, seq_len, LANES), lambda p, j: (0, 0, 0)),
        ],
        out_specs=[block, block, block, pl.BlockSpec((1, 3, LANES), lambda p, j: (p, 0, 0))],
        out_shape=[wide, wide, wide, jax.ShapeDtypeStruct((pairs, 3, LANES), F32)],
        scratch_shapes=[pltpu.VMEM((seq_len, LANES), F32)] * 3,
        cost_estimate=pl.CostEstimate(
            flops=elements * 10 * LANES,
            bytes_accessed=7 * seq_len * width * 2,
            transcendentals=elements,
        ),
        name="attention_backward",
    )(q, k, v, grad, lse, tables)


def pick(x, index):
    return lax.dynamic_index_in_dim(x, index, 0, keepdims=False)


class Cube:
    def __init__(self, axis, size):
        self.axis, self.size = axis, size
        self.bits = [b for b in range(size.bit_length()) if 1 << b < size]
        me = lax.axis_index(axis)
        self.own = [lax.rem(lax.div(me, 1 << b), 2) for b in self.bits]

    def swap(self, x, b):
        return lax.ppermute(x, self.axis, [(i, i ^ (1 << b)) for i in range(self.size)])

    def sum_all(self, x):
        for b in self.bits:
            x = x + self.swap(x, b)
        return x

    def contract(self, left, right):
        depth, rows = left.shape
        columns = right.shape[1]
        core, others = self.bits[0], self.bits[1:]
        half = rows // 2
        mine = self.own[0]
        first = lax.dynamic_slice_in_dim(left, (1 - mine) * half, half, 1)
        second = lax.dynamic_slice_in_dim(left, mine * half, half, 1)
        away = dot(first, right, 0, 0, BF16)
        came = self.swap(away, core)
        keep = dot(second, right, 0, 0, BF16)
        orders = [others, others[::-1]]
        quarter = half // 2
        done = []
        for n, order in enumerate(orders):
            small = quarter >> len(order)
            shape = (2,) * len(order) + (small, columns)
            cur = (
                keep[n * quarter : (n + 1) * quarter].astype(F32)
                + came[n * quarter : (n + 1) * quarter].astype(F32)
            ).reshape(shape)
            for b in order:
                own = self.own[b]
                send = pick(cur, 1 - own).astype(BF16)
                got = self.swap(send, b)
                cur = pick(cur, own) + got.astype(F32)
            buf = cur.astype(BF16)
            for b in order[::-1]:
                own = self.own[b]
                got = self.swap(buf, b)
                low = jnp.where(own == 0, buf, got)
                high = jnp.where(own == 0, got, buf)
                buf = jnp.stack([low, high])
            done.append(buf.reshape(quarter, columns))
        whole = jnp.concatenate(done, axis=0)
        other = self.swap(whole, core)
        low = jnp.where(mine == 0, whole, other)
        high = jnp.where(mine == 0, other, whole)
        return jnp.concatenate([low, high], axis=0).astype(F32)


LAG = 2
BLOCK = 128
PIECES = 16
WIDE = 256
STEP = 32
MESH = pl.DeviceIdType.MESH


def item_places(n_d, n_g, n_q):
    d_at = -(-n_g // n_d) * n_d
    q_at = -(-(d_at + n_d) // n_q) * n_q
    return d_at, 0, q_at, q_at + n_q


class Places:
    def __init__(self, n_dp, n_z):
        self.me = lax.axis_index("dp")
        self.z = z = lax.axis_index("mp")
        self.core = lax.rem(self.me, 2)
        self.x = lax.rem(lax.div(self.me, 2), 2)
        self.y = lax.div(self.me, 4)
        self.core_peer = (self.me + 1 - 2 * self.core, z)
        self.x_peer = (self.me + 2 - 4 * self.x, z)
        self.y_peer = (self.me + 4 - 8 * self.y, z)
        self.dp_others = [lax.rem(self.me + n, n_dp) for n in range(1, n_dp)]
        self.dp_peers = [(other, z) for other in self.dp_others]
        self.z_of = [lax.rem(z + d, n_z) for d in range(n_z)]
        self.z_peers = [(self.me, to) for to in self.z_of]
        self.above = jnp.minimum(z + 1, n_z - 1)
        self.below = jnp.maximum(z - 1, 0)
        self.far = n_z - 1 - z
        self.has_above, self.has_below = z < n_z - 1, z > 0
        self.end = jnp.logical_or(z == 0, z == n_z - 1)
        self.inner = jnp.where(z == 0, 1, n_z - 2)
        self.middle = jnp.logical_not(self.end)
        self.order = [
            z,
            jnp.where(z == 0, 1, z - 1),
            jnp.where(z == 0, 2, jnp.where(z == 1, 2, jnp.where(z == 2, 3, 1))),
            jnp.where(z <= 1, 3, 0),
        ]


def rdma(src, dst, send_sem, recv_sem, peer):
    return pltpu.make_async_remote_copy(
        src_ref=src,
        dst_ref=dst,
        send_sem=send_sem,
        recv_sem=recv_sem,
        device_id=peer,
        device_id_type=MESH,
    )


def start(copies):
    for copy in copies:
        copy.start()


def wait(copies):
    for copy in copies:
        copy.wait()


def at_block(i, size):
    return pl.ds(pl.multiple_of(i * size, size), size)


def both(a, b):
    return jnp.logical_and(a, b)


def causal_block():
    key = lax.broadcasted_iota(jnp.int32, (QB, QB), 0)
    query = lax.broadcasted_iota(jnp.int32, (QB, QB), 1)
    return key <= query


def head_part(x, mask):
    return jnp.where(mask, x, jnp.zeros_like(x))


def attend_unit(u, qkv_v, attn_v, hat_v, lse_v, first_row):
    seq_len = qkv_v.shape[1]
    pair, j = lax.div(u, 2), lax.rem(u, 2)
    lanes = at_block(pair, LANES)
    mask = lane_mask(QB, j)
    causal = causal_block()
    for i in range(seq_len // QB):
        rows = pl.ds(i * QB, QB)
        q = head_part(qkv_v[0, rows, lanes] * 0.125, mask)
        parts = []
        if i:
            parts.append(dot(qkv_v[1, pl.ds(0, i * QB), lanes], q, 1, 1))
        parts.append(jnp.where(causal, dot(qkv_v[1, rows, lanes], q, 1, 1), -1e30))
        top = functools.reduce(
            jnp.maximum, [jnp.max(s, axis=0, keepdims=True) for s in parts]
        )
        exps = [jnp.exp(s - top) for s in parts]
        total = sum(jnp.sum(e, axis=0, keepdims=True) for e in exps)
        inv = 1.0 / total
        probs = jnp.concatenate([(e * inv).astype(BF16) for e in exps], axis=0)
        out = dot(probs, qkv_v[2, pl.ds(0, (i + 1) * QB), lanes], 0, 0).astype(BF16)
        attn_v[rows, lanes] = jnp.where(mask, out, attn_v[rows, lanes])
        lse_v[u, :, i * QB : (i + 1) * QB] = top + jnp.log(total)

    @pl.when(j == 1)
    def _():
        for i in range(seq_len // QB):
            rows = pl.ds(i * QB, QB)
            to = pl.ds(pl.multiple_of(first_row + pair * LANES, LANES), LANES)
            hat_v[to, rows] = jnp.transpose(attn_v[rows, lanes])


def attend_back_unit(u, qkv_v, do_v, lse_v, tab_v, dqkv_v, small, dq, dk, dv):
    seq_len, width = qkv_v.shape[1:]
    pair, j = lax.div(u, 2), lax.rem(u, 2)
    lanes = at_block(pair, LANES)
    mask = lane_mask(QB, j)
    causal = causal_block()

    @pl.when(j == 0)
    def _():
        dk[...] = jnp.zeros_like(dk)
        dv[...] = jnp.zeros_like(dv)
        dq[...] = jnp.zeros_like(dq)

    for i in range(seq_len // QB):
        rows = pl.ds(i * QB, QB)
        q = head_part(qkv_v[0, rows, lanes] * 0.125, mask)
        do = head_part(do_v[rows, lanes], mask)
        lse = lse_v[u, :, i * QB : (i + 1) * QB]
        pieces = [(pl.ds(0, i * QB), False)] if i else []
        pieces.append((rows, True))
        probs, grads = [], []
        inner = 0.0
        for where, diagonal in pieces:
            s = dot(qkv_v[1, where, lanes], q, 1, 1)
            if diagonal:
                s = jnp.where(causal, s, -1e30)
            p = jnp.exp(s - lse)
            dp = dot(qkv_v[2, where, lanes], do, 1, 1)
            inner = inner + jnp.sum(p * dp, axis=0, keepdims=True)
            probs.append(p)
            grads.append(dp)
        acc = 0.0
        for (where, diagonal), p, dp in zip(pieces, probs, grads):
            ds = (p * (dp - inner)).astype(BF16)
            dv[where, :] += dot(p.astype(BF16), do, 1, 0)
            dk[where, :] += dot(ds, q, 1, 0)
            acc = acc + dot(ds, qkv_v[1, where, lanes], 0, 0)
        dq[rows, :] = jnp.where(mask, acc * 0.125, dq[rows, :])

    @pl.when(j == 1)
    def _():
        tables = (tab_v[0], tab_v[1])
        out = (
            turn(dq[...], tables, -1.0).astype(BF16),
            turn(dk[...], tables, -1.0).astype(BF16),
            dv[...].astype(BF16),
        )
        for t, g in enumerate(out):
            dqkv_v[:, pl.ds(pl.multiple_of(t * width + pair * LANES, LANES), LANES)] = g
            small[2 + t : 3 + t, lanes] = jnp.sum(g.astype(F32), axis=0, keepdims=True)


def layer_kernel(
    n_dp, n_z, tokens, grad_out, table_c, table_s, w_gate_up, w_qkv, w_down, w_out, gain_ref, shift_ref, bias_ref,
    sums_out, layer_out, grad_tokens_out, gain_out, shift_out, bias_out, w_gate, w_up,
    lhs_v, dy_v, nrm, rhs, a1_v, a2_v, qkv_v, attn_v, hq_v, do_v, lse_v, tab_v, tok_v,
    wf, zsend, zin, zout, far_v, mid, own, small, small_in, share_in,
    acc, rcv0, rcv1, rcv2, fin,
    load, s_raw, s_wf, s_back, s_wd, s_wn, s_tok, b_sems, m_sems,
    n_send, n_recv, y_send, y_recv, z_sems, small_sems, share_sems,
    s0, s1, s2, s3, s4, s5, s_fin,
):
    at = Places(n_dp, n_z)
    seq_len, model = dy_v.shape
    own_rows = tok_v.shape[0]
    width = qkv_v.shape[2]
    local_ff = a1_v.shape[1]
    blocks_h, blocks_o = local_ff // BLOCK, width // BLOCK
    columns = model // WIDE
    n_d = columns
    n_g, n_q = blocks_h, 3 * width // WIDE
    total = n_d + n_g + n_q
    d_place, g_place, q_place, _ = item_places(n_d, n_g, n_q)
    per = width // WIDE
    fill = n_g + n_q
    dy_chunks = y_recv.shape[1]
    dy_wide = model // dy_chunks
    units = width // HD

    dqkv_v = hq_v
    away_slots = LAG + 1
    own_slots = acc.shape[0] - away_slots
    hat_v, nt_v = lhs_v.at[0], lhs_v.at[1]

    def slot_of(buf, it):
        return lax.rem(it, own_slots if buf is acc else buf.shape[0])

    def quarter(bit, half):
        return half * 4 + bit * 2

    def stage0(it):
        sa, s = own_slots + lax.rem(it, away_slots), slot_of(rcv0, it)
        return [rdma(acc.at[sa], rcv0.at[s], s0.at[0, s], s0.at[1, s], at.core_peer)]

    def stage1(it):
        sa, s = slot_of(acc, it), slot_of(rcv1, it)
        a, b = pl.ds(quarter(1 - at.x, 0), 2), pl.ds(quarter(1 - at.y, 1), 2)
        return [
            rdma(acc.at[sa, a], rcv1.at[s, 0], s1.at[0, s], s1.at[1, s], at.x_peer),
            rdma(acc.at[sa, b], rcv1.at[s, 1], s1.at[2, s], s1.at[3, s], at.y_peer),
        ]

    def stage2(it):
        sa, s = slot_of(acc, it), slot_of(rcv2, it)
        a, b = quarter(at.x, 0) + 1 - at.y, quarter(at.y, 1) + 1 - at.x
        return [
            rdma(acc.at[sa, a], rcv2.at[s, 0], s2.at[0, s], s2.at[1, s], at.y_peer),
            rdma(acc.at[sa, b], rcv2.at[s, 1], s2.at[2, s], s2.at[3, s], at.x_peer),
        ]

    def piece_a():
        return at.core * 8 + quarter(at.x, 0) + at.y

    def piece_b():
        return at.core * 8 + quarter(at.y, 1) + at.x

    def place(it):
        late = jnp.where(it < n_d + n_g, g_place - n_d, q_place - n_d - n_g)
        return it + jnp.where(it < n_d, d_place, late)

    def stage3(it):
        s, n = slot_of(fin, it), lax.rem(it, s3.shape[1])
        a, b = sums_out.at[place(it), piece_a()], sums_out.at[place(it), piece_b()]
        return [
            rdma(fin.at[s, 0], a, s3.at[0, n], s3.at[1, n], at.y_peer),
            rdma(fin.at[s, 1], b, s3.at[2, n], s3.at[3, n], at.x_peer),
        ]

    def keep3(it):
        s = slot_of(fin, it)
        return [
            pltpu.make_async_copy(fin.at[s, 0], sums_out.at[place(it), piece_a()], s_fin.at[0, s]),
            pltpu.make_async_copy(fin.at[s, 1], sums_out.at[place(it), piece_b()], s_fin.at[1, s]),
        ]

    def stage4(it):
        n = lax.rem(it, s4.shape[1])
        a = sums_out.at[place(it), pl.ds(at.core * 8 + quarter(at.x, 0), 2)]
        b = sums_out.at[place(it), pl.ds(at.core * 8 + quarter(at.y, 1), 2)]
        return [
            rdma(a, a, s4.at[0, n], s4.at[1, n], at.x_peer),
            rdma(b, b, s4.at[2, n], s4.at[3, n], at.y_peer),
        ]

    def stage5(it):
        n = lax.rem(it, s5.shape[1])
        part = sums_out.at[place(it), pl.ds(at.core * 8, 8)]
        return [rdma(part, part, s5.at[0, n], s5.at[1, n], at.core_peer)]

    def product(it):
        left = jnp.where(it < n_d, 0, 1)

        @pl.when(it < n_d)
        def _():
            rhs[...] = dy_v[:, at_block(it, WIDE)]

        @pl.when(both(it >= n_d, it < n_d + n_g))
        def _():
            lanes = at_block(it - n_d, BLOCK)
            rhs[:, :BLOCK] = a1_v[:, lanes]
            rhs[:, BLOCK:] = a2_v[:, lanes]

        @pl.when(it >= n_d + n_g)
        def _():
            rhs[...] = dqkv_v[:, at_block(it - n_d - n_g, WIDE)]

        @pl.loop(0, 2)
        def _(h):
            which = jnp.where(h == 0, 1 - at.core, at.core)
            slot = jnp.where(h == 0, own_slots + lax.rem(it, away_slots), lax.rem(it, own_slots))
            tile = dot(lhs_v[left, at_block(which, 8 * BLOCK), :], rhs[...], 1, 0, BF16)
            for p in range(8):
                acc[slot, p] = tile[p * BLOCK : (p + 1) * BLOCK]

            @pl.when(h == 0)
            def _():
                start(stage0(it))

    def shard(origin):
        return at_block(origin, own_rows)

    def n_copy(kind, origin, to):
        rows = nrm.at[shard(origin)]
        return rdma(rows, rows, n_send.at[kind], n_recv.at[origin], (at.me, to))

    def y_copy(kind, origin, to, c):
        part = dy_v.at[shard(origin), at_block(c, dy_wide)]
        return rdma(part, part, y_send.at[kind, c], y_recv.at[origin, c], (at.me, to))

    def route(make, what):
        def when(condition, copy):
            @pl.when(condition)
            def _():
                getattr(copy, what)()

        def first():
            when(at.has_above, make(0, at.z, at.above))
            when(at.has_below, make(1, at.z, at.below))
            when(at.end, make(2, at.z, at.far))

        def passed(up):
            if up:
                when(at.middle, make(3, at.below, at.above))
            else:
                when(at.middle, make(4, at.above, at.below))

        return first, passed

    def n_arrived(origin):
        n_copy(0, origin, at.z_of[1]).wait_recv()

    def y_arrived(origin, c):
        y_copy(0, origin, at.z_of[1], c).wait_recv()

    def norm_rows(rows):
        tok = tok_v[rows, :].astype(F32)
        centered = tok - jnp.mean(tok, axis=1, keepdims=True)
        inv_std = lax.rsqrt(jnp.mean(centered * centered, axis=1, keepdims=True) + EPS)
        return centered * inv_std, inv_std

    gain = gain_ref[...].astype(F32).reshape(1, model)
    shift = shift_ref[...].astype(F32).reshape(1, model)

    def normalize():
        @pl.loop(0, own_rows // STEP)
        def _(r):
            xhat, _ = norm_rows(at_block(r, STEP))
            to = pl.ds(pl.multiple_of(at.z * own_rows + r * STEP, STEP), STEP)
            nrm[to, :] = (xhat * gain + shift).astype(BF16)

    def raw_copy(wint, f):
        s = lax.rem(f, 2)
        return pltpu.make_async_copy(
            w_gate_up.at[:, :, at_block(f, BLOCK)], wint.at[s], s_raw.at[s]
        )

    def back_copies(f):
        s = lax.rem(f, 2)
        return [
            pltpu.make_async_copy(
                wf.at[s, :, pl.ds(n * BLOCK, BLOCK)], w.at[:, at_block(f, BLOCK)], s_back.at[n, s]
            )
            for n, w in enumerate((w_gate, w_up))
        ]

    def pair_copies(f, s):
        return [
            pltpu.make_async_copy(
                w.at[:, at_block(f, BLOCK)], wf.at[s, :, pl.ds(n * BLOCK, BLOCK)], s_wf.at[n, s]
            )
            for n, w in enumerate((w_gate, w_up))
        ]

    def qkv_copies(m, s):
        return [
            pltpu.make_async_copy(
                w_qkv.at[lax.div(m, per), :, at_block(lax.rem(m, per), WIDE)], wf.at[s], s_wf.at[0, s]
            )
        ]

    def rows_of(rows):
        parts = [nrm[r, :] for r in rows]
        return parts[0] if len(parts) == 1 else jnp.concatenate(parts, axis=0)

    def hidden_tile(f, s, rows):
        product_of = dot(rows_of(rows), wf[s], 1, 0)
        lanes = at_block(f, BLOCK)
        for n, r in enumerate(rows):
            part = product_of[n * own_rows : (n + 1) * own_rows]
            g, u = part[:, :BLOCK], part[:, BLOCK:]
            sig = jax.nn.sigmoid(g)
            silu = g * sig
            h = (silu * u).astype(BF16)
            hq_v[r, lanes] = h
            hat_v[lanes, r] = jnp.transpose(h)
            a1_v[r, lanes] = (u * (sig + silu * (1.0 - sig))).astype(BF16)
            a2_v[r, lanes] = silu.astype(BF16)

    def qkv_tile(m, s, rows):
        t = lax.div(m, per)
        biases = bias_ref[...].astype(F32)
        bias = jnp.where(t == 0, biases[0:1], jnp.where(t == 1, biases[1:2], biases[2:3]))
        part = bias[:, :WIDE]
        for n in range(1, per):
            part = jnp.where(lax.rem(m, per) == n, bias[:, n * WIDE : (n + 1) * WIDE], part)
        product_of = dot(rows_of(rows), wf[s], 1, 0) + part
        for k, r in enumerate(rows):
            for n in range(WIDE // LANES):
                x = product_of[k * own_rows : (k + 1) * own_rows, n * LANES : (n + 1) * LANES]
                turned = turn(x, (tab_v[0, r, :], tab_v[1, r, :]), 1.0)
                lanes = pl.ds(pl.multiple_of(lax.rem(m, per) * WIDE + n * LANES, LANES), LANES)
                qkv_v[t, r, lanes] = jnp.where(t < 2, turned, x).astype(BF16)

    def turn_over(origin):
        rows = shard(origin)
        for n in range(columns):
            cols = pl.ds(n * WIDE, WIDE)
            nt_v[cols, rows] = jnp.transpose(nrm[rows, cols])

    def own_pass(wint):
        r = lax.broadcasted_iota(jnp.int32, (WIDE, WIDE), 0)
        c = lax.broadcasted_iota(jnp.int32, (WIDE, WIDE), 1)
        source = jnp.where(r < BLOCK, 2 * r, 2 * (r - BLOCK) + 1)
        parting = (source == c).astype(F32).astype(BF16)
        rows = shard(at.z)

        @pl.loop(0, n_g)
        def _(f):
            s = lax.rem(f, 2)

            @pl.when(f + 1 < n_g)
            def _():
                raw_copy(wint, f + 1).start()

            raw_copy(wint, f).wait()

            @pl.when(f >= 2)
            def _():
                wait(back_copies(f - 2))

            for n in range(model // BLOCK):
                part = pl.ds(n * BLOCK, BLOCK)
                raw = wint[s, part].reshape(WIDE, BLOCK)
                parted = dot(parting, raw, 1, 0, BF16)
                wf[s, part, :BLOCK] = parted[:BLOCK]
                wf[s, part, BLOCK:] = parted[BLOCK:]
            start(back_copies(f))
            hidden_tile(f, s, [rows])

        for f in (n_g - 2, n_g - 1):
            wait(back_copies(f))
        start(qkv_copies(0, n_g % 2))

        @pl.loop(0, n_q)
        def _(m):
            n = n_g + m
            s = lax.rem(n, 2)

            @pl.when(m + 1 < n_q)
            def _():
                start(qkv_copies(m + 1, 1 - s))

            @pl.when(m + 1 == n_q)
            def _():
                start(pair_copies(0, 1 - s))

            wait(qkv_copies(m, s))
            qkv_tile(m, s, [rows])

    def later_pass(k, origins, aside=None):
        rows = [shard(origin) for origin in origins]
        base = k * fill

        @pl.loop(0, n_g)
        def _(f):
            s = lax.rem(base + f, 2)

            @pl.when(f + 1 < n_g)
            def _():
                start(pair_copies(f + 1, 1 - s))

            @pl.when(f + 1 == n_g)
            def _():
                start(qkv_copies(0, 1 - s))

            if aside is not None:

                @pl.when(f == n_g - 1)
                def _():
                    aside()

            wait(pair_copies(f, s))
            hidden_tile(f, s, rows)

        @pl.loop(0, n_q)
        def _(m):
            s = lax.rem(base + n_g + m, 2)

            @pl.when(m + 1 < n_q)
            def _():
                start(qkv_copies(m + 1, 1 - s))

            if k < 2:

                @pl.when(m + 1 == n_q)
                def _():
                    start(pair_copies(0, 1 - s))

            wait(qkv_copies(m, s))
            qkv_tile(m, s, rows)

        for origin in origins:
            turn_over(origin)

    def straight(d):
        return {1: at.z != n_z - 1, 2: at.end, n_z - 1: at.z != 0}[d]

    def comes(d):
        return {1: at.z != 0, 2: at.z >= 0, n_z - 1: at.z != n_z - 1}[d]

    def under(condition, act):
        @pl.when(condition)
        def _():
            act()

    def z_copy(c, d, onward=False):
        columns_c = at_block(c, WIDE)
        src = far_v.at[:, columns_c] if onward else zsend.at[slot_of(zsend, c), shard(at.z_of[d])]
        dst = zin.at[d - 1, :, columns_c]
        return rdma(src, dst, z_sems.at[0, d - 1, c], z_sems.at[1, d - 1, c], at.z_peers[d])

    def mid_copy(c):
        src = zsend.at[slot_of(zsend, c), shard(at.far)]
        dst = mid.at[:, at_block(c, WIDE)]
        return rdma(src, dst, m_sems.at[0, c], m_sems.at[1, c], (at.me, at.inner))

    def z_out(c, what):
        for d in range(1, n_z):
            under(straight(d), getattr(z_copy(c, d), what))
        under(at.end, getattr(mid_copy(c), what))

    def far_job(c):
        @pl.when(at.middle)
        def _():
            mid_copy(c).wait_recv()
            cols = at_block(c, WIDE)
            far_v[:, cols] = (far_v[:, cols].astype(F32) + mid[:, cols].astype(F32)).astype(BF16)
            z_copy(c, 2, True).start()

    def branch_load(c):
        s = lax.rem(c, 2)
        cols = at_block(c, WIDE)
        return [
            pltpu.make_async_copy(
                w_down.at[:, cols], wf.at[s, pl.ds(0, local_ff)], s_wf.at[0, s]
            ),
            pltpu.make_async_copy(
                w_out.at[:, cols], wf.at[s, pl.ds(local_ff, width)], s_wf.at[1, s]
            ),
        ]

    def branch_job(c):
        s = lax.rem(c, 2)
        wait(branch_load(c))

        @pl.when(c + 1 < columns)
        def _():
            start(branch_load(c + 1))

        value = dot(hq_v[:, :local_ff], wf[s, :local_ff], 1, 0) + dot(
            attn_v[...], wf[s, local_ff : local_ff + width], 1, 0
        )
        nrm[:, at_block(c, WIDE)] = value.astype(BF16)

    def branch_copy(d):
        src, dst = nrm.at[shard(at.z_of[d])], zout.at[d - 1]
        return rdma(src, dst, b_sems.at[0, d - 1], b_sems.at[1, d - 1], at.z_peers[d])

    def branch_mid():
        return rdma(
            nrm.at[shard(at.far)], far_v, b_sems.at[0, n_z - 1], b_sems.at[1, n_z - 1],
            (at.me, at.inner),
        )

    def branch_first():
        under(at.end, lambda: branch_mid().start())

        @pl.when(at.middle)
        def _():
            for d in (1, n_z - 1):
                branch_copy(d).start()

    def branch_second():
        @pl.when(at.end)
        def _():
            for d in range(1, n_z):
                under(straight(d), branch_copy(d).start)

        @pl.when(at.middle)
        def _():
            branch_mid().wait_recv()

            @pl.loop(0, own_rows // STEP)
            def _(r):
                rows = at_block(r, STEP)
                to = pl.ds(pl.multiple_of(at.z_of[2] * own_rows + r * STEP, STEP), STEP)
                nrm[to, :] = (nrm[to, :].astype(F32) + far_v[rows, :].astype(F32)).astype(BF16)

            branch_copy(2).start()

    def layer_out_copy():
        return pltpu.make_async_copy(nrm.at[shard(at.z)], layer_out, s_tok.at[0])

    def layer_out_job():
        under(at.end, branch_mid().wait_send)
        under(at.middle, branch_copy(2).wait_send)
        for d in range(1, n_z):
            under(straight(d), branch_copy(d).wait_send)
            under(comes(d), branch_copy(d).wait_recv)

        @pl.loop(0, own_rows // STEP)
        def _(r):
            rows = at_block(r, STEP)
            here = pl.ds(pl.multiple_of(at.z * own_rows + r * STEP, STEP), STEP)
            value = tok_v[rows, :].astype(F32) + nrm[here, :].astype(F32)
            for n in range(n_z - 1):
                value = value + jnp.where(comes(n + 1), zout[n, rows, :].astype(F32), 0.0)
            nrm[here, :] = value.astype(BF16)

        layer_out_copy().start()

    def hidden_load(g, wd):
        def one(n, what):
            b = 2 * g + n
            dst = wd.at[pl.ds(n * BLOCK, BLOCK)]

            @pl.when(b < blocks_h)
            def _():
                rows = at_block(jnp.minimum(b, blocks_h - 1), BLOCK)
                getattr(pltpu.make_async_copy(w_down.at[rows], dst, s_wd.at[n]), what)()

            @pl.when(both(b >= blocks_h, b < blocks_h + blocks_o))
            def _():
                rows = at_block(jnp.clip(b - blocks_h, 0, blocks_o - 1), BLOCK)
                getattr(pltpu.make_async_copy(w_out.at[rows], dst, s_wd.at[n]), what)()

        return one

    def hidden_job(g, wd):
        for n in range(2):
            hidden_load(g, wd)(n, "wait")
        dh = dot(dy_v[...], wd[...], 1, 1)
        for n in range(2):
            b = 2 * g + n
            part = dh[:, n * BLOCK : (n + 1) * BLOCK]

            @pl.when(b < blocks_h)
            def _(part=part, b=b):
                lanes = at_block(jnp.minimum(b, blocks_h - 1), BLOCK)
                a1_v[:, lanes] = (part * a1_v[:, lanes].astype(F32)).astype(BF16)
                a2_v[:, lanes] = (part * a2_v[:, lanes].astype(F32)).astype(BF16)

            @pl.when(both(b >= blocks_h, b < blocks_h + blocks_o))
            def _(part=part, b=b):
                do_v[:, at_block(jnp.clip(b - blocks_h, 0, blocks_o - 1), BLOCK)] = part.astype(BF16)

    def normed_load(c, wg, wu, wq):
        rows = at_block(c, WIDE)
        return [
            pltpu.make_async_copy(w_gate.at[rows], wg, s_wn.at[0]),
            pltpu.make_async_copy(w_up.at[rows], wu, s_wn.at[1]),
            pltpu.make_async_copy(w_qkv.at[:, rows], wq, s_wn.at[2]),
        ]

    def normed_job(c, wg, wu, wq):
        wait(normed_load(c, wg, wu, wq))
        part = dot(a1_v[...], wg[...], 1, 1) + dot(a2_v[...], wu[...], 1, 1)
        for t in range(3):
            part = part + dot(dqkv_v[:, t * width : (t + 1) * width], wq[t], 1, 1)
        s = slot_of(zsend, c)

        @pl.when(c >= zsend.shape[0])
        def _():
            z_out(c - zsend.shape[0], "wait_send")

        zsend[s] = part.astype(BF16)
        z_out(c, "start")

        @pl.when(at.middle)
        def _():
            far_v[:, at_block(c, WIDE)] = zsend[s, shard(at.z_of[2]), :]

        @pl.when(c + 1 < columns)
        def _():
            start(normed_load(c + 1, wg, wu, wq))

        own[:, at_block(c, WIDE)] = zsend[s, shard(at.z), :]

    def tokens_copy():
        return pltpu.make_async_copy(tok_v, grad_tokens_out, s_tok.at[1])

    def norm_job():
        @pl.loop(0, columns)
        def _(c):
            @pl.when(c >= columns - zsend.shape[0])
            def _():
                z_out(c, "wait_send")

            under(at.middle, z_copy(c, 2, True).wait_send)
            for d in range(1, n_z):
                under(comes(d), z_copy(c, d).wait_recv)

        @pl.loop(0, own_rows // STEP)
        def _(r):
            rows = at_block(r, STEP)
            d = own[rows, :].astype(F32)
            for n in range(n_z - 1):
                d = d + jnp.where(comes(n + 1), zin[n, rows, :].astype(F32), 0.0)
            xhat, inv_std = norm_rows(rows)
            scaled = d * gain
            here = pl.ds(pl.multiple_of(at.z * own_rows + r * STEP, STEP), STEP)
            out = dy_v[here, :].astype(F32) + inv_std * (
                scaled
                - jnp.mean(scaled, axis=1, keepdims=True)
                - xhat * jnp.mean(scaled * xhat, axis=1, keepdims=True)
            )
            small[0:1, :] += jnp.sum(d * xhat, axis=0, keepdims=True)
            small[1:2, :] += jnp.sum(d, axis=0, keepdims=True)
            tok_v[rows, :] = out.astype(BF16)

        tokens_copy().start()

    share = model // n_z

    def share_copies():
        return [
            rdma(
                small.at[:, at_block(at.z_of[d], share)],
                share_in.at[d - 1],
                share_sems.at[0, d - 1],
                share_sems.at[1, d - 1],
                at.z_peers[d],
            )
            for d in range(1, n_z)
        ]

    def spread_copies():
        return [
            rdma(
                small_in.at[at.me],
                small_in.at[at.me],
                small_sems.at[0, n],
                small_sems.at[1, at.me],
                peer,
            )
            for n, peer in enumerate(at.dp_peers)
        ]

    def small_spread():
        wait(share_copies())
        mine = small[0:2, at_block(at.z, share)]
        for n in range(n_z - 1):
            mine = mine + share_in[n, 0:2, :]
        small_in[at.me] = small[:, 0:share]
        small_in[at.me, 0:2, :] = mine
        start(spread_copies())

    def small_end():
        for copy in spread_copies():
            copy.wait_send()
        for n, source in enumerate(at.dp_others):
            rdma(
                small_in.at[source], small_in.at[source], small_sems.at[0, n],
                small_sems.at[1, source], at.dp_peers[n],
            ).wait_recv()
        value = small_in[0]
        for n in range(1, small_in.shape[0]):
            value = value + small_in[n]
        gain_out[...] = value[0]
        shift_out[...] = value[1]
        bias_out[...] = value[2:5]

    loads = [
        pltpu.make_async_copy(tokens, tok_v, load.at[0]),
        pltpu.make_async_copy(grad_out, dy_v.at[shard(at.z)], load.at[1]),
        pltpu.make_async_copy(table_c, tab_v.at[0], load.at[2]),
        pltpu.make_async_copy(table_s, tab_v.at[1], load.at[3]),
    ]
    start(loads)
    barrier = pltpu.get_barrier_semaphore()
    peers = at.dp_peers + at.z_peers[1:]
    for peer in peers:
        pl.semaphore_signal(barrier, inc=1, device_id=peer, device_id_type=MESH)
    loads[0].wait()
    normalize()
    pl.semaphore_wait(barrier, len(peers))

    def forward(wint):
        raw_copy(wint, 0).start()
        route(n_copy, "start")[0]()
        small[...] = jnp.zeros_like(small)
        rest = model - local_ff
        hat_v[pl.ds(local_ff, rest), :] = jnp.zeros((rest, seq_len), BF16)
        loads[2].wait()
        loads[3].wait()
        own_pass(wint)
        turn_over(at.z)

    pl.run_scoped(forward, pltpu.VMEM((2, model, 2, BLOCK), BF16))
    o1, o2, o3 = at.order[1:]
    n_arrived(o1)
    onward = route(n_copy, "start")[1]

    @pl.when(at.middle)
    def _():
        n_arrived(o2)
        onward(True)
        onward(False)
        later_pass(1, [o1, o2])
        n_arrived(o3)

    @pl.when(at.end)
    def _():
        later_pass(1, [o1])
        n_arrived(o2)
        n_arrived(o3)

    def dy_route(c, what):
        return route(lambda *a: y_copy(*a, c), what)

    def send_dy(c):
        dy_route(c, "start")[0]()

    def pass_dy_on(c):
        @pl.when(at.middle)
        def _():
            y_arrived(o1, c)
            y_arrived(o2, c)

        onward = dy_route(c, "start")[1]
        onward(True)
        onward(False)

    def rest_of_dy(c):
        y_arrived(o3, c)

        @pl.when(at.end)
        def _():
            y_arrived(o1, c)
            y_arrived(o2, c)

    loads[1].wait()
    send_dy(0)

    @pl.when(at.middle)
    def _():
        later_pass(2, [o3], lambda: send_dy(1))

    @pl.when(at.end)
    def _():
        later_pass(2, [o2, o3], lambda: send_dy(1))

    start(branch_load(0))
    pass_dy_on(0)

    first, passed = route(n_copy, "wait_send")
    first()
    passed(True)
    passed(False)

    def attend(first, count):
        @pl.loop(first, first + count)
        def _(u):
            attend_unit(u, qkv_v, attn_v, hat_v, lse_v, local_ff)

    attend(0, units // 2)
    pass_dy_on(1)
    send_dy(2)
    attend(units // 2, units - units // 2)

    early = [0, 1, 2, 3, 6, 7]
    behind = 4
    branches = {4: 0, 5: 2, 8: 4, 9: 6}

    def meanwhile(tick):
        for t, c in ((2, 2), (5, 3)):

            @pl.when(tick == t)
            def _(c=c):
                pass_dy_on(c)
                if c + 1 < dy_chunks:
                    send_dy(c + 1)

        from_, to = 0, 0
        for t, c in branches.items():
            from_ = jnp.where(tick == t, c, from_)
            to = jnp.where(tick == t, c + 2, to)

        @pl.loop(from_, to)
        def _(c):
            branch_job(c)

        for t, c in ((0, 0), (2, 1), (6, 2), (10, 3)):

            @pl.when(tick == t)
            def _(c=c):
                rest_of_dy(c)

    def item_at(tick):
        it = tick - behind
        for n, t in enumerate(early):
            it = jnp.where(tick == t, n, it)
        return it

    def live(tick):
        ready_tick = both(tick >= len(early) + behind, tick < total + behind)
        for t in early:
            ready_tick = jnp.logical_or(ready_tick, tick == t)
        return ready_tick

    hidden_jobs = -(-(blocks_h + blocks_o) // 2)
    split = blocks_h // 2
    hidden_at = len(early) + behind
    back_at = hidden_at + 2 + hidden_jobs - split
    normed_at = max(back_at + units // 2 + units // 4, hidden_at + hidden_jobs)
    out_at = normed_at + 4
    norm_at = normed_at + columns + 3

    def hidden_index(n):
        late = hidden_jobs - split
        return jnp.where(n < 2, n, jnp.where(n < late + 2, n + split - 2, n - late))

    def ticks(wide, wq, dq, dk, dv):
        wd = wide.at[0]
        wg, wu = wide.at[0, :, pl.ds(0, local_ff)], wide.at[1, :, pl.ds(0, local_ff)]

        for n in range(2):
            hidden_load(hidden_index(0), wd)(n, "start")

        @pl.loop(0, max(total + behind + 2 + 4 * LAG, norm_at + 6))
        def _(tick):
            one = item_at(tick - 1)

            @pl.when(live(tick - 1))
            def _():
                wait(stage0(one))
                sa, s = slot_of(acc, one), slot_of(rcv0, one)

                @pl.loop(0, 8)
                def _(p):
                    acc[sa, p] = (acc[sa, p].astype(F32) + rcv0[s, p].astype(F32)).astype(BF16)

                start(stage1(one))

            two = item_at(tick - (1 + LAG))

            @pl.when(live(tick - (1 + LAG)))
            def _():
                wait(stage1(two))
                sa, s = slot_of(acc, two), slot_of(rcv1, two)
                for n, bit in ((0, at.x), (1, at.y)):
                    for m in range(2):
                        p = quarter(bit, n) + m
                        acc[sa, p] = (
                            acc[sa, p].astype(F32) + rcv1[s, n, m].astype(F32)
                        ).astype(BF16)
                start(stage2(two))

            three = item_at(tick - (1 + 2 * LAG))

            @pl.when(live(tick - (1 + 2 * LAG)))
            def _():
                wait(stage2(three))
                sa, s, d = slot_of(acc, three), slot_of(rcv2, three), slot_of(fin, three)
                for n, p in ((0, quarter(at.x, 0) + at.y), (1, quarter(at.y, 1) + at.x)):
                    fin[d, n] = (acc[sa, p].astype(F32) + rcv2[s, n].astype(F32)).astype(BF16)
                start(stage3(three))
                start(keep3(three))

            four = item_at(tick - (1 + 3 * LAG))

            @pl.when(live(tick - (1 + 3 * LAG)))
            def _():
                wait(keep3(four))
                wait(stage3(four))
                start(stage4(four))

            five = item_at(tick - (1 + 4 * LAG))

            @pl.when(live(tick - (1 + 4 * LAG)))
            def _():
                wait(stage4(five))
                start(stage5(five))

            six = item_at(tick - (2 + 4 * LAG))

            @pl.when(live(tick - (2 + 4 * LAG)))
            def _():
                wait(stage5(six))

            meanwhile(tick)
            item = item_at(tick)

            @pl.when(live(tick))
            def _():
                product(item)

            @pl.when(tick == hidden_at)
            def _():
                branch_first()

            @pl.when(tick == hidden_at + 4)
            def _():
                branch_second()

            @pl.when(both(tick >= hidden_at, tick < hidden_at + hidden_jobs))
            def _():
                n = tick - hidden_at
                hidden_job(hidden_index(n), wd)

                @pl.when(n + 1 < hidden_jobs)
                def _():
                    for m in range(2):
                        hidden_load(hidden_index(n + 1), wd)(m, "start")

            half = units // 2
            first = tick - back_at + jnp.clip(tick - back_at - half, 0, half)
            count = jnp.where(tick - back_at < half, 1, 2)

            @pl.loop(first, jnp.where(both(first >= 0, first < units), first + count, first))
            def _(u):
                attend_back_unit(
                    u, qkv_v, do_v, lse_v, tab_v, dqkv_v, small, dq, dk, dv
                )

            @pl.when(tick == normed_at - 1)
            def _():
                start(normed_load(0, wg, wu, wq))

            @pl.when(both(tick >= normed_at, tick < normed_at + columns))
            def _():
                normed_job(tick - normed_at, wg, wu, wq)

            @pl.when(both(tick >= normed_at + 1, tick < normed_at + 1 + columns))
            def _():
                far_job(tick - normed_at - 1)

            @pl.when(tick == out_at)
            def _():
                layer_out_job()
                for c in range(dy_chunks):
                    first, passed = dy_route(c, "wait_send")
                    first()
                    passed(True)
                    passed(False)

            @pl.when(tick == norm_at)
            def _():
                norm_job()
                start(share_copies())

            @pl.when(tick == norm_at + 2)
            def _():
                small_spread()

            @pl.when(tick == norm_at + 5)
            def _():
                small_end()
                tokens_copy().wait()
                layer_out_copy().wait()

    pl.run_scoped(
        ticks,
        pltpu.VMEM((2, WIDE, model), BF16),
        pltpu.VMEM((3, WIDE, width), BF16),
        *[pltpu.VMEM((seq_len, LANES), F32)] * 3,
    )


def run_layer(
    tokens, grad_out, tables, w_gate_up, w_qkv, w_down, w_out, gain, shift, bias, n_dp, n_z
):
    own, model = tokens.shape
    seq_len = own * n_z
    local_ff, width = w_down.shape[0], w_out.shape[0]
    columns = model // WIDE
    places = item_places(columns, local_ff // BLOCK, 3 * width // WIDE)[3]
    bf = lambda *shape: pltpu.VMEM(shape, BF16)
    fl = lambda *shape: pltpu.VMEM(shape, F32)
    sems = lambda *shape: pltpu.SemaphoreType.DMA(shape)
    slots = 2 * LAG + 2
    dy_chunks = 4
    hbm = pl.BlockSpec(memory_space=pl.ANY)
    vmem = pl.BlockSpec(memory_space=pltpu.VMEM)
    return pl.pallas_call(
        functools.partial(layer_kernel, n_dp, n_z),
        in_specs=[hbm] * 8 + [vmem] * 3,
        out_specs=[hbm, hbm, hbm, vmem, vmem, vmem, hbm, hbm],
        out_shape=[
            jax.ShapeDtypeStruct((places, PIECES, BLOCK, WIDE), BF16),
            jax.ShapeDtypeStruct((own, model), BF16),
            jax.ShapeDtypeStruct((own, model), BF16),
            jax.ShapeDtypeStruct((model // n_z,), F32),
            jax.ShapeDtypeStruct((model // n_z,), F32),
            jax.ShapeDtypeStruct((3, width), F32),
            jax.ShapeDtypeStruct((model, local_ff), BF16),
            jax.ShapeDtypeStruct((model, local_ff), BF16),
        ],
        scratch_shapes=[
            bf(2, model, seq_len), bf(seq_len, model), bf(seq_len, model), bf(seq_len, WIDE),
            bf(seq_len, local_ff), bf(seq_len, local_ff),
            bf(3, seq_len, width), bf(seq_len, width), bf(seq_len, max(local_ff, 3 * width)),
            bf(seq_len, width), fl(width // HD, 1, seq_len), fl(2, seq_len, LANES), bf(own, model),
            bf(2, model, WIDE), bf(3, seq_len, WIDE), bf(n_z - 1, own, model), bf(n_z - 1, own, model), bf(own, model), bf(own, model), bf(own, model),
            fl(8, model), fl(n_dp, 8, model // n_z), fl(n_z - 1, 8, model // n_z),
            bf(4 * LAG + 2, 8, BLOCK, WIDE),
            bf(slots - 1, 8, BLOCK, WIDE), bf(slots, 2, 2, BLOCK, WIDE), bf(slots, 2, BLOCK, WIDE),
            bf(LAG + 1, 2, BLOCK, WIDE),
            sems(4), sems(2), sems(2, 2), sems(2, 2), sems(2), sems(3), sems(2),
            sems(2, n_z), sems(2, columns),
            sems(5), sems(n_z), sems(5, dy_chunks), sems(n_z, dy_chunks),
            sems(2, n_z - 1, columns), sems(2, n_dp), sems(2, n_z - 1),
            sems(2, slots), sems(4, slots), sems(4, slots),
            sems(4, slots), sems(4, slots), sems(2, slots), sems(2, LAG + 1),
        ],
        compiler_params=pltpu.CompilerParams(
            collective_id=0, has_side_effects=True, vmem_limit_bytes=67043328
        ),
        name="layer",
    )(tokens, grad_out, *tables, w_gate_up, w_qkv, w_down, w_out, gain, shift, bias)


def unpack_kernel(n_down, n_out, n_g, d_ref, g_ref, q_ref, *refs):
    passed = len(refs) // 2 - 2
    kept, (down, out, gate_up, qkv), outs = refs[:passed], refs[passed : passed + 4], refs[passed + 4 :]
    i = pl.program_id(0)
    for src, dst in zip(kept, outs):
        dst[...] = src[...]

    def columns(n):
        return pl.ds(n * WIDE, WIDE)

    @pl.when(i < n_down)
    def _():
        for n in range(d_ref.shape[0]):
            down[:, columns(n)] = d_ref[n, 0].astype(F32)

    @pl.when(both(i >= n_down, i < n_down + n_out))
    def _():
        for n in range(d_ref.shape[0]):
            out[:, columns(n)] = d_ref[n, 0].astype(F32)

    @pl.when(i < n_g)
    def _():
        flat = gate_up.reshape(2 * gate_up.shape[0], BLOCK)
        for p in range(PIECES):
            value = g_ref[0, p].astype(F32)
            for n in range(2):
                flat[pl.ds(2 * p * BLOCK + n, BLOCK, stride=2), :] = value[
                    :, n * BLOCK : (n + 1) * BLOCK
                ]

    per = q_ref.shape[0] // 3
    for n in range(q_ref.shape[0]):
        qkv[n // per, :, columns(n % per)] = q_ref[n, 0].astype(F32)


def unpack(items, kept, local_ff, width, model):
    n_d, n_g, n_q = model // WIDE, local_ff // BLOCK, 3 * width // WIDE
    d_at, g_at, q_at, _ = item_places(n_d, n_g, n_q)
    n_down, n_out = local_ff // BLOCK, width // BLOCK

    def piece(n, at):
        return pl.BlockSpec((n, 1, BLOCK, WIDE), lambda i: (at // n, i, 0, 0))

    def whole(x):
        if x.ndim == 2 and x.shape[0] % 256 == 0:
            return pl.BlockSpec((x.shape[0] // PIECES, x.shape[1]), lambda i: (i, 0))
        return pl.BlockSpec(x.shape, lambda i: (0,) * x.ndim)

    down, out, gate_up, qkv, *kept = pl.pallas_call(
        functools.partial(unpack_kernel, n_down, n_out, n_g),
        grid=(PIECES,),
        in_specs=[
            piece(n_d, d_at),
            pl.BlockSpec(
                (1, PIECES, BLOCK, WIDE), lambda i: (g_at + jnp.minimum(i, n_g - 1), 0, 0, 0)
            ),
            piece(n_q, q_at),
            *[whole(x) for x in kept],
        ],
        out_specs=[
            pl.BlockSpec((BLOCK, model), lambda i: (jnp.minimum(i, n_down - 1), 0)),
            pl.BlockSpec((BLOCK, model), lambda i: (jnp.clip(i - n_down, 0, n_out - 1), 0)),
            pl.BlockSpec((model, 2, BLOCK), lambda i: (0, 0, jnp.minimum(i, n_g - 1))),
            pl.BlockSpec((3, BLOCK, width), lambda i: (0, i, 0)),
            *[whole(x) for x in kept],
        ],
        out_shape=[
            jax.ShapeDtypeStruct((local_ff, model), F32),
            jax.ShapeDtypeStruct((width, model), F32),
            jax.ShapeDtypeStruct((model, 2, local_ff), F32),
            jax.ShapeDtypeStruct((3, model, width), F32),
            *[jax.ShapeDtypeStruct(x.shape, x.dtype) for x in kept],
        ],
        name="unpack",
    )(items, items, items, *kept)
    return (down, out, gate_up, qkv.transpose(1, 0, 2), *kept)


def fast_path(n_dp, n_mp, rows, model_width, local_width, local_ff):
    blocks_h, blocks_o = local_ff // BLOCK, local_width // BLOCK
    return (
        n_dp == 8
        and n_mp == 4
        and rows == QB
        and model_width == PIECES * BLOCK
        and local_width == model_width // n_mp
        and local_ff % BLOCK == 0
        and blocks_h % 2 == 1
        and blocks_h + blocks_o < PIECES
    )


def fused_layer(
    n_dp,
    n_mp,
    tables,
    tokens,
    norm_gain,
    layernorm_bias,
    qkv_weight,
    qkv_bias,
    out_weight,
    gate_up_weight,
    down_weight,
    grad_out,
):
    model_width = tokens.shape[1]
    local_width, local_ff = qkv_weight.shape[2], gate_up_weight.shape[2]
    items, *kept = run_layer(
        tokens,
        grad_out,
        tables,
        gate_up_weight,
        qkv_weight.transpose(1, 0, 2),
        down_weight,
        out_weight,
        norm_gain,
        layernorm_bias,
        qkv_bias,
        n_dp,
        n_mp,
    )
    grad_down_w, grad_out_w, grad_gate_up_w, grad_qkv_w, *kept = unpack(
        items, kept[:5], local_ff, local_width, model_width
    )
    layer_out, grad_tokens, grad_gain, grad_shift, grad_bias = kept
    return (
        layer_out,
        grad_tokens,
        grad_gain,
        grad_shift,
        grad_qkv_w,
        grad_bias,
        grad_out_w,
        grad_gate_up_w,
        grad_down_w,
    )


def on_device(
    n_dp,
    n_mp,
    tokens,
    norm_gain,
    layernorm_bias,
    qkv_weight,
    qkv_bias,
    out_weight,
    gate_up_weight,
    down_weight,
    grad_out,
):
    rows, model_width = tokens.shape
    local_width = qkv_weight.shape[2]
    seq_len = rows * n_mp
    tables = rotary_tables(seq_len)
    if fast_path(n_dp, n_mp, rows, model_width, local_width, gate_up_weight.shape[2]):
        return fused_layer(
            n_dp, n_mp, tables, tokens, norm_gain, layernorm_bias, qkv_weight, qkv_bias, out_weight,
            gate_up_weight, down_weight, grad_out,
        )
    cube = Cube("dp", n_dp)
    tables = jnp.stack(tables)
    gain = norm_gain.astype(F32)
    token_f32 = tokens.astype(F32)
    row_mean = jnp.mean(token_f32, axis=1, keepdims=True)
    centered = token_f32 - row_mean
    inv_std = lax.rsqrt(jnp.mean(centered * centered, axis=1, keepdims=True) + EPS)
    xhat = centered * inv_std
    normed_own = (xhat * gain + layernorm_bias.astype(F32)).astype(BF16)
    normed = lax.all_gather(normed_own, "mp", axis=0, tiled=True)
    dy = lax.all_gather(grad_out, "mp", axis=0, tiled=True)

    w_qkv = [qkv_weight[:, t, :] for t in range(3)]
    w_gate, w_up = gate_up_weight[:, 0, :], gate_up_weight[:, 1, :]

    gate = dot(normed, w_gate, 1, 0)
    up = dot(normed, w_up, 1, 0)
    sig = jax.nn.sigmoid(gate)
    hidden = (gate * sig * up).astype(BF16)
    qkv = jnp.concatenate([dot(normed, w, 1, 0) for w in w_qkv], axis=1)
    q, k, v, attended, lse = attention_forward(qkv, qkv_bias.astype(F32), tables)
    branch = (dot(attended, out_weight, 1, 0) + dot(hidden, down_weight, 1, 0)).astype(BF16)
    share = lax.psum_scatter(branch, "mp", scatter_dimension=0, tiled=True)
    layer_out = (token_f32 + share.astype(F32)).astype(BF16)

    share_width = model_width // n_mp
    d_hidden = dot(dy, down_weight, 1, 1)
    silu = gate * sig
    d_gate = (d_hidden * up * (sig + silu * (1.0 - sig))).astype(BF16)
    d_up = (d_hidden * silu).astype(BF16)
    d_attended = dot(dy, out_weight, 1, 1, BF16)
    dq, dk, dv, sums = attention_backward(q, k, v, d_attended, lse, tables)
    d_normed = (
        dot(d_gate, w_gate, 1, 1)
        + dot(d_up, w_up, 1, 1)
        + dot(dq, w_qkv[0], 1, 1)
        + dot(dk, w_qkv[1], 1, 1)
        + dot(dv, w_qkv[2], 1, 1)
    ).astype(BF16)
    d_own = lax.psum_scatter(d_normed, "mp", scatter_dimension=0, tiled=True).astype(F32)
    d_qkv = jnp.concatenate([dq, dk, dv], axis=1)
    grad_down_w = cube.contract(hidden, dy)
    grad_out_w = cube.contract(attended, dy)
    grad_gate_up_w = jnp.stack(
        [cube.contract(normed, d_gate), cube.contract(normed, d_up)], axis=1
    )
    grad_qkv_w = cube.contract(normed, d_qkv).reshape(model_width, 3, local_width)

    scaled = d_own * gain
    grad_tokens = grad_out.astype(F32) + inv_std * (
        scaled
        - jnp.mean(scaled, axis=1, keepdims=True)
        - xhat * jnp.mean(scaled * xhat, axis=1, keepdims=True)
    )
    terms = jnp.stack([jnp.sum(d_own * xhat, axis=0), jnp.sum(d_own, axis=0)])
    bias_sum = cube.sum_all(sums)
    grad_bias = bias_sum.swapaxes(0, 1).reshape(3, local_width)
    terms = Cube("mp", n_mp).sum_all(cube.sum_all(terms))
    terms = lax.dynamic_slice_in_dim(
        terms, lax.axis_index("mp") * share_width, share_width, 1
    )
    return (
        layer_out,
        grad_tokens.astype(BF16),
        terms[0],
        terms[1],
        grad_qkv_w,
        grad_bias,
        grad_out_w,
        grad_gate_up_w,
        grad_down_w,
    )


def solution(mesh):
    return jax.shard_map(
        functools.partial(on_device, mesh.shape["dp"], mesh.shape["mp"]),
        mesh=mesh,
        in_specs=(
            P(("dp", "mp"), None),
            P(),
            P(),
            P(None, None, "mp"),
            P(None, "mp"),
            P("mp", None),
            P(None, None, "mp"),
            P("mp", None),
            P(("dp", "mp"), None),
        ),
        out_specs=(
            P(("dp", "mp"), None),
            P(("dp", "mp"), None),
            P("mp"),
            P("mp"),
            P(None, None, "mp"),
            P(None, "mp"),
            P("mp", None),
            P(None, None, "mp"),
            P("mp", None),
        ),
        check_vma=False,
    )
```
